32 devices in a mesh: batch: 4 (over y, x), field: 2 (over core), dim: 4 (over z).
Axes of the slice: x: 2, y: 2, z: 4, core: 2. Of those that a mesh axis runs over, the one named last changes fastest.
Arguments:
- features: bfloat16 [26, 128, 4096], P('field', 'dim', 'batch'), may hold values from -6 to 6
- cross_weight: bfloat16 [2, 26, 128, 26, 128], P(None, 'field', 'dim'), may hold values from -0.109375 to 0.109375
- cross_bias: float32 [2, 26, 128], P(None, 'field', 'dim'), may hold values from -3 to 3
- tower_weight: bfloat16 [1024, 26, 128], P(('field', 'dim')), may hold values from -0.109375 to 0.109375
- tower_bias: float32 [1024], P(('field', 'dim')), may hold values from -3 to 3
- query_weight: bfloat16 [1024, 128], P(('field', 'dim')), may hold values from -0.1875 to 0.1875
- user_vec: bfloat16 [4096, 128], P('batch'), may hold values from -6 to 6
- candidates: bfloat16 [1024, 128], P('batch'), may hold values from -6 to 6
- positive: int32 [4096], P('batch'), may hold values from 0 to 1023
Outputs:
- crossed: bfloat16 [26, 128, 4096], P('field', 'dim', 'batch')
- losses: float32 [4096], P('batch')
The draws below stay inside these ranges and needn't reach their ends.
All inputs are finite; a program needn't handle non-finite values.
Results may differ from the reference program's by a relative error of at most 0.0049.
Values may be sent and summed in bfloat16 or wider, within the bound.
A program may use at most 64 MiB of HBM per device.

```python
import math
import jax
import jax.numpy as jnp
from jax import lax

FIELDS = 26
EMB = 128
TOWER = 1024
CROSS = 2
EX_DEV = 1024
BATCH = 4096
CANDS = 1024
N_BATCH = 4


def draw_user_vec(key, part):
    row_total = BATCH
    values = jnp.clip(jax.random.normal(jax.random.fold_in(key, 11), (row_total, EMB), jnp.float32), -6.0, 6.0)
    return values.astype(jnp.bfloat16)


def draw_candidates(key, part):
    row_total = CANDS
    values = jnp.clip(jax.random.normal(jax.random.fold_in(key, 23), (row_total, EMB), jnp.float32), -6.0, 6.0)
    return values.astype(jnp.bfloat16)


def plant(entries, rng, low, top_value):
    extent = entries.shape
    spot = [jax.random.randint(jax.random.fold_in(rng, axis), (), 0, extent[axis]) for axis in range(len(extent))]
    entries = entries.at[tuple(spot)].set(low)
    longest = extent.index(max(extent))
    spot[longest] = (spot[longest] + 1) % extent[longest]
    return entries.at[tuple(spot)].set(top_value)


def steps_of(rng, dims, split, least, largest):
    loudness = 1.0
    for dim, parts in split:
        draws = jax.random.uniform(jax.random.fold_in(jax.random.fold_in(rng, 6), dim), (parts,), jnp.float32, least / len(split), largest / len(split))
        loudness = loudness * jnp.repeat(jnp.exp(draws), dims[dim] // parts).reshape((-1,) + (1,) * (len(dims) - 1 - dim))
    return loudness


def normal_values(own_key, shape, deviation, most, cuts=(), kind=jnp.bfloat16):
    values = deviation * jax.random.normal(own_key, shape, jnp.float32)
    if cuts:
        values = values * steps_of(own_key, shape, cuts, -0.22, 0.18)
    return jnp.clip(values, -most, most).astype(kind)


def setup_inputs(seed: int = 0) -> dict:
    key_of = jax.random.split(jax.random.key(seed), 10)
    return {
        "features": normal_values(key_of[0], (FIELDS, EMB, BATCH), 1.0, 6.0, ((0, 2), (1, 4), (2, 4))),
        "cross_weight": normal_values(key_of[1], (CROSS, FIELDS, EMB, FIELDS, EMB), (FIELDS * EMB) ** -0.5, 0.109375, ((1, 2), (2, 4))),
        "cross_bias": normal_values(key_of[2], (CROSS, FIELDS, EMB), 0.5, 3.0, ((1, 2), (2, 4)), jnp.float32),
        "tower_weight": normal_values(key_of[3], (TOWER, FIELDS, EMB), (FIELDS * EMB) ** -0.5, 0.109375, ((0, 8),)),
        "tower_bias": normal_values(key_of[4], (TOWER,), 0.5, 3.0, ((0, 8),), jnp.float32),
        "query_weight": normal_values(key_of[5], (TOWER, EMB), TOWER ** -0.5, 0.1875, ((0, 8),)),
        "user_vec": draw_user_vec(jax.random.fold_in(key_of[9], 71), 0),
        "candidates": draw_candidates(jax.random.fold_in(key_of[9], 71), 0),
        "positive": plant(jax.random.randint(key_of[8], (BATCH,), 0, CANDS), jax.random.fold_in(key_of[8], 1), 0, CANDS - 1).astype(jnp.int32),
    }


def reference(features, cross_weight, cross_bias, tower_weight, tower_bias, query_weight, user_vec, candidates, positive):
    width_all = FIELDS * EMB
    anchor = features.reshape(width_all, BATCH).T
    current = anchor
    for level_idx in range(CROSS):
        matrix = cross_weight[level_idx].reshape(width_all, width_all).T
        product = jnp.dot(current, matrix, preferred_element_type=jnp.float32) + cross_bias[level_idx].reshape(width_all)
        current = (anchor.astype(jnp.float32) * product + current.astype(jnp.float32)).astype(jnp.bfloat16)
    crossed = current.T.reshape(FIELDS, EMB, BATCH)
    tower_matrix = tower_weight.reshape(TOWER, width_all).T
    hidden = jax.nn.relu(jnp.dot(current, tower_matrix, preferred_element_type=jnp.float32) + tower_bias).astype(jnp.bfloat16)
    query_vec = (jnp.dot(hidden, query_weight, preferred_element_type=jnp.float32) + user_vec.astype(jnp.float32)).astype(jnp.bfloat16)
    score_scale = 1.0 / math.sqrt(EMB)

    def block_loss(inputs):
        queries, targets = inputs
        logits = jnp.dot(queries, candidates.T, preferred_element_type=jnp.float32) * score_scale
        picked = jnp.take_along_axis(logits, targets[:, None], axis=1)[:, 0]
        return jax.nn.logsumexp(logits, axis=1) - picked
    losses = lax.map(block_loss, (query_vec.reshape(N_BATCH, EX_DEV, EMB), positive.reshape(N_BATCH, EX_DEV)))
    return (crossed, losses.reshape(BATCH))
```

```python
import functools
import math

import jax
import jax.numpy as jnp
from jax import lax
from jax.experimental import pallas as pl
from jax.experimental.pallas import tpu as pltpu
from jax.sharding import PartitionSpec as P

CROSS = 2
MESH = pl.DeviceIdType.MESH


def tower_levels(dim_count):
    held = min(2, dim_count)
    return (dim_count - held) // 2, held


def chunk_count(row_count, field_count, held):
    chunks = 2
    while chunks > field_count and row_count % (chunks * held * 128):
        chunks //= 2
    return chunks


def rank_kernel(
    counts, splits,
    feat, weight, bias, tower, tower_bias, query_weight, user, cand, positive,
    out, loss_out,
    x0, x1, flat, sent, rows, towers, biases, columns_bias, queries, cands, losses,
    feat_sem, weight_sem, tower_sem, small_sem,
    right_sem, left_sem, pair_sem, recv_sem, pair_recv,
    row_send, row_recv, chain_right, chain_left, chain_recv, both_send, both_recv,
    plane_send, plane_recv, plane_pair, plane_pair_recv,
    cand_send, cand_recv, loss_send, loss_recv,
):
    batch_count, field_count, dim_count = counts
    chunks, split = splits
    b = lax.axis_index("batch")
    f = lax.axis_index("field")
    d = lax.axis_index("dim")
    me = f * dim_count + d
    members = field_count * dim_count
    fl, el, row_count = feat.shape
    columns = fl * el
    fields, width, rc = x0.shape[1:]
    low, held = tower_levels(dim_count)
    high = low + held - 1
    level_of = d - low
    active = (d >= low) & (d <= high)
    sub = rc // held
    run = chunks // field_count
    share = run * sub
    part = towers.shape[2]
    units = split * part
    buffers = (x0, x1)
    other = field_count - 1 - f
    mine = b if split > 1 else 0
    to_right = jnp.minimum(d + 1, dim_count - 1)
    to_left = jnp.maximum(d - 1, 0)

    def remote(ref, send, recv, **where):
        return pltpu.make_async_remote_copy(
            ref, ref, send, recv, device_id=where, device_id_type=MESH)

    def place(ff, o):
        return pl.ds(ff * fl, fl), pl.ds(pl.multiple_of(o * el, el), el)

    def piece(ph, c, ff, o):
        fs, ds = place(ff, o)
        return buffers[ph].at[c, fs, ds, :]

    def right(ph, c, o):
        return remote(piece(ph, c, f, o), right_sem.at[ph, c, o], recv_sem.at[ph, c, o], dim=to_right)

    def left(ph, c, o):
        return remote(piece(ph, c, f, o), left_sem.at[ph, c, o], recv_sem.at[ph, c, o], dim=to_left)

    def pair(ph, c, o, ff):
        return remote(
            piece(ph, c, ff, o), pair_sem.at[ph, c, o], pair_recv.at[ph, c, o], field=other)

    def issue_own(ph, c):
        @pl.when(d < dim_count - 1)
        def _():
            right(ph, c, d).start()

        @pl.when(d > 0)
        def _():
            left(ph, c, d).start()

        pair(ph, c, d, f).start()

    def forwards(ph, c):
        for s in range(1, dim_count):
            @pl.when(d - s >= 0)
            def _():
                right(ph, c, d - s).wait_recv()

                @pl.when(d < dim_count - 1)
                def _():
                    right(ph, c, d - s).start()

                pair(ph, c, d - s, f).start()

            @pl.when(d + s < dim_count)
            def _():
                left(ph, c, d + s).wait_recv()

                @pl.when(d > 0)
                def _():
                    left(ph, c, d + s).start()

                pair(ph, c, d + s, f).start()
        for o in range(dim_count):
            pair(ph, c, o, other).wait_recv()

    def weight_copy(level, ff):
        return pltpu.make_async_copy(
            weight.at[level, :, ff],
            flat.at[level, :, :, pl.ds(pl.multiple_of(ff * width, width), width)],
            weight_sem.at[level, ff])

    def tower_copy(ff):
        return pltpu.make_async_copy(
            tower.at[ff, pl.ds(pl.multiple_of(mine * part, part), part), :],
            towers.at[mine, me, :, pl.ds(pl.multiple_of(ff * width, width), width)],
            tower_sem.at[ff])

    def each_field(act):
        def step(ff, carry):
            act(ff)
            return carry

        lax.fori_loop(0, fields, step, 0)

    small_refs = (
        lambda o: towers.at[mine, f * dim_count + o],
        lambda o: queries.at[:, f * dim_count + o],
        lambda o: biases.at[f * dim_count + o],
    )
    small_wide = (
        lambda ff: towers.at[mine, pl.ds(ff * dim_count, dim_count)],
        lambda ff: queries.at[:, pl.ds(ff * dim_count, dim_count)],
        lambda ff: biases.at[pl.ds(ff * dim_count, dim_count)],
    )

    def chain_to(k, o, sems, target):
        return remote(small_refs[k](o), sems.at[k, o], chain_recv.at[k, o], dim=target)

    def chain_own():
        for k in range(3):
            @pl.when(d < high)
            def _():
                chain_to(k, d, chain_right, to_right).start()

            @pl.when(d > low)
            def _():
                chain_to(k, d, chain_left, to_left).start()

    def chain_step(s):
        for k in range(3):
            @pl.when((d - s >= 0) & (d <= high))
            def _():
                chain_to(k, d - s, chain_right, to_right).wait_recv()

                @pl.when(d < high)
                def _():
                    chain_to(k, d - s, chain_right, to_right).start()

            @pl.when((d + s < dim_count) & (d >= low))
            def _():
                chain_to(k, d + s, chain_left, to_left).wait_recv()

                @pl.when(d > low)
                def _():
                    chain_to(k, d + s, chain_left, to_left).start()

    def both(k, ff):
        return remote(small_wide[k](ff), both_send.at[k], both_recv.at[k], field=other)

    def plane(t, source):
        return remote(
            towers.at[source, pl.ds(f * dim_count, dim_count)],
            plane_send.at[t], plane_recv.at[source], batch=t)

    def plane_both(source, ff):
        return remote(
            towers.at[source, pl.ds(ff * dim_count, dim_count)],
            plane_pair.at[source], plane_pair_recv.at[source], field=other)

    def cand_copy(t, source):
        return remote(cands.at[source], cand_send.at[t], cand_recv.at[source], batch=t)

    def loss_copy(m, ff, level):
        ref = losses.at[level, pl.ds(ff * run, run)]
        return remote(
            ref, loss_send.at[m], loss_recv.at[ff, level], field=m // dim_count, dim=m % dim_count)

    def row_copy(c, level):
        fs, ds = place(f, d)
        return pltpu.make_async_remote_copy(
            sent.at[c, level],
            rows.at[fs, ds, pl.ds(pl.multiple_of(lax.rem(c, run) * sub, sub), sub)],
            row_send.at[c, level], row_recv.at[lax.rem(c, run), me],
            device_id={"field": c // run, "dim": low + level}, device_id_type=MESH)

    def own_rows(c, level):
        return (c // run == f) & (level_of == level)

    def advance(ph, c):
        whole = buffers[ph][c].reshape(fields * width, rc)
        matrix = flat[ph].reshape(columns, fields * width)
        product = jnp.dot(matrix, whole, preferred_element_type=jnp.float32) + bias[ph]
        fs, ds = place(f, d)
        anchor = x0[c, fs, ds, :].astype(jnp.float32).reshape(columns, rc)
        current = buffers[ph][c, fs, ds, :].astype(jnp.float32).reshape(columns, rc)
        return (anchor * product + current).astype(jnp.bfloat16).reshape(fl, el, rc)

    own_copies = []
    for c in range(chunks):
        own_copies.append(pltpu.make_async_copy(
            feat.at[:, :, pl.ds(c * rc, rc)], piece(0, c, f, d), feat_sem.at[c]))
    small_copies = [
        pltpu.make_async_copy(query_weight, queries.at[:, me], small_sem.at[0]),
        pltpu.make_async_copy(tower_bias, biases.at[me], small_sem.at[1]),
        pltpu.make_async_copy(cand, cands.at[b], small_sem.at[2]),
    ]
    for copy in own_copies + small_copies:
        copy.start()
    each_field(lambda ff: tower_copy(ff).start())
    for level in range(CROSS):
        each_field(lambda ff: weight_copy(level, ff).start())

    barrier = pltpu.get_barrier_semaphore()
    for k in range(1, members):
        m = lax.rem(me + k, members)
        pl.semaphore_signal(
            barrier, inc=1, device_id={"field": m // dim_count, "dim": m % dim_count},
            device_id_type=MESH)
    for k in range(1, batch_count):
        pl.semaphore_signal(
            barrier, inc=1, device_id={"batch": lax.rem(b + k, batch_count)}, device_id_type=MESH)
    pl.semaphore_wait(barrier, members + batch_count - 2)
    for copy in own_copies:
        copy.wait()
    issue_own(0, 0)
    if chunks > 1:
        issue_own(0, 1)
    each_field(lambda ff: tower_copy(ff).wait())
    for copy in small_copies:
        copy.wait()
    chain_own()

    @pl.when(active)
    def _():
        for k in range(1, batch_count):
            cand_copy(lax.rem(b + k, batch_count), b).start()

    for level in range(CROSS):
        each_field(lambda ff: weight_copy(level, ff).wait())

    def first(c, carry):
        @pl.when(c + 2 < chunks)
        def _():
            issue_own(0, c + 2)

        forwards(0, c)
        fs, ds = place(f, d)
        x1[c, fs, ds, :] = advance(0, c)
        issue_own(1, c)

        for s in range(1, min(chunks, dim_count)):
            @pl.when(c == s)
            def _():
                chain_step(s)

        return carry

    lax.fori_loop(0, chunks, first, 0)
    for s in range(min(chunks, dim_count), dim_count):
        chain_step(s)

    @pl.when(active)
    def _():
        for k in range(3):
            both(k, f).start()
        if split > 1:
            for k in range(1, split):
                plane(lax.rem(b + k, split), b).start()

    def second(c, carry):
        forwards(1, c)
        new = advance(1, c)
        out[:, :, pl.ds(pl.multiple_of(c * rc, 128), rc)] = new
        for level in range(held):
            block = new[:, :, level * sub:(level + 1) * sub]

            @pl.when(own_rows(c, level))
            def _():
                fs, ds = place(f, d)
                rows[fs, ds, pl.ds(pl.multiple_of(lax.rem(c, run) * sub, sub), sub)] = block

            @pl.when(jnp.logical_not(own_rows(c, level)))
            def _():
                sent[c, level] = block
                row_copy(c, level).start()

        return carry

    lax.fori_loop(0, chunks, second, 0)

    def tower_block(s, query):
        matrix = towers[s].reshape(members * part, fields * width)
        pre = jnp.dot(
            matrix, rows[...].reshape(fields * width, share), preferred_element_type=jnp.float32)
        pre = pre + columns_bias[s].reshape(members * part, share)
        hidden = jnp.maximum(pre, 0.0).astype(jnp.bfloat16)
        return query + lax.dot_general(
            hidden, queries[s].reshape(members * part, width), (((0,), (0,)), ((), ())),
            preferred_element_type=jnp.float32)

    @pl.when(active)
    def _():
        if split > 1:
            for k in range(1, split):
                source = lax.rem(b + k, split)
                plane(source, source).wait_recv()
                plane_both(source, f).start()
        for k in range(3):
            both(k, other).wait_recv()
        for k in range(1, batch_count):
            source = lax.rem(b + k, batch_count)
            cand_copy(source, source).wait_recv()
        for m in range(members):
            block = jnp.broadcast_to(biases[m], (share, units)).T
            columns_bias[:, m] = block.reshape(split, part, share)
        if split > 1:
            for k in range(1, split):
                plane_both(lax.rem(b + k, split), other).wait_recv()
        for j in range(run):
            for k in range(1, members):
                m = lax.rem(me + k, members)
                fs, ds = place(m // dim_count, m % dim_count)
                remote(rows.at[fs, ds, pl.ds(j * sub, sub)], row_send.at[0, 0], row_recv.at[j, m],
                       field=m // dim_count, dim=m % dim_count).wait_recv()

        query = lax.fori_loop(0, split, tower_block, jnp.zeros((share, width), jnp.float32))
        all_cands = cands[...].reshape(-1, width)
        for j in range(run):
            c = f * run + j
            start = pl.multiple_of(c * rc + level_of * sub, sub)
            query_vec = (
                query[j * sub:(j + 1) * sub] + user[pl.ds(start, sub), :].astype(jnp.float32)
            ).astype(jnp.bfloat16)
            logits = lax.dot_general(
                all_cands, query_vec, (((1,), (1,)), ((), ())), preferred_element_type=jnp.float32
            ) * (1.0 / math.sqrt(width))
            labels = lax.broadcasted_iota(jnp.int32, logits.shape, 0)
            target = positive[c * held + level_of]
            picked = jnp.sum(jnp.where(labels == target, logits, 0.0), axis=0, keepdims=True)
            best = jnp.max(logits, axis=0, keepdims=True)
            total = jnp.sum(jnp.exp(logits - best), axis=0, keepdims=True)
            losses[level_of, c] = best + jnp.log(total) - picked
        for k in range(1, members):
            loss_copy(lax.rem(me + k, members), f, level_of).start()

    def drain(c, carry):
        for ph in range(CROSS):
            for o in range(dim_count):
                @pl.when((o <= d) & (d < dim_count - 1))
                def _():
                    right(ph, c, o).wait_send()

                @pl.when((o >= d) & (d > 0))
                def _():
                    left(ph, c, o).wait_send()

                pair(ph, c, o, f).wait_send()
        return carry

    lax.fori_loop(0, chunks, drain, 0)
    for k in range(3):
        for o in range(dim_count):
            @pl.when((o <= d) & (d < high))
            def _():
                chain_to(k, o, chain_right, to_right).wait_send()

            @pl.when((o >= d) & (d > low))
            def _():
                chain_to(k, o, chain_left, to_left).wait_send()

    @pl.when(active)
    def _():
        for k in range(3):
            both(k, f).wait_send()
        if split > 1:
            for k in range(1, split):
                t = lax.rem(b + k, split)
                plane(t, b).wait_send()
                plane_both(t, f).wait_send()
        for k in range(1, batch_count):
            cand_copy(lax.rem(b + k, batch_count), b).wait_send()
        for k in range(1, members):
            loss_copy(lax.rem(me + k, members), f, level_of).wait_send()

    for c in range(chunks):
        for level in range(held):
            @pl.when(jnp.logical_not(own_rows(c, level)))
            def _():
                row_copy(c, level).wait_send()

    for ff in range(field_count):
        for level in range(held):
            @pl.when(jnp.logical_not((f == ff) & (level_of == level)))
            def _():
                loss_copy(ff * dim_count + low + level, ff, level).wait_recv()

    for c in range(chunks):
        for level in range(held):
            loss_out[c * held + level] = losses[level, c]


def line_pieces(count, parts):
    base, extra = divmod(count, parts)
    bounds, start = [], 0
    for k in range(parts):
        size = base + (k < extra)
        bounds.append((start, size))
        start += size
    return bounds


def line_fits(counts, features, tower_weight, candidates):
    batch_count, field_count, dim_count = counts
    fl, el, row_count = features.shape
    units, fields, width = tower_weight.shape
    return (
        dim_count == 4 and batch_count == 4 and field_count == 2
        and fields % 2 == 0 and fl >= PIECES and el % 32 == 0 and 4 * el == width and width == 128
        and row_count % (CHUNKS * field_count * 128) == 0 and units % (16 * batch_count) == 0)


PIECES = 4
CHUNKS = 4


def line_kernel(
    counts,
    feat, weight, bias, tower, tower_bias, query_weight, user, cand, positive,
    out, loss_out,
    x0, x1, y, x2, flat, tw, tw_near, tw_far, tw_raw, q_raw, pre_out, pre_in, pre_own,
    bias_raw, bias_cols, unit_raw, unit_cols, cands, users, targets, losses,
    feat_sem, weight_sem, small_sem,
    end_send, end_recv, cross_send, cross_recv, pair_send, pair_recv, one_send, one_recv,
    piece_send, piece_recv, plane_send, plane_recv, tower_send, tower_recv, both_send, both_recv,
    bias_send, bias_recv, unit_send, unit_recv, cand_send, cand_recv,
    two_send, two_recv, out_sem, give_send, give_recv, part_send, part_recv, loss_send, loss_recv,
):
    batch_count, field_count, dim_count = counts
    b = lax.axis_index("batch")
    f = lax.axis_index("field")
    d = lax.axis_index("dim")
    members = field_count * dim_count
    me = f * dim_count + d
    chunks, fields, width, rc = x0.shape
    fl, el, _ = feat.shape
    wide = 2 * el
    half_k = fields // 2 * width
    quarter_units = tw_near.shape[0]
    units = tw.shape[1]
    side_k = fields * wide
    lanes = rc // field_count
    rows_in_part = el // 2
    side = d // 2
    mid = 1 + side
    far = 2 - side
    end = 3 * side
    far_end = 3 - end
    is_mid = d == mid
    is_end = d == end
    other = field_count - 1 - f
    x_next = b + 1 - 2 * lax.rem(b, 2)
    y_next = lax.rem(b + 2, 4)
    diagonal = 3 - b
    fs = pl.ds(f * fl, fl)
    ss = pl.ds(pl.multiple_of(side * wide, wide), wide)

    def remote(ref, send, recv, to=None, **where):
        return pltpu.make_async_remote_copy(
            ref, ref if to is None else to, send, recv, device_id=where, device_id_type=MESH)

    def entries(o):
        return pl.ds(pl.multiple_of(o * el, el), el)

    def within(o):
        return pl.ds(pl.multiple_of(lax.rem(o, 2) * el, el), el)

    def block(c, ff, o):
        return x0.at[c, pl.ds(ff * fl, fl), entries(o), :]

    def from_end(c, target):
        return remote(block(c, f, end), end_send.at[c], end_recv.at[c], dim=target)

    def cross(k, c, o):
        return remote(block(c, f, o), cross_send.at[k, c], cross_recv.at[k, c], dim=far)

    def cross_one(c, s):
        ref = x1.at[c, fs, pl.ds(pl.multiple_of(s * wide, wide), wide), :]
        return remote(ref, cross_send.at[2, c], cross_recv.at[2, c], dim=far)

    def pair(c, o, ff):
        return remote(block(c, ff, o), pair_send.at[o, c], pair_recv.at[o, c], field=other)

    def pair_one(c, s, ff):
        ref = x1.at[c, pl.ds(ff * fl, fl), pl.ds(pl.multiple_of(s * wide, wide), wide), :]
        return remote(ref, one_send.at[s, c], one_recv.at[s, c], field=other)

    def weight_piece(level, p, source):
        start, size = line_pieces(fl, PIECES)[p]
        row = pl.multiple_of(lax.rem(end, 2) * el + lax.rem(source, 2) * rows_in_part, rows_in_part)
        lane = pl.multiple_of(source // 2 * half_k, half_k)
        return flat.at[level, pl.ds(start, size), pl.ds(row, rows_in_part), pl.ds(lane, half_k)]

    def piece(level, p, target):
        ref = weight_piece(level, p, b)
        return remote(ref, piece_send.at[level, p], piece_recv.at[level, p], dim=target)

    def tower_rows(member, source):
        return tw.at[member, pl.ds(pl.multiple_of(source * quarter_units, quarter_units), quarter_units), :]

    def item(i, source):
        if i < CROSS * PIECES:
            return weight_piece(i // PIECES, i % PIECES, source)
        return tower_rows(f * dim_count + i - CROSS * PIECES, source)

    def plane(i, slot, source, target):
        return remote(item(i, source), plane_send.at[i, slot], plane_recv.at[i, source], batch=target)

    def plane_out(i):
        plane(i, 0, b, x_next).start()
        plane(i, 1, b, y_next).start()

    def relay(i):
        return (x_next, y_next) if i % 2 == 0 else (y_next, x_next)

    def plane_forward(i):
        source, target = relay(i)
        plane(i, 2, source, target).wait_recv()
        plane(i, 2, source, target).start()

    def plane_rest(i):
        plane(i, 2, relay(i)[1], x_next).wait_recv()
        plane(i, 2, diagonal, x_next).wait_recv()

    def tower_item(z):
        return CROSS * PIECES + z

    def tower_copy(slot, ref, source, target):
        return remote(
            ref, tower_send.at[slot], tower_recv.at[source],
            to=tower_rows(f * dim_count + source, b), dim=target)

    def both(ff):
        return remote(tw.at[pl.ds(ff * dim_count, dim_count)], both_send, both_recv, field=other)

    def bias_copy(target):
        return remote(bias_raw.at[lax.rem(end, 2)], bias_send, bias_recv, dim=target)

    def unit_copy(k, source, ff, z):
        return remote(unit_raw.at[source], unit_send.at[k], unit_recv.at[source], field=ff, dim=z)

    def cand_copy(k, source):
        t = lax.rem(b + k, batch_count)
        return remote(cands.at[source], cand_send.at[k], cand_recv.at[source], batch=t)

    def two(c, ff):
        lane = pl.multiple_of((1 - ff) * lanes, lanes)
        return remote(
            y.at[c, :, :, pl.ds(lane, lanes)], two_send.at[c], two_recv.at[c],
            to=x2.at[c, pl.ds(ff * fl, fl)], field=other)

    def rows_of(c):
        return pl.ds(pl.multiple_of(c * rc, rc), rc)

    def keep(c):
        return pltpu.make_async_copy(y.at[c, :, within(mid), :], out.at[:, :, rows_of(c)], out_sem.at[c])

    def give(c):
        return remote(
            y.at[c, :, within(end), :], give_send.at[c], give_recv.at[c],
            to=out.at[:, :, rows_of(c)], dim=end)

    def part(j):
        return remote(pre_out.at[j], part_send.at[j], part_recv.at[j], to=pre_in.at[j], dim=far)

    def loss_copy(k, c, ff):
        m = lax.rem(me + k, members)
        return remote(
            losses.at[c, ff], loss_send.at[c, k], loss_recv.at[c, ff],
            field=m // dim_count, dim=lax.rem(m, dim_count))

    def own_weight(level, ff):
        return pltpu.make_async_copy(
            weight.at[level, :, ff],
            flat.at[level, :, within(mid), pl.ds(pl.multiple_of(ff * width, width), width)],
            weight_sem.at[level, ff])

    def end_weight(level, k):
        row = pl.multiple_of(lax.rem(b, 2) * rows_in_part, rows_in_part)
        ff = b // 2 * (fields // 2) + k
        to = pl.multiple_of(lax.rem(end, 2) * el + row, rows_in_part)
        return pltpu.make_async_copy(
            weight.at[level, :, ff, pl.ds(row, rows_in_part), :],
            flat.at[level, :, pl.ds(to, rows_in_part), pl.ds(pl.multiple_of(ff * width, width), width)],
            weight_sem.at[level, k])

    def each(count, act):
        def step(k, carry):
            act(k)
            return carry

        lax.fori_loop(0, count, step, 0)

    own_features = [
        pltpu.make_async_copy(feat.at[:, :, pl.ds(c * rc, rc)], block(c, f, d), feat_sem.at[c])
        for c in range(chunks)]
    quarter = pl.ds(pl.multiple_of(b * quarter_units, quarter_units), quarter_units)
    small = [
        pltpu.make_async_copy(bias, bias_raw.at[lax.rem(d, 2)], small_sem.at[0]),
        pltpu.make_async_copy(tower_bias, unit_raw.at[me], small_sem.at[1]),
        pltpu.make_async_copy(cand, cands.at[b], small_sem.at[2]),
        pltpu.make_async_copy(tower.at[:, quarter, :], tw_raw, small_sem.at[3]),
        pltpu.make_async_copy(query_weight.at[quarter, :], q_raw, small_sem.at[4]),
        pltpu.make_async_copy(user, users, small_sem.at[5]),
        pltpu.make_async_copy(positive, targets, small_sem.at[6]),
    ]
    for copy in own_features:
        copy.start()

    @pl.when(is_end)
    def _():
        each(fields // 2, lambda k: end_weight(0, k).start())

    for copy in small:
        copy.start()

    @pl.when(is_mid)
    def _():
        each(fields, lambda k: own_weight(0, k).start())
        each(fields, lambda k: own_weight(1, k).start())

    @pl.when(is_end)
    def _():
        each(fields // 2, lambda k: end_weight(1, k).start())

    barrier = pltpu.get_barrier_semaphore()
    for k in range(1, members):
        m = lax.rem(me + k, members)
        pl.semaphore_signal(
            barrier, inc=1, device_id={"field": m // dim_count, "dim": lax.rem(m, dim_count)},
            device_id_type=MESH)
    for k in range(1, batch_count):
        pl.semaphore_signal(
            barrier, inc=1, device_id={"batch": lax.rem(b + k, batch_count)}, device_id_type=MESH)
    pl.semaphore_wait(barrier, members + batch_count - 2)

    def unit_sends(act):
        k = 0
        for ff in range(field_count):
            for z in (1, 2):
                @pl.when((f != ff) | (d != z))
                def _():
                    act(unit_copy(k, me, ff, z))
                k += 1

    def pack_tower():
        for s, ref in ((0, tw_near), (1, tw_far)):
            start = jnp.where(s == 0, side, 1 - side)
            for j in range(fields // 2):
                first = tw_raw[2 * j]
                second = tw_raw[2 * j + 1]
                low = jnp.concatenate([first[:, :wide], second[:, :wide]], axis=1)
                high = jnp.concatenate([first[:, wide:], second[:, wide:]], axis=1)
                ref[:, j * width:(j + 1) * width] = jnp.where(start == 0, low, high)
            ref[:, side_k:] = q_raw[...]

    @pl.when(is_end)
    def _():
        each(fields // 2, lambda k: end_weight(0, k).wait())
        piece(0, 0, mid).start()
        piece(0, 1, mid).start()
        for copy in own_features:
            copy.wait()
        from_end(0, mid).start()
        piece(0, 2, mid).start()
        piece(0, 3, mid).start()
        for c in range(1, chunks):
            from_end(c, mid).start()
        for copy in small:
            copy.wait()
        bias_copy(mid).start()
        unit_sends(lambda copy: copy.start())
        pack_tower()
        tower_copy(0, tw_near, d, mid).start()
        tower_copy(1, tw_far, d, far).start()
        each(fields // 2, lambda k: end_weight(1, k).wait())
        for p in range(PIECES):
            piece(1, p, mid).start()

    def expect_piece(level, p):
        piece(level, p, end).wait_recv()
        plane_out(level * PIECES + p)

    def expect_end(c):
        from_end(c, end).wait_recv()
        cross(1, c, end).start()
        pair(c, end, f).start()

    def expect_far(k, c, o):
        cross(k, c, o).wait_recv()
        pair(c, o, f).start()

    def expect_tower(z):
        tower_copy(0, tw_near, z, end).wait_recv()
        for k in range(dim_count):
            @pl.when(z == k)
            def _():
                plane_out(tower_item(k))

    def on_tower(z, act):
        for k in range(dim_count):
            @pl.when(z == k)
            def _():
                act(tower_item(k))

    def advance(source, level, c):
        product = jnp.dot(
            flat[level].reshape(fl * wide, fields * width), source[c].reshape(fields * width, rc),
            preferred_element_type=jnp.float32)
        column = bias_cols[level]
        product = product + jnp.concatenate([column] * (rc // column.shape[1]), axis=1)
        anchor = x0[c, fs, ss, :].astype(jnp.float32).reshape(fl * wide, rc)
        current = source[c, fs, ss, :].astype(jnp.float32).reshape(fl * wide, rc)
        return (anchor * product + current).astype(jnp.bfloat16).reshape(fl, wide, rc)

    def build_bias():
        pick = (lax.broadcasted_iota(jnp.int32, (el, el), 0) == lax.broadcasted_iota(jnp.int32, (el, el), 1))
        for level in range(CROSS):
            for k in range(fl):
                for s in range(2):
                    line = bias_raw[s, level, k:k + 1, :]
                    column = jnp.sum(jnp.where(pick, line, 0.0), axis=1, keepdims=True)
                    start = (2 * k + s) * el
                    bias_cols[level, start:start + el, :] = jnp.broadcast_to(column, (el, width))

    def build_units():
        for m in range(members):
            unit_cols[m * units:(m + 1) * units, :] = jnp.broadcast_to(unit_raw[m], (lanes, units)).T

    def first(c, carry):
        @pl.when(c == 1)
        def _():
            expect_end(3)

        @pl.when(c == 2)
        def _():
            expect_far(1, 2, far_end)

        @pl.when(c == 3)
        def _():
            expect_tower(end)
            expect_far(1, 3, far_end)

        for o in range(dim_count):
            pair(c, o, other).wait_recv()
        x1[c, fs, ss, :] = advance(x0, 0, c)
        cross_one(c, side).start()
        pair_one(c, side, f).start()
        return carry

    def tower_part(c):
        matrix = tw[:, :, :side_k].reshape(members * units, side_k)
        return jnp.dot(matrix, x2[c].reshape(side_k, lanes), preferred_element_type=jnp.float32)

    def second(c, carry):
        cross_one(c, 1 - side).wait_recv()
        pair_one(c, 1 - side, f).start()
        pair_one(c, side, other).wait_recv()
        pair_one(c, 1 - side, other).wait_recv()
        new = advance(x1, 1, c)
        y[c] = new
        two(c, f).start()
        for ff in range(field_count):
            @pl.when(f == ff)
            def _():
                x2[c, fs] = new[:, :, ff * lanes:(ff + 1) * lanes]
        give(c).start()
        keep(c).start()
        two(c, other).wait_recv()
        pre = tower_part(c)
        j = c // 2

        @pl.when(lax.rem(c, 2) == side)
        def _():
            pre_own[j] = pre

        @pl.when(lax.rem(c, 2) != side)
        def _():
            pre_out[j] = pre.astype(jnp.bfloat16)
            part(j).start()

        return carry

    def finish(j, carry):
        c = 2 * j + side
        part(j).wait_recv()
        pre = pre_own[j] + pre_in[j].astype(jnp.float32) + unit_cols[...]
        hidden = jnp.maximum(pre, 0.0).astype(jnp.bfloat16)
        query = lax.dot_general(
            hidden, tw[:, :, side_k:].reshape(members * units, width), (((0,), (0,)), ((), ())),
            preferred_element_type=jnp.float32)
        start = pl.multiple_of(c * rc + f * lanes, lanes)
        query_vec = (query + users[pl.ds(start, lanes), :].astype(jnp.float32)).astype(jnp.bfloat16)
        logits = lax.dot_general(
            cands[...].reshape(-1, width), query_vec, (((1,), (1,)), ((), ())),
            preferred_element_type=jnp.float32) * (1.0 / math.sqrt(width))
        labels = lax.broadcasted_iota(jnp.int32, logits.shape, 0)
        target = targets[c * field_count + f]
        picked = jnp.sum(jnp.where(labels == target, logits, 0.0), axis=0, keepdims=True)
        best = jnp.max(logits, axis=0, keepdims=True)
        total = jnp.sum(jnp.exp(logits - best), axis=0, keepdims=True)
        losses[c, f] = best + jnp.log(total) - picked
        for k in range(1, members):
            loss_copy(k, c, f).start()
        return carry

    @pl.when(is_mid)
    def _():
        for c in range(chunks):
            own_features[c].wait()
            cross(0, c, mid).start()
            pair(c, mid, f).start()
        for copy in small:
            copy.wait()
        unit_sends(lambda copy: copy.start())
        for k in range(1, batch_count):
            cand_copy(k, b).start()
        pack_tower()
        tower_copy(1, tw_far, d, far).start()
        tw[me, quarter, :] = tw_near[...]
        expect_piece(0, 0)
        expect_far(0, 0, far)
        expect_piece(0, 1)
        plane_forward(0)
        expect_far(0, 1, far)
        expect_end(0)
        plane_forward(1)
        expect_far(0, 2, far)
        expect_piece(0, 2)
        expect_far(0, 3, far)
        bias_copy(end).wait_recv()
        build_bias()
        expect_piece(0, 3)
        plane_forward(2)
        on_tower(d, plane_out)
        expect_tower(far)
        expect_end(1)
        expect_far(1, 0, far_end)
        plane_forward(3)
        expect_end(2)
        expect_far(1, 1, far_end)
        for level in range(CROSS):
            each(fields, lambda k: own_weight(level, k).wait())
        for p in range(PIECES):
            plane_rest(p)
        lax.fori_loop(0, chunks, first, 0)
        on_tower(d, plane_forward)
        on_tower(far, plane_forward)
        expect_piece(1, 0)
        on_tower(end, plane_forward)
        expect_tower(far_end)
        expect_piece(1, 1)
        plane_forward(PIECES)
        on_tower(far_end, plane_forward)
        expect_piece(1, 2)
        plane_forward(PIECES + 1)
        for k in range(1, batch_count):
            cand_copy(0, lax.rem(b + k, batch_count)).wait_recv()
        for m in range(members):
            @pl.when(me != m)
            def _():
                unit_copy(0, m, f, d).wait_recv()
        build_units()
        for z in range(dim_count):
            plane_rest(tower_item(z))
        both(f).start()
        expect_piece(1, 3)
        plane_forward(PIECES + 2)
        plane_forward(PIECES + 3)
        for p in range(PIECES):
            plane_rest(PIECES + p)
        both(other).wait_recv()
        lax.fori_loop(0, chunks, second, 0)
        lax.fori_loop(0, chunks // 2, finish, 0)

    for c in range(chunks):
        for ff in range(field_count):
            @pl.when(jnp.logical_not((d == 1 + c % 2) & (f == ff)))
            def _():
                loss_copy(1, c, ff).wait_recv()

    for c in range(chunks):
        for ff in range(field_count):
            loss_out[c * field_count + ff] = losses[c, ff]

    @pl.when(is_end)
    def _():
        for level in range(CROSS):
            for p in range(PIECES):
                piece(level, p, mid).wait_send()
        for c in range(chunks):
            from_end(c, mid).wait_send()
            give(c).wait_recv()
        bias_copy(mid).wait_send()
        tower_copy(0, tw_near, d, mid).wait_send()
        tower_copy(1, tw_far, d, far).wait_send()

    unit_sends(lambda copy: copy.wait_send())

    @pl.when(is_mid)
    def _():
        tower_copy(1, tw_far, d, far).wait_send()
        for k in range(1, batch_count):
            cand_copy(k, b).wait_send()
        both(f).wait_send()

        def drain(c, carry):
            cross(0, c, mid).wait_send()
            cross(1, c, end).wait_send()
            cross_one(c, side).wait_send()
            for o in range(dim_count):
                pair(c, o, f).wait_send()
            for s in range(2):
                pair_one(c, s, f).wait_send()
            two(c, f).wait_send()
            give(c).wait_send()
            keep(c).wait()
            return carry

        lax.fori_loop(0, chunks, drain, 0)

        for i in range(CROSS * PIECES + dim_count):
            plane(i, 0, b, x_next).wait_send()
            plane(i, 1, b, y_next).wait_send()
            plane(i, 2, *relay(i)).wait_send()

        def drain_half(j, carry):
            part(j).wait_send()
            for k in range(1, members):
                loss_copy(k, 2 * j + side, f).wait_send()
            return carry

        lax.fori_loop(0, chunks // 2, drain_half, 0)


def line_body(
    counts, features, cross_weight, cross_bias, tower_weight, tower_bias, query_weight,
    user_vec, candidates, positive,
):
    batch_count, field_count, dim_count = counts
    members = field_count * dim_count
    fl, el, row_count = features.shape
    units, fields, width = tower_weight.shape
    rc = row_count // CHUNKS
    lanes = rc // field_count
    wide = 2 * el
    quarter = units // batch_count
    packed = fields * wide + width
    pairs = CHUNKS // 2
    items = CROSS * PIECES + dim_count
    dma = pltpu.SemaphoreType.DMA
    vmem = pltpu.VMEM
    bf16 = jnp.bfloat16
    f32 = jnp.float32
    far = pl.BlockSpec(memory_space=pl.ANY)
    near = pl.BlockSpec(memory_space=pltpu.VMEM)
    crossed, losses = pl.pallas_call(
        functools.partial(line_kernel, counts),
        out_shape=(
            jax.ShapeDtypeStruct(features.shape, bf16),
            jax.ShapeDtypeStruct((CHUNKS * field_count, 1, lanes), f32),
        ),
        in_specs=[far] * 9,
        out_specs=(far, near),
        scratch_shapes=[
            vmem((CHUNKS, fields, width, rc), bf16),
            vmem((CHUNKS, fields, width, rc), bf16),
            vmem((CHUNKS, fl, wide, rc), bf16),
            vmem((CHUNKS, fields, wide, lanes), bf16),
            vmem((CROSS, fl, wide, fields * width), bf16),
            vmem((members, units, packed), bf16),
            vmem((quarter, packed), bf16),
            vmem((quarter, packed), bf16),
            vmem((fields, quarter, width), bf16),
            vmem((quarter, width), bf16),
            vmem((pairs, members * units, lanes), bf16),
            vmem((pairs, members * units, lanes), bf16),
            vmem((pairs, members * units, lanes), f32),
            vmem((2, CROSS, fl, el), f32),
            vmem((CROSS, fl * wide, width), f32),
            vmem((members, 1, units), f32),
            vmem((members * units, lanes), f32),
            vmem((batch_count,) + candidates.shape, bf16),
            vmem(user_vec.shape, bf16),
            vmem((CHUNKS * field_count, 1, lanes), jnp.int32),
            vmem((CHUNKS, field_count, 1, lanes), f32),
            dma((CHUNKS,)), dma((CROSS, fields)), dma((7,)),
            dma((CHUNKS,)), dma((CHUNKS,)), dma((3, CHUNKS)), dma((3, CHUNKS)),
            dma((dim_count, CHUNKS)), dma((dim_count, CHUNKS)), dma((2, CHUNKS)), dma((2, CHUNKS)),
            dma((CROSS, PIECES)), dma((CROSS, PIECES)), dma((items, 3)), dma((items, batch_count)),
            dma((2,)), dma((dim_count,)), dma, dma,
            dma, dma, dma((members,)), dma((members,)), dma((batch_count,)), dma((batch_count,)),
            dma((CHUNKS,)), dma((CHUNKS,)), dma((CHUNKS,)), dma((CHUNKS,)), dma((CHUNKS,)),
            dma((pairs,)), dma((pairs,)), dma((CHUNKS, members)), dma((CHUNKS, field_count)),
        ],
        compiler_params=pltpu.CompilerParams(
            collective_id=0, has_side_effects=True, vmem_limit_bytes=60 * 2**20),
        name="line_forward",
    )(
        features,
        cross_weight.transpose(0, 1, 3, 2, 4),
        cross_bias,
        tower_weight.transpose(1, 0, 2),
        tower_bias.reshape(1, units),
        query_weight,
        user_vec,
        candidates,
        positive.reshape(CHUNKS * field_count, 1, lanes),
    )
    return (crossed, losses.reshape(row_count))


def body(
    features, cross_weight, cross_bias, tower_weight, tower_bias, query_weight,
    user_vec, candidates, positive,
):
    counts = tuple(lax.axis_size(name) for name in ("batch", "field", "dim"))
    if line_fits(counts, features, tower_weight, candidates):
        return line_body(
            counts, features, cross_weight, cross_bias, tower_weight, tower_bias, query_weight,
            user_vec, candidates, positive)
    batch_count, field_count, dim_count = counts
    members = field_count * dim_count
    fl, el, row_count = features.shape
    columns = fl * el
    units, fields, width = tower_weight.shape
    low, held = tower_levels(dim_count)
    chunks = chunk_count(row_count, field_count, held)
    split = batch_count if units % (batch_count * 16) == 0 else 1
    part = units // split
    rc = row_count // chunks
    sub = rc // held
    run = chunks // field_count
    share = run * sub
    steps = (CROSS, chunks, dim_count)
    small = (3, dim_count)
    dma = pltpu.SemaphoreType.DMA
    vmem = pltpu.VMEM
    bf16 = jnp.bfloat16
    far = pl.BlockSpec(memory_space=pl.ANY)
    near = pl.BlockSpec(memory_space=pltpu.VMEM)
    crossed, losses = pl.pallas_call(
        functools.partial(rank_kernel, counts, (chunks, split)),
        out_shape=(
            jax.ShapeDtypeStruct(features.shape, bf16),
            jax.ShapeDtypeStruct((chunks * held, 1, sub), jnp.float32),
        ),
        in_specs=[far, far, near, far, far, far, near, far, near],
        out_specs=(near, near),
        scratch_shapes=[
            vmem((chunks, fields, width, rc), bf16),
            vmem((chunks, fields, width, rc), bf16),
            vmem((CROSS, fl, el, fields * width), bf16),
            vmem((chunks, held, fl, el, sub), bf16),
            vmem((fields, width, share), bf16),
            vmem((split, members, part, fields * width), bf16),
            vmem((members, 1, units), jnp.float32),
            vmem((split, members, part, share), jnp.float32),
            vmem((split, members, part, width), bf16),
            vmem((batch_count,) + candidates.shape, bf16),
            vmem((held, chunks, 1, sub), jnp.float32),
            dma((chunks,)), dma((CROSS, fields)), dma((fields,)), dma((3,)),
            dma(steps), dma(steps), dma(steps), dma(steps), dma(steps),
            dma((chunks, held)), dma((run, members)), dma(small), dma(small), dma(small),
            dma((3,)), dma((3,)),
            dma((split,)), dma((split,)), dma((split,)), dma((split,)),
            dma((batch_count,)), dma((batch_count,)), dma((members,)), dma((field_count, held)),
        ],
        compiler_params=pltpu.CompilerParams(
            collective_id=0, has_side_effects=True, vmem_limit_bytes=56 * 2**20),
        name="rank_forward",
    )(
        features,
        cross_weight.transpose(0, 1, 3, 2, 4),
        cross_bias.reshape(CROSS, columns, 1),
        tower_weight.transpose(1, 0, 2),
        tower_bias.reshape(1, units),
        query_weight.reshape(split, part, width),
        user_vec,
        candidates,
        positive.reshape(chunks * held, 1, sub),
    )
    return (crossed, losses.reshape(row_count))


def solution(mesh):
    placed = (
        P("field", "dim", "batch"),
        P(None, "field", "dim", None, None),
        P(None, "field", "dim"),
        P(("field", "dim"), None, None),
        P(("field", "dim")),
        P(("field", "dim"), None),
        P("batch", None),
        P("batch", None),
        P("batch"),
    )
    return jax.shard_map(
        body,
        mesh=mesh,
        in_specs=placed,
        out_specs=(P("field", "dim", "batch"), P("batch")),
        check_vma=False,
    )
```

```python
import functools
import math

import jax
import jax.numpy as jnp
from jax import lax
from jax.experimental import pallas as pl
from jax.experimental.pallas import tpu as pltpu
from jax.sharding import PartitionSpec as P

CROSS = 2
MESH = pl.DeviceIdType.MESH


def tower_levels(dim_count):
    held = min(2, dim_count)
    return (dim_count - held) // 2, held


def chunk_count(row_count, field_count, held):
    chunks = 2
    while chunks > field_count and row_count % (chunks * held * 128):
        chunks //= 2
    return chunks


def rank_kernel(
    counts, splits,
    feat, weight, bias, tower, tower_bias, query_weight, user, cand, positive,
    out, loss_out,
    x0, x1, flat, sent, rows, towers, biases, columns_bias, queries, cands, losses,
    feat_sem, weight_sem, tower_sem, small_sem,
    right_sem, left_sem, pair_sem, recv_sem, pair_recv,
    row_send, row_recv, chain_right, chain_left, chain_recv, both_send, both_recv,
    plane_send, plane_recv, plane_pair, plane_pair_recv,
    cand_send, cand_recv, loss_send, loss_recv,
):
    batch_count, field_count, dim_count = counts
    chunks, split = splits
    b = lax.axis_index("batch")
    f = lax.axis_index("field")
    d = lax.axis_index("dim")
    me = f * dim_count + d
    members = field_count * dim_count
    fl, el, row_count = feat.shape
    columns = fl * el
    fields, width, rc = x0.shape[1:]
    low, held = tower_levels(dim_count)
    high = low + held - 1
    level_of = d - low
    active = (d >= low) & (d <= high)
    sub = rc // held
    run = chunks // field_count
    share = run * sub
    part = towers.shape[2]
    units = split * part
    buffers = (x0, x1)
    other = field_count - 1 - f
    mine = b if split > 1 else 0
    to_right = jnp.minimum(d + 1, dim_count - 1)
    to_left = jnp.maximum(d - 1, 0)

    def remote(ref, send, recv, **where):
        return pltpu.make_async_remote_copy(
            ref, ref, send, recv, device_id=where, device_id_type=MESH)

    def place(ff, o):
        return pl.ds(ff * fl, fl), pl.ds(pl.multiple_of(o * el, el), el)

    def piece(ph, c, ff, o):
        fs, ds = place(ff, o)
        return buffers[ph].at[c, fs, ds, :]

    def right(ph, c, o):
        return remote(piece(ph, c, f, o), right_sem.at[ph, c, o], recv_sem.at[ph, c, o], dim=to_right)

    def left(ph, c, o):
        return remote(piece(ph, c, f, o), left_sem.at[ph, c, o], recv_sem.at[ph, c, o], dim=to_left)

    def pair(ph, c, o, ff):
        return remote(
            piece(ph, c, ff, o), pair_sem.at[ph, c, o], pair_recv.at[ph, c, o], field=other)

    def issue_own(ph, c):
        @pl.when(d < dim_count - 1)
        def _():
            right(ph, c, d).start()

        @pl.when(d > 0)
        def _():
            left(ph, c, d).start()

        pair(ph, c, d, f).start()

    def forwards(ph, c):
        for s in range(1, dim_count):
            @pl.when(d - s >= 0)
            def _():
                right(ph, c, d - s).wait_recv()

                @pl.when(d < dim_count - 1)
                def _():
                    right(ph, c, d - s).start()

                pair(ph, c, d - s, f).start()

            @pl.when(d + s < dim_count)
            def _():
                left(ph, c, d + s).wait_recv()

                @pl.when(d > 0)
                def _():
                    left(ph, c, d + s).start()

                pair(ph, c, d + s, f).start()
        for o in range(dim_count):
            pair(ph, c, o, other).wait_recv()

    def weight_copy(level, ff):
        return pltpu.make_async_copy(
            weight.at[level, :, ff],
            flat.at[level, :, :, pl.ds(pl.multiple_of(ff * width, width), width)],
            weight_sem.at[level, ff])

    def tower_copy(ff):
        return pltpu.make_async_copy(
            tower.at[ff, pl.ds(pl.multiple_of(mine * part, part), part), :],
            towers.at[mine, me, :, pl.ds(pl.multiple_of(ff * width, width), width)],
            tower_sem.at[ff])

    def each_field(act):
        def step(ff, carry):
            act(ff)
            return carry

        lax.fori_loop(0, fields, step, 0)

    small_refs = (
        lambda o: towers.at[mine, f * dim_count + o],
        lambda o: queries.at[:, f * dim_count + o],
        lambda o: biases.at[f * dim_count + o],
    )
    small_wide = (
        lambda ff: towers.at[mine, pl.ds(ff * dim_count, dim_count)],
        lambda ff: queries.at[:, pl.ds(ff * dim_count, dim_count)],
        lambda ff: biases.at[pl.ds(ff * dim_count, dim_count)],
    )

    def chain_to(k, o, sems, target):
        return remote(small_refs[k](o), sems.at[k, o], chain_recv.at[k, o], dim=target)

    def chain_own():
        for k in range(3):
            @pl.when(d < high)
            def _():
                chain_to(k, d, chain_right, to_right).start()

            @pl.when(d > low)
            def _():
                chain_to(k, d, chain_left, to_left).start()

    def chain_step(s):
        for k in range(3):
            @pl.when((d - s >= 0) & (d <= high))
            def _():
                chain_to(k, d - s, chain_right, to_right).wait_recv()

                @pl.when(d < high)
                def _():
                    chain_to(k, d - s, chain_right, to_right).start()

            @pl.when((d + s < dim_count) & (d >= low))
            def _():
                chain_to(k, d + s, chain_left, to_left).wait_recv()

                @pl.when(d > low)
                def _():
                    chain_to(k, d + s, chain_left, to_left).start()

    def both(k, ff):
        return remote(small_wide[k](ff), both_send.at[k], both_recv.at[k], field=other)

    def plane(t, source):
        return remote(
            towers.at[source, pl.ds(f * dim_count, dim_count)],
            plane_send.at[t], plane_recv.at[source], batch=t)

    def plane_both(source, ff):
        return remote(
            towers.at[source, pl.ds(ff * dim_count, dim_count)],
            plane_pair.at[source], plane_pair_recv.at[source], field=other)

    def cand_copy(t, source):
        return remote(cands.at[source], cand_send.at[t], cand_recv.at[source], batch=t)

    def loss_copy(m, ff, level):
        ref = losses.at[level, pl.ds(ff * run, run)]
        return remote(
            ref, loss_send.at[m], loss_recv.at[ff, level], field=m // dim_count, dim=m % dim_count)

    def row_copy(c, level):
        fs, ds = place(f, d)
        return pltpu.make_async_remote_copy(
            sent.at[c, level],
            rows.at[fs, ds, pl.ds(pl.multiple_of(lax.rem(c, run) * sub, sub), sub)],
            row_send.at[c, level], row_recv.at[lax.rem(c, run), me],
            device_id={"field": c // run, "dim": low + level}, device_id_type=MESH)

    def own_rows(c, level):
        return (c // run == f) & (level_of == level)

    def advance(ph, c):
        whole = buffers[ph][c].reshape(fields * width, rc)
        matrix = flat[ph].reshape(columns, fields * width)
        product = jnp.dot(matrix, whole, preferred_element_type=jnp.float32) + bias[ph]
        fs, ds = place(f, d)
        anchor = x0[c, fs, ds, :].astype(jnp.float32).reshape(columns, rc)
        current = buffers[ph][c, fs, ds, :].astype(jnp.float32).reshape(columns, rc)
        return (anchor * product + current).astype(jnp.bfloat16).reshape(fl, el, rc)

    own_copies = []
    for c in range(chunks):
        own_copies.append(pltpu.make_async_copy(
            feat.at[:, :, pl.ds(c * rc, rc)], piece(0, c, f, d), feat_sem.at[c]))
    small_copies = [
        pltpu.make_async_copy(query_weight, queries.at[:, me], small_sem.at[0]),
        pltpu.make_async_copy(tower_bias, biases.at[me], small_sem.at[1]),
        pltpu.make_async_copy(cand, cands.at[b], small_sem.at[2]),
    ]
    for copy in own_copies + small_copies:
        copy.start()
    each_field(lambda ff: tower_copy(ff).start())
    for level in range(CROSS):
        each_field(lambda ff: weight_copy(level, ff).start())

    barrier = pltpu.get_barrier_semaphore()
    for k in range(1, members):
        m = lax.rem(me + k, members)
        pl.semaphore_signal(
            barrier, inc=1, device_id={"field": m // dim_count, "dim": m % dim_count},
            device_id_type=MESH)
    for k in range(1, batch_count):
        pl.semaphore_signal(
            barrier, inc=1, device_id={"batch": lax.rem(b + k, batch_count)}, device_id_type=MESH)
    pl.semaphore_wait(barrier, members + batch_count - 2)
    for copy in own_copies:
        copy.wait()
    issue_own(0, 0)
    if chunks > 1:
        issue_own(0, 1)
    each_field(lambda ff: tower_copy(ff).wait())
    for copy in small_copies:
        copy.wait()
    chain_own()

    @pl.when(active)
    def _():
        for k in range(1, batch_count):
            cand_copy(lax.rem(b + k, batch_count), b).start()

    for level in range(CROSS):
        each_field(lambda ff: weight_copy(level, ff).wait())

    def first(c, carry):
        @pl.when(c + 2 < chunks)
        def _():
            issue_own(0, c + 2)

        forwards(0, c)
        fs, ds = place(f, d)
        x1[c, fs, ds, :] = advance(0, c)
        issue_own(1, c)

        for s in range(1, min(chunks, dim_count)):
            @pl.when(c == s)
            def _():
                chain_step(s)

        return carry

    lax.fori_loop(0, chunks, first, 0)
    for s in range(min(chunks, dim_count), dim_count):
        chain_step(s)

    @pl.when(active)
    def _():
        for k in range(3):
            both(k, f).start()
        if split > 1:
            for k in range(1, split):
                plane(lax.rem(b + k, split), b).start()

    def second(c, carry):
        forwards(1, c)
        new = advance(1, c)
        out[:, :, pl.ds(pl.multiple_of(c * rc, 128), rc)] = new
        for level in range(held):
            block = new[:, :, level * sub:(level + 1) * sub]

            @pl.when(own_rows(c, level))
            def _():
                fs, ds = place(f, d)
                rows[fs, ds, pl.ds(pl.multiple_of(lax.rem(c, run) * sub, sub), sub)] = block

            @pl.when(jnp.logical_not(own_rows(c, level)))
            def _():
                sent[c, level] = block
                row_copy(c, level).start()

        return carry

    lax.fori_loop(0, chunks, second, 0)

    def tower_block(s, query):
        matrix = towers[s].reshape(members * part, fields * width)
        pre = jnp.dot(
            matrix, rows[...].reshape(fields * width, share), preferred_element_type=jnp.float32)
        pre = pre + columns_bias[s].reshape(members * part, share)
        hidden = jnp.maximum(pre, 0.0).astype(jnp.bfloat16)
        return query + lax.dot_general(
            hidden, queries[s].reshape(members * part, width), (((0,), (0,)), ((), ())),
            preferred_element_type=jnp.float32)

    @pl.when(active)
    def _():
        if split > 1:
            for k in range(1, split):
                source = lax.rem(b + k, split)
                plane(source, source).wait_recv()
                plane_both(source, f).start()
        for k in range(3):
            both(k, other).wait_recv()
        for k in range(1, batch_count):
            source = lax.rem(b + k, batch_count)
            cand_copy(source, source).wait_recv()
        for m in range(members):
            block = jnp.broadcast_to(biases[m], (share, units)).T
            columns_bias[:, m] = block.reshape(split, part, share)
        if split > 1:
            for k in range(1, split):
                plane_both(lax.rem(b + k, split), other).wait_recv()
        for j in range(run):
            for k in range(1, members):
                m = lax.rem(me + k, members)
                fs, ds = place(m // dim_count, m % dim_count)
                remote(rows.at[fs, ds, pl.ds(j * sub, sub)], row_send.at[0, 0], row_recv.at[j, m],
                       field=m // dim_count, dim=m % dim_count).wait_recv()

        query = lax.fori_loop(0, split, tower_block, jnp.zeros((share, width), jnp.float32))
        all_cands = cands[...].reshape(-1, width)
        for j in range(run):
            c = f * run + j
            start = pl.multiple_of(c * rc + level_of * sub, sub)
            query_vec = (
                query[j * sub:(j + 1) * sub] + user[pl.ds(start, sub), :].astype(jnp.float32)
            ).astype(jnp.bfloat16)
            logits = lax.dot_general(
                all_cands, query_vec, (((1,), (1,)), ((), ())), preferred_element_type=jnp.float32
            ) * (1.0 / math.sqrt(width))
            labels = lax.broadcasted_iota(jnp.int32, logits.shape, 0)
            target = positive[c * held + level_of]
            picked = jnp.sum(jnp.where(labels == target, logits, 0.0), axis=0, keepdims=True)
            best = jnp.max(logits, axis=0, keepdims=True)
            total = jnp.sum(jnp.exp(logits - best), axis=0, keepdims=True)
            losses[level_of, c] = best + jnp.log(total) - picked
        for k in range(1, members):
            loss_copy(lax.rem(me + k, members), f, level_of).start()

    def drain(c, carry):
        for ph in range(CROSS):
            for o in range(dim_count):
                @pl.when((o <= d) & (d < dim_count - 1))
                def _():
                    right(ph, c, o).wait_send()

                @pl.when((o >= d) & (d > 0))
                def _():
                    left(ph, c, o).wait_send()

                pair(ph, c, o, f).wait_send()
        return carry

    lax.fori_loop(0, chunks, drain, 0)
    for k in range(3):
        for o in range(dim_count):
            @pl.when((o <= d) & (d < high))
            def _():
                chain_to(k, o, chain_right, to_right).wait_send()

            @pl.when((o >= d) & (d > low))
            def _():
                chain_to(k, o, chain_left, to_left).wait_send()

    @pl.when(active)
    def _():
        for k in range(3):
            both(k, f).wait_send()
        if split > 1:
            for k in range(1, split):
                t = lax.rem(b + k, split)
                plane(t, b).wait_send()
                plane_both(t, f).wait_send()
        for k in range(1, batch_count):
            cand_copy(lax.rem(b + k, batch_count), b).wait_send()
        for k in range(1, members):
            loss_copy(lax.rem(me + k, members), f, level_of).wait_send()

    for c in range(chunks):
        for level in range(held):
            @pl.when(jnp.logical_not(own_rows(c, level)))
            def _():
                row_copy(c, level).wait_send()

    for ff in range(field_count):
        for level in range(held):
            @pl.when(jnp.logical_not((f == ff) & (level_of == level)))
            def _():
                loss_copy(ff * dim_count + low + level, ff, level).wait_recv()

    for c in range(chunks):
        for level in range(held):
            loss_out[c * held + level] = losses[level, c]


def line_pieces(count, parts):
    base, extra = divmod(count, parts)
    bounds, start = [], 0
    for k in range(parts):
        size = base + (k < extra)
        bounds.append((start, size))
        start += size
    return bounds


def line_fits(counts, features, tower_weight, candidates):
    batch_count, field_count, dim_count = counts
    fl, el, row_count = features.shape
    units, fields, width = tower_weight.shape
    return (
        dim_count == 4 and batch_count == 4 and field_count == 2
        and fields % 2 == 0 and fl >= PIECES and el % 32 == 0 and 4 * el == width and width == 128
        and row_count % (CHUNKS * field_count * 128) == 0 and units % (16 * batch_count) == 0)


PIECES = 4
CHUNKS = 4
FAR_TOWER = CROSS * PIECES
END_TOWER = FAR_TOWER + 1


def line_kernel(
    counts,
    feat, weight, bias, tower, tower_bias, query_weight, user, cand, positive,
    out, loss_out,
    x0, x1, y, x2, flat, tw, tw_near, tw_far, tw_raw, q_raw, pre_out, pre_in, pre_own,
    bias_raw, bias_cols, unit_raw, unit_cols, cands, users, targets, losses,
    feat_sem, weight_sem, small_sem,
    end_send, end_recv, cross_send, cross_recv, pair_send, pair_recv, one_send, one_recv,
    piece_send, piece_recv, plane_send, plane_recv, tower_send, tower_recv, both_send, both_recv,
    bias_send, bias_recv, unit_send, unit_recv, cand_send, cand_recv,
    two_send, two_recv, out_sem, give_send, give_recv, part_send, part_recv, loss_send, loss_recv,
):
    batch_count, field_count, dim_count = counts
    b = lax.axis_index("batch")
    f = lax.axis_index("field")
    d = lax.axis_index("dim")
    members = field_count * dim_count
    me = f * dim_count + d
    chunks, fields, width, rc = x0.shape
    fl, el, _ = feat.shape
    wide = 2 * el
    half_k = fields // 2 * width
    quarter_units = tw_far.shape[0]
    units = tw.shape[1]
    side_k = fields * wide
    lanes = rc // field_count
    rows_in_part = el // 2
    side = d // 2
    mid = 1 + side
    far = 2 - side
    end = 3 * side
    far_end = 3 - end
    is_mid = d == mid
    is_end = d == end
    owner = is_mid & (f == side)
    giver = is_mid & (f != side)
    other = field_count - 1 - f
    x_next = b + 1 - 2 * lax.rem(b, 2)
    y_next = lax.rem(b + 2, 4)
    diagonal = 3 - b
    fs = pl.ds(f * fl, fl)
    ss = pl.ds(pl.multiple_of(side * wide, wide), wide)

    def remote(ref, send, recv, to=None, **where):
        return pltpu.make_async_remote_copy(
            ref, ref if to is None else to, send, recv, device_id=where, device_id_type=MESH)

    def entries(o):
        return pl.ds(pl.multiple_of(o * el, el), el)

    def within(o):
        return pl.ds(pl.multiple_of(lax.rem(o, 2) * el, el), el)

    def block(c, ff, o):
        return x0.at[c, pl.ds(ff * fl, fl), entries(o), :]

    def from_end(c, target):
        return remote(block(c, f, end), end_send.at[c], end_recv.at[c], dim=target)

    def cross(k, c, o):
        return remote(block(c, f, o), cross_send.at[k, c], cross_recv.at[k, c], dim=far)

    def cross_one(c, s):
        ref = x1.at[c, fs, pl.ds(pl.multiple_of(s * wide, wide), wide), :]
        return remote(ref, cross_send.at[2, c], cross_recv.at[2, c], dim=far)

    def pair(c, o, ff):
        return remote(block(c, ff, o), pair_send.at[o, c], pair_recv.at[o, c], field=other)

    def pair_one(c, s, ff):
        ref = x1.at[c, pl.ds(ff * fl, fl), pl.ds(pl.multiple_of(s * wide, wide), wide), :]
        return remote(ref, one_send.at[s, c], one_recv.at[s, c], field=other)

    def weight_piece(level, p, source):
        start, size = line_pieces(fl, PIECES)[p]
        row = pl.multiple_of(lax.rem(end, 2) * el + lax.rem(source, 2) * rows_in_part, rows_in_part)
        lane = pl.multiple_of(source // 2 * half_k, half_k)
        return flat.at[level, pl.ds(start, size), pl.ds(row, rows_in_part), pl.ds(lane, half_k)]

    def piece(level, p, target):
        ref = weight_piece(level, p, b)
        return remote(ref, piece_send.at[level, p], piece_recv.at[level, p], dim=target)

    def tower_rows(member, source):
        return tw.at[member, pl.ds(pl.multiple_of(source * quarter_units, quarter_units), quarter_units), :]

    def item(i, source):
        if i < CROSS * PIECES:
            return weight_piece(i // PIECES, i % PIECES, source)
        return tower_rows(f * dim_count + (far if i == FAR_TOWER else far_end), source)

    def plane(i, slot, source, target):
        return remote(item(i, source), plane_send.at[i, slot], plane_recv.at[i, source], batch=target)

    def plane_out(i):
        plane(i, 0, b, x_next).start()
        plane(i, 1, b, y_next).start()

    def relay(i):
        return (x_next, y_next) if i % 2 == 0 else (y_next, x_next)

    def plane_forward(i):
        source, target = relay(i)
        plane(i, 2, source, target).wait_recv()
        plane(i, 2, source, target).start()

    def plane_rest(i):
        plane(i, 2, relay(i)[1], x_next).wait_recv()
        plane(i, 2, diagonal, x_next).wait_recv()

    def near_tower(target):
        return remote(
            tw_near, tower_send.at[0], tower_recv.at[end], to=tw.at[f * dim_count + end], dim=target)

    def far_tower(source, target):
        return remote(
            tw_far, tower_send.at[1], tower_recv.at[source],
            to=tower_rows(f * dim_count + source, b), dim=target)

    def both(z, ff):
        return remote(tw.at[ff * dim_count + z], both_send.at[z], both_recv.at[z], field=other)

    def bias_copy(target):
        return remote(bias_raw.at[lax.rem(end, 2)], bias_send, bias_recv, dim=target)

    def unit_copy(k, source, ff, z):
        return remote(unit_raw.at[source], unit_send.at[k], unit_recv.at[source], field=ff, dim=z)

    def cand_copy(k, source):
        t = lax.rem(b + k, batch_count)
        return remote(cands.at[source], cand_send.at[k], cand_recv.at[source], batch=t)

    def two(c, ff):
        lane = pl.multiple_of((1 - ff) * lanes, lanes)
        return remote(
            y.at[c, :, :, pl.ds(lane, lanes)], two_send.at[c], two_recv.at[c],
            to=x2.at[c, pl.ds(ff * fl, fl)], field=other)

    def rows_of(c):
        return pl.ds(pl.multiple_of(c * rc, rc), rc)

    def keep(c):
        return pltpu.make_async_copy(y.at[c, :, within(mid), :], out.at[:, :, rows_of(c)], out_sem.at[c])

    def give(c):
        return remote(
            y.at[c, :, within(end), :], give_send.at[c], give_recv.at[c],
            to=out.at[:, :, rows_of(c)], dim=end)

    def part(c):
        return remote(pre_out.at[c], part_send.at[c], part_recv.at[c], to=pre_in.at[c], dim=far)

    def loss_copy(k, c, ff):
        m = lax.rem(me + k, members)
        return remote(
            losses.at[c, ff], loss_send.at[c, k], loss_recv.at[c, ff],
            field=m // dim_count, dim=lax.rem(m, dim_count))

    def own_weight(level, ff):
        return pltpu.make_async_copy(
            weight.at[level, :, ff],
            flat.at[level, :, within(mid), pl.ds(pl.multiple_of(ff * width, width), width)],
            weight_sem.at[level, ff])

    def end_weight(level, k):
        row = pl.multiple_of(lax.rem(b, 2) * rows_in_part, rows_in_part)
        ff = b // 2 * (fields // 2) + k
        to = pl.multiple_of(lax.rem(end, 2) * el + row, rows_in_part)
        return pltpu.make_async_copy(
            weight.at[level, :, ff, pl.ds(row, rows_in_part), :],
            flat.at[level, :, pl.ds(to, rows_in_part), pl.ds(pl.multiple_of(ff * width, width), width)],
            weight_sem.at[level, k])

    def each(count, act):
        def step(k, carry):
            act(k)
            return carry

        lax.fori_loop(0, count, step, 0)

    own_features = [
        pltpu.make_async_copy(feat.at[:, :, pl.ds(c * rc, rc)], block(c, f, d), feat_sem.at[c])
        for c in range(chunks)]
    quarter = pl.ds(pl.multiple_of(b * quarter_units, quarter_units), quarter_units)
    small = [
        pltpu.make_async_copy(bias, bias_raw.at[lax.rem(d, 2)], small_sem.at[0]),
        pltpu.make_async_copy(tower_bias, unit_raw.at[me], small_sem.at[1]),
        pltpu.make_async_copy(cand, cands.at[b], small_sem.at[2]),
        pltpu.make_async_copy(tower, tw_raw, small_sem.at[3]),
        pltpu.make_async_copy(query_weight, q_raw, small_sem.at[4]),
        pltpu.make_async_copy(user, users, small_sem.at[5]),
        pltpu.make_async_copy(positive, targets, small_sem.at[6]),
    ]
    for copy in own_features:
        copy.start()

    @pl.when(is_end)
    def _():
        each(fields // 2, lambda k: end_weight(0, k).start())

    for copy in small:
        copy.start()

    @pl.when(is_mid)
    def _():
        each(fields, lambda k: own_weight(0, k).start())
        each(fields, lambda k: own_weight(1, k).start())

    @pl.when(is_end)
    def _():
        each(fields // 2, lambda k: end_weight(1, k).start())

    barrier = pltpu.get_barrier_semaphore()
    for k in range(1, members):
        m = lax.rem(me + k, members)
        pl.semaphore_signal(
            barrier, inc=1, device_id={"field": m // dim_count, "dim": lax.rem(m, dim_count)},
            device_id_type=MESH)
    for k in range(1, batch_count):
        pl.semaphore_signal(
            barrier, inc=1, device_id={"batch": lax.rem(b + k, batch_count)}, device_id_type=MESH)
    pl.semaphore_wait(barrier, members + batch_count - 2)

    def unit_sends(act):
        k = 0
        for ff in range(field_count):
            for z in (1, 2):
                @pl.when((f != ff) | (d != z))
                def _():
                    act(unit_copy(k, me, ff, z))
                k += 1

    def pack_tower():
        def halves(rows, j):
            first = tw_raw[2 * j, rows, :]
            second = tw_raw[2 * j + 1, rows, :]
            low = jnp.concatenate([first[:, :wide], second[:, :wide]], axis=1)
            high = jnp.concatenate([first[:, wide:], second[:, wide:]], axis=1)
            return low, high

        for j in range(fields // 2):
            low, high = halves(slice(None), j)
            tw_near[:, j * width:(j + 1) * width] = jnp.where(side == 0, low, high)
            low, high = halves(quarter, j)
            tw_far[:, j * width:(j + 1) * width] = jnp.where(side == 0, high, low)
        tw_near[:, side_k:] = q_raw[...]
        tw_far[:, side_k:] = q_raw[quarter, :]

    @pl.when(is_end)
    def _():
        small[0].wait()
        bias_copy(mid).start()
        small[1].wait()
        unit_sends(lambda copy: copy.start())
        each(fields // 2, lambda k: end_weight(0, k).wait())
        for p in range(PIECES - 1):
            piece(0, p, mid).start()
        own_features[0].wait()
        from_end(0, mid).start()
        piece(0, PIECES - 1, mid).start()
        for c in range(1, chunks):
            own_features[c].wait()
            from_end(c, mid).start()
        for copy in small[2:]:
            copy.wait()
        pack_tower()
        far_tower(d, far).start()
        each(fields // 2, lambda k: end_weight(1, k).wait())
        for p in range(PIECES):
            piece(1, p, mid).start()
        near_tower(mid).start()

    def expect_piece(level, p):
        piece(level, p, end).wait_recv()
        plane_out(level * PIECES + p)

    def expect_end(c):
        from_end(c, end).wait_recv()
        cross(1, c, end).start()
        pair(c, end, f).start()

    def expect_far(k, c, o):
        cross(k, c, o).wait_recv()
        pair(c, o, f).start()

    def expect_tower(i, z):
        far_tower(z, end).wait_recv()
        plane_out(i)

    def half(source, level, c, ff):
        matrix = flat[level, :, :, pl.ds(pl.multiple_of(ff * half_k, half_k), half_k)]
        return jnp.dot(
            matrix.reshape(fl * wide, half_k), source[c, pl.ds(ff * fl, fl)].reshape(half_k, rc),
            preferred_element_type=jnp.float32)

    def advance(source, level, c, wait_pair):
        product = half(source, level, c, f)
        wait_pair()
        product = product + half(source, level, c, other)
        column = bias_cols[level]
        product = product + jnp.concatenate([column] * (rc // column.shape[1]), axis=1)
        anchor = x0[c, fs, ss, :].astype(jnp.float32).reshape(fl * wide, rc)
        current = source[c, fs, ss, :].astype(jnp.float32).reshape(fl * wide, rc)
        return (anchor * product + current).astype(jnp.bfloat16).reshape(fl, wide, rc)

    def build_bias():
        pick = (lax.broadcasted_iota(jnp.int32, (el, el), 0) == lax.broadcasted_iota(jnp.int32, (el, el), 1))
        for level in range(CROSS):
            for k in range(fl):
                for s in range(2):
                    line = bias_raw[s, k, level:level + 1, :]
                    column = jnp.sum(jnp.where(pick, line, 0.0), axis=1, keepdims=True)
                    start = (2 * k + s) * el
                    bias_cols[level, start:start + el, :] = jnp.broadcast_to(column, (el, width))

    def build_units():
        for m in range(members):
            unit_cols[m * units:(m + 1) * units, :] = jnp.broadcast_to(unit_raw[m], (lanes, units)).T

    def first(c, carry):
        @pl.when(c == 1)
        def _():
            expect_end(3)
            cross_one(0, side).start()

        @pl.when(c == 2)
        def _():
            plane_forward(FAR_TOWER)
            expect_far(1, 2, far_end)

        @pl.when(c == 3)
        def _():
            expect_tower(END_TOWER, far_end)
            expect_far(1, 3, far_end)
            expect_piece(1, 0)

        def wait_pair():
            for o in range(dim_count):
                pair(c, o, other).wait_recv()

        x1[c, fs, ss, :] = advance(x0, 0, c, wait_pair)
        pair_one(c, side, f).start()

        @pl.when(c > 0)
        def _():
            cross_one(c, side).start()

        return carry

    def tower_part(c):
        matrix = tw[:, :, :side_k].reshape(members * units, side_k)
        return jnp.dot(matrix, x2[c].reshape(side_k, lanes), preferred_element_type=jnp.float32)

    def layer_two(c):
        cross_one(c, 1 - side).wait_recv()
        pair_one(c, 1 - side, f).start()

        def wait_pair():
            pair_one(c, side, other).wait_recv()
            pair_one(c, 1 - side, other).wait_recv()

        y[c] = advance(x1, 1, c, wait_pair)
        two(c, f).start()
        give(c).start()
        keep(c).start()
        for ff in range(field_count):
            @pl.when(f == ff)
            def _():
                x2[c, fs] = y[c, :, :, ff * lanes:(ff + 1) * lanes]

    def layer_three(c):
        two(c, other).wait_recv()
        pre = tower_part(c)

        @pl.when(owner)
        def _():
            pre_own[c] = pre

        @pl.when(giver)
        def _():
            pre_out[c] = pre.astype(jnp.bfloat16)
            part(c).start()

    def second(c, carry):
        @pl.when(c < chunks)
        def _():
            layer_two(c)

        @pl.when(c > 0)
        def _():
            layer_three(c - 1)

        @pl.when(owner & (c > 1))
        def _():
            finish(c - 2)

        return carry

    def finish(c):
        part(c).wait_recv()
        pre = pre_own[c] + pre_in[c].astype(jnp.float32) + unit_cols[...]
        hidden = jnp.maximum(pre, 0.0).astype(jnp.bfloat16)
        query = lax.dot_general(
            hidden, tw[:, :, side_k:].reshape(members * units, width), (((0,), (0,)), ((), ())),
            preferred_element_type=jnp.float32)
        start = pl.multiple_of(c * rc + f * lanes, lanes)
        query_vec = (query + users[pl.ds(start, lanes), :].astype(jnp.float32)).astype(jnp.bfloat16)
        logits = lax.dot_general(
            cands[...].reshape(-1, width), query_vec, (((1,), (1,)), ((), ())),
            preferred_element_type=jnp.float32) * (1.0 / math.sqrt(width))
        labels = lax.broadcasted_iota(jnp.int32, logits.shape, 0)
        target = targets[c * field_count + f]
        picked = jnp.sum(jnp.where(labels == target, logits, 0.0), axis=0, keepdims=True)
        best = jnp.max(logits, axis=0, keepdims=True)
        total = jnp.sum(jnp.exp(logits - best), axis=0, keepdims=True)
        losses[c, f] = best + jnp.log(total) - picked
        for k in range(1, members):
            loss_copy(k, c, f).start()

    @pl.when(is_mid)
    def _():
        for c in range(chunks):
            own_features[c].wait()
            cross(0, c, mid).start()
            pair(c, mid, f).start()
        small[1].wait()
        unit_sends(lambda copy: copy.start())
        for copy in small[:1] + small[2:]:
            copy.wait()
        for k in range(1, batch_count):
            cand_copy(k, b).start()
        pack_tower()
        far_tower(d, far).start()
        tw[me] = tw_near[...]
        both(mid, f).start()
        bias_copy(end).wait_recv()
        build_bias()
        expect_piece(0, 0)
        expect_far(0, 0, far)
        expect_piece(0, 1)
        expect_far(0, 1, far)
        plane_forward(0)
        expect_piece(0, 2)
        expect_far(0, 2, far)
        plane_forward(1)
        expect_end(0)
        expect_far(0, 3, far)
        plane_forward(2)
        expect_tower(FAR_TOWER, far)
        expect_piece(0, 3)
        expect_far(1, 0, far_end)
        expect_end(1)
        plane_forward(3)
        for level in range(CROSS):
            each(fields, lambda k: own_weight(level, k).wait())
        expect_end(2)
        for p in range(PIECES):
            plane_rest(p)
        expect_far(1, 1, far_end)
        lax.fori_loop(0, chunks, first, 0)
        plane_forward(END_TOWER)
        for k in range(1, batch_count):
            cand_copy(0, lax.rem(b + k, batch_count)).wait_recv()
        for m in range(members):
            @pl.when(me != m)
            def _():
                unit_copy(0, m, f, d).wait_recv()
        build_units()
        expect_piece(1, 1)
        plane_forward(PIECES)
        expect_piece(1, 2)
        plane_forward(PIECES + 1)
        expect_piece(1, 3)
        for i, z in ((FAR_TOWER, far), (END_TOWER, far_end)):
            plane_rest(i)
            both(z, f).start()
        plane_forward(PIECES + 2)
        plane_forward(PIECES + 3)
        near_tower(end).wait_recv()
        both(end, f).start()
        for p in range(PIECES):
            plane_rest(PIECES + p)
        for z in range(dim_count):
            both(z, other).wait_recv()
        lax.fori_loop(0, chunks + 1, second, 0)

        @pl.when(owner)
        def _():
            finish(chunks - 1)

    for c in range(chunks):
        for ff in range(field_count):
            @pl.when(jnp.logical_not((d == 1 + ff) & (f == ff)))
            def _():
                loss_copy(1, c, ff).wait_recv()

    for c in range(chunks):
        for ff in range(field_count):
            loss_out[c * field_count + ff] = losses[c, ff]

    @pl.when(is_end)
    def _():
        for level in range(CROSS):
            for p in range(PIECES):
                piece(level, p, mid).wait_send()
        for c in range(chunks):
            from_end(c, mid).wait_send()
            give(c).wait_recv()
        bias_copy(mid).wait_send()
        near_tower(mid).wait_send()
        far_tower(d, far).wait_send()

    unit_sends(lambda copy: copy.wait_send())

    @pl.when(is_mid)
    def _():
        far_tower(d, far).wait_send()
        for k in range(1, batch_count):
            cand_copy(k, b).wait_send()
        for z in range(dim_count):
            both(z, f).wait_send()

        def drain(c, carry):
            cross(0, c, mid).wait_send()
            cross(1, c, end).wait_send()
            cross_one(c, side).wait_send()
            for o in range(dim_count):
                pair(c, o, f).wait_send()
            for s in range(2):
                pair_one(c, s, f).wait_send()
            two(c, f).wait_send()
            give(c).wait_send()
            keep(c).wait()
            return carry

        lax.fori_loop(0, chunks, drain, 0)

        for i in range(END_TOWER + 1):
            plane(i, 0, b, x_next).wait_send()
            plane(i, 1, b, y_next).wait_send()
            plane(i, 2, *relay(i)).wait_send()

    @pl.when(giver)
    def _():
        for c in range(chunks):
            part(c).wait_send()

    @pl.when(owner)
    def _():
        def drain_losses(c, carry):
            for k in range(1, members):
                loss_copy(k, c, f).wait_send()
            return carry

        lax.fori_loop(0, chunks, drain_losses, 0)


def line_body(
    counts, features, cross_weight, cross_bias, tower_weight, tower_bias, query_weight,
    user_vec, candidates, positive,
):
    batch_count, field_count, dim_count = counts
    members = field_count * dim_count
    fl, el, row_count = features.shape
    units, fields, width = tower_weight.shape
    rc = row_count // CHUNKS
    lanes = rc // field_count
    wide = 2 * el
    quarter = units // batch_count
    packed = fields * wide + width
    items = END_TOWER + 1
    dma = pltpu.SemaphoreType.DMA
    vmem = pltpu.VMEM
    bf16 = jnp.bfloat16
    f32 = jnp.float32
    far = pl.BlockSpec(memory_space=pl.ANY)
    near = pl.BlockSpec(memory_space=pltpu.VMEM)
    crossed, losses = pl.pallas_call(
        functools.partial(line_kernel, counts),
        out_shape=(
            jax.ShapeDtypeStruct(features.shape, bf16),
            jax.ShapeDtypeStruct((CHUNKS * field_count, 1, lanes), f32),
        ),
        in_specs=[far] * 9,
        out_specs=(far, near),
        scratch_shapes=[
            vmem((CHUNKS, fields, width, rc), bf16),
            vmem((CHUNKS, fields, width, rc), bf16),
            vmem((CHUNKS, fl, wide, rc), bf16),
            vmem((CHUNKS, fields, wide, lanes), bf16),
            vmem((CROSS, fl, wide, fields * width), bf16),
            vmem((members, units, packed), bf16),
            vmem((units, packed), bf16),
            vmem((quarter, packed), bf16),
            vmem((fields, units, width), bf16),
            vmem((units, width), bf16),
            vmem((CHUNKS, members * units, lanes), bf16),
            vmem((CHUNKS, members * units, lanes), bf16),
            vmem((CHUNKS, members * units, lanes), f32),
            vmem((2, fl, CROSS, el), f32),
            vmem((CROSS, fl * wide, width), f32),
            vmem((members, 1, units), f32),
            vmem((members * units, lanes), f32),
            vmem((batch_count,) + candidates.shape, bf16),
            vmem(user_vec.shape, bf16),
            vmem((CHUNKS * field_count, 1, lanes), jnp.int32),
            vmem((CHUNKS, field_count, 1, lanes), f32),
            dma((CHUNKS,)), dma((CROSS, fields)), dma((7,)),
            dma((CHUNKS,)), dma((CHUNKS,)), dma((3, CHUNKS)), dma((3, CHUNKS)),
            dma((dim_count, CHUNKS)), dma((dim_count, CHUNKS)), dma((2, CHUNKS)), dma((2, CHUNKS)),
            dma((CROSS, PIECES)), dma((CROSS, PIECES)), dma((items, 3)), dma((items, batch_count)),
            dma((2,)), dma((dim_count,)), dma((dim_count,)), dma((dim_count,)),
            dma, dma, dma((members,)), dma((members,)), dma((batch_count,)), dma((batch_count,)),
            dma((CHUNKS,)), dma((CHUNKS,)), dma((CHUNKS,)), dma((CHUNKS,)), dma((CHUNKS,)),
            dma((CHUNKS,)), dma((CHUNKS,)), dma((CHUNKS, members)), dma((CHUNKS, field_count)),
        ],
        compiler_params=pltpu.CompilerParams(
            collective_id=0, has_side_effects=True, vmem_limit_bytes=60 * 2**20),
        name="line_forward",
    )(
        features,
        cross_weight.transpose(0, 1, 3, 2, 4),
        cross_bias.transpose(1, 0, 2),
        tower_weight.transpose(1, 0, 2),
        tower_bias.reshape(1, units),
        query_weight,
        user_vec,
        candidates,
        positive.reshape(CHUNKS * field_count, 1, lanes),
    )
    return (crossed, losses.reshape(row_count))


def body(
    features, cross_weight, cross_bias, tower_weight, tower_bias, query_weight,
    user_vec, candidates, positive,
):
    counts = tuple(lax.axis_size(name) for name in ("batch", "field", "dim"))
    if line_fits(counts, features, tower_weight, candidates):
        return line_body(
            counts, features, cross_weight, cross_bias, tower_weight, tower_bias, query_weight,
            user_vec, candidates, positive)
    batch_count, field_count, dim_count = counts
    members = field_count * dim_count
    fl, el, row_count = features.shape
    columns = fl * el
    units, fields, width = tower_weight.shape
    low, held = tower_levels(dim_count)
    chunks = chunk_count(row_count, field_count, held)
    split = batch_count if units % (batch_count * 16) == 0 else 1
    part = units // split
    rc = row_count // chunks
    sub = rc // held
    run = chunks // field_count
    share = run * sub
    steps = (CROSS, chunks, dim_count)
    small = (3, dim_count)
    dma = pltpu.SemaphoreType.DMA
    vmem = pltpu.VMEM
    bf16 = jnp.bfloat16
    far = pl.BlockSpec(memory_space=pl.ANY)
    near = pl.BlockSpec(memory_space=pltpu.VMEM)
    crossed, losses = pl.pallas_call(
        functools.partial(rank_kernel, counts, (chunks, split)),
        out_shape=(
            jax.ShapeDtypeStruct(features.shape, bf16),
            jax.ShapeDtypeStruct((chunks * held, 1, sub), jnp.float32),
        ),
        in_specs=[far, far, near, far, far, far, near, far, near],
        out_specs=(near, near),
        scratch_shapes=[
            vmem((chunks, fields, width, rc), bf16),
            vmem((chunks, fields, width, rc), bf16),
            vmem((CROSS, fl, el, fields * width), bf16),
            vmem((chunks, held, fl, el, sub), bf16),
            vmem((fields, width, share), bf16),
            vmem((split, members, part, fields * width), bf16),
            vmem((members, 1, units), jnp.float32),
            vmem((split, members, part, share), jnp.float32),
            vmem((split, members, part, width), bf16),
            vmem((batch_count,) + candidates.shape, bf16),
            vmem((held, chunks, 1, sub), jnp.float32),
            dma((chunks,)), dma((CROSS, fields)), dma((fields,)), dma((3,)),
            dma(steps), dma(steps), dma(steps), dma(steps), dma(steps),
            dma((chunks, held)), dma((run, members)), dma(small), dma(small), dma(small),
            dma((3,)), dma((3,)),
            dma((split,)), dma((split,)), dma((split,)), dma((split,)),
            dma((batch_count,)), dma((batch_count,)), dma((members,)), dma((field_count, held)),
        ],
        compiler_params=pltpu.CompilerParams(
            collective_id=0, has_side_effects=True, vmem_limit_bytes=56 * 2**20),
        name="rank_forward",
    )(
        features,
        cross_weight.transpose(0, 1, 3, 2, 4),
        cross_bias.reshape(CROSS, columns, 1),
        tower_weight.transpose(1, 0, 2),
        tower_bias.reshape(1, units),
        query_weight.reshape(split, part, width),
        user_vec,
        candidates,
        positive.reshape(chunks * held, 1, sub),
    )
    return (crossed, losses.reshape(row_count))


def solution(mesh):
    placed = (
        P("field", "dim", "batch"),
        P(None, "field", "dim", None, None),
        P(None, "field", "dim"),
        P(("field", "dim"), None, None),
        P(("field", "dim")),
        P(("field", "dim"), None),
        P("batch", None),
        P("batch", None),
        P("batch"),
    )
    return jax.shard_map(
        body,
        mesh=mesh,
        in_specs=placed,
        out_specs=(P("field", "dim", "batch"), P("batch")),
        check_vma=False,
    )
```

```python
import functools
import math

import jax
import jax.numpy as jnp
from jax import lax
from jax.experimental import pallas as pl
from jax.experimental.pallas import tpu as pltpu
from jax.sharding import PartitionSpec as P

CROSS = 2
MESH = pl.DeviceIdType.MESH


def tower_levels(dim_count):
    held = min(2, dim_count)
    return (dim_count - held) // 2, held


def chunk_count(row_count, field_count, held):
    chunks = 2
    while chunks > field_count and row_count % (chunks * held * 128):
        chunks //= 2
    return chunks


def rank_kernel(
    counts, splits,
    feat, weight, bias, tower, tower_bias, query_weight, user, cand, positive,
    out, loss_out,
    x0, x1, flat, sent, rows, towers, biases, columns_bias, queries, cands, losses,
    feat_sem, weight_sem, tower_sem, small_sem,
    right_sem, left_sem, pair_sem, recv_sem, pair_recv,
    row_send, row_recv, chain_right, chain_left, chain_recv, both_send, both_recv,
    plane_send, plane_recv, plane_pair, plane_pair_recv,
    cand_send, cand_recv, loss_send, loss_recv,
):
    batch_count, field_count, dim_count = counts
    chunks, split = splits
    b = lax.axis_index("batch")
    f = lax.axis_index("field")
    d = lax.axis_index("dim")
    me = f * dim_count + d
    members = field_count * dim_count
    fl, el, row_count = feat.shape
    columns = fl * el
    fields, width, rc = x0.shape[1:]
    low, held = tower_levels(dim_count)
    high = low + held - 1
    level_of = d - low
    active = (d >= low) & (d <= high)
    sub = rc // held
    run = chunks // field_count
    share = run * sub
    part = towers.shape[2]
    units = split * part
    buffers = (x0, x1)
    other = field_count - 1 - f
    mine = b if split > 1 else 0
    to_right = jnp.minimum(d + 1, dim_count - 1)
    to_left = jnp.maximum(d - 1, 0)

    def remote(ref, send, recv, **where):
        return pltpu.make_async_remote_copy(
            ref, ref, send, recv, device_id=where, device_id_type=MESH)

    def place(ff, o):
        return pl.ds(ff * fl, fl), pl.ds(pl.multiple_of(o * el, el), el)

    def piece(ph, c, ff, o):
        fs, ds = place(ff, o)
        return buffers[ph].at[c, fs, ds, :]

    def right(ph, c, o):
        return remote(piece(ph, c, f, o), right_sem.at[ph, c, o], recv_sem.at[ph, c, o], dim=to_right)

    def left(ph, c, o):
        return remote(piece(ph, c, f, o), left_sem.at[ph, c, o], recv_sem.at[ph, c, o], dim=to_left)

    def pair(ph, c, o, ff):
        return remote(
            piece(ph, c, ff, o), pair_sem.at[ph, c, o], pair_recv.at[ph, c, o], field=other)

    def issue_own(ph, c):
        @pl.when(d < dim_count - 1)
        def _():
            right(ph, c, d).start()

        @pl.when(d > 0)
        def _():
            left(ph, c, d).start()

        pair(ph, c, d, f).start()

    def forwards(ph, c):
        for s in range(1, dim_count):
            @pl.when(d - s >= 0)
            def _():
                right(ph, c, d - s).wait_recv()

                @pl.when(d < dim_count - 1)
                def _():
                    right(ph, c, d - s).start()

                pair(ph, c, d - s, f).start()

            @pl.when(d + s < dim_count)
            def _():
                left(ph, c, d + s).wait_recv()

                @pl.when(d > 0)
                def _():
                    left(ph, c, d + s).start()

                pair(ph, c, d + s, f).start()
        for o in range(dim_count):
            pair(ph, c, o, other).wait_recv()

    def weight_copy(level, ff):
        return pltpu.make_async_copy(
            weight.at[level, :, ff],
            flat.at[level, :, :, pl.ds(pl.multiple_of(ff * width, width), width)],
            weight_sem.at[level, ff])

    def tower_copy(ff):
        return pltpu.make_async_copy(
            tower.at[ff, pl.ds(pl.multiple_of(mine * part, part), part), :],
            towers.at[mine, me, :, pl.ds(pl.multiple_of(ff * width, width), width)],
            tower_sem.at[ff])

    def each_field(act):
        def step(ff, carry):
            act(ff)
            return carry

        lax.fori_loop(0, fields, step, 0)

    small_refs = (
        lambda o: towers.at[mine, f * dim_count + o],
        lambda o: queries.at[:, f * dim_count + o],
        lambda o: biases.at[f * dim_count + o],
    )
    small_wide = (
        lambda ff: towers.at[mine, pl.ds(ff * dim_count, dim_count)],
        lambda ff: queries.at[:, pl.ds(ff * dim_count, dim_count)],
        lambda ff: biases.at[pl.ds(ff * dim_count, dim_count)],
    )

    def chain_to(k, o, sems, target):
        return remote(small_refs[k](o), sems.at[k, o], chain_recv.at[k, o], dim=target)

    def chain_own():
        for k in range(3):
            @pl.when(d < high)
            def _():
                chain_to(k, d, chain_right, to_right).start()

            @pl.when(d > low)
            def _():
                chain_to(k, d, chain_left, to_left).start()

    def chain_step(s):
        for k in range(3):
            @pl.when((d - s >= 0) & (d <= high))
            def _():
                chain_to(k, d - s, chain_right, to_right).wait_recv()

                @pl.when(d < high)
                def _():
                    chain_to(k, d - s, chain_right, to_right).start()

            @pl.when((d + s < dim_count) & (d >= low))
            def _():
                chain_to(k, d + s, chain_left, to_left).wait_recv()

                @pl.when(d > low)
                def _():
                    chain_to(k, d + s, chain_left, to_left).start()

    def both(k, ff):
        return remote(small_wide[k](ff), both_send.at[k], both_recv.at[k], field=other)

    def plane(t, source):
        return remote(
            towers.at[source, pl.ds(f * dim_count, dim_count)],
            plane_send.at[t], plane_recv.at[source], batch=t)

    def plane_both(source, ff):
        return remote(
            towers.at[source, pl.ds(ff * dim_count, dim_count)],
            plane_pair.at[source], plane_pair_recv.at[source], field=other)

    def cand_copy(t, source):
        return remote(cands.at[source], cand_send.at[t], cand_recv.at[source], batch=t)

    def loss_copy(m, ff, level):
        ref = losses.at[level, pl.ds(ff * run, run)]
        return remote(
            ref, loss_send.at[m], loss_recv.at[ff, level], field=m // dim_count, dim=m % dim_count)

    def row_copy(c, level):
        fs, ds = place(f, d)
        return pltpu.make_async_remote_copy(
            sent.at[c, level],
            rows.at[fs, ds, pl.ds(pl.multiple_of(lax.rem(c, run) * sub, sub), sub)],
            row_send.at[c, level], row_recv.at[lax.rem(c, run), me],
            device_id={"field": c // run, "dim": low + level}, device_id_type=MESH)

    def own_rows(c, level):
        return (c // run == f) & (level_of == level)

    def advance(ph, c):
        whole = buffers[ph][c].reshape(fields * width, rc)
        matrix = flat[ph].reshape(columns, fields * width)
        product = jnp.dot(matrix, whole, preferred_element_type=jnp.float32) + bias[ph]
        fs, ds = place(f, d)
        anchor = x0[c, fs, ds, :].astype(jnp.float32).reshape(columns, rc)
        current = buffers[ph][c, fs, ds, :].astype(jnp.float32).reshape(columns, rc)
        return (anchor * product + current).astype(jnp.bfloat16).reshape(fl, el, rc)

    own_copies = []
    for c in range(chunks):
        own_copies.append(pltpu.make_async_copy(
            feat.at[:, :, pl.ds(c * rc, rc)], piece(0, c, f, d), feat_sem.at[c]))
    small_copies = [
        pltpu.make_async_copy(query_weight, queries.at[:, me], small_sem.at[0]),
        pltpu.make_async_copy(tower_bias, biases.at[me], small_sem.at[1]),
        pltpu.make_async_copy(cand, cands.at[b], small_sem.at[2]),
    ]
    for copy in own_copies + small_copies:
        copy.start()
    each_field(lambda ff: tower_copy(ff).start())
    for level in range(CROSS):
        each_field(lambda ff: weight_copy(level, ff).start())

    barrier = pltpu.get_barrier_semaphore()
    for k in range(1, members):
        m = lax.rem(me + k, members)
        pl.semaphore_signal(
            barrier, inc=1, device_id={"field": m // dim_count, "dim": m % dim_count},
            device_id_type=MESH)
    for k in range(1, batch_count):
        pl.semaphore_signal(
            barrier, inc=1, device_id={"batch": lax.rem(b + k, batch_count)}, device_id_type=MESH)
    pl.semaphore_wait(barrier, members + batch_count - 2)
    for copy in own_copies:
        copy.wait()
    issue_own(0, 0)
    if chunks > 1:
        issue_own(0, 1)
    each_field(lambda ff: tower_copy(ff).wait())
    for copy in small_copies:
        copy.wait()
    chain_own()

    @pl.when(active)
    def _():
        for k in range(1, batch_count):
            cand_copy(lax.rem(b + k, batch_count), b).start()

    for level in range(CROSS):
        each_field(lambda ff: weight_copy(level, ff).wait())

    def first(c, carry):
        @pl.when(c + 2 < chunks)
        def _():
            issue_own(0, c + 2)

        forwards(0, c)
        fs, ds = place(f, d)
        x1[c, fs, ds, :] = advance(0, c)
        issue_own(1, c)

        for s in range(1, min(chunks, dim_count)):
            @pl.when(c == s)
            def _():
                chain_step(s)

        return carry

    lax.fori_loop(0, chunks, first, 0)
    for s in range(min(chunks, dim_count), dim_count):
        chain_step(s)

    @pl.when(active)
    def _():
        for k in range(3):
            both(k, f).start()
        if split > 1:
            for k in range(1, split):
                plane(lax.rem(b + k, split), b).start()

    def second(c, carry):
        forwards(1, c)
        new = advance(1, c)
        out[:, :, pl.ds(pl.multiple_of(c * rc, 128), rc)] = new
        for level in range(held):
            block = new[:, :, level * sub:(level + 1) * sub]

            @pl.when(own_rows(c, level))
            def _():
                fs, ds = place(f, d)
                rows[fs, ds, pl.ds(pl.multiple_of(lax.rem(c, run) * sub, sub), sub)] = block

            @pl.when(jnp.logical_not(own_rows(c, level)))
            def _():
                sent[c, level] = block
                row_copy(c, level).start()

        return carry

    lax.fori_loop(0, chunks, second, 0)

    def tower_block(s, query):
        matrix = towers[s].reshape(members * part, fields * width)
        pre = jnp.dot(
            matrix, rows[...].reshape(fields * width, share), preferred_element_type=jnp.float32)
        pre = pre + columns_bias[s].reshape(members * part, share)
        hidden = jnp.maximum(pre, 0.0).astype(jnp.bfloat16)
        return query + lax.dot_general(
            hidden, queries[s].reshape(members * part, width), (((0,), (0,)), ((), ())),
            preferred_element_type=jnp.float32)

    @pl.when(active)
    def _():
        if split > 1:
            for k in range(1, split):
                source = lax.rem(b + k, split)
                plane(source, source).wait_recv()
                plane_both(source, f).start()
        for k in range(3):
            both(k, other).wait_recv()
        for k in range(1, batch_count):
            source = lax.rem(b + k, batch_count)
            cand_copy(source, source).wait_recv()
        for m in range(members):
            block = jnp.broadcast_to(biases[m], (share, units)).T
            columns_bias[:, m] = block.reshape(split, part, share)
        if split > 1:
            for k in range(1, split):
                plane_both(lax.rem(b + k, split), other).wait_recv()
        for j in range(run):
            for k in range(1, members):
                m = lax.rem(me + k, members)
                fs, ds = place(m // dim_count, m % dim_count)
                remote(rows.at[fs, ds, pl.ds(j * sub, sub)], row_send.at[0, 0], row_recv.at[j, m],
                       field=m // dim_count, dim=m % dim_count).wait_recv()

        query = lax.fori_loop(0, split, tower_block, jnp.zeros((share, width), jnp.float32))
        all_cands = cands[...].reshape(-1, width)
        for j in range(run):
            c = f * run + j
            start = pl.multiple_of(c * rc + level_of * sub, sub)
            query_vec = (
                query[j * sub:(j + 1) * sub] + user[pl.ds(start, sub), :].astype(jnp.float32)
            ).astype(jnp.bfloat16)
            logits = lax.dot_general(
                all_cands, query_vec, (((1,), (1,)), ((), ())), preferred_element_type=jnp.float32
            ) * (1.0 / math.sqrt(width))
            labels = lax.broadcasted_iota(jnp.int32, logits.shape, 0)
            target = positive[c * held + level_of]
            picked = jnp.sum(jnp.where(labels == target, logits, 0.0), axis=0, keepdims=True)
            best = jnp.max(logits, axis=0, keepdims=True)
            total = jnp.sum(jnp.exp(logits - best), axis=0, keepdims=True)
            losses[level_of, c] = best + jnp.log(total) - picked
        for k in range(1, members):
            loss_copy(lax.rem(me + k, members), f, level_of).start()

    def drain(c, carry):
        for ph in range(CROSS):
            for o in range(dim_count):
                @pl.when((o <= d) & (d < dim_count - 1))
                def _():
                    right(ph, c, o).wait_send()

                @pl.when((o >= d) & (d > 0))
                def _():
                    left(ph, c, o).wait_send()

                pair(ph, c, o, f).wait_send()
        return carry

    lax.fori_loop(0, chunks, drain, 0)
    for k in range(3):
        for o in range(dim_count):
            @pl.when((o <= d) & (d < high))
            def _():
                chain_to(k, o, chain_right, to_right).wait_send()

            @pl.when((o >= d) & (d > low))
            def _():
                chain_to(k, o, chain_left, to_left).wait_send()

    @pl.when(active)
    def _():
        for k in range(3):
            both(k, f).wait_send()
        if split > 1:
            for k in range(1, split):
                t = lax.rem(b + k, split)
                plane(t, b).wait_send()
                plane_both(t, f).wait_send()
        for k in range(1, batch_count):
            cand_copy(lax.rem(b + k, batch_count), b).wait_send()
        for k in range(1, members):
            loss_copy(lax.rem(me + k, members), f, level_of).wait_send()

    for c in range(chunks):
        for level in range(held):
            @pl.when(jnp.logical_not(own_rows(c, level)))
            def _():
                row_copy(c, level).wait_send()

    for ff in range(field_count):
        for level in range(held):
            @pl.when(jnp.logical_not((f == ff) & (level_of == level)))
            def _():
                loss_copy(ff * dim_count + low + level, ff, level).wait_recv()

    for c in range(chunks):
        for level in range(held):
            loss_out[c * held + level] = losses[level, c]


def line_pieces(count, parts):
    base, extra = divmod(count, parts)
    bounds, start = [], 0
    for k in range(parts):
        size = base + (k < extra)
        bounds.append((start, size))
        start += size
    return bounds


def line_fits(counts, features, tower_weight, candidates):
    batch_count, field_count, dim_count = counts
    fl, el, row_count = features.shape
    units, fields, width = tower_weight.shape
    return (
        dim_count == 4 and batch_count == 4 and field_count == 2
        and fields % 2 == 0 and fl >= PIECES and el % 32 == 0 and 4 * el == width and width == 128
        and row_count % (CHUNKS * field_count * 128) == 0 and units % (16 * batch_count) == 0)


PIECES = 4
CHUNKS = 4
FAR_TOWER = CROSS * PIECES
END_TOWER = FAR_TOWER + 1


def line_kernel(
    counts,
    feat, weight, bias, tower, tower_bias, query_weight, user, cand, positive,
    out, loss_out,
    x0, x1, y, x2, flat, tw, tw_near, tw_far, tw_raw, q_raw, pre_out, pre_in, pre_own,
    bias_raw, bias_cols, unit_raw, unit_cols, cands, users, targets, losses,
    feat_sem, weight_sem, small_sem,
    end_send, end_recv, cross_send, cross_recv, pair_send, pair_recv, one_send, one_recv,
    piece_send, piece_recv, plane_send, plane_recv, rest_recv,
    tower_send, tower_recv, both_send, both_recv,
    bias_send, bias_recv, unit_send, unit_recv, cand_send, cand_recv,
    two_send, two_recv, out_sem, give_send, give_recv, part_send, part_recv, loss_send, loss_recv,
):
    batch_count, field_count, dim_count = counts
    b = lax.axis_index("batch")
    f = lax.axis_index("field")
    d = lax.axis_index("dim")
    members = field_count * dim_count
    me = f * dim_count + d
    chunks, fields, width, rc = x0.shape
    fl, el, _ = feat.shape
    wide = 2 * el
    half_k = fields // 2 * width
    quarter_units = tw_far.shape[0]
    units = tw.shape[1]
    side_k = fields * wide
    lanes = rc // field_count
    rows_in_part = el // 2
    side = d // 2
    mid = 1 + side
    far = 2 - side
    end = 3 * side
    far_end = 3 - end
    is_mid = d == mid
    is_end = d == end
    owner = is_mid & (f == side)
    giver = is_mid & (f != side)
    other = field_count - 1 - f
    x_next = b + 1 - 2 * lax.rem(b, 2)
    y_next = lax.rem(b + 2, 4)
    diagonal = 3 - b
    fs = pl.ds(f * fl, fl)
    ss = pl.ds(pl.multiple_of(side * wide, wide), wide)

    def remote(ref, send, recv, to=None, **where):
        return pltpu.make_async_remote_copy(
            ref, ref if to is None else to, send, recv, device_id=where, device_id_type=MESH)

    def sent(ref, sem):
        remote(ref, sem, sem, field=other).wait_send()

    def landed(ref, sem):
        remote(ref, sem, sem, field=other).wait_recv()

    def entries(o):
        return pl.ds(pl.multiple_of(o * el, el), el)

    def within(o):
        return pl.ds(pl.multiple_of(lax.rem(o, 2) * el, el), el)

    def block(c, ff, o):
        return x0.at[c, pl.ds(ff * fl, fl), entries(o), :]

    def from_end(c, target):
        return remote(block(c, f, end), end_send, end_recv.at[c], dim=target)

    def cross(k, c, o):
        return remote(block(c, f, o), cross_send.at[k], cross_recv.at[k, c], dim=far)

    def cross_one(c, s):
        ref = x1.at[c, fs, pl.ds(pl.multiple_of(s * wide, wide), wide), :]
        return remote(ref, cross_send.at[2], cross_recv.at[2, c], dim=far)

    def pair(c, o):
        return remote(block(c, f, o), pair_send, pair_recv.at[c], field=other)

    def pair_one(c, s):
        ref = x1.at[c, fs, pl.ds(pl.multiple_of(s * wide, wide), wide), :]
        return remote(ref, one_send, one_recv.at[c], field=other)

    def weight_piece(level, p, source):
        start, size = line_pieces(fl, PIECES)[p]
        return weight_part(level, start, size, source)

    def weight_part(level, start, size, source):
        row = pl.multiple_of(lax.rem(end, 2) * el + lax.rem(source, 2) * rows_in_part, rows_in_part)
        lane = pl.multiple_of(source // 2 * half_k, half_k)
        return flat.at[level, pl.ds(start, size), pl.ds(row, rows_in_part), pl.ds(lane, half_k)]

    def piece(level, p, target):
        ref = weight_piece(level, p, b)
        return remote(ref, piece_send.at[level], piece_recv.at[level, p], dim=target)

    def tower_rows(member, source):
        return tw.at[member, pl.ds(pl.multiple_of(source * quarter_units, quarter_units), quarter_units), :]

    def item(i, source):
        if i < CROSS * PIECES:
            return weight_piece(i // PIECES, i % PIECES, source)
        return tower_rows(f * dim_count + (far if i == FAR_TOWER else far_end), source)

    def relay(i):
        return (x_next, y_next) if i % 2 == 0 else (y_next, x_next)

    def plane(i, source, target, arrival):
        group = i // PIECES
        return remote(item(i, source), plane_send.at[group], arrival, batch=target)

    def plane_out(i):
        first, second = relay(i)
        plane(i, b, first, plane_recv.at[i]).start()
        plane(i, b, second, rest_recv.at[i // PIECES]).start()

    def plane_forward(i):
        source, target = relay(i)
        plane(i, source, target, plane_recv.at[i]).wait_recv()
        plane(i, source, target, rest_recv.at[i // PIECES]).start()

    def plane_rest(group):
        landed(plane_bytes(group, 2), rest_recv.at[group])

    def plane_bytes(group, copies):
        if group < CROSS:
            return flat.at[group, :, pl.ds(0, copies * rows_in_part), pl.ds(0, half_k)]
        return tw.at[pl.ds(0, copies * 2), pl.ds(0, quarter_units), :]

    def near_tower(target):
        return remote(
            tw_near, tower_send.at[0], tower_recv.at[end], to=tw.at[f * dim_count + end], dim=target)

    def far_tower(source, target):
        return remote(
            tw_far, tower_send.at[1], tower_recv.at[source],
            to=tower_rows(f * dim_count + source, b), dim=target)

    def both(z, ff):
        return remote(tw.at[ff * dim_count + z], both_send, both_recv, field=other)

    def bias_copy(target):
        return remote(bias_raw.at[lax.rem(end, 2)], bias_send, bias_recv, dim=target)

    def unit_copy(ff, z):
        return remote(unit_raw.at[me], unit_send, unit_recv, field=ff, dim=z)

    def cand_copy(k):
        return remote(cands.at[b], cand_send, cand_recv, batch=lax.rem(b + k, batch_count))

    def two(c, ff):
        lane = pl.multiple_of((1 - ff) * lanes, lanes)
        return remote(
            y.at[c, :, :, pl.ds(lane, lanes)], two_send, two_recv.at[c],
            to=x2.at[c, pl.ds(ff * fl, fl)], field=other)

    def rows_of(c):
        return pl.ds(pl.multiple_of(c * rc, rc), rc)

    def keep(c):
        return pltpu.make_async_copy(y.at[c, :, within(mid), :], out.at[:, :, rows_of(c)], out_sem)

    def give(c):
        return remote(
            y.at[c, :, within(end), :], give_send, give_recv,
            to=out.at[:, :, rows_of(c)], dim=end)

    def part(c):
        return remote(pre_out.at[c], part_send, part_recv.at[c], to=pre_in.at[c], dim=far)

    def loss_copy(k, c):
        m = lax.rem(me + k, members)
        return remote(
            losses.at[f, c], loss_send.at[k], loss_recv,
            field=m // dim_count, dim=lax.rem(m, dim_count))

    def own_weight(level, ff):
        return pltpu.make_async_copy(
            weight.at[level, :, ff],
            flat.at[level, :, within(mid), pl.ds(pl.multiple_of(ff * width, width), width)],
            weight_sem.at[level])

    def end_weight(level, k):
        row = pl.multiple_of(lax.rem(b, 2) * rows_in_part, rows_in_part)
        ff = b // 2 * (fields // 2) + k
        to = pl.multiple_of(lax.rem(end, 2) * el + row, rows_in_part)
        return pltpu.make_async_copy(
            weight.at[level, :, ff, pl.ds(row, rows_in_part), :],
            flat.at[level, :, pl.ds(to, rows_in_part), pl.ds(pl.multiple_of(ff * width, width), width)],
            weight_sem.at[level])

    def each(count, act):
        def step(k, carry):
            act(k)
            return carry

        lax.fori_loop(0, count, step, 0)

    own_features = [
        pltpu.make_async_copy(feat.at[:, :, pl.ds(c * rc, rc)], block(c, f, d), feat_sem.at[c])
        for c in range(chunks)]
    quarter = pl.ds(pl.multiple_of(b * quarter_units, quarter_units), quarter_units)
    small = [
        pltpu.make_async_copy(bias, bias_raw.at[lax.rem(d, 2)], small_sem.at[0]),
        pltpu.make_async_copy(tower_bias, unit_raw.at[me], small_sem.at[1]),
        pltpu.make_async_copy(cand, cands.at[b], small_sem.at[2]),
        pltpu.make_async_copy(tower, tw_raw, small_sem.at[3]),
        pltpu.make_async_copy(query_weight, q_raw, small_sem.at[4]),
        pltpu.make_async_copy(user, users, small_sem.at[5]),
        pltpu.make_async_copy(positive, targets, small_sem.at[6]),
    ]
    for copy in own_features:
        copy.start()

    @pl.when(is_end)
    def _():
        each(fields // 2, lambda k: end_weight(0, k).start())

    for copy in small:
        copy.start()

    @pl.when(is_mid)
    def _():
        each(fields, lambda k: own_weight(0, k).start())
        each(fields, lambda k: own_weight(1, k).start())

    @pl.when(is_end)
    def _():
        each(fields // 2, lambda k: end_weight(1, k).start())

    barrier = pltpu.get_barrier_semaphore()
    for k in range(1, members):
        m = lax.rem(me + k, members)
        pl.semaphore_signal(
            barrier, inc=1, device_id={"field": m // dim_count, "dim": lax.rem(m, dim_count)},
            device_id_type=MESH)
    for k in range(1, batch_count):
        pl.semaphore_signal(
            barrier, inc=1, device_id={"batch": lax.rem(b + k, batch_count)}, device_id_type=MESH)
    pl.semaphore_wait(barrier, members + batch_count - 2)

    def unit_sends():
        for ff in range(field_count):
            for z in (1, 2):
                @pl.when((f != ff) | (d != z))
                def _():
                    unit_copy(ff, z).start()

    def loaded_own(level):
        ref = flat.at[level, :, within(mid), :]
        pltpu.make_async_copy(ref, ref, weight_sem.at[level]).wait()

    def loaded_end(level):
        ref = weight_part(level, 0, fl, b)
        pltpu.make_async_copy(ref, ref, weight_sem.at[level]).wait()

    def pack_tower():
        def halves(rows, j):
            first = tw_raw[2 * j, rows, :]
            second = tw_raw[2 * j + 1, rows, :]
            low = jnp.concatenate([first[:, :wide], second[:, :wide]], axis=1)
            high = jnp.concatenate([first[:, wide:], second[:, wide:]], axis=1)
            return low, high

        for j in range(fields // 2):
            low, high = halves(slice(None), j)
            tw_near[:, j * width:(j + 1) * width] = jnp.where(side == 0, low, high)
            low, high = halves(quarter, j)
            tw_far[:, j * width:(j + 1) * width] = jnp.where(side == 0, high, low)
        tw_near[:, side_k:] = q_raw[...]
        tw_far[:, side_k:] = q_raw[quarter, :]

    @pl.when(is_end)
    def _():
        loaded_end(0)
        for p in range(PIECES - 1):
            piece(0, p, mid).start()
        for copy in small:
            copy.wait()
        pack_tower()
        far_tower(d, far).start()
        for copy in own_features:
            copy.wait()
        from_end(0, mid).start()
        piece(0, PIECES - 1, mid).start()
        from_end(1, mid).start()
        bias_copy(mid).start()
        for c in range(2, chunks):
            from_end(c, mid).start()
        loaded_end(1)
        for p in range(PIECES):
            piece(1, p, mid).start()
        near_tower(mid).start()
        unit_sends()

    def expect_piece(level, p):
        piece(level, p, end).wait_recv()
        plane_out(level * PIECES + p)

    def expect_end(c):
        from_end(c, end).wait_recv()
        cross(1, c, end).start()
        pair(c, end).start()

    def expect_far(k, c, o):
        cross(k, c, o).wait_recv()
        pair(c, o).start()

    def expect_tower(i, z):
        far_tower(z, end).wait_recv()
        plane_out(i)

    def half(source, level, c, ff):
        matrix = flat[level, :, :, pl.ds(pl.multiple_of(ff * half_k, half_k), half_k)]
        return jnp.dot(
            matrix.reshape(fl * wide, half_k), source[c, pl.ds(ff * fl, fl)].reshape(half_k, rc),
            preferred_element_type=jnp.float32)

    def advance(source, level, c, wait_pair):
        product = half(source, level, c, f)
        wait_pair()
        product = product + half(source, level, c, other)
        column = bias_cols[level]
        product = product + jnp.concatenate([column] * (rc // column.shape[1]), axis=1)
        anchor = x0[c, fs, ss, :].astype(jnp.float32).reshape(fl * wide, rc)
        current = source[c, fs, ss, :].astype(jnp.float32).reshape(fl * wide, rc)
        return (anchor * product + current).astype(jnp.bfloat16).reshape(fl, wide, rc)

    def build_bias():
        pick = (lax.broadcasted_iota(jnp.int32, (el, el), 0) == lax.broadcasted_iota(jnp.int32, (el, el), 1))
        for level in range(CROSS):
            for k in range(fl):
                for s in range(2):
                    line = bias_raw[s, k, level:level + 1, :]
                    column = jnp.sum(jnp.where(pick, line, 0.0), axis=1, keepdims=True)
                    start = (2 * k + s) * el
                    bias_cols[level, start:start + el, :] = jnp.broadcast_to(column, (el, width))

    def build_units():
        for m in range(members):
            unit_cols[m * units:(m + 1) * units, :] = jnp.broadcast_to(unit_raw[m], (lanes, units)).T

    def first(c, carry):
        @pl.when(c == 1)
        def _():
            expect_end(3)
            cross_one(0, side).start()

        @pl.when(c == 2)
        def _():
            expect_far(1, 2, far_end)
            plane_forward(FAR_TOWER)
            plane_forward(END_TOWER)
            expect_piece(1, 0)

        @pl.when(c == 3)
        def _():
            expect_far(1, 3, far_end)
            expect_piece(1, 1)

        def wait_pair():
            landed(x0.at[c, fs], pair_recv.at[c])

        x1[c, fs, ss, :] = advance(x0, 0, c, wait_pair)
        pair_one(c, side).start()

        @pl.when(c > 0)
        def _():
            cross_one(c, side).start()

        return carry

    def tower_part(c):
        matrix = tw[:, :, :side_k].reshape(members * units, side_k)
        return jnp.dot(matrix, x2[c].reshape(side_k, lanes), preferred_element_type=jnp.float32)

    def expect_one(c):
        cross_one(c, 1 - side).wait_recv()
        pair_one(c, 1 - side).start()

    def layer_two(c):
        def wait_pair():
            landed(x1.at[c, fs], one_recv.at[c])

        y[c] = advance(x1, 1, c, wait_pair)
        two(c, f).start()
        give(c).start()
        keep(c).start()
        for ff in range(field_count):
            @pl.when(f == ff)
            def _():
                x2[c, fs] = y[c, :, :, ff * lanes:(ff + 1) * lanes]

    def layer_three(c):
        two(c, other).wait_recv()
        pre = tower_part(c)

        @pl.when(owner)
        def _():
            pre_own[c] = pre

        @pl.when(giver)
        def _():
            pre_out[c] = pre.astype(jnp.bfloat16)
            part(c).start()

    def second(c, carry):
        layer_two(c)

        @pl.when(c == 1)
        def _():
            expect_one(2)

        def tower_step(k, carry):
            layer_three(k)
            return carry

        last = c == chunks - 1
        lax.fori_loop(
            jnp.where(last, c, jnp.maximum(c - 1, 0)), jnp.where(c < chunks - 2, c, c + 1),
            tower_step, 0)

        @pl.when(c == 2)
        def _():
            expect_one(3)

        return carry

    def finish(c):
        part(c).wait_recv()
        pre = pre_own[c] + pre_in[c].astype(jnp.float32) + unit_cols[...]
        hidden = jnp.maximum(pre, 0.0).astype(jnp.bfloat16)
        query = lax.dot_general(
            hidden, tw[:, :, side_k:].reshape(members * units, width), (((0,), (0,)), ((), ())),
            preferred_element_type=jnp.float32)
        start = pl.multiple_of(c * rc + f * lanes, lanes)
        query_vec = (query + users[pl.ds(start, lanes), :].astype(jnp.float32)).astype(jnp.bfloat16)
        logits = lax.dot_general(
            cands[...].reshape(-1, width), query_vec, (((1,), (1,)), ((), ())),
            preferred_element_type=jnp.float32) * (1.0 / math.sqrt(width))
        labels = lax.broadcasted_iota(jnp.int32, logits.shape, 0)
        target = targets[c * field_count + f]
        picked = jnp.sum(jnp.where(labels == target, logits, 0.0), axis=0, keepdims=True)
        best = jnp.max(logits, axis=0, keepdims=True)
        total = jnp.sum(jnp.exp(logits - best), axis=0, keepdims=True)
        losses[f, c] = best + jnp.log(total) - picked
        for k in range(1, members):
            loss_copy(k, c).start()

    @pl.when(is_mid)
    def _():
        for c in range(chunks):
            own_features[c].wait()
            cross(0, c, mid).start()
            pair(c, mid).start()
        for copy in small:
            copy.wait()
        for k in range(1, batch_count):
            cand_copy(k).start()
        pack_tower()
        far_tower(d, far).start()
        tw[me] = tw_near[...]
        both(mid, f).start()
        expect_piece(0, 0)
        expect_far(0, 0, far)
        expect_piece(0, 1)
        expect_far(0, 1, far)
        expect_piece(0, 2)
        expect_far(0, 2, far)
        plane_forward(0)
        plane_forward(1)
        expect_far(0, 3, far)
        expect_end(0)
        expect_piece(0, 3)
        plane_forward(2)
        expect_far(1, 0, far_end)
        expect_end(1)
        plane_forward(3)
        expect_tower(FAR_TOWER, far)
        expect_tower(END_TOWER, far_end)
        bias_copy(end).wait_recv()
        build_bias()
        unit_sends()
        for level in range(CROSS):
            loaded_own(level)
        expect_end(2)
        plane_rest(0)
        expect_far(1, 1, far_end)
        lax.fori_loop(0, chunks, first, 0)
        landed(cands.at[pl.ds(0, batch_count - 1)], cand_recv)
        plane_rest(2)
        both(far, f).start()
        both(far_end, f).start()
        expect_piece(1, 2)
        expect_piece(1, 3)
        plane_forward(PIECES)
        plane_forward(PIECES + 1)
        expect_one(0)
        plane_forward(PIECES + 2)
        plane_forward(PIECES + 3)
        expect_one(1)
        near_tower(end).wait_recv()
        both(end, f).start()
        landed(unit_raw.at[pl.ds(0, members - 1)], unit_recv)
        build_units()
        plane_rest(1)
        landed(tw.at[pl.ds(0, dim_count)], both_recv)
        lax.fori_loop(0, chunks, second, 0)

        @pl.when(owner)
        def _():
            for c in range(chunks):
                finish(c)

    @pl.when(owner)
    def _():
        landed(losses.at[0], loss_recv)

    @pl.when(jnp.logical_not(owner))
    def _():
        landed(losses, loss_recv)

    for ff in range(field_count):
        for c in range(chunks):
            loss_out[c * field_count + ff] = losses[ff, c]

    @pl.when(is_end)
    def _():
        for level in range(CROSS):
            sent(weight_part(level, 0, fl, b), piece_send.at[level])
        sent(x0.at[:, fs, entries(d), :], end_send)
        bias_copy(mid).wait_send()
        near_tower(mid).wait_send()
        far_tower(d, far).wait_send()
        sent(unit_raw.at[pl.ds(0, 4)], unit_send)
        landed(out, give_recv)

    @pl.when(is_mid)
    def _():
        far_tower(d, far).wait_send()
        sent(cands.at[pl.ds(0, batch_count - 1)], cand_send)
        sent(tw.at[pl.ds(0, dim_count)], both_send)
        sent(unit_raw.at[pl.ds(0, 3)], unit_send)
        sent(x0.at[:, fs, entries(mid), :], cross_send.at[0])
        sent(x0.at[:, fs, entries(end), :], cross_send.at[1])
        sent(x1.at[:, fs, ss, :], cross_send.at[2])
        sent(x0.at[:, fs], pair_send)
        sent(x1.at[:, fs], one_send)
        sent(y.at[:, :, :, pl.ds(0, lanes)], two_send)
        sent(out, give_send)
        pltpu.make_async_copy(out, out, out_sem).wait()
        for group in range(CROSS + 1):
            sent(plane_bytes(group, 3), plane_send.at[group])

    @pl.when(giver)
    def _():
        sent(pre_out, part_send)

    @pl.when(owner)
    def _():
        for k in range(1, members):
            sent(losses.at[0], loss_send.at[k])


def line_body(
    counts, features, cross_weight, cross_bias, tower_weight, tower_bias, query_weight,
    user_vec, candidates, positive,
):
    batch_count, field_count, dim_count = counts
    members = field_count * dim_count
    fl, el, row_count = features.shape
    units, fields, width = tower_weight.shape
    rc = row_count // CHUNKS
    lanes = rc // field_count
    wide = 2 * el
    quarter = units // batch_count
    packed = fields * wide + width
    items = END_TOWER + 1
    dma = pltpu.SemaphoreType.DMA
    vmem = pltpu.VMEM
    bf16 = jnp.bfloat16
    f32 = jnp.float32
    far = pl.BlockSpec(memory_space=pl.ANY)
    near = pl.BlockSpec(memory_space=pltpu.VMEM)
    crossed, losses = pl.pallas_call(
        functools.partial(line_kernel, counts),
        out_shape=(
            jax.ShapeDtypeStruct(features.shape, bf16),
            jax.ShapeDtypeStruct((CHUNKS * field_count, 1, lanes), f32),
        ),
        in_specs=[far] * 9,
        out_specs=(far, near),
        scratch_shapes=[
            vmem((CHUNKS, fields, width, rc), bf16),
            vmem((CHUNKS, fields, width, rc), bf16),
            vmem((CHUNKS, fl, wide, rc), bf16),
            vmem((CHUNKS, fields, wide, lanes), bf16),
            vmem((CROSS, fl, wide, fields * width), bf16),
            vmem((members, units, packed), bf16),
            vmem((units, packed), bf16),
            vmem((quarter, packed), bf16),
            vmem((fields, units, width), bf16),
            vmem((units, width), bf16),
            vmem((CHUNKS, members * units, lanes), bf16),
            vmem((CHUNKS, members * units, lanes), bf16),
            vmem((CHUNKS, members * units, lanes), f32),
            vmem((2, fl, CROSS, el), f32),
            vmem((CROSS, fl * wide, width), f32),
            vmem((members, 1, units), f32),
            vmem((members * units, lanes), f32),
            vmem((batch_count,) + candidates.shape, bf16),
            vmem(user_vec.shape, bf16),
            vmem((CHUNKS * field_count, 1, lanes), jnp.int32),
            vmem((field_count, CHUNKS, 1, lanes), f32),
            dma((CHUNKS,)), dma((CROSS,)), dma((7,)),
            dma, dma((CHUNKS,)), dma((3,)), dma((3, CHUNKS)),
            dma, dma((CHUNKS,)), dma, dma((CHUNKS,)),
            dma((CROSS,)), dma((CROSS, PIECES)), dma((CROSS + 1,)), dma((items,)), dma((CROSS + 1,)),
            dma((2,)), dma((dim_count,)), dma, dma,
            dma, dma, dma, dma, dma, dma,
            dma, dma((CHUNKS,)), dma, dma, dma, dma, dma((CHUNKS,)), dma((members,)), dma,
        ],
        compiler_params=pltpu.CompilerParams(
            collective_id=0, has_side_effects=True, vmem_limit_bytes=60 * 2**20),
        name="line_forward",
    )(
        features,
        cross_weight.transpose(0, 1, 3, 2, 4),
        cross_bias.transpose(1, 0, 2),
        tower_weight.transpose(1, 0, 2),
        tower_bias.reshape(1, units),
        query_weight,
        user_vec,
        candidates,
        positive.reshape(CHUNKS * field_count, 1, lanes),
    )
    return (crossed, losses.reshape(row_count))


def body(
    features, cross_weight, cross_bias, tower_weight, tower_bias, query_weight,
    user_vec, candidates, positive,
):
    counts = tuple(lax.axis_size(name) for name in ("batch", "field", "dim"))
    if line_fits(counts, features, tower_weight, candidates):
        return line_body(
            counts, features, cross_weight, cross_bias, tower_weight, tower_bias, query_weight,
            user_vec, candidates, positive)
    batch_count, field_count, dim_count = counts
    members = field_count * dim_count
    fl, el, row_count = features.shape
    columns = fl * el
    units, fields, width = tower_weight.shape
    low, held = tower_levels(dim_count)
    chunks = chunk_count(row_count, field_count, held)
    split = batch_count if units % (batch_count * 16) == 0 else 1
    part = units // split
    rc = row_count // chunks
    sub = rc // held
    run = chunks // field_count
    share = run * sub
    steps = (CROSS, chunks, dim_count)
    small = (3, dim_count)
    dma = pltpu.SemaphoreType.DMA
    vmem = pltpu.VMEM
    bf16 = jnp.bfloat16
    far = pl.BlockSpec(memory_space=pl.ANY)
    near = pl.BlockSpec(memory_space=pltpu.VMEM)
    crossed, losses = pl.pallas_call(
        functools.partial(rank_kernel, counts, (chunks, split)),
        out_shape=(
            jax.ShapeDtypeStruct(features.shape, bf16),
            jax.ShapeDtypeStruct((chunks * held, 1, sub), jnp.float32),
        ),
        in_specs=[far, far, near, far, far, far, near, far, near],
        out_specs=(near, near),
        scratch_shapes=[
            vmem((chunks, fields, width, rc), bf16),
            vmem((chunks, fields, width, rc), bf16),
            vmem((CROSS, fl, el, fields * width), bf16),
            vmem((chunks, held, fl, el, sub), bf16),
            vmem((fields, width, share), bf16),
            vmem((split, members, part, fields * width), bf16),
            vmem((members, 1, units), jnp.float32),
            vmem((split, members, part, share), jnp.float32),
            vmem((split, members, part, width), bf16),
            vmem((batch_count,) + candidates.shape, bf16),
            vmem((held, chunks, 1, sub), jnp.float32),
            dma((chunks,)), dma((CROSS, fields)), dma((fields,)), dma((3,)),
            dma(steps), dma(steps), dma(steps), dma(steps), dma(steps),
            dma((chunks, held)), dma((run, members)), dma(small), dma(small), dma(small),
            dma((3,)), dma((3,)),
            dma((split,)), dma((split,)), dma((split,)), dma((split,)),
            dma((batch_count,)), dma((batch_count,)), dma((members,)), dma((field_count, held)),
        ],
        compiler_params=pltpu.CompilerParams(
            collective_id=0, has_side_effects=True, vmem_limit_bytes=56 * 2**20),
        name="rank_forward",
    )(
        features,
        cross_weight.transpose(0, 1, 3, 2, 4),
        cross_bias.reshape(CROSS, columns, 1),
        tower_weight.transpose(1, 0, 2),
        tower_bias.reshape(1, units),
        query_weight.reshape(split, part, width),
        user_vec,
        candidates,
        positive.reshape(chunks * held, 1, sub),
    )
    return (crossed, losses.reshape(row_count))


def solution(mesh):
    placed = (
        P("field", "dim", "batch"),
        P(None, "field", "dim", None, None),
        P(None, "field", "dim"),
        P(("field", "dim"), None, None),
        P(("field", "dim")),
        P(("field", "dim"), None),
        P("batch", None),
        P("batch", None),
        P("batch"),
    )
    return jax.shard_map(
        body,
        mesh=mesh,
        in_specs=placed,
        out_specs=(P("field", "dim", "batch"), P("batch")),
        check_vma=False,
    )
```

```python
import functools
import math

import jax
import jax.numpy as jnp
from jax import lax
from jax.experimental import pallas as pl
from jax.experimental.pallas import tpu as pltpu
from jax.sharding import PartitionSpec as P

CROSS = 2
MESH = pl.DeviceIdType.MESH


def tower_levels(dim_count):
    held = min(2, dim_count)
    return (dim_count - held) // 2, held


def chunk_count(row_count, field_count, held):
    chunks = 2
    while chunks > field_count and row_count % (chunks * held * 128):
        chunks //= 2
    return chunks


def rank_kernel(
    counts, splits,
    feat, weight, bias, tower, tower_bias, query_weight, user, cand, positive,
    out, loss_out,
    x0, x1, flat, sent, rows, towers, biases, columns_bias, queries, cands, losses,
    feat_sem, weight_sem, tower_sem, small_sem,
    right_sem, left_sem, pair_sem, recv_sem, pair_recv,
    row_send, row_recv, chain_right, chain_left, chain_recv, both_send, both_recv,
    plane_send, plane_recv, plane_pair, plane_pair_recv,
    cand_send, cand_recv, loss_send, loss_recv,
):
    batch_count, field_count, dim_count = counts
    chunks, split = splits
    b = lax.axis_index("batch")
    f = lax.axis_index("field")
    d = lax.axis_index("dim")
    me = f * dim_count + d
    members = field_count * dim_count
    fl, el, row_count = feat.shape
    columns = fl * el
    fields, width, rc = x0.shape[1:]
    low, held = tower_levels(dim_count)
    high = low + held - 1
    level_of = d - low
    active = (d >= low) & (d <= high)
    sub = rc // held
    run = chunks // field_count
    share = run * sub
    part = towers.shape[2]
    units = split * part
    buffers = (x0, x1)
    other = field_count - 1 - f
    mine = b if split > 1 else 0
    to_right = jnp.minimum(d + 1, dim_count - 1)
    to_left = jnp.maximum(d - 1, 0)

    def remote(ref, send, recv, **where):
        return pltpu.make_async_remote_copy(
            ref, ref, send, recv, device_id=where, device_id_type=MESH)

    def place(ff, o):
        return pl.ds(ff * fl, fl), pl.ds(pl.multiple_of(o * el, el), el)

    def piece(ph, c, ff, o):
        fs, ds = place(ff, o)
        return buffers[ph].at[c, fs, ds, :]

    def right(ph, c, o):
        return remote(piece(ph, c, f, o), right_sem.at[ph, c, o], recv_sem.at[ph, c, o], dim=to_right)

    def left(ph, c, o):
        return remote(piece(ph, c, f, o), left_sem.at[ph, c, o], recv_sem.at[ph, c, o], dim=to_left)

    def pair(ph, c, o, ff):
        return remote(
            piece(ph, c, ff, o), pair_sem.at[ph, c, o], pair_recv.at[ph, c, o], field=other)

    def issue_own(ph, c):
        @pl.when(d < dim_count - 1)
        def _():
            right(ph, c, d).start()

        @pl.when(d > 0)
        def _():
            left(ph, c, d).start()

        pair(ph, c, d, f).start()

    def forwards(ph, c):
        for s in range(1, dim_count):
            @pl.when(d - s >= 0)
            def _():
                right(ph, c, d - s).wait_recv()

                @pl.when(d < dim_count - 1)
                def _():
                    right(ph, c, d - s).start()

                pair(ph, c, d - s, f).start()

            @pl.when(d + s < dim_count)
            def _():
                left(ph, c, d + s).wait_recv()

                @pl.when(d > 0)
                def _():
                    left(ph, c, d + s).start()

                pair(ph, c, d + s, f).start()
        for o in range(dim_count):
            pair(ph, c, o, other).wait_recv()

    def weight_copy(level, ff):
        return pltpu.make_async_copy(
            weight.at[level, :, ff],
            flat.at[level, :, :, pl.ds(pl.multiple_of(ff * width, width), width)],
            weight_sem.at[level, ff])

    def tower_copy(ff):
        return pltpu.make_async_copy(
            tower.at[ff, pl.ds(pl.multiple_of(mine * part, part), part), :],
            towers.at[mine, me, :, pl.ds(pl.multiple_of(ff * width, width), width)],
            tower_sem.at[ff])

    def each_field(act):
        def step(ff, carry):
            act(ff)
            return carry

        lax.fori_loop(0, fields, step, 0)

    small_refs = (
        lambda o: towers.at[mine, f * dim_count + o],
        lambda o: queries.at[:, f * dim_count + o],
        lambda o: biases.at[f * dim_count + o],
    )
    small_wide = (
        lambda ff: towers.at[mine, pl.ds(ff * dim_count, dim_count)],
        lambda ff: queries.at[:, pl.ds(ff * dim_count, dim_count)],
        lambda ff: biases.at[pl.ds(ff * dim_count, dim_count)],
    )

    def chain_to(k, o, sems, target):
        return remote(small_refs[k](o), sems.at[k, o], chain_recv.at[k, o], dim=target)

    def chain_own():
        for k in range(3):
            @pl.when(d < high)
            def _():
                chain_to(k, d, chain_right, to_right).start()

            @pl.when(d > low)
            def _():
                chain_to(k, d, chain_left, to_left).start()

    def chain_step(s):
        for k in range(3):
            @pl.when((d - s >= 0) & (d <= high))
            def _():
                chain_to(k, d - s, chain_right, to_right).wait_recv()

                @pl.when(d < high)
                def _():
                    chain_to(k, d - s, chain_right, to_right).start()

            @pl.when((d + s < dim_count) & (d >= low))
            def _():
                chain_to(k, d + s, chain_left, to_left).wait_recv()

                @pl.when(d > low)
                def _():
                    chain_to(k, d + s, chain_left, to_left).start()

    def both(k, ff):
        return remote(small_wide[k](ff), both_send.at[k], both_recv.at[k], field=other)

    def plane(t, source):
        return remote(
            towers.at[source, pl.ds(f * dim_count, dim_count)],
            plane_send.at[t], plane_recv.at[source], batch=t)

    def plane_both(source, ff):
        return remote(
            towers.at[source, pl.ds(ff * dim_count, dim_count)],
            plane_pair.at[source], plane_pair_recv.at[source], field=other)

    def cand_copy(t, source):
        return remote(cands.at[source], cand_send.at[t], cand_recv.at[source], batch=t)

    def loss_copy(m, ff, level):
        ref = losses.at[level, pl.ds(ff * run, run)]
        return remote(
            ref, loss_send.at[m], loss_recv.at[ff, level], field=m // dim_count, dim=m % dim_count)

    def row_copy(c, level):
        fs, ds = place(f, d)
        return pltpu.make_async_remote_copy(
            sent.at[c, level],
            rows.at[fs, ds, pl.ds(pl.multiple_of(lax.rem(c, run) * sub, sub), sub)],
            row_send.at[c, level], row_recv.at[lax.rem(c, run), me],
            device_id={"field": c // run, "dim": low + level}, device_id_type=MESH)

    def own_rows(c, level):
        return (c // run == f) & (level_of == level)

    def advance(ph, c):
        whole = buffers[ph][c].reshape(fields * width, rc)
        matrix = flat[ph].reshape(columns, fields * width)
        product = jnp.dot(matrix, whole, preferred_element_type=jnp.float32) + bias[ph]
        fs, ds = place(f, d)
        anchor = x0[c, fs, ds, :].astype(jnp.float32).reshape(columns, rc)
        current = buffers[ph][c, fs, ds, :].astype(jnp.float32).reshape(columns, rc)
        return (anchor * product + current).astype(jnp.bfloat16).reshape(fl, el, rc)

    own_copies = []
    for c in range(chunks):
        own_copies.append(pltpu.make_async_copy(
            feat.at[:, :, pl.ds(c * rc, rc)], piece(0, c, f, d), feat_sem.at[c]))
    small_copies = [
        pltpu.make_async_copy(query_weight, queries.at[:, me], small_sem.at[0]),
        pltpu.make_async_copy(tower_bias, biases.at[me], small_sem.at[1]),
        pltpu.make_async_copy(cand, cands.at[b], small_sem.at[2]),
    ]
    for copy in own_copies + small_copies:
        copy.start()
    each_field(lambda ff: tower_copy(ff).start())
    for level in range(CROSS):
        each_field(lambda ff: weight_copy(level, ff).start())

    barrier = pltpu.get_barrier_semaphore()
    for k in range(1, members):
        m = lax.rem(me + k, members)
        pl.semaphore_signal(
            barrier, inc=1, device_id={"field": m // dim_count, "dim": m % dim_count},
            device_id_type=MESH)
    for k in range(1, batch_count):
        pl.semaphore_signal(
            barrier, inc=1, device_id={"batch": lax.rem(b + k, batch_count)}, device_id_type=MESH)
    pl.semaphore_wait(barrier, members + batch_count - 2)
    for copy in own_copies:
        copy.wait()
    issue_own(0, 0)
    if chunks > 1:
        issue_own(0, 1)
    each_field(lambda ff: tower_copy(ff).wait())
    for copy in small_copies:
        copy.wait()
    chain_own()

    @pl.when(active)
    def _():
        for k in range(1, batch_count):
            cand_copy(lax.rem(b + k, batch_count), b).start()

    for level in range(CROSS):
        each_field(lambda ff: weight_copy(level, ff).wait())

    def first(c, carry):
        @pl.when(c + 2 < chunks)
        def _():
            issue_own(0, c + 2)

        forwards(0, c)
        fs, ds = place(f, d)
        x1[c, fs, ds, :] = advance(0, c)
        issue_own(1, c)

        for s in range(1, min(chunks, dim_count)):
            @pl.when(c == s)
            def _():
                chain_step(s)

        return carry

    lax.fori_loop(0, chunks, first, 0)
    for s in range(min(chunks, dim_count), dim_count):
        chain_step(s)

    @pl.when(active)
    def _():
        for k in range(3):
            both(k, f).start()
        if split > 1:
            for k in range(1, split):
                plane(lax.rem(b + k, split), b).start()

    def second(c, carry):
        forwards(1, c)
        new = advance(1, c)
        out[:, :, pl.ds(pl.multiple_of(c * rc, 128), rc)] = new
        for level in range(held):
            block = new[:, :, level * sub:(level + 1) * sub]

            @pl.when(own_rows(c, level))
            def _():
                fs, ds = place(f, d)
                rows[fs, ds, pl.ds(pl.multiple_of(lax.rem(c, run) * sub, sub), sub)] = block

            @pl.when(jnp.logical_not(own_rows(c, level)))
            def _():
                sent[c, level] = block
                row_copy(c, level).start()

        return carry

    lax.fori_loop(0, chunks, second, 0)

    def tower_block(s, query):
        matrix = towers[s].reshape(members * part, fields * width)
        pre = jnp.dot(
            matrix, rows[...].reshape(fields * width, share), preferred_element_type=jnp.float32)
        pre = pre + columns_bias[s].reshape(members * part, share)
        hidden = jnp.maximum(pre, 0.0).astype(jnp.bfloat16)
        return query + lax.dot_general(
            hidden, queries[s].reshape(members * part, width), (((0,), (0,)), ((), ())),
            preferred_element_type=jnp.float32)

    @pl.when(active)
    def _():
        if split > 1:
            for k in range(1, split):
                source = lax.rem(b + k, split)
                plane(source, source).wait_recv()
                plane_both(source, f).start()
        for k in range(3):
            both(k, other).wait_recv()
        for k in range(1, batch_count):
            source = lax.rem(b + k, batch_count)
            cand_copy(source, source).wait_recv()
        for m in range(members):
            block = jnp.broadcast_to(biases[m], (share, units)).T
            columns_bias[:, m] = block.reshape(split, part, share)
        if split > 1:
            for k in range(1, split):
                plane_both(lax.rem(b + k, split), other).wait_recv()
        for j in range(run):
            for k in range(1, members):
                m = lax.rem(me + k, members)
                fs, ds = place(m // dim_count, m % dim_count)
                remote(rows.at[fs, ds, pl.ds(j * sub, sub)], row_send.at[0, 0], row_recv.at[j, m],
                       field=m // dim_count, dim=m % dim_count).wait_recv()

        query = lax.fori_loop(0, split, tower_block, jnp.zeros((share, width), jnp.float32))
        all_cands = cands[...].reshape(-1, width)
        for j in range(run):
            c = f * run + j
            start = pl.multiple_of(c * rc + level_of * sub, sub)
            query_vec = (
                query[j * sub:(j + 1) * sub] + user[pl.ds(start, sub), :].astype(jnp.float32)
            ).astype(jnp.bfloat16)
            logits = lax.dot_general(
                all_cands, query_vec, (((1,), (1,)), ((), ())), preferred_element_type=jnp.float32
            ) * (1.0 / math.sqrt(width))
            labels = lax.broadcasted_iota(jnp.int32, logits.shape, 0)
            target = positive[c * held + level_of]
            picked = jnp.sum(jnp.where(labels == target, logits, 0.0), axis=0, keepdims=True)
            best = jnp.max(logits, axis=0, keepdims=True)
            total = jnp.sum(jnp.exp(logits - best), axis=0, keepdims=True)
            losses[level_of, c] = best + jnp.log(total) - picked
        for k in range(1, members):
            loss_copy(lax.rem(me + k, members), f, level_of).start()

    def drain(c, carry):
        for ph in range(CROSS):
            for o in range(dim_count):
                @pl.when((o <= d) & (d < dim_count - 1))
                def _():
                    right(ph, c, o).wait_send()

                @pl.when((o >= d) & (d > 0))
                def _():
                    left(ph, c, o).wait_send()

                pair(ph, c, o, f).wait_send()
        return carry

    lax.fori_loop(0, chunks, drain, 0)
    for k in range(3):
        for o in range(dim_count):
            @pl.when((o <= d) & (d < high))
            def _():
                chain_to(k, o, chain_right, to_right).wait_send()

            @pl.when((o >= d) & (d > low))
            def _():
                chain_to(k, o, chain_left, to_left).wait_send()

    @pl.when(active)
    def _():
        for k in range(3):
            both(k, f).wait_send()
        if split > 1:
            for k in range(1, split):
                t = lax.rem(b + k, split)
                plane(t, b).wait_send()
                plane_both(t, f).wait_send()
        for k in range(1, batch_count):
            cand_copy(lax.rem(b + k, batch_count), b).wait_send()
        for k in range(1, members):
            loss_copy(lax.rem(me + k, members), f, level_of).wait_send()

    for c in range(chunks):
        for level in range(held):
            @pl.when(jnp.logical_not(own_rows(c, level)))
            def _():
                row_copy(c, level).wait_send()

    for ff in range(field_count):
        for level in range(held):
            @pl.when(jnp.logical_not((f == ff) & (level_of == level)))
            def _():
                loss_copy(ff * dim_count + low + level, ff, level).wait_recv()

    for c in range(chunks):
        for level in range(held):
            loss_out[c * held + level] = losses[level, c]


def line_pieces(count, parts):
    base, extra = divmod(count, parts)
    bounds, start = [], 0
    for k in range(parts):
        size = base + (k < extra)
        bounds.append((start, size))
        start += size
    return bounds


def line_fits(counts, features, tower_weight, candidates):
    batch_count, field_count, dim_count = counts
    fl, el, row_count = features.shape
    units, fields, width = tower_weight.shape
    return (
        dim_count == 4 and batch_count == 4 and field_count == 2
        and fields % 2 == 0 and fl >= PIECES and el % 32 == 0 and 4 * el == width and width == 128
        and row_count % (CHUNKS * field_count * 128) == 0 and units % (16 * batch_count) == 0)


PIECES = 4
CHUNKS = 4
FAR_TOWER = CROSS * PIECES
END_TOWER = FAR_TOWER + 1


def line_kernel(
    counts,
    feat, weight, bias, tower, tower_bias, query_weight, user, cand, positive,
    out, loss_out,
    x0, x1, y, x2, flat, tw, tw_near, tw_far, tw_raw, q_raw, pre_out, pre_in, pre_own,
    bias_raw, bias_cols, unit_raw, unit_cols, cands, users, targets, losses,
    feat_sem, weight_sem, small_sem,
    end_send, end_recv, cross_send, cross_recv, pair_send, pair_recv, one_send, one_recv,
    piece_send, piece_recv, plane_send, plane_recv, rest_recv,
    tower_send, tower_recv, both_send, both_recv,
    bias_send, bias_recv, unit_send, unit_recv, cand_send, cand_recv,
    two_send, two_recv, out_sem, give_send, give_recv, part_send, part_recv, loss_send, loss_recv,
):
    batch_count, field_count, dim_count = counts
    b = lax.axis_index("batch")
    f = lax.axis_index("field")
    d = lax.axis_index("dim")
    members = field_count * dim_count
    me = f * dim_count + d
    chunks, fields, width, rc = x0.shape
    fl, el, _ = feat.shape
    wide = 2 * el
    half_k = fields // 2 * width
    quarter_units = tw_far.shape[0]
    units = tw.shape[1]
    side_k = fields * wide
    lanes = rc // field_count
    rows_in_part = el // 2
    side = d // 2
    mid = 1 + side
    far = 2 - side
    end = 3 * side
    far_end = 3 - end
    is_mid = d == mid
    is_end = d == end
    owner = is_mid & (f == side)
    giver = is_mid & (f != side)
    other = field_count - 1 - f
    x_next = b + 1 - 2 * lax.rem(b, 2)
    y_next = lax.rem(b + 2, 4)
    diagonal = 3 - b
    fs = pl.ds(f * fl, fl)
    ss = pl.ds(pl.multiple_of(side * wide, wide), wide)

    def remote(ref, send, recv, to=None, **where):
        return pltpu.make_async_remote_copy(
            ref, ref if to is None else to, send, recv, device_id=where, device_id_type=MESH)

    def sent(ref, sem):
        remote(ref, sem, sem, field=other).wait_send()

    def landed(ref, sem):
        remote(ref, sem, sem, field=other).wait_recv()

    def entries(o):
        return pl.ds(pl.multiple_of(o * el, el), el)

    def within(o):
        return pl.ds(pl.multiple_of(lax.rem(o, 2) * el, el), el)

    def block(c, ff, o):
        return x0.at[c, pl.ds(ff * fl, fl), entries(o), :]

    def from_end(c, target):
        return remote(block(c, f, end), end_send, end_recv.at[c], dim=target)

    def cross(k, c, o):
        return remote(block(c, f, o), cross_send.at[k], cross_recv.at[k, c], dim=far)

    def cross_one(c, s):
        ref = x1.at[c, fs, pl.ds(pl.multiple_of(s * wide, wide), wide), :]
        return remote(ref, cross_send.at[2], cross_recv.at[2, c], dim=far)

    def pair(c, o):
        return remote(block(c, f, o), pair_send, pair_recv.at[c], field=other)

    def pair_one(c, s):
        ref = x1.at[c, fs, pl.ds(pl.multiple_of(s * wide, wide), wide), :]
        return remote(ref, one_send, one_recv.at[c], field=other)

    def weight_piece(level, p, source):
        start, size = line_pieces(fl, PIECES)[p]
        return weight_part(level, start, size, source)

    def weight_part(level, start, size, source):
        row = pl.multiple_of(lax.rem(end, 2) * el + lax.rem(source, 2) * rows_in_part, rows_in_part)
        lane = pl.multiple_of(source // 2 * half_k, half_k)
        return flat.at[level, pl.ds(start, size), pl.ds(row, rows_in_part), pl.ds(lane, half_k)]

    def piece(level, p, target):
        ref = weight_piece(level, p, b)
        return remote(ref, piece_send.at[level], piece_recv.at[level, p], dim=target)

    def tower_rows(member, source):
        return tw.at[member, pl.ds(pl.multiple_of(source * quarter_units, quarter_units), quarter_units), :]

    def item(i, source):
        if i < CROSS * PIECES:
            return weight_piece(i // PIECES, i % PIECES, source)
        return tower_rows(f * dim_count + (far if i == FAR_TOWER else far_end), source)

    def relay(i):
        return (x_next, y_next) if i % 2 == 0 else (y_next, x_next)

    def plane(i, source, target, arrival):
        group = i // PIECES
        return remote(item(i, source), plane_send.at[group], arrival, batch=target)

    def plane_out(i):
        first, second = relay(i)
        plane(i, b, first, plane_recv.at[i]).start()
        plane(i, b, second, rest_recv.at[i // PIECES]).start()

    def plane_forward(i):
        source, target = relay(i)
        plane(i, source, target, plane_recv.at[i]).wait_recv()
        plane(i, source, target, rest_recv.at[i // PIECES]).start()

    def plane_rest(group):
        landed(plane_bytes(group, 2), rest_recv.at[group])

    def plane_bytes(group, copies):
        if group < CROSS:
            return flat.at[group, :, pl.ds(0, copies * rows_in_part), pl.ds(0, half_k)]
        return tw.at[pl.ds(0, copies * 2), pl.ds(0, quarter_units), :]

    def near_tower(target):
        return remote(
            tw_near, tower_send.at[0], tower_recv.at[end], to=tw.at[f * dim_count + end], dim=target)

    def far_tower(source, target):
        return remote(
            tw_far, tower_send.at[1], tower_recv.at[source],
            to=tower_rows(f * dim_count + source, b), dim=target)

    def both(z, ff):
        return remote(tw.at[ff * dim_count + z], both_send, both_recv, field=other)

    def bias_copy(target):
        return remote(bias_raw.at[lax.rem(end, 2)], bias_send, bias_recv, dim=target)

    def unit_copy(ff, z):
        return remote(unit_raw.at[me], unit_send, unit_recv, field=ff, dim=z)

    def cand_copy(k):
        return remote(cands.at[b], cand_send, cand_recv, batch=lax.rem(b + k, batch_count))

    def two(c, ff):
        lane = pl.multiple_of((1 - ff) * lanes, lanes)
        return remote(
            y.at[c, :, :, pl.ds(lane, lanes)], two_send, two_recv.at[c],
            to=x2.at[c, pl.ds(ff * fl, fl)], field=other)

    def rows_of(c):
        return pl.ds(pl.multiple_of(c * rc, rc), rc)

    def keep(c):
        return pltpu.make_async_copy(y.at[c, :, within(mid), :], out.at[:, :, rows_of(c)], out_sem)

    def give(c):
        return remote(
            y.at[c, :, within(end), :], give_send, give_recv,
            to=out.at[:, :, rows_of(c)], dim=end)

    def part(c):
        return remote(pre_out.at[c], part_send, part_recv.at[c], to=pre_in.at[c], dim=far)

    def loss_copy(k, c):
        m = lax.rem(me + k, members)
        return remote(
            losses.at[c], loss_send.at[k], loss_recv, to=loss_out.at[c * field_count + f],
            field=m // dim_count, dim=lax.rem(m, dim_count))

    def keep_loss(c):
        return pltpu.make_async_copy(losses.at[c], loss_out.at[c * field_count + f], loss_send.at[0])

    def own_weight(level, ff):
        return pltpu.make_async_copy(
            weight.at[level, :, ff],
            flat.at[level, :, within(mid), pl.ds(pl.multiple_of(ff * width, width), width)],
            weight_sem.at[level])

    def end_weight(level, k):
        row = pl.multiple_of(lax.rem(b, 2) * rows_in_part, rows_in_part)
        ff = b // 2 * (fields // 2) + k
        to = pl.multiple_of(lax.rem(end, 2) * el + row, rows_in_part)
        return pltpu.make_async_copy(
            weight.at[level, :, ff, pl.ds(row, rows_in_part), :],
            flat.at[level, :, pl.ds(to, rows_in_part), pl.ds(pl.multiple_of(ff * width, width), width)],
            weight_sem.at[level])

    def each(count, act):
        def step(k, carry):
            act(k)
            return carry

        lax.fori_loop(0, count, step, 0)

    own_features = [
        pltpu.make_async_copy(feat.at[:, :, pl.ds(c * rc, rc)], block(c, f, d), feat_sem.at[c])
        for c in range(chunks)]
    quarter = pl.ds(pl.multiple_of(b * quarter_units, quarter_units), quarter_units)
    small = [
        pltpu.make_async_copy(bias, bias_raw.at[lax.rem(d, 2)], small_sem.at[0]),
        pltpu.make_async_copy(tower_bias, unit_raw.at[me], small_sem.at[1]),
        pltpu.make_async_copy(cand, cands.at[b], small_sem.at[2]),
        pltpu.make_async_copy(tower, tw_raw, small_sem.at[3]),
        pltpu.make_async_copy(query_weight, q_raw, small_sem.at[4]),
        pltpu.make_async_copy(user, users, small_sem.at[5]),
        pltpu.make_async_copy(positive, targets, small_sem.at[6]),
    ]
    barrier = pltpu.get_barrier_semaphore()
    for k in range(1, members):
        m = lax.rem(me + k, members)
        pl.semaphore_signal(
            barrier, inc=1, device_id={"field": m // dim_count, "dim": lax.rem(m, dim_count)},
            device_id_type=MESH)
    for k in range(1, batch_count):
        pl.semaphore_signal(
            barrier, inc=1, device_id={"batch": lax.rem(b + k, batch_count)}, device_id_type=MESH)
    for copy in own_features:
        copy.start()

    @pl.when(is_end)
    def _():
        each(fields // 2, lambda k: end_weight(0, k).start())

    for copy in small:
        copy.start()

    @pl.when(is_mid)
    def _():
        each(fields, lambda k: own_weight(0, k).start())
        each(fields, lambda k: own_weight(1, k).start())

    @pl.when(is_end)
    def _():
        each(fields // 2, lambda k: end_weight(1, k).start())

    pl.semaphore_wait(barrier, members + batch_count - 2)

    def unit_sends():
        for ff in range(field_count):
            for z in (1, 2):
                @pl.when((f != ff) | (d != z))
                def _():
                    unit_copy(ff, z).start()

    def loaded_own(level):
        ref = flat.at[level, :, within(mid), :]
        pltpu.make_async_copy(ref, ref, weight_sem.at[level]).wait()

    def loaded_end(level):
        ref = weight_part(level, 0, fl, b)
        pltpu.make_async_copy(ref, ref, weight_sem.at[level]).wait()

    def pack_tower():
        def halves(rows, j):
            first = tw_raw[2 * j, rows, :]
            second = tw_raw[2 * j + 1, rows, :]
            low = jnp.concatenate([first[:, :wide], second[:, :wide]], axis=1)
            high = jnp.concatenate([first[:, wide:], second[:, wide:]], axis=1)
            return low, high

        for j in range(fields // 2):
            low, high = halves(slice(None), j)
            tw_near[:, j * width:(j + 1) * width] = jnp.where(side == 0, low, high)
            low, high = halves(quarter, j)
            tw_far[:, j * width:(j + 1) * width] = jnp.where(side == 0, high, low)
        tw_near[:, side_k:] = q_raw[...]
        tw_far[:, side_k:] = q_raw[quarter, :]

    @pl.when(is_end)
    def _():
        loaded_end(0)
        for p in range(PIECES - 1):
            piece(0, p, mid).start()
        for copy in small:
            copy.wait()
        pack_tower()
        far_tower(d, far).start()
        for copy in own_features:
            copy.wait()
        from_end(0, mid).start()
        piece(0, PIECES - 1, mid).start()
        from_end(1, mid).start()
        bias_copy(mid).start()
        for c in range(2, chunks):
            from_end(c, mid).start()
        loaded_end(1)
        for p in range(PIECES):
            piece(1, p, mid).start()
        near_tower(mid).start()
        unit_sends()

    def expect_piece(level, p):
        piece(level, p, end).wait_recv()
        plane_out(level * PIECES + p)

    def expect_end(c):
        from_end(c, end).wait_recv()
        cross(1, c, end).start()
        pair(c, end).start()

    def expect_far(k, c, o):
        cross(k, c, o).wait_recv()
        pair(c, o).start()

    def expect_tower(i, z):
        far_tower(z, end).wait_recv()
        plane_out(i)

    def half(source, level, c, ff):
        matrix = flat[level, :, :, pl.ds(pl.multiple_of(ff * half_k, half_k), half_k)]
        return jnp.dot(
            matrix.reshape(fl * wide, half_k), source[c, pl.ds(ff * fl, fl)].reshape(half_k, rc),
            preferred_element_type=jnp.float32)

    def advance(source, level, c, wait_pair):
        product = half(source, level, c, f)
        wait_pair()
        product = product + half(source, level, c, other)
        column = bias_cols[level]
        product = product + jnp.concatenate([column] * (rc // column.shape[1]), axis=1)
        anchor = x0[c, fs, ss, :].astype(jnp.float32).reshape(fl * wide, rc)
        current = source[c, fs, ss, :].astype(jnp.float32).reshape(fl * wide, rc)
        return (anchor * product + current).astype(jnp.bfloat16).reshape(fl, wide, rc)

    def build_bias():
        pick = (lax.broadcasted_iota(jnp.int32, (el, el), 0) == lax.broadcasted_iota(jnp.int32, (el, el), 1))
        for level in range(CROSS):
            for k in range(fl):
                for s in range(2):
                    line = bias_raw[s, k, level:level + 1, :]
                    column = jnp.sum(jnp.where(pick, line, 0.0), axis=1, keepdims=True)
                    start = (2 * k + s) * el
                    bias_cols[level, start:start + el, :] = jnp.broadcast_to(column, (el, width))

    def build_units():
        for m in range(members):
            unit_cols[m * units:(m + 1) * units, :] = jnp.broadcast_to(unit_raw[m], (lanes, units)).T

    def first(c, carry):
        @pl.when(c == 1)
        def _():
            expect_end(3)
            cross_one(0, side).start()

        @pl.when(c == 2)
        def _():
            expect_far(1, 2, far_end)
            plane_forward(FAR_TOWER)
            plane_forward(END_TOWER)
            expect_piece(1, 0)

        @pl.when(c == 3)
        def _():
            expect_far(1, 3, far_end)
            expect_piece(1, 1)

        def wait_pair():
            landed(x0.at[c, fs], pair_recv.at[c])

        x1[c, fs, ss, :] = advance(x0, 0, c, wait_pair)
        pair_one(c, side).start()

        @pl.when(c > 0)
        def _():
            cross_one(c, side).start()

        return carry

    def tower_part(c):
        matrix = tw[:, :, :side_k].reshape(members * units, side_k)
        return jnp.dot(matrix, x2[c].reshape(side_k, lanes), preferred_element_type=jnp.float32)

    def expect_one(c):
        cross_one(c, 1 - side).wait_recv()
        pair_one(c, 1 - side).start()

    def layer_two(c):
        def wait_pair():
            landed(x1.at[c, fs], one_recv.at[c])

        y[c] = advance(x1, 1, c, wait_pair)
        two(c, f).start()
        give(c).start()
        keep(c).start()
        for ff in range(field_count):
            @pl.when(f == ff)
            def _():
                x2[c, fs] = y[c, :, :, ff * lanes:(ff + 1) * lanes]

    def layer_three(c):
        two(c, other).wait_recv()
        pre = tower_part(c)

        @pl.when(owner)
        def _():
            pre_own[c] = pre

        @pl.when(giver)
        def _():
            pre_out[c] = pre.astype(jnp.bfloat16)
            part(c).start()

    def second(c, carry):
        layer_two(c)

        @pl.when(c == 1)
        def _():
            expect_one(2)

        def tower_step(k, carry):
            layer_three(k)
            return carry

        last = c == chunks - 1
        lax.fori_loop(
            jnp.where(last, c, jnp.maximum(c - 1, 0)), jnp.where(c < chunks - 2, c, c + 1),
            tower_step, 0)

        @pl.when(c == 2)
        def _():
            expect_one(3)

        return carry

    def finish(c):
        part(c).wait_recv()
        pre = pre_own[c] + pre_in[c].astype(jnp.float32) + unit_cols[...]
        hidden = jnp.maximum(pre, 0.0).astype(jnp.bfloat16)
        query = lax.dot_general(
            hidden, tw[:, :, side_k:].reshape(members * units, width), (((0,), (0,)), ((), ())),
            preferred_element_type=jnp.float32)
        start = pl.multiple_of(c * rc + f * lanes, lanes)
        query_vec = (query + users[pl.ds(start, lanes), :].astype(jnp.float32)).astype(jnp.bfloat16)
        logits = lax.dot_general(
            cands[...].reshape(-1, width), query_vec, (((1,), (1,)), ((), ())),
            preferred_element_type=jnp.float32) * (1.0 / math.sqrt(width))
        labels = lax.broadcasted_iota(jnp.int32, logits.shape, 0)
        target = targets[c * field_count + f]
        picked = jnp.sum(jnp.where(labels == target, logits, 0.0), axis=0, keepdims=True)
        best = jnp.max(logits, axis=0, keepdims=True)
        total = jnp.sum(jnp.exp(logits - best), axis=0, keepdims=True)
        losses[c] = best + jnp.log(total) - picked
        for k in range(1, members):
            loss_copy(k, c).start()
        keep_loss(c).start()

    @pl.when(is_mid)
    def _():
        for c in range(chunks):
            own_features[c].wait()
            cross(0, c, mid).start()
            pair(c, mid).start()
        for copy in small:
            copy.wait()
        for k in range(1, batch_count):
            cand_copy(k).start()
        pack_tower()
        far_tower(d, far).start()
        tw[me] = tw_near[...]
        both(mid, f).start()
        expect_piece(0, 0)
        expect_far(0, 0, far)
        expect_piece(0, 1)
        expect_far(0, 1, far)
        expect_piece(0, 2)
        expect_far(0, 2, far)
        plane_forward(0)
        plane_forward(1)
        expect_far(0, 3, far)
        expect_end(0)
        expect_piece(0, 3)
        plane_forward(2)
        expect_far(1, 0, far_end)
        expect_end(1)
        plane_forward(3)
        expect_tower(FAR_TOWER, far)
        expect_tower(END_TOWER, far_end)
        bias_copy(end).wait_recv()
        build_bias()
        unit_sends()
        for level in range(CROSS):
            loaded_own(level)
        expect_end(2)
        plane_rest(0)
        expect_far(1, 1, far_end)
        lax.fori_loop(0, chunks, first, 0)
        landed(cands.at[pl.ds(0, batch_count - 1)], cand_recv)
        plane_rest(2)
        both(far, f).start()
        both(far_end, f).start()
        expect_piece(1, 2)
        expect_piece(1, 3)
        plane_forward(PIECES)
        plane_forward(PIECES + 1)
        expect_one(0)
        plane_forward(PIECES + 2)
        plane_forward(PIECES + 3)
        expect_one(1)
        near_tower(end).wait_recv()
        both(end, f).start()
        landed(unit_raw.at[pl.ds(0, members - 1)], unit_recv)
        build_units()
        plane_rest(1)
        landed(tw.at[pl.ds(0, dim_count)], both_recv)
        lax.fori_loop(0, chunks, second, 0)

        @pl.when(owner)
        def _():
            for c in range(chunks):
                finish(c)

    @pl.when(owner)
    def _():
        landed(losses, loss_recv)

    @pl.when(jnp.logical_not(owner))
    def _():
        landed(loss_out, loss_recv)

    @pl.when(is_end)
    def _():
        for level in range(CROSS):
            sent(weight_part(level, 0, fl, b), piece_send.at[level])
        sent(x0.at[:, fs, entries(d), :], end_send)
        bias_copy(mid).wait_send()
        near_tower(mid).wait_send()
        far_tower(d, far).wait_send()
        sent(unit_raw.at[pl.ds(0, 4)], unit_send)
        landed(out, give_recv)

    @pl.when(is_mid)
    def _():
        far_tower(d, far).wait_send()
        sent(cands.at[pl.ds(0, batch_count - 1)], cand_send)
        sent(tw.at[pl.ds(0, dim_count)], both_send)
        sent(unit_raw.at[pl.ds(0, 3)], unit_send)
        sent(x0.at[:, fs, entries(mid), :], cross_send.at[0])
        sent(x0.at[:, fs, entries(end), :], cross_send.at[1])
        sent(x1.at[:, fs, ss, :], cross_send.at[2])
        sent(x0.at[:, fs], pair_send)
        sent(x1.at[:, fs], one_send)
        sent(y.at[:, :, :, pl.ds(0, lanes)], two_send)
        sent(out, give_send)
        pltpu.make_async_copy(out, out, out_sem).wait()
        for group in range(CROSS + 1):
            sent(plane_bytes(group, 3), plane_send.at[group])

    @pl.when(giver)
    def _():
        sent(pre_out, part_send)

    @pl.when(owner)
    def _():
        for k in range(1, members):
            sent(losses, loss_send.at[k])
        pltpu.make_async_copy(losses, losses, loss_send.at[0]).wait()


def line_body(
    counts, features, cross_weight, cross_bias, tower_weight, tower_bias, query_weight,
    user_vec, candidates, positive,
):
    batch_count, field_count, dim_count = counts
    members = field_count * dim_count
    fl, el, row_count = features.shape
    units, fields, width = tower_weight.shape
    rc = row_count // CHUNKS
    lanes = rc // field_count
    wide = 2 * el
    quarter = units // batch_count
    packed = fields * wide + width
    items = END_TOWER + 1
    dma = pltpu.SemaphoreType.DMA
    vmem = pltpu.VMEM
    bf16 = jnp.bfloat16
    f32 = jnp.float32
    far = pl.BlockSpec(memory_space=pl.ANY)
    crossed, losses = pl.pallas_call(
        functools.partial(line_kernel, counts),
        out_shape=(
            jax.ShapeDtypeStruct(features.shape, bf16),
            jax.ShapeDtypeStruct((CHUNKS * field_count, 1, lanes), f32),
        ),
        in_specs=[far] * 9,
        out_specs=(far, far),
        scratch_shapes=[
            vmem((CHUNKS, fields, width, rc), bf16),
            vmem((CHUNKS, fields, width, rc), bf16),
            vmem((CHUNKS, fl, wide, rc), bf16),
            vmem((CHUNKS, fields, wide, lanes), bf16),
            vmem((CROSS, fl, wide, fields * width), bf16),
            vmem((members, units, packed), bf16),
            vmem((units, packed), bf16),
            vmem((quarter, packed), bf16),
            vmem((fields, units, width), bf16),
            vmem((units, width), bf16),
            vmem((CHUNKS, members * units, lanes), bf16),
            vmem((CHUNKS, members * units, lanes), bf16),
            vmem((CHUNKS, members * units, lanes), f32),
            vmem((2, fl, CROSS, el), f32),
            vmem((CROSS, fl * wide, width), f32),
            vmem((members, 1, units), f32),
            vmem((members * units, lanes), f32),
            vmem((batch_count,) + candidates.shape, bf16),
            vmem(user_vec.shape, bf16),
            vmem((CHUNKS * field_count, 1, lanes), jnp.int32),
            vmem((CHUNKS, 1, lanes), f32),
            dma((CHUNKS,)), dma((CROSS,)), dma((7,)),
            dma, dma((CHUNKS,)), dma((3,)), dma((3, CHUNKS)),
            dma, dma((CHUNKS,)), dma, dma((CHUNKS,)),
            dma((CROSS,)), dma((CROSS, PIECES)), dma((CROSS + 1,)), dma((items,)), dma((CROSS + 1,)),
            dma((2,)), dma((dim_count,)), dma, dma,
            dma, dma, dma, dma, dma, dma,
            dma, dma((CHUNKS,)), dma, dma, dma, dma, dma((CHUNKS,)), dma((members,)), dma,
        ],
        compiler_params=pltpu.CompilerParams(
            collective_id=0, has_side_effects=True, vmem_limit_bytes=48 * 2**20),
        name="line_forward",
    )(*(pltpu.with_memory_space_constraint(value, pltpu.HBM) for value in (
        features,
        cross_weight.transpose(0, 1, 3, 2, 4),
        cross_bias.transpose(1, 0, 2),
        tower_weight.transpose(1, 0, 2),
        tower_bias.reshape(1, units),
        query_weight,
        user_vec,
        candidates,
        positive.reshape(CHUNKS * field_count, 1, lanes),
    )))
    return (crossed, losses.reshape(row_count))


def body(
    features, cross_weight, cross_bias, tower_weight, tower_bias, query_weight,
    user_vec, candidates, positive,
):
    counts = tuple(lax.axis_size(name) for name in ("batch", "field", "dim"))
    if line_fits(counts, features, tower_weight, candidates):
        return line_body(
            counts, features, cross_weight, cross_bias, tower_weight, tower_bias, query_weight,
            user_vec, candidates, positive)
    batch_count, field_count, dim_count = counts
    members = field_count * dim_count
    fl, el, row_count = features.shape
    columns = fl * el
    units, fields, width = tower_weight.shape
    low, held = tower_levels(dim_count)
    chunks = chunk_count(row_count, field_count, held)
    split = batch_count if units % (batch_count * 16) == 0 else 1
    part = units // split
    rc = row_count // chunks
    sub = rc // held
    run = chunks // field_count
    share = run * sub
    steps = (CROSS, chunks, dim_count)
    small = (3, dim_count)
    dma = pltpu.SemaphoreType.DMA
    vmem = pltpu.VMEM
    bf16 = jnp.bfloat16
    far = pl.BlockSpec(memory_space=pl.ANY)
    near = pl.BlockSpec(memory_space=pltpu.VMEM)
    crossed, losses = pl.pallas_call(
        functools.partial(rank_kernel, counts, (chunks, split)),
        out_shape=(
            jax.ShapeDtypeStruct(features.shape, bf16),
            jax.ShapeDtypeStruct((chunks * held, 1, sub), jnp.float32),
        ),
        in_specs=[far, far, near, far, far, far, near, far, near],
        out_specs=(near, near),
        scratch_shapes=[
            vmem((chunks, fields, width, rc), bf16),
            vmem((chunks, fields, width, rc), bf16),
            vmem((CROSS, fl, el, fields * width), bf16),
            vmem((chunks, held, fl, el, sub), bf16),
            vmem((fields, width, share), bf16),
            vmem((split, members, part, fields * width), bf16),
            vmem((members, 1, units), jnp.float32),
            vmem((split, members, part, share), jnp.float32),
            vmem((split, members, part, width), bf16),
            vmem((batch_count,) + candidates.shape, bf16),
            vmem((held, chunks, 1, sub), jnp.float32),
            dma((chunks,)), dma((CROSS, fields)), dma((fields,)), dma((3,)),
            dma(steps), dma(steps), dma(steps), dma(steps), dma(steps),
            dma((chunks, held)), dma((run, members)), dma(small), dma(small), dma(small),
            dma((3,)), dma((3,)),
            dma((split,)), dma((split,)), dma((split,)), dma((split,)),
            dma((batch_count,)), dma((batch_count,)), dma((members,)), dma((field_count, held)),
        ],
        compiler_params=pltpu.CompilerParams(
            collective_id=0, has_side_effects=True, vmem_limit_bytes=56 * 2**20),
        name="rank_forward",
    )(
        features,
        cross_weight.transpose(0, 1, 3, 2, 4),
        cross_bias.reshape(CROSS, columns, 1),
        tower_weight.transpose(1, 0, 2),
        tower_bias.reshape(1, units),
        query_weight.reshape(split, part, width),
        user_vec,
        candidates,
        positive.reshape(chunks * held, 1, sub),
    )
    return (crossed, losses.reshape(row_count))


def solution(mesh):
    placed = (
        P("field", "dim", "batch"),
        P(None, "field", "dim", None, None),
        P(None, "field", "dim"),
        P(("field", "dim"), None, None),
        P(("field", "dim")),
        P(("field", "dim"), None),
        P("batch", None),
        P("batch", None),
        P("batch"),
    )
    return jax.shard_map(
        body,
        mesh=mesh,
        in_specs=placed,
        out_specs=(P("field", "dim", "batch"), P("batch")),
        check_vma=False,
    )
```

```python
import functools
import math

import jax
import jax.numpy as jnp
from jax import lax
from jax.experimental import pallas as pl
from jax.experimental.pallas import tpu as pltpu
from jax.sharding import PartitionSpec as P

CROSS = 2
MESH = pl.DeviceIdType.MESH


def tower_levels(dim_count):
    held = min(2, dim_count)
    return (dim_count - held) // 2, held


def chunk_count(row_count, field_count, held):
    chunks = 2
    while chunks > field_count and row_count % (chunks * held * 128):
        chunks //= 2
    return chunks


def rank_kernel(
    counts, splits,
    feat, weight, bias, tower, tower_bias, query_weight, user, cand, positive,
    out, loss_out,
    x0, x1, flat, sent, rows, towers, biases, columns_bias, queries, cands, losses,
    feat_sem, weight_sem, tower_sem, small_sem,
    right_sem, left_sem, pair_sem, recv_sem, pair_recv,
    row_send, row_recv, chain_right, chain_left, chain_recv, both_send, both_recv,
    plane_send, plane_recv, plane_pair, plane_pair_recv,
    cand_send, cand_recv, loss_send, loss_recv,
):
    batch_count, field_count, dim_count = counts
    chunks, split = splits
    b = lax.axis_index("batch")
    f = lax.axis_index("field")
    d = lax.axis_index("dim")
    me = f * dim_count + d
    members = field_count * dim_count
    fl, el, row_count = feat.shape
    columns = fl * el
    fields, width, rc = x0.shape[1:]
    low, held = tower_levels(dim_count)
    high = low + held - 1
    level_of = d - low
    active = (d >= low) & (d <= high)
    sub = rc // held
    run = chunks // field_count
    share = run * sub
    part = towers.shape[2]
    units = split * part
    buffers = (x0, x1)
    other = field_count - 1 - f
    mine = b if split > 1 else 0
    to_right = jnp.minimum(d + 1, dim_count - 1)
    to_left = jnp.maximum(d - 1, 0)

    def remote(ref, send, recv, **where):
        return pltpu.make_async_remote_copy(
            ref, ref, send, recv, device_id=where, device_id_type=MESH)

    def place(ff, o):
        return pl.ds(ff * fl, fl), pl.ds(pl.multiple_of(o * el, el), el)

    def piece(ph, c, ff, o):
        fs, ds = place(ff, o)
        return buffers[ph].at[c, fs, ds, :]

    def right(ph, c, o):
        return remote(piece(ph, c, f, o), right_sem.at[ph, c, o], recv_sem.at[ph, c, o], dim=to_right)

    def left(ph, c, o):
        return remote(piece(ph, c, f, o), left_sem.at[ph, c, o], recv_sem.at[ph, c, o], dim=to_left)

    def pair(ph, c, o, ff):
        return remote(
            piece(ph, c, ff, o), pair_sem.at[ph, c, o], pair_recv.at[ph, c, o], field=other)

    def issue_own(ph, c):
        @pl.when(d < dim_count - 1)
        def _():
            right(ph, c, d).start()

        @pl.when(d > 0)
        def _():
            left(ph, c, d).start()

        pair(ph, c, d, f).start()

    def forwards(ph, c):
        for s in range(1, dim_count):
            @pl.when(d - s >= 0)
            def _():
                right(ph, c, d - s).wait_recv()

                @pl.when(d < dim_count - 1)
                def _():
                    right(ph, c, d - s).start()

                pair(ph, c, d - s, f).start()

            @pl.when(d + s < dim_count)
            def _():
                left(ph, c, d + s).wait_recv()

                @pl.when(d > 0)
                def _():
                    left(ph, c, d + s).start()

                pair(ph, c, d + s, f).start()
        for o in range(dim_count):
            pair(ph, c, o, other).wait_recv()

    def weight_copy(level, ff):
        return pltpu.make_async_copy(
            weight.at[level, :, ff],
            flat.at[level, :, :, pl.ds(pl.multiple_of(ff * width, width), width)],
            weight_sem.at[level, ff])

    def tower_copy(ff):
        return pltpu.make_async_copy(
            tower.at[ff, pl.ds(pl.multiple_of(mine * part, part), part), :],
            towers.at[mine, me, :, pl.ds(pl.multiple_of(ff * width, width), width)],
            tower_sem.at[ff])

    def each_field(act):
        def step(ff, carry):
            act(ff)
            return carry

        lax.fori_loop(0, fields, step, 0)

    small_refs = (
        lambda o: towers.at[mine, f * dim_count + o],
        lambda o: queries.at[:, f * dim_count + o],
        lambda o: biases.at[f * dim_count + o],
    )
    small_wide = (
        lambda ff: towers.at[mine, pl.ds(ff * dim_count, dim_count)],
        lambda ff: queries.at[:, pl.ds(ff * dim_count, dim_count)],
        lambda ff: biases.at[pl.ds(ff * dim_count, dim_count)],
    )

    def chain_to(k, o, sems, target):
        return remote(small_refs[k](o), sems.at[k, o], chain_recv.at[k, o], dim=target)

    def chain_own():
        for k in range(3):
            @pl.when(d < high)
            def _():
                chain_to(k, d, chain_right, to_right).start()

            @pl.when(d > low)
            def _():
                chain_to(k, d, chain_left, to_left).start()

    def chain_step(s):
        for k in range(3):
            @pl.when((d - s >= 0) & (d <= high))
            def _():
                chain_to(k, d - s, chain_right, to_right).wait_recv()

                @pl.when(d < high)
                def _():
                    chain_to(k, d - s, chain_right, to_right).start()

            @pl.when((d + s < dim_count) & (d >= low))
            def _():
                chain_to(k, d + s, chain_left, to_left).wait_recv()

                @pl.when(d > low)
                def _():
                    chain_to(k, d + s, chain_left, to_left).start()

    def both(k, ff):
        return remote(small_wide[k](ff), both_send.at[k], both_recv.at[k], field=other)

    def plane(t, source):
        return remote(
            towers.at[source, pl.ds(f * dim_count, dim_count)],
            plane_send.at[t], plane_recv.at[source], batch=t)

    def plane_both(source, ff):
        return remote(
            towers.at[source, pl.ds(ff * dim_count, dim_count)],
            plane_pair.at[source], plane_pair_recv.at[source], field=other)

    def cand_copy(t, source):
        return remote(cands.at[source], cand_send.at[t], cand_recv.at[source], batch=t)

    def loss_copy(m, ff, level):
        ref = losses.at[level, pl.ds(ff * run, run)]
        return remote(
            ref, loss_send.at[m], loss_recv.at[ff, level], field=m // dim_count, dim=m % dim_count)

    def row_copy(c, level):
        fs, ds = place(f, d)
        return pltpu.make_async_remote_copy(
            sent.at[c, level],
            rows.at[fs, ds, pl.ds(pl.multiple_of(lax.rem(c, run) * sub, sub), sub)],
            row_send.at[c, level], row_recv.at[lax.rem(c, run), me],
            device_id={"field": c // run, "dim": low + level}, device_id_type=MESH)

    def own_rows(c, level):
        return (c // run == f) & (level_of == level)

    def advance(ph, c):
        whole = buffers[ph][c].reshape(fields * width, rc)
        matrix = flat[ph].reshape(columns, fields * width)
        product = jnp.dot(matrix, whole, preferred_element_type=jnp.float32) + bias[ph]
        fs, ds = place(f, d)
        anchor = x0[c, fs, ds, :].astype(jnp.float32).reshape(columns, rc)
        current = buffers[ph][c, fs, ds, :].astype(jnp.float32).reshape(columns, rc)
        return (anchor * product + current).astype(jnp.bfloat16).reshape(fl, el, rc)

    own_copies = []
    for c in range(chunks):
        own_copies.append(pltpu.make_async_copy(
            feat.at[:, :, pl.ds(c * rc, rc)], piece(0, c, f, d), feat_sem.at[c]))
    small_copies = [
        pltpu.make_async_copy(query_weight, queries.at[:, me], small_sem.at[0]),
        pltpu.make_async_copy(tower_bias, biases.at[me], small_sem.at[1]),
        pltpu.make_async_copy(cand, cands.at[b], small_sem.at[2]),
    ]
    for copy in own_copies + small_copies:
        copy.start()
    each_field(lambda ff: tower_copy(ff).start())
    for level in range(CROSS):
        each_field(lambda ff: weight_copy(level, ff).start())

    barrier = pltpu.get_barrier_semaphore()
    for k in range(1, members):
        m = lax.rem(me + k, members)
        pl.semaphore_signal(
            barrier, inc=1, device_id={"field": m // dim_count, "dim": m % dim_count},
            device_id_type=MESH)
    for k in range(1, batch_count):
        pl.semaphore_signal(
            barrier, inc=1, device_id={"batch": lax.rem(b + k, batch_count)}, device_id_type=MESH)
    pl.semaphore_wait(barrier, members + batch_count - 2)
    for copy in own_copies:
        copy.wait()
    issue_own(0, 0)
    if chunks > 1:
        issue_own(0, 1)
    each_field(lambda ff: tower_copy(ff).wait())
    for copy in small_copies:
        copy.wait()
    chain_own()

    @pl.when(active)
    def _():
        for k in range(1, batch_count):
            cand_copy(lax.rem(b + k, batch_count), b).start()

    for level in range(CROSS):
        each_field(lambda ff: weight_copy(level, ff).wait())

    def first(c, carry):
        @pl.when(c + 2 < chunks)
        def _():
            issue_own(0, c + 2)

        forwards(0, c)
        fs, ds = place(f, d)
        x1[c, fs, ds, :] = advance(0, c)
        issue_own(1, c)

        for s in range(1, min(chunks, dim_count)):
            @pl.when(c == s)
            def _():
                chain_step(s)

        return carry

    lax.fori_loop(0, chunks, first, 0)
    for s in range(min(chunks, dim_count), dim_count):
        chain_step(s)

    @pl.when(active)
    def _():
        for k in range(3):
            both(k, f).start()
        if split > 1:
            for k in range(1, split):
                plane(lax.rem(b + k, split), b).start()

    def second(c, carry):
        forwards(1, c)
        new = advance(1, c)
        out[:, :, pl.ds(pl.multiple_of(c * rc, 128), rc)] = new
        for level in range(held):
            block = new[:, :, level * sub:(level + 1) * sub]

            @pl.when(own_rows(c, level))
            def _():
                fs, ds = place(f, d)
                rows[fs, ds, pl.ds(pl.multiple_of(lax.rem(c, run) * sub, sub), sub)] = block

            @pl.when(jnp.logical_not(own_rows(c, level)))
            def _():
                sent[c, level] = block
                row_copy(c, level).start()

        return carry

    lax.fori_loop(0, chunks, second, 0)

    def tower_block(s, query):
        matrix = towers[s].reshape(members * part, fields * width)
        pre = jnp.dot(
            matrix, rows[...].reshape(fields * width, share), preferred_element_type=jnp.float32)
        pre = pre + columns_bias[s].reshape(members * part, share)
        hidden = jnp.maximum(pre, 0.0).astype(jnp.bfloat16)
        return query + lax.dot_general(
            hidden, queries[s].reshape(members * part, width), (((0,), (0,)), ((), ())),
            preferred_element_type=jnp.float32)

    @pl.when(active)
    def _():
        if split > 1:
            for k in range(1, split):
                source = lax.rem(b + k, split)
                plane(source, source).wait_recv()
                plane_both(source, f).start()
        for k in range(3):
            both(k, other).wait_recv()
        for k in range(1, batch_count):
            source = lax.rem(b + k, batch_count)
            cand_copy(source, source).wait_recv()
        for m in range(members):
            block = jnp.broadcast_to(biases[m], (share, units)).T
            columns_bias[:, m] = block.reshape(split, part, share)
        if split > 1:
            for k in range(1, split):
                plane_both(lax.rem(b + k, split), other).wait_recv()
        for j in range(run):
            for k in range(1, members):
                m = lax.rem(me + k, members)
                fs, ds = place(m // dim_count, m % dim_count)
                remote(rows.at[fs, ds, pl.ds(j * sub, sub)], row_send.at[0, 0], row_recv.at[j, m],
                       field=m // dim_count, dim=m % dim_count).wait_recv()

        query = lax.fori_loop(0, split, tower_block, jnp.zeros((share, width), jnp.float32))
        all_cands = cands[...].reshape(-1, width)
        for j in range(run):
            c = f * run + j
            start = pl.multiple_of(c * rc + level_of * sub, sub)
            query_vec = (
                query[j * sub:(j + 1) * sub] + user[pl.ds(start, sub), :].astype(jnp.float32)
            ).astype(jnp.bfloat16)
            logits = lax.dot_general(
                all_cands, query_vec, (((1,), (1,)), ((), ())), preferred_element_type=jnp.float32
            ) * (1.0 / math.sqrt(width))
            labels = lax.broadcasted_iota(jnp.int32, logits.shape, 0)
            target = positive[c * held + level_of]
            picked = jnp.sum(jnp.where(labels == target, logits, 0.0), axis=0, keepdims=True)
            best = jnp.max(logits, axis=0, keepdims=True)
            total = jnp.sum(jnp.exp(logits - best), axis=0, keepdims=True)
            losses[level_of, c] = best + jnp.log(total) - picked
        for k in range(1, members):
            loss_copy(lax.rem(me + k, members), f, level_of).start()

    def drain(c, carry):
        for ph in range(CROSS):
            for o in range(dim_count):
                @pl.when((o <= d) & (d < dim_count - 1))
                def _():
                    right(ph, c, o).wait_send()

                @pl.when((o >= d) & (d > 0))
                def _():
                    left(ph, c, o).wait_send()

                pair(ph, c, o, f).wait_send()
        return carry

    lax.fori_loop(0, chunks, drain, 0)
    for k in range(3):
        for o in range(dim_count):
            @pl.when((o <= d) & (d < high))
            def _():
                chain_to(k, o, chain_right, to_right).wait_send()

            @pl.when((o >= d) & (d > low))
            def _():
                chain_to(k, o, chain_left, to_left).wait_send()

    @pl.when(active)
    def _():
        for k in range(3):
            both(k, f).wait_send()
        if split > 1:
            for k in range(1, split):
                t = lax.rem(b + k, split)
                plane(t, b).wait_send()
                plane_both(t, f).wait_send()
        for k in range(1, batch_count):
            cand_copy(lax.rem(b + k, batch_count), b).wait_send()
        for k in range(1, members):
            loss_copy(lax.rem(me + k, members), f, level_of).wait_send()

    for c in range(chunks):
        for level in range(held):
            @pl.when(jnp.logical_not(own_rows(c, level)))
            def _():
                row_copy(c, level).wait_send()

    for ff in range(field_count):
        for level in range(held):
            @pl.when(jnp.logical_not((f == ff) & (level_of == level)))
            def _():
                loss_copy(ff * dim_count + low + level, ff, level).wait_recv()

    for c in range(chunks):
        for level in range(held):
            loss_out[c * held + level] = losses[level, c]


def line_pieces(count, parts):
    base, extra = divmod(count, parts)
    bounds, start = [], 0
    for k in range(parts):
        size = base + (k < extra)
        bounds.append((start, size))
        start += size
    return bounds


def line_fits(counts, features, tower_weight, candidates):
    batch_count, field_count, dim_count = counts
    fl, el, row_count = features.shape
    units, fields, width = tower_weight.shape
    return (
        dim_count == 4 and batch_count == 4 and field_count == 2
        and fields % 2 == 0 and fl >= PIECES and el % 32 == 0 and 4 * el == width and width == 128
        and row_count % (CHUNKS * field_count * 128) == 0 and units % (16 * batch_count) == 0)


PIECES = 4
CHUNKS = 4
FAR_TOWER = CROSS * PIECES
END_TOWER = FAR_TOWER + 1
CANDS = END_TOWER + 1


def line_kernel(
    counts,
    feat, weight, bias, tower, tower_bias, query_weight, user, cand, positive,
    out, loss_out,
    x0, x1, y, x2, flat, tw, tw_near, tw_far, tw_pass, tw_raw, q_raw, pre_out, pre_in, pre_own,
    bias_raw, bias_cols, unit_raw, unit_cols, cands, users, targets, losses,
    feat_sem, weight_sem, small_sem,
    end_send, end_recv, cross_send, cross_recv, pair_send, pair_recv, one_send, one_recv,
    piece_send, piece_recv, plane_send, plane_recv, rest_recv,
    tower_send, tower_recv, near_recv, both_send, both_recv,
    bias_send, bias_recv, unit_send, unit_recv, near_unit,
    two_send, two_recv, out_sem, give_send, give_recv, part_send, part_recv, loss_send, loss_recv,
):
    batch_count, field_count, dim_count = counts
    b = lax.axis_index("batch")
    f = lax.axis_index("field")
    d = lax.axis_index("dim")
    members = field_count * dim_count
    me = f * dim_count + d
    chunks, fields, width, rc = x0.shape
    fl, el, _ = feat.shape
    wide = 2 * el
    half_k = fields // 2 * width
    quarter_units = tw_far.shape[0]
    units = tw.shape[1]
    side_k = fields * wide
    lanes = rc // field_count
    rows_in_part = el // 2
    side = d // 2
    mid = 1 + side
    far = 2 - side
    end = 3 * side
    far_end = 3 - end
    is_mid = d == mid
    is_end = d == end
    owner = is_mid & (f == side)
    giver = is_mid & (f != side)
    other = field_count - 1 - f
    x_next = b + 1 - 2 * lax.rem(b, 2)
    y_next = lax.rem(b + 2, 4)
    diagonal = 3 - b
    fs = pl.ds(f * fl, fl)
    ss = pl.ds(pl.multiple_of(side * wide, wide), wide)

    def remote(ref, send, recv, to=None, **where):
        return pltpu.make_async_remote_copy(
            ref, ref if to is None else to, send, recv, device_id=where, device_id_type=MESH)

    def sent(ref, sem):
        remote(ref, sem, sem, field=other).wait_send()

    def landed(ref, sem):
        remote(ref, sem, sem, field=other).wait_recv()

    def entries(o):
        return pl.ds(pl.multiple_of(o * el, el), el)

    def within(o):
        return pl.ds(pl.multiple_of(lax.rem(o, 2) * el, el), el)

    def block(c, ff, o):
        return x0.at[c, pl.ds(ff * fl, fl), entries(o), :]

    def from_end(c, target):
        return remote(block(c, f, end), end_send, end_recv.at[c], dim=target)

    def cross(k, c, o):
        return remote(block(c, f, o), cross_send.at[k], cross_recv.at[k, c], dim=far)

    def cross_one(c, s):
        ref = x1.at[c, fs, pl.ds(pl.multiple_of(s * wide, wide), wide), :]
        return remote(ref, cross_send.at[2], cross_recv.at[2, c], dim=far)

    def pair(c, o):
        return remote(block(c, f, o), pair_send, pair_recv.at[c], field=other)

    def pair_one(c, s):
        ref = x1.at[c, fs, pl.ds(pl.multiple_of(s * wide, wide), wide), :]
        return remote(ref, one_send, one_recv.at[c], field=other)

    def weight_piece(level, p, source):
        start, size = line_pieces(fl, PIECES)[p]
        return weight_part(level, start, size, source)

    def weight_part(level, start, size, source):
        row = pl.multiple_of(lax.rem(end, 2) * el + lax.rem(source, 2) * rows_in_part, rows_in_part)
        lane = pl.multiple_of(source // 2 * half_k, half_k)
        return flat.at[level, pl.ds(start, size), pl.ds(row, rows_in_part), pl.ds(lane, half_k)]

    def piece(level, p, target):
        ref = weight_piece(level, p, b)
        return remote(ref, piece_send.at[level], piece_recv.at[level, p], dim=target)

    def tower_rows(member, source):
        return tw.at[member, pl.ds(pl.multiple_of(source * quarter_units, quarter_units), quarter_units), :]

    def item(i, source):
        if i < CROSS * PIECES:
            return weight_piece(i // PIECES, i % PIECES, source)
        if i == CANDS:
            return cands.at[source]
        return tower_rows(f * dim_count + (far if i == FAR_TOWER else far_end), source)

    def relay(i):
        return (x_next, y_next) if i % 2 == 0 else (y_next, x_next)

    def group_of(i):
        return CROSS + 1 if i == CANDS else i // PIECES

    def plane(i, source, target, arrival):
        return remote(item(i, source), plane_send.at[group_of(i)], arrival, batch=target)

    def plane_out(i):
        first, second = relay(i)
        plane(i, b, first, plane_recv.at[i]).start()
        plane(i, b, second, rest_recv.at[group_of(i)]).start()

    def plane_forward(i):
        source, target = relay(i)
        plane(i, source, target, plane_recv.at[i]).wait_recv()
        plane(i, source, target, rest_recv.at[group_of(i)]).start()

    def plane_rest(group):
        landed(plane_bytes(group, 2), rest_recv.at[group])

    def plane_bytes(group, copies):
        if group < CROSS:
            return flat.at[group, :, pl.ds(0, copies * rows_in_part), pl.ds(0, half_k)]
        if group == CROSS + 1:
            return cands.at[pl.ds(0, copies)]
        return tw.at[pl.ds(0, copies * 2), pl.ds(0, quarter_units), :]

    def near_tower(target):
        return remote(
            tw_near, tower_send.at[0], near_recv, to=tw.at[f * dim_count + end], dim=target)

    def far_tower(source, target):
        return remote(
            tw_far, tower_send.at[1], tower_recv.at[source],
            to=tower_rows(f * dim_count + source, b), dim=target)

    def pass_in(target):
        return remote(tw_far, tower_send.at[1], tower_recv.at[mid], to=tw_pass, dim=target)

    def pass_on():
        return remote(
            tw_pass, tower_send.at[0], tower_recv.at[end],
            to=tower_rows(f * dim_count + end, b), dim=far)

    def both(z, ff):
        return remote(tw.at[ff * dim_count + z], both_send, both_recv, field=other)

    def bias_copy(target):
        return remote(bias_raw.at[lax.rem(end, 2)], bias_send, bias_recv, dim=target)

    def unit_in(target):
        return remote(unit_raw.at[f * dim_count + end], unit_send, near_unit, dim=target)

    def unit_out(ff, z):
        rows = unit_raw.at[pl.ds(f * dim_count + 2 * side, 2)]
        return remote(rows, unit_send, unit_recv, field=ff, dim=z)

    def two(c, ff):
        lane = pl.multiple_of((1 - ff) * lanes, lanes)
        return remote(
            y.at[c, :, :, pl.ds(lane, lanes)], two_send, two_recv.at[c],
            to=x2.at[c, pl.ds(ff * fl, fl)], field=other)

    def rows_of(c):
        return pl.ds(pl.multiple_of(c * rc, rc), rc)

    def keep(c):
        return pltpu.make_async_copy(y.at[c, :, within(mid), :], out.at[:, :, rows_of(c)], out_sem)

    def give(c):
        return remote(
            y.at[c, :, within(end), :], give_send, give_recv,
            to=out.at[:, :, rows_of(c)], dim=end)

    def part(c):
        return remote(pre_out.at[c], part_send, part_recv.at[c], to=pre_in.at[c], dim=far)

    def loss_copy(k, c):
        m = lax.rem(me + k, members)
        return remote(
            losses.at[c], loss_send.at[k], loss_recv, to=loss_out.at[c * field_count + f],
            field=m // dim_count, dim=lax.rem(m, dim_count))

    def keep_loss(c):
        return pltpu.make_async_copy(losses.at[c], loss_out.at[c * field_count + f], loss_send.at[0])

    def own_weight(level, ff):
        return pltpu.make_async_copy(
            weight.at[level, :, ff],
            flat.at[level, :, within(mid), pl.ds(pl.multiple_of(ff * width, width), width)],
            weight_sem.at[level])

    def end_weight(level, k):
        row = pl.multiple_of(lax.rem(b, 2) * rows_in_part, rows_in_part)
        ff = b // 2 * (fields // 2) + k
        to = pl.multiple_of(lax.rem(end, 2) * el + row, rows_in_part)
        return pltpu.make_async_copy(
            weight.at[level, :, ff, pl.ds(row, rows_in_part), :],
            flat.at[level, :, pl.ds(to, rows_in_part), pl.ds(pl.multiple_of(ff * width, width), width)],
            weight_sem.at[level])

    def each(count, act):
        def step(k, carry):
            act(k)
            return carry

        lax.fori_loop(0, count, step, 0)

    own_features = [
        pltpu.make_async_copy(feat.at[:, :, pl.ds(c * rc, rc)], block(c, f, d), feat_sem.at[c])
        for c in range(chunks)]
    quarter = pl.ds(pl.multiple_of(b * quarter_units, quarter_units), quarter_units)
    small = [
        pltpu.make_async_copy(bias, bias_raw.at[lax.rem(d, 2)], small_sem.at[0]),
        pltpu.make_async_copy(tower_bias, unit_raw.at[me], small_sem.at[1]),
        pltpu.make_async_copy(cand, cands.at[b], small_sem.at[2]),
        pltpu.make_async_copy(tower, tw_raw, small_sem.at[3]),
        pltpu.make_async_copy(query_weight, q_raw, small_sem.at[4]),
        pltpu.make_async_copy(user, users, small_sem.at[5]),
        pltpu.make_async_copy(positive, targets, small_sem.at[6]),
    ]
    barrier = pltpu.get_barrier_semaphore()

    def greet(**where):
        pl.semaphore_signal(barrier, inc=1, device_id=where, device_id_type=MESH)

    @pl.when(is_end)
    def _():
        for ff in range(field_count):
            for z in (1, 2):
                greet(field=ff, dim=z)

    @pl.when(is_mid)
    def _():
        greet(dim=end)
        greet(dim=far)
        greet(batch=x_next)
        greet(batch=y_next)
        greet(field=other, dim=far)
        greet(field=other)

    for copy in own_features:
        copy.start()

    @pl.when(is_end)
    def _():
        each(fields // 2, lambda k: end_weight(0, k).start())

    for copy in small:
        copy.start()

    @pl.when(is_mid)
    def _():
        each(fields, lambda k: own_weight(0, k).start())
        each(fields, lambda k: own_weight(1, k).start())

    @pl.when(is_end)
    def _():
        each(fields // 2, lambda k: end_weight(1, k).start())

    pl.semaphore_wait(barrier, jnp.where(is_mid, 2 * field_count + 5, 1))

    def loaded_own(level):
        ref = flat.at[level, :, within(mid), :]
        pltpu.make_async_copy(ref, ref, weight_sem.at[level]).wait()

    def loaded_end(level):
        ref = weight_part(level, 0, fl, b)
        pltpu.make_async_copy(ref, ref, weight_sem.at[level]).wait()

    def pack_tower():
        def halves(rows, j):
            first = tw_raw[2 * j, rows, :]
            second = tw_raw[2 * j + 1, rows, :]
            low = jnp.concatenate([first[:, :wide], second[:, :wide]], axis=1)
            high = jnp.concatenate([first[:, wide:], second[:, wide:]], axis=1)
            return low, high

        for j in range(fields // 2):
            low, high = halves(slice(None), j)
            tw_near[:, j * width:(j + 1) * width] = jnp.where(side == 0, low, high)
            low, high = halves(quarter, j)
            tw_far[:, j * width:(j + 1) * width] = jnp.where(side == 0, high, low)
        tw_near[:, side_k:] = q_raw[...]
        tw_far[:, side_k:] = q_raw[quarter, :]

    @pl.when(is_end)
    def _():
        loaded_end(0)
        for p in range(PIECES - 1):
            piece(0, p, mid).start()
        for copy in small:
            copy.wait()
        pack_tower()
        pass_in(mid).start()
        for copy in own_features:
            copy.wait()
        from_end(0, mid).start()
        piece(0, PIECES - 1, mid).start()
        from_end(1, mid).start()
        bias_copy(mid).start()
        unit_in(mid).start()
        for c in range(2, chunks):
            from_end(c, mid).start()
        loaded_end(1)
        for p in range(PIECES):
            piece(1, p, mid).start()
        near_tower(mid).start()

    def expect_piece(level, p):
        piece(level, p, end).wait_recv()
        plane_out(level * PIECES + p)

    def expect_end(c):
        from_end(c, end).wait_recv()
        cross(1, c, end).start()
        pair(c, end).start()

    def expect_far(k, c, o):
        cross(k, c, o).wait_recv()
        pair(c, o).start()

    def expect_tower(i, z):
        far_tower(z, end).wait_recv()
        plane_out(i)

    def half(source, level, c, ff):
        matrix = flat[level, :, :, pl.ds(pl.multiple_of(ff * half_k, half_k), half_k)]
        return jnp.dot(
            matrix.reshape(fl * wide, half_k), source[c, pl.ds(ff * fl, fl)].reshape(half_k, rc),
            preferred_element_type=jnp.float32)

    def advance(source, level, c, wait_pair):
        product = half(source, level, c, f)
        wait_pair()
        product = product + half(source, level, c, other)
        column = bias_cols[level]
        product = product + jnp.concatenate([column] * (rc // column.shape[1]), axis=1)
        anchor = x0[c, fs, ss, :].astype(jnp.float32).reshape(fl * wide, rc)
        current = source[c, fs, ss, :].astype(jnp.float32).reshape(fl * wide, rc)
        return (anchor * product + current).astype(jnp.bfloat16).reshape(fl, wide, rc)

    def build_bias():
        pick = (lax.broadcasted_iota(jnp.int32, (el, el), 0) == lax.broadcasted_iota(jnp.int32, (el, el), 1))
        for level in range(CROSS):
            for k in range(fl):
                for s in range(2):
                    line = bias_raw[s, k, level:level + 1, :]
                    column = jnp.sum(jnp.where(pick, line, 0.0), axis=1, keepdims=True)
                    start = (2 * k + s) * el
                    bias_cols[level, start:start + el, :] = jnp.broadcast_to(column, (el, width))

    def build_units():
        for m in range(members):
            unit_cols[m * units:(m + 1) * units, :] = jnp.broadcast_to(unit_raw[m], (lanes, units)).T

    def first(c, carry):
        @pl.when(c == 2)
        def _():
            expect_far(1, 2, far_end)
            plane_forward(FAR_TOWER)
            plane_forward(END_TOWER)
            expect_piece(1, 0)

        @pl.when(c == 3)
        def _():
            expect_far(1, 3, far_end)
            expect_piece(1, 1)

        def wait_pair():
            landed(x0.at[c, fs], pair_recv.at[c])

        x1[c, fs, ss, :] = advance(x0, 0, c, wait_pair)
        cross_one(c, side).start()
        pair_one(c, side).start()
        return carry

    def tower_part(c):
        matrix = tw[:, :, :side_k].reshape(members * units, side_k)
        return jnp.dot(matrix, x2[c].reshape(side_k, lanes), preferred_element_type=jnp.float32)

    def expect_one(c):
        cross_one(c, 1 - side).wait_recv()
        pair_one(c, 1 - side).start()

    def layer_two(c):
        def wait_pair():
            landed(x1.at[c, fs], one_recv.at[c])

        y[c] = advance(x1, 1, c, wait_pair)
        two(c, f).start()
        give(c).start()
        keep(c).start()
        for ff in range(field_count):
            @pl.when(f == ff)
            def _():
                x2[c, fs] = y[c, :, :, ff * lanes:(ff + 1) * lanes]

    def layer_three(c):
        two(c, other).wait_recv()
        pre = tower_part(c)

        @pl.when(owner)
        def _():
            pre_own[c] = pre

        @pl.when(giver)
        def _():
            pre_out[c] = pre.astype(jnp.bfloat16)
            part(c).start()

    def second(c, carry):
        layer_two(c)

        @pl.when(c == 1)
        def _():
            expect_one(2)

        def tower_step(k, carry):
            layer_three(k)
            return carry

        last = c == chunks - 1
        lax.fori_loop(
            jnp.where(last, c, jnp.maximum(c - 1, 0)), jnp.where(c < chunks - 2, c, c + 1),
            tower_step, 0)

        @pl.when(c == 2)
        def _():
            expect_one(3)

        return carry

    def finish(c):
        part(c).wait_recv()
        pre = pre_own[c] + pre_in[c].astype(jnp.float32) + unit_cols[...]
        hidden = jnp.maximum(pre, 0.0).astype(jnp.bfloat16)
        query = lax.dot_general(
            hidden, tw[:, :, side_k:].reshape(members * units, width), (((0,), (0,)), ((), ())),
            preferred_element_type=jnp.float32)
        start = pl.multiple_of(c * rc + f * lanes, lanes)
        query_vec = (query + users[pl.ds(start, lanes), :].astype(jnp.float32)).astype(jnp.bfloat16)
        logits = lax.dot_general(
            cands[...].reshape(-1, width), query_vec, (((1,), (1,)), ((), ())),
            preferred_element_type=jnp.float32) * (1.0 / math.sqrt(width))
        labels = lax.broadcasted_iota(jnp.int32, logits.shape, 0)
        target = targets[c * field_count + f]
        picked = jnp.sum(jnp.where(labels == target, logits, 0.0), axis=0, keepdims=True)
        best = jnp.max(logits, axis=0, keepdims=True)
        total = jnp.sum(jnp.exp(logits - best), axis=0, keepdims=True)
        losses[c] = best + jnp.log(total) - picked
        for k in range(1, members):
            loss_copy(k, c).start()
        keep_loss(c).start()

    @pl.when(is_mid)
    def _():
        for c in range(chunks):
            own_features[c].wait()
            cross(0, c, mid).start()
            pair(c, mid).start()
        for copy in small:
            copy.wait()
        plane_out(CANDS)
        pack_tower()
        far_tower(d, far).start()
        tw[me] = tw_near[...]
        both(mid, f).start()
        expect_piece(0, 0)
        expect_far(0, 0, far)
        expect_piece(0, 1)
        expect_far(0, 1, far)
        plane_forward(CANDS)
        expect_piece(0, 2)
        pass_in(end).wait_recv()
        pass_on().start()
        expect_far(0, 2, far)
        plane_forward(0)
        plane_forward(1)
        expect_far(0, 3, far)
        expect_end(0)
        expect_piece(0, 3)
        plane_forward(2)
        expect_end(1)
        plane_forward(3)
        expect_far(1, 0, far_end)
        expect_tower(FAR_TOWER, far)
        expect_tower(END_TOWER, far_end)
        bias_copy(end).wait_recv()
        build_bias()
        unit_in(end).wait_recv()
        unit_out(other, d).start()
        unit_out(f, far).start()
        unit_out(other, far).start()
        for level in range(CROSS):
            loaded_own(level)
        expect_end(2)
        plane_rest(0)
        expect_far(1, 1, far_end)
        expect_end(3)
        lax.fori_loop(0, chunks, first, 0)
        plane_rest(3)
        plane_rest(2)
        both(far, f).start()
        both(far_end, f).start()
        expect_piece(1, 2)
        expect_piece(1, 3)
        plane_forward(PIECES)
        plane_forward(PIECES + 1)
        expect_one(0)
        plane_forward(PIECES + 2)
        plane_forward(PIECES + 3)
        expect_one(1)
        near_tower(end).wait_recv()
        both(end, f).start()
        landed(unit_raw.at[pl.ds(0, 6)], unit_recv)
        build_units()
        plane_rest(1)
        landed(tw.at[pl.ds(0, dim_count)], both_recv)
        lax.fori_loop(0, chunks, second, 0)

        @pl.when(owner)
        def _():
            for c in range(chunks):
                finish(c)

    @pl.when(owner)
    def _():
        landed(losses, loss_recv)

    @pl.when(jnp.logical_not(owner))
    def _():
        landed(loss_out, loss_recv)

    @pl.when(is_end)
    def _():
        for level in range(CROSS):
            sent(weight_part(level, 0, fl, b), piece_send.at[level])
        sent(x0.at[:, fs, entries(d), :], end_send)
        bias_copy(mid).wait_send()
        near_tower(mid).wait_send()
        pass_in(mid).wait_send()
        unit_in(mid).wait_send()
        landed(out, give_recv)

    @pl.when(is_mid)
    def _():
        far_tower(d, far).wait_send()
        pass_on().wait_send()
        sent(tw.at[pl.ds(0, dim_count)], both_send)
        sent(unit_raw.at[pl.ds(0, 6)], unit_send)
        sent(x0.at[:, fs, entries(mid), :], cross_send.at[0])
        sent(x0.at[:, fs, entries(end), :], cross_send.at[1])
        sent(x1.at[:, fs, ss, :], cross_send.at[2])
        sent(x0.at[:, fs], pair_send)
        sent(x1.at[:, fs], one_send)
        sent(y.at[:, :, :, pl.ds(0, lanes)], two_send)
        sent(out, give_send)
        pltpu.make_async_copy(out, out, out_sem).wait()
        for group in range(CROSS + 2):
            sent(plane_bytes(group, 3), plane_send.at[group])

    @pl.when(giver)
    def _():
        sent(pre_out, part_send)

    @pl.when(owner)
    def _():
        for k in range(1, members):
            sent(losses, loss_send.at[k])
        pltpu.make_async_copy(losses, losses, loss_send.at[0]).wait()


def line_body(
    counts, features, cross_weight, cross_bias, tower_weight, tower_bias, query_weight,
    user_vec, candidates, positive,
):
    batch_count, field_count, dim_count = counts
    members = field_count * dim_count
    fl, el, row_count = features.shape
    units, fields, width = tower_weight.shape
    rc = row_count // CHUNKS
    lanes = rc // field_count
    wide = 2 * el
    quarter = units // batch_count
    packed = fields * wide + width
    items = CANDS + 1
    dma = pltpu.SemaphoreType.DMA
    vmem = pltpu.VMEM
    bf16 = jnp.bfloat16
    f32 = jnp.float32
    far = pl.BlockSpec(memory_space=pl.ANY)
    crossed, losses = pl.pallas_call(
        functools.partial(line_kernel, counts),
        out_shape=(
            jax.ShapeDtypeStruct(features.shape, bf16),
            jax.ShapeDtypeStruct((CHUNKS * field_count, 1, lanes), f32),
        ),
        in_specs=[far] * 9,
        out_specs=(far, far),
        scratch_shapes=[
            vmem((CHUNKS, fields, width, rc), bf16),
            vmem((CHUNKS, fields, width, rc), bf16),
            vmem((CHUNKS, fl, wide, rc), bf16),
            vmem((CHUNKS, fields, wide, lanes), bf16),
            vmem((CROSS, fl, wide, fields * width), bf16),
            vmem((members, units, packed), bf16),
            vmem((units, packed), bf16),
            vmem((quarter, packed), bf16),
            vmem((quarter, packed), bf16),
            vmem((fields, units, width), bf16),
            vmem((units, width), bf16),
            vmem((CHUNKS, members * units, lanes), bf16),
            vmem((CHUNKS, members * units, lanes), bf16),
            vmem((CHUNKS, members * units, lanes), f32),
            vmem((2, fl, CROSS, el), f32),
            vmem((CROSS, fl * wide, width), f32),
            vmem((members, 1, units), f32),
            vmem((members * units, lanes), f32),
            vmem((batch_count,) + candidates.shape, bf16),
            vmem(user_vec.shape, bf16),
            vmem((CHUNKS * field_count, 1, lanes), jnp.int32),
            vmem((CHUNKS, 1, lanes), f32),
            dma((CHUNKS,)), dma((CROSS,)), dma((7,)),
            dma, dma((CHUNKS,)), dma((3,)), dma((3, CHUNKS)),
            dma, dma((CHUNKS,)), dma, dma((CHUNKS,)),
            dma((CROSS,)), dma((CROSS, PIECES)), dma((CROSS + 2,)), dma((items,)), dma((CROSS + 2,)),
            dma((2,)), dma((dim_count,)), dma, dma, dma,
            dma, dma, dma, dma, dma,
            dma, dma((CHUNKS,)), dma, dma, dma, dma, dma((CHUNKS,)), dma((members,)), dma,
        ],
        compiler_params=pltpu.CompilerParams(
            collective_id=0, has_side_effects=True, vmem_limit_bytes=48 * 2**20),
        name="line_forward",
    )(*(pltpu.with_memory_space_constraint(value, pltpu.HBM) for value in (
        features,
        cross_weight.transpose(0, 1, 3, 2, 4),
        cross_bias.transpose(1, 0, 2),
        tower_weight.transpose(1, 0, 2),
        tower_bias.reshape(1, units),
        query_weight,
        user_vec,
        candidates,
        positive.reshape(CHUNKS * field_count, 1, lanes),
    )))
    return (crossed, losses.reshape(row_count))


def body(
    features, cross_weight, cross_bias, tower_weight, tower_bias, query_weight,
    user_vec, candidates, positive,
):
    counts = tuple(lax.axis_size(name) for name in ("batch", "field", "dim"))
    if line_fits(counts, features, tower_weight, candidates):
        return line_body(
            counts, features, cross_weight, cross_bias, tower_weight, tower_bias, query_weight,
            user_vec, candidates, positive)
    batch_count, field_count, dim_count = counts
    members = field_count * dim_count
    fl, el, row_count = features.shape
    columns = fl * el
    units, fields, width = tower_weight.shape
    low, held = tower_levels(dim_count)
    chunks = chunk_count(row_count, field_count, held)
    split = batch_count if units % (batch_count * 16) == 0 else 1
    part = units // split
    rc = row_count // chunks
    sub = rc // held
    run = chunks // field_count
    share = run * sub
    steps = (CROSS, chunks, dim_count)
    small = (3, dim_count)
    dma = pltpu.SemaphoreType.DMA
    vmem = pltpu.VMEM
    bf16 = jnp.bfloat16
    far = pl.BlockSpec(memory_space=pl.ANY)
    near = pl.BlockSpec(memory_space=pltpu.VMEM)
    crossed, losses = pl.pallas_call(
        functools.partial(rank_kernel, counts, (chunks, split)),
        out_shape=(
            jax.ShapeDtypeStruct(features.shape, bf16),
            jax.ShapeDtypeStruct((chunks * held, 1, sub), jnp.float32),
        ),
        in_specs=[far, far, near, far, far, far, near, far, near],
        out_specs=(near, near),
        scratch_shapes=[
            vmem((chunks, fields, width, rc), bf16),
            vmem((chunks, fields, width, rc), bf16),
            vmem((CROSS, fl, el, fields * width), bf16),
            vmem((chunks, held, fl, el, sub), bf16),
            vmem((fields, width, share), bf16),
            vmem((split, members, part, fields * width), bf16),
            vmem((members, 1, units), jnp.float32),
            vmem((split, members, part, share), jnp.float32),
            vmem((split, members, part, width), bf16),
            vmem((batch_count,) + candidates.shape, bf16),
            vmem((held, chunks, 1, sub), jnp.float32),
            dma((chunks,)), dma((CROSS, fields)), dma((fields,)), dma((3,)),
            dma(steps), dma(steps), dma(steps), dma(steps), dma(steps),
            dma((chunks, held)), dma((run, members)), dma(small), dma(small), dma(small),
            dma((3,)), dma((3,)),
            dma((split,)), dma((split,)), dma((split,)), dma((split,)),
            dma((batch_count,)), dma((batch_count,)), dma((members,)), dma((field_count, held)),
        ],
        compiler_params=pltpu.CompilerParams(
            collective_id=0, has_side_effects=True, vmem_limit_bytes=56 * 2**20),
        name="rank_forward",
    )(
        features,
        cross_weight.transpose(0, 1, 3, 2, 4),
        cross_bias.reshape(CROSS, columns, 1),
        tower_weight.transpose(1, 0, 2),
        tower_bias.reshape(1, units),
        query_weight.reshape(split, part, width),
        user_vec,
        candidates,
        positive.reshape(chunks * held, 1, sub),
    )
    return (crossed, losses.reshape(row_count))


def solution(mesh):
    placed = (
        P("field", "dim", "batch"),
        P(None, "field", "dim", None, None),
        P(None, "field", "dim"),
        P(("field", "dim"), None, None),
        P(("field", "dim")),
        P(("field", "dim"), None),
        P("batch", None),
        P("batch", None),
        P("batch"),
    )
    return jax.shard_map(
        body,
        mesh=mesh,
        in_specs=placed,
        out_specs=(P("field", "dim", "batch"), P("batch")),
        check_vma=False,
    )
```

```python
import functools
import math

import jax
import jax.numpy as jnp
from jax import lax
from jax.experimental import pallas as pl
from jax.experimental.pallas import tpu as pltpu
from jax.sharding import PartitionSpec as P

CROSS = 2
MESH = pl.DeviceIdType.MESH


def tower_levels(dim_count):
    held = min(2, dim_count)
    return (dim_count - held) // 2, held


def chunk_count(row_count, field_count, held):
    chunks = 2
    while chunks > field_count and row_count % (chunks * held * 128):
        chunks //= 2
    return chunks


def rank_kernel(
    counts, splits,
    feat, weight, bias, tower, tower_bias, query_weight, user, cand, positive,
    out, loss_out,
    x0, x1, flat, sent, rows, towers, biases, columns_bias, queries, cands, losses,
    feat_sem, weight_sem, tower_sem, small_sem,
    right_sem, left_sem, pair_sem, recv_sem, pair_recv,
    row_send, row_recv, chain_right, chain_left, chain_recv, both_send, both_recv,
    plane_send, plane_recv, plane_pair, plane_pair_recv,
    cand_send, cand_recv, loss_send, loss_recv,
):
    batch_count, field_count, dim_count = counts
    chunks, split = splits
    b = lax.axis_index("batch")
    f = lax.axis_index("field")
    d = lax.axis_index("dim")
    me = f * dim_count + d
    members = field_count * dim_count
    fl, el, row_count = feat.shape
    columns = fl * el
    fields, width, rc = x0.shape[1:]
    low, held = tower_levels(dim_count)
    high = low + held - 1
    level_of = d - low
    active = (d >= low) & (d <= high)
    sub = rc // held
    run = chunks // field_count
    share = run * sub
    part = towers.shape[2]
    units = split * part
    buffers = (x0, x1)
    other = field_count - 1 - f
    mine = b if split > 1 else 0
    to_right = jnp.minimum(d + 1, dim_count - 1)
    to_left = jnp.maximum(d - 1, 0)

    def remote(ref, send, recv, **where):
        return pltpu.make_async_remote_copy(
            ref, ref, send, recv, device_id=where, device_id_type=MESH)

    def place(ff, o):
        return pl.ds(ff * fl, fl), pl.ds(pl.multiple_of(o * el, el), el)

    def piece(ph, c, ff, o):
        fs, ds = place(ff, o)
        return buffers[ph].at[c, fs, ds, :]

    def right(ph, c, o):
        return remote(piece(ph, c, f, o), right_sem.at[ph, c, o], recv_sem.at[ph, c, o], dim=to_right)

    def left(ph, c, o):
        return remote(piece(ph, c, f, o), left_sem.at[ph, c, o], recv_sem.at[ph, c, o], dim=to_left)

    def pair(ph, c, o, ff):
        return remote(
            piece(ph, c, ff, o), pair_sem.at[ph, c, o], pair_recv.at[ph, c, o], field=other)

    def issue_own(ph, c):
        @pl.when(d < dim_count - 1)
        def _():
            right(ph, c, d).start()

        @pl.when(d > 0)
        def _():
            left(ph, c, d).start()

        pair(ph, c, d, f).start()

    def forwards(ph, c):
        for s in range(1, dim_count):
            @pl.when(d - s >= 0)
            def _():
                right(ph, c, d - s).wait_recv()

                @pl.when(d < dim_count - 1)
                def _():
                    right(ph, c, d - s).start()

                pair(ph, c, d - s, f).start()

            @pl.when(d + s < dim_count)
            def _():
                left(ph, c, d + s).wait_recv()

                @pl.when(d > 0)
                def _():
                    left(ph, c, d + s).start()

                pair(ph, c, d + s, f).start()
        for o in range(dim_count):
            pair(ph, c, o, other).wait_recv()

    def weight_copy(level, ff):
        return pltpu.make_async_copy(
            weight.at[level, :, ff],
            flat.at[level, :, :, pl.ds(pl.multiple_of(ff * width, width), width)],
            weight_sem.at[level, ff])

    def tower_copy(ff):
        return pltpu.make_async_copy(
            tower.at[ff, pl.ds(pl.multiple_of(mine * part, part), part), :],
            towers.at[mine, me, :, pl.ds(pl.multiple_of(ff * width, width), width)],
            tower_sem.at[ff])

    def each_field(act):
        def step(ff, carry):
            act(ff)
            return carry

        lax.fori_loop(0, fields, step, 0)

    small_refs = (
        lambda o: towers.at[mine, f * dim_count + o],
        lambda o: queries.at[:, f * dim_count + o],
        lambda o: biases.at[f * dim_count + o],
    )
    small_wide = (
        lambda ff: towers.at[mine, pl.ds(ff * dim_count, dim_count)],
        lambda ff: queries.at[:, pl.ds(ff * dim_count, dim_count)],
        lambda ff: biases.at[pl.ds(ff * dim_count, dim_count)],
    )

    def chain_to(k, o, sems, target):
        return remote(small_refs[k](o), sems.at[k, o], chain_recv.at[k, o], dim=target)

    def chain_own():
        for k in range(3):
            @pl.when(d < high)
            def _():
                chain_to(k, d, chain_right, to_right).start()

            @pl.when(d > low)
            def _():
                chain_to(k, d, chain_left, to_left).start()

    def chain_step(s):
        for k in range(3):
            @pl.when((d - s >= 0) & (d <= high))
            def _():
                chain_to(k, d - s, chain_right, to_right).wait_recv()

                @pl.when(d < high)
                def _():
                    chain_to(k, d - s, chain_right, to_right).start()

            @pl.when((d + s < dim_count) & (d >= low))
            def _():
                chain_to(k, d + s, chain_left, to_left).wait_recv()

                @pl.when(d > low)
                def _():
                    chain_to(k, d + s, chain_left, to_left).start()

    def both(k, ff):
        return remote(small_wide[k](ff), both_send.at[k], both_recv.at[k], field=other)

    def plane(t, source):
        return remote(
            towers.at[source, pl.ds(f * dim_count, dim_count)],
            plane_send.at[t], plane_recv.at[source], batch=t)

    def plane_both(source, ff):
        return remote(
            towers.at[source, pl.ds(ff * dim_count, dim_count)],
            plane_pair.at[source], plane_pair_recv.at[source], field=other)

    def cand_copy(t, source):
        return remote(cands.at[source], cand_send.at[t], cand_recv.at[source], batch=t)

    def loss_copy(m, ff, level):
        ref = losses.at[level, pl.ds(ff * run, run)]
        return remote(
            ref, loss_send.at[m], loss_recv.at[ff, level], field=m // dim_count, dim=m % dim_count)

    def row_copy(c, level):
        fs, ds = place(f, d)
        return pltpu.make_async_remote_copy(
            sent.at[c, level],
            rows.at[fs, ds, pl.ds(pl.multiple_of(lax.rem(c, run) * sub, sub), sub)],
            row_send.at[c, level], row_recv.at[lax.rem(c, run), me],
            device_id={"field": c // run, "dim": low + level}, device_id_type=MESH)

    def own_rows(c, level):
        return (c // run == f) & (level_of == level)

    def advance(ph, c):
        whole = buffers[ph][c].reshape(fields * width, rc)
        matrix = flat[ph].reshape(columns, fields * width)
        product = jnp.dot(matrix, whole, preferred_element_type=jnp.float32) + bias[ph]
        fs, ds = place(f, d)
        anchor = x0[c, fs, ds, :].astype(jnp.float32).reshape(columns, rc)
        current = buffers[ph][c, fs, ds, :].astype(jnp.float32).reshape(columns, rc)
        return (anchor * product + current).astype(jnp.bfloat16).reshape(fl, el, rc)

    own_copies = []
    for c in range(chunks):
        own_copies.append(pltpu.make_async_copy(
            feat.at[:, :, pl.ds(c * rc, rc)], piece(0, c, f, d), feat_sem.at[c]))
    small_copies = [
        pltpu.make_async_copy(query_weight, queries.at[:, me], small_sem.at[0]),
        pltpu.make_async_copy(tower_bias, biases.at[me], small_sem.at[1]),
        pltpu.make_async_copy(cand, cands.at[b], small_sem.at[2]),
    ]
    for copy in own_copies + small_copies:
        copy.start()
    each_field(lambda ff: tower_copy(ff).start())
    for level in range(CROSS):
        each_field(lambda ff: weight_copy(level, ff).start())

    barrier = pltpu.get_barrier_semaphore()
    for k in range(1, members):
        m = lax.rem(me + k, members)
        pl.semaphore_signal(
            barrier, inc=1, device_id={"field": m // dim_count, "dim": m % dim_count},
            device_id_type=MESH)
    for k in range(1, batch_count):
        pl.semaphore_signal(
            barrier, inc=1, device_id={"batch": lax.rem(b + k, batch_count)}, device_id_type=MESH)
    pl.semaphore_wait(barrier, members + batch_count - 2)
    for copy in own_copies:
        copy.wait()
    issue_own(0, 0)
    if chunks > 1:
        issue_own(0, 1)
    each_field(lambda ff: tower_copy(ff).wait())
    for copy in small_copies:
        copy.wait()
    chain_own()

    @pl.when(active)
    def _():
        for k in range(1, batch_count):
            cand_copy(lax.rem(b + k, batch_count), b).start()

    for level in range(CROSS):
        each_field(lambda ff: weight_copy(level, ff).wait())

    def first(c, carry):
        @pl.when(c + 2 < chunks)
        def _():
            issue_own(0, c + 2)

        forwards(0, c)
        fs, ds = place(f, d)
        x1[c, fs, ds, :] = advance(0, c)
        issue_own(1, c)

        for s in range(1, min(chunks, dim_count)):
            @pl.when(c == s)
            def _():
                chain_step(s)

        return carry

    lax.fori_loop(0, chunks, first, 0)
    for s in range(min(chunks, dim_count), dim_count):
        chain_step(s)

    @pl.when(active)
    def _():
        for k in range(3):
            both(k, f).start()
        if split > 1:
            for k in range(1, split):
                plane(lax.rem(b + k, split), b).start()

    def second(c, carry):
        forwards(1, c)
        new = advance(1, c)
        out[:, :, pl.ds(pl.multiple_of(c * rc, 128), rc)] = new
        for level in range(held):
            block = new[:, :, level * sub:(level + 1) * sub]

            @pl.when(own_rows(c, level))
            def _():
                fs, ds = place(f, d)
                rows[fs, ds, pl.ds(pl.multiple_of(lax.rem(c, run) * sub, sub), sub)] = block

            @pl.when(jnp.logical_not(own_rows(c, level)))
            def _():
                sent[c, level] = block
                row_copy(c, level).start()

        return carry

    lax.fori_loop(0, chunks, second, 0)

    def tower_block(s, query):
        matrix = towers[s].reshape(members * part, fields * width)
        pre = jnp.dot(
            matrix, rows[...].reshape(fields * width, share), preferred_element_type=jnp.float32)
        pre = pre + columns_bias[s].reshape(members * part, share)
        hidden = jnp.maximum(pre, 0.0).astype(jnp.bfloat16)
        return query + lax.dot_general(
            hidden, queries[s].reshape(members * part, width), (((0,), (0,)), ((), ())),
            preferred_element_type=jnp.float32)

    @pl.when(active)
    def _():
        if split > 1:
            for k in range(1, split):
                source = lax.rem(b + k, split)
                plane(source, source).wait_recv()
                plane_both(source, f).start()
        for k in range(3):
            both(k, other).wait_recv()
        for k in range(1, batch_count):
            source = lax.rem(b + k, batch_count)
            cand_copy(source, source).wait_recv()
        for m in range(members):
            block = jnp.broadcast_to(biases[m], (share, units)).T
            columns_bias[:, m] = block.reshape(split, part, share)
        if split > 1:
            for k in range(1, split):
                plane_both(lax.rem(b + k, split), other).wait_recv()
        for j in range(run):
            for k in range(1, members):
                m = lax.rem(me + k, members)
                fs, ds = place(m // dim_count, m % dim_count)
                remote(rows.at[fs, ds, pl.ds(j * sub, sub)], row_send.at[0, 0], row_recv.at[j, m],
                       field=m // dim_count, dim=m % dim_count).wait_recv()

        query = lax.fori_loop(0, split, tower_block, jnp.zeros((share, width), jnp.float32))
        all_cands = cands[...].reshape(-1, width)
        for j in range(run):
            c = f * run + j
            start = pl.multiple_of(c * rc + level_of * sub, sub)
            query_vec = (
                query[j * sub:(j + 1) * sub] + user[pl.ds(start, sub), :].astype(jnp.float32)
            ).astype(jnp.bfloat16)
            logits = lax.dot_general(
                all_cands, query_vec, (((1,), (1,)), ((), ())), preferred_element_type=jnp.float32
            ) * (1.0 / math.sqrt(width))
            labels = lax.broadcasted_iota(jnp.int32, logits.shape, 0)
            target = positive[c * held + level_of]
            picked = jnp.sum(jnp.where(labels == target, logits, 0.0), axis=0, keepdims=True)
            best = jnp.max(logits, axis=0, keepdims=True)
            total = jnp.sum(jnp.exp(logits - best), axis=0, keepdims=True)
            losses[level_of, c] = best + jnp.log(total) - picked
        for k in range(1, members):
            loss_copy(lax.rem(me + k, members), f, level_of).start()

    def drain(c, carry):
        for ph in range(CROSS):
            for o in range(dim_count):
                @pl.when((o <= d) & (d < dim_count - 1))
                def _():
                    right(ph, c, o).wait_send()

                @pl.when((o >= d) & (d > 0))
                def _():
                    left(ph, c, o).wait_send()

                pair(ph, c, o, f).wait_send()
        return carry

    lax.fori_loop(0, chunks, drain, 0)
    for k in range(3):
        for o in range(dim_count):
            @pl.when((o <= d) & (d < high))
            def _():
                chain_to(k, o, chain_right, to_right).wait_send()

            @pl.when((o >= d) & (d > low))
            def _():
                chain_to(k, o, chain_left, to_left).wait_send()

    @pl.when(active)
    def _():
        for k in range(3):
            both(k, f).wait_send()
        if split > 1:
            for k in range(1, split):
                t = lax.rem(b + k, split)
                plane(t, b).wait_send()
                plane_both(t, f).wait_send()
        for k in range(1, batch_count):
            cand_copy(lax.rem(b + k, batch_count), b).wait_send()
        for k in range(1, members):
            loss_copy(lax.rem(me + k, members), f, level_of).wait_send()

    for c in range(chunks):
        for level in range(held):
            @pl.when(jnp.logical_not(own_rows(c, level)))
            def _():
                row_copy(c, level).wait_send()

    for ff in range(field_count):
        for level in range(held):
            @pl.when(jnp.logical_not((f == ff) & (level_of == level)))
            def _():
                loss_copy(ff * dim_count + low + level, ff, level).wait_recv()

    for c in range(chunks):
        for level in range(held):
            loss_out[c * held + level] = losses[level, c]


def line_pieces(count, parts):
    base, extra = divmod(count, parts)
    bounds, start = [], 0
    for k in range(parts):
        size = base + (k < extra)
        bounds.append((start, size))
        start += size
    return bounds


def line_fits(counts, features, tower_weight, candidates):
    batch_count, field_count, dim_count = counts
    fl, el, row_count = features.shape
    units, fields, width = tower_weight.shape
    relayed = line_pieces(fl, PIECES)[RELAYED][0]
    return (
        (fl + relayed) % 2 == 0 and (2 * fl + relayed) % 3 == 0 and
        dim_count == 4 and batch_count == 4 and field_count == 2
        and fields % 2 == 0 and fl >= PIECES and el % 32 == 0 and 4 * el == width and width == 128
        and row_count % (CHUNKS * field_count * 128) == 0 and units % (16 * batch_count) == 0)


PIECES = 4
RELAYED = 2
CHUNKS = 4
FAR_TOWER = CROSS * PIECES
END_TOWER = FAR_TOWER + 1
CANDS = END_TOWER + 1


def line_kernel(
    counts,
    feat, weight, bias, tower, tower_bias, query_weight, user, cand, positive,
    out, loss_out,
    x0, x1, y, x2, flat, tw, tw_near, tw_far, tw_pass, tw_raw, q_raw, pre_out, pre_in, pre_own,
    bias_raw, bias_cols, unit_raw, unit_cols, cands, users, targets, losses,
    feat_sem, weight_sem, small_sem,
    end_send, end_recv, cross_send, cross_recv, pair_send, pair_recv, one_send, one_recv,
    piece_send, piece_recv, direct_load, direct_send, direct_recv, plane_send, plane_recv, rest_recv,
    tower_send, tower_recv, near_recv, both_send, both_recv,
    bias_send, bias_recv, unit_send, unit_recv, near_unit,
    two_send, two_recv, out_sem, give_send, give_recv, part_send, part_recv, loss_send, loss_recv,
):
    batch_count, field_count, dim_count = counts
    b = lax.axis_index("batch")
    f = lax.axis_index("field")
    d = lax.axis_index("dim")
    members = field_count * dim_count
    me = f * dim_count + d
    chunks, fields, width, rc = x0.shape
    fl, el, _ = feat.shape
    wide = 2 * el
    half_k = fields // 2 * width
    quarter_units = tw_far.shape[0]
    units = tw.shape[1]
    side_k = fields * wide
    lanes = rc // field_count
    rows_in_part = el // 2
    side = d // 2
    mid = 1 + side
    far = 2 - side
    end = 3 * side
    far_end = 3 - end
    is_mid = d == mid
    is_end = d == end
    owner = is_mid & (f == 1)
    giver = is_mid & (f == 0)
    part_of = jnp.where(f == 1, side, 1 - side)
    other = field_count - 1 - f
    x_next = b + 1 - 2 * lax.rem(b, 2)
    y_next = lax.rem(b + 2, 4)
    diagonal = 3 - b
    fs = pl.ds(f * fl, fl)
    ss = pl.ds(pl.multiple_of(side * wide, wide), wide)

    def remote(ref, send, recv, to=None, **where):
        return pltpu.make_async_remote_copy(
            ref, ref if to is None else to, send, recv, device_id=where, device_id_type=MESH)

    def sent(ref, sem):
        remote(ref, sem, sem, field=other).wait_send()

    def landed(ref, sem):
        remote(ref, sem, sem, field=other).wait_recv()

    def entries(o):
        return pl.ds(pl.multiple_of(o * el, el), el)

    def within(o):
        return pl.ds(pl.multiple_of(lax.rem(o, 2) * el, el), el)

    def block(c, ff, o):
        return x0.at[c, pl.ds(ff * fl, fl), entries(o), :]

    def from_end(c, target):
        return remote(block(c, f, end), end_send, end_recv.at[c], dim=target)

    def cross(k, c, o):
        return remote(block(c, f, o), cross_send.at[k], cross_recv.at[k, c], dim=far)

    def cross_one(c, s):
        ref = x1.at[c, fs, pl.ds(pl.multiple_of(s * wide, wide), wide), :]
        return remote(ref, cross_send.at[2], cross_recv.at[2, c], dim=far)

    def pair(c, o):
        return remote(block(c, f, o), pair_send, pair_recv.at[c], field=other)

    def pair_one(c, s):
        ref = x1.at[c, fs, pl.ds(pl.multiple_of(s * wide, wide), wide), :]
        return remote(ref, one_send, one_recv.at[c], field=other)

    def weight_piece(level, p, source):
        start, size = line_pieces(fl, PIECES)[p]
        return weight_part(level, start, size, source)

    def weight_part(level, start, size, source):
        row = pl.multiple_of(lax.rem(end, 2) * el + lax.rem(source, 2) * rows_in_part, rows_in_part)
        lane = pl.multiple_of(source // 2 * half_k, half_k)
        return flat.at[level, pl.ds(start, size), pl.ds(row, rows_in_part), pl.ds(lane, half_k)]

    def piece(level, p, target):
        ref = weight_piece(level, p, b)
        return remote(ref, piece_send.at[level], piece_recv.at[level, p], dim=target)

    def direct(p, target):
        ref = weight_piece(1, p, diagonal)
        return remote(ref, direct_send, direct_recv, dim=target)

    def direct_part():
        start = line_pieces(fl, PIECES)[RELAYED][0]
        return weight_part(1, start, fl - start, diagonal)

    def tower_rows(member, source):
        return tw.at[member, pl.ds(pl.multiple_of(source * quarter_units, quarter_units), quarter_units), :]

    def item(i, source):
        if i < CROSS * PIECES:
            return weight_piece(i // PIECES, i % PIECES, source)
        if i == CANDS:
            return cands.at[source]
        return tower_rows(f * dim_count + (far if i == FAR_TOWER else far_end), source)

    def relay(i):
        return (x_next, y_next) if i % 2 == 0 else (y_next, x_next)

    def group_of(i):
        return i // PIECES if i < FAR_TOWER else CROSS + i - FAR_TOWER

    def plane(i, source, target, arrival):
        return remote(item(i, source), plane_send.at[group_of(i)], arrival, batch=target)

    def plane_out(i):
        first, second = relay(i)
        plane(i, b, first, plane_recv.at[i]).start()
        plane(i, b, second, rest_recv.at[group_of(i)]).start()

    def plane_forward(i):
        source, target = relay(i)
        plane(i, source, target, plane_recv.at[i]).wait_recv()
        plane(i, source, target, rest_recv.at[group_of(i)]).start()

    def plane_keep(i):
        source, target = relay(i)
        plane(i, source, target, plane_recv.at[i]).wait_recv()

    def plane_rest(group):
        landed(plane_bytes(group, 2), rest_recv.at[group])

    def plane_bytes(group, copies):
        if group == 1:
            total = (copies - 1) * fl + line_pieces(fl, PIECES)[RELAYED][0]
            return flat.at[1, pl.ds(0, total // copies), pl.ds(0, copies * rows_in_part), pl.ds(0, half_k)]
        if group < CROSS:
            return flat.at[group, :, pl.ds(0, copies * rows_in_part), pl.ds(0, half_k)]
        if group == CROSS + 2:
            return cands.at[pl.ds(0, copies)]
        return tw.at[pl.ds(0, copies), pl.ds(0, quarter_units), :]

    def near_tower(target):
        return remote(
            tw_near, tower_send.at[0], near_recv, to=tw.at[f * dim_count + end], dim=target)

    def far_tower(source, target):
        return remote(
            tw_far, tower_send.at[1], tower_recv.at[source],
            to=tower_rows(f * dim_count + source, b), dim=target)

    def pass_in(target):
        return remote(tw_far, tower_send.at[1], tower_recv.at[mid], to=tw_pass, dim=target)

    def pass_on():
        return remote(
            tw_pass, tower_send.at[0], tower_recv.at[end],
            to=tower_rows(f * dim_count + end, b), dim=far)

    def both(z, ff):
        return remote(tw.at[ff * dim_count + z], both_send, both_recv, field=other)

    def bias_copy(target):
        return remote(bias_raw.at[lax.rem(end, 2)], bias_send, bias_recv, dim=target)

    def unit_in(target):
        return remote(unit_raw.at[f * dim_count + end], unit_send, near_unit, dim=target)

    def unit_out(ff, z):
        rows = unit_raw.at[pl.ds(f * dim_count + 2 * side, 2)]
        return remote(rows, unit_send, unit_recv, field=ff, dim=z)

    def two(c, ff):
        lane = pl.multiple_of((1 - part_of) * lanes, lanes)
        return remote(
            y.at[c, :, :, pl.ds(lane, lanes)], two_send, two_recv.at[c],
            to=x2.at[c, pl.ds(ff * fl, fl)], field=other)

    def rows_of(c):
        return pl.ds(pl.multiple_of(c * rc, rc), rc)

    def keep(c):
        return pltpu.make_async_copy(y.at[c, :, within(mid), :], out.at[:, :, rows_of(c)], out_sem)

    def give(c):
        return remote(
            y.at[c, :, within(end), :], give_send, give_recv,
            to=out.at[:, :, rows_of(c)], dim=end)

    def part(c):
        return remote(
            pre_out.at[c], part_send, part_recv.at[c], to=pre_in.at[c], field=other, dim=far)

    def loss_copy(k, c):
        m = lax.rem(me + k, members)
        return remote(
            losses.at[c], loss_send.at[k], loss_recv, to=loss_out.at[c * field_count + part_of],
            field=m // dim_count, dim=lax.rem(m, dim_count))

    def keep_loss(c):
        return pltpu.make_async_copy(losses.at[c], loss_out.at[c * field_count + part_of], loss_send.at[0])

    def own_weight(level, ff):
        return pltpu.make_async_copy(
            weight.at[level, :, ff],
            flat.at[level, :, within(mid), pl.ds(pl.multiple_of(ff * width, width), width)],
            weight_sem.at[level])

    def end_weight(level, k):
        row = pl.multiple_of(lax.rem(b, 2) * rows_in_part, rows_in_part)
        ff = b // 2 * (fields // 2) + k
        to = pl.multiple_of(lax.rem(end, 2) * el + row, rows_in_part)
        return pltpu.make_async_copy(
            weight.at[level, :, ff, pl.ds(row, rows_in_part), :],
            flat.at[level, :, pl.ds(to, rows_in_part), pl.ds(pl.multiple_of(ff * width, width), width)],
            weight_sem.at[level])

    def direct_weight(k):
        start = line_pieces(fl, PIECES)[RELAYED][0]
        row = pl.multiple_of(lax.rem(diagonal, 2) * rows_in_part, rows_in_part)
        ff = diagonal // 2 * (fields // 2) + k
        to = pl.multiple_of(lax.rem(end, 2) * el + row, rows_in_part)
        return pltpu.make_async_copy(
            weight.at[1, pl.ds(start, fl - start), ff, pl.ds(row, rows_in_part), :],
            flat.at[1, pl.ds(start, fl - start), pl.ds(to, rows_in_part),
                    pl.ds(pl.multiple_of(ff * width, width), width)],
            direct_load)

    def each(count, act):
        def step(k, carry):
            act(k)
            return carry

        lax.fori_loop(0, count, step, 0)

    own_features = [
        pltpu.make_async_copy(feat.at[:, :, pl.ds(c * rc, rc)], block(c, f, d), feat_sem.at[c])
        for c in range(chunks)]
    quarter = pl.ds(pl.multiple_of(b * quarter_units, quarter_units), quarter_units)
    small = [
        pltpu.make_async_copy(bias, bias_raw.at[lax.rem(d, 2)], small_sem.at[0]),
        pltpu.make_async_copy(tower_bias, unit_raw.at[me], small_sem.at[1]),
        pltpu.make_async_copy(cand, cands.at[b], small_sem.at[2]),
        pltpu.make_async_copy(tower, tw_raw, small_sem.at[3]),
        pltpu.make_async_copy(query_weight, q_raw, small_sem.at[4]),
        pltpu.make_async_copy(user, users, small_sem.at[5]),
        pltpu.make_async_copy(positive, targets, small_sem.at[6]),
    ]
    barrier = pltpu.get_barrier_semaphore()

    def greet(**where):
        pl.semaphore_signal(barrier, inc=1, device_id=where, device_id_type=MESH)

    @pl.when(is_end)
    def _():
        for ff in range(field_count):
            for z in (1, 2):
                greet(field=ff, dim=z)

    @pl.when(is_mid)
    def _():
        greet(dim=end)
        greet(dim=far)
        greet(batch=x_next)
        greet(batch=y_next)
        greet(field=other, dim=far)
        greet(field=other)

    for copy in own_features:
        copy.start()

    @pl.when(is_end)
    def _():
        each(fields // 2, lambda k: end_weight(0, k).start())

    for copy in small:
        copy.start()

    @pl.when(is_mid)
    def _():
        each(fields, lambda k: own_weight(0, k).start())
        each(fields, lambda k: own_weight(1, k).start())

    @pl.when(is_end)
    def _():
        each(fields // 2, lambda k: end_weight(1, k).start())
        each(fields // 2, lambda k: direct_weight(k).start())

    pl.semaphore_wait(barrier, jnp.where(is_mid, 2 * field_count + 5, 1))

    def loaded_own(level):
        ref = flat.at[level, :, within(mid), :]
        pltpu.make_async_copy(ref, ref, weight_sem.at[level]).wait()

    def loaded_end(level):
        ref = weight_part(level, 0, fl, b)
        pltpu.make_async_copy(ref, ref, weight_sem.at[level]).wait()

    def pack_tower():
        def halves(rows, j):
            first = tw_raw[2 * j, rows, :]
            second = tw_raw[2 * j + 1, rows, :]
            low = jnp.concatenate([first[:, :wide], second[:, :wide]], axis=1)
            high = jnp.concatenate([first[:, wide:], second[:, wide:]], axis=1)
            return low, high

        for j in range(fields // 2):
            low, high = halves(slice(None), j)
            tw_near[:, j * width:(j + 1) * width] = jnp.where(side == 0, low, high)
            low, high = halves(quarter, j)
            tw_far[:, j * width:(j + 1) * width] = jnp.where(side == 0, high, low)
        tw_near[:, side_k:] = q_raw[...]
        tw_far[:, side_k:] = q_raw[quarter, :]

    @pl.when(is_end)
    def _():
        loaded_end(0)
        for p in range(PIECES - 1):
            piece(0, p, mid).start()
        for copy in own_features:
            copy.wait()
        from_end(0, mid).start()
        piece(0, PIECES - 1, mid).start()
        from_end(1, mid).start()
        for copy in small:
            copy.wait()
        bias_copy(mid).start()
        unit_in(mid).start()
        for c in range(2, chunks):
            from_end(c, mid).start()
        pack_tower()
        pass_in(mid).start()
        loaded_end(1)
        for p in range(PIECES):
            piece(1, p, mid).start()
        pltpu.make_async_copy(direct_part(), direct_part(), direct_load).wait()
        for p in range(RELAYED, PIECES):
            direct(p, mid).start()
        near_tower(mid).start()

    def expect_piece(level, p):
        piece(level, p, end).wait_recv()
        plane_out(level * PIECES + p)

    def expect_end(c):
        from_end(c, end).wait_recv()
        cross(1, c, end).start()
        pair(c, end).start()

    def expect_far(k, c, o):
        cross(k, c, o).wait_recv()
        pair(c, o).start()

    def expect_tower(i, z):
        far_tower(z, end).wait_recv()
        plane_out(i)

    def half(source, level, c, ff):
        matrix = flat[level, :, :, pl.ds(pl.multiple_of(ff * half_k, half_k), half_k)]
        return jnp.dot(
            matrix.reshape(fl * wide, half_k), source[c, pl.ds(ff * fl, fl)].reshape(half_k, rc),
            preferred_element_type=jnp.float32)

    def advance(source, level, c, wait_pair):
        product = half(source, level, c, f)
        wait_pair()
        product = product + half(source, level, c, other)
        column = bias_cols[level]
        product = product + jnp.concatenate([column] * (rc // column.shape[1]), axis=1)
        anchor = x0[c, fs, ss, :].astype(jnp.float32).reshape(fl * wide, rc)
        current = source[c, fs, ss, :].astype(jnp.float32).reshape(fl * wide, rc)
        return (anchor * product + current).astype(jnp.bfloat16).reshape(fl, wide, rc)

    def build_bias():
        pick = (lax.broadcasted_iota(jnp.int32, (el, el), 0) == lax.broadcasted_iota(jnp.int32, (el, el), 1))
        for level in range(CROSS):
            for k in range(fl):
                for s in range(2):
                    line = bias_raw[s, k, level:level + 1, :]
                    column = jnp.sum(jnp.where(pick, line, 0.0), axis=1, keepdims=True)
                    start = (2 * k + s) * el
                    bias_cols[level, start:start + el, :] = jnp.broadcast_to(column, (el, width))

    def build_units():
        for m in range(members):
            unit_cols[m * units:(m + 1) * units, :] = jnp.broadcast_to(unit_raw[m], (lanes, units)).T

    def first(c, carry):
        @pl.when(c == 1)
        def _():
            pass_in(end).wait_recv()
            pass_on().start()

        @pl.when(c == 2)
        def _():
            expect_far(1, 2, far_end)
            plane_forward(FAR_TOWER)
            expect_piece(1, 0)

        @pl.when(c == 3)
        def _():
            expect_far(1, 3, far_end)
            expect_piece(1, 1)

        def wait_pair():
            landed(x0.at[c, fs], pair_recv.at[c])

        x1[c, fs, ss, :] = advance(x0, 0, c, wait_pair)
        cross_one(c, side).start()
        pair_one(c, side).start()
        return carry

    def tower_part(c):
        matrix = tw[:, :, :side_k].reshape(members * units, side_k)
        return jnp.dot(matrix, x2[c].reshape(side_k, lanes), preferred_element_type=jnp.float32)

    def expect_one(c):
        cross_one(c, 1 - side).wait_recv()
        pair_one(c, 1 - side).start()

    def layer_two(c):
        def wait_pair():
            landed(x1.at[c, fs], one_recv.at[c])

        y[c] = advance(x1, 1, c, wait_pair)
        two(c, f).start()
        give(c).start()
        keep(c).start()
        for k in range(2):
            @pl.when(part_of == k)
            def _():
                x2[c, fs] = y[c, :, :, k * lanes:(k + 1) * lanes]

    def layer_three(c):
        two(c, other).wait_recv()
        pre = tower_part(c)

        @pl.when(owner)
        def _():
            pre_own[c] = pre

        @pl.when(giver)
        def _():
            pre_out[c] = pre.astype(jnp.bfloat16)
            part(c).start()

    def second(c, carry):
        layer_two(c)

        @pl.when(c == 1)
        def _():
            near_tower(end).wait_recv()
            both(end, f).start()
            expect_one(2)
            landed(tw.at[pl.ds(0, dim_count)], both_recv)

        def tower_step(k, carry):
            layer_three(k)
            return carry

        last = c == chunks - 1
        lax.fori_loop(
            jnp.where(last, c, jnp.maximum(c - 1, 0)), jnp.where(c < chunks - 2, c, c + 1),
            tower_step, 0)

        @pl.when(c == 2)
        def _():
            expect_one(3)

        return carry

    def finish(c):
        part(c).wait_recv()
        pre = pre_own[c] + pre_in[c].astype(jnp.float32) + unit_cols[...]
        hidden = jnp.maximum(pre, 0.0).astype(jnp.bfloat16)
        query = lax.dot_general(
            hidden, tw[:, :, side_k:].reshape(members * units, width), (((0,), (0,)), ((), ())),
            preferred_element_type=jnp.float32)
        start = pl.multiple_of(c * rc + part_of * lanes, lanes)
        query_vec = (query + users[pl.ds(start, lanes), :].astype(jnp.float32)).astype(jnp.bfloat16)
        logits = lax.dot_general(
            cands[...].reshape(-1, width), query_vec, (((1,), (1,)), ((), ())),
            preferred_element_type=jnp.float32) * (1.0 / math.sqrt(width))
        labels = lax.broadcasted_iota(jnp.int32, logits.shape, 0)
        target = targets[c * field_count + part_of]
        picked = jnp.sum(jnp.where(labels == target, logits, 0.0), axis=0, keepdims=True)
        best = jnp.max(logits, axis=0, keepdims=True)
        total = jnp.sum(jnp.exp(logits - best), axis=0, keepdims=True)
        losses[c] = best + jnp.log(total) - picked
        for k in range(1, members):
            loss_copy(k, c).start()
        keep_loss(c).start()

    @pl.when(is_mid)
    def _():
        for c in range(chunks):
            own_features[c].wait()
            cross(0, c, mid).start()
            pair(c, mid).start()
        for copy in small:
            copy.wait()
        plane_out(CANDS)
        pack_tower()
        far_tower(d, far).start()
        tw[me] = tw_near[...]
        both(mid, f).start()
        expect_piece(0, 0)
        expect_far(0, 0, far)
        expect_piece(0, 1)
        expect_far(0, 1, far)
        plane_forward(CANDS)
        expect_piece(0, 2)
        expect_far(0, 2, far)
        plane_forward(0)
        plane_forward(1)
        expect_far(0, 3, far)
        expect_end(0)
        expect_piece(0, 3)
        plane_forward(2)
        expect_end(1)
        plane_forward(3)
        expect_far(1, 0, far_end)
        expect_tower(FAR_TOWER, far)
        bias_copy(end).wait_recv()
        build_bias()
        unit_in(end).wait_recv()
        unit_out(other, d).start()
        unit_out(f, far).start()
        unit_out(other, far).start()
        for level in range(CROSS):
            loaded_own(level)
        expect_end(2)
        plane_rest(0)
        expect_far(1, 1, far_end)
        expect_end(3)
        lax.fori_loop(0, chunks, first, 0)
        plane_rest(4)
        plane_rest(2)
        both(far, f).start()
        expect_piece(1, 2)
        expect_piece(1, 3)
        expect_tower(END_TOWER, far_end)
        for p in range(RELAYED):
            plane_forward(PIECES + p)
        expect_one(0)
        plane_forward(END_TOWER)
        for p in range(RELAYED, PIECES):
            plane_keep(PIECES + p)
        expect_one(1)
        landed(unit_raw.at[pl.ds(0, 6)], unit_recv)
        build_units()
        plane_rest(3)
        both(far_end, f).start()
        landed(direct_part(), direct_recv)
        plane_rest(1)
        lax.fori_loop(0, chunks, second, 0)

        @pl.when(owner)
        def _():
            for c in range(chunks):
                finish(c)

    @pl.when(owner)
    def _():
        landed(losses, loss_recv)

    @pl.when(jnp.logical_not(owner))
    def _():
        landed(loss_out, loss_recv)

    @pl.when(is_end)
    def _():
        for level in range(CROSS):
            sent(weight_part(level, 0, fl, b), piece_send.at[level])
        sent(direct_part(), direct_send)
        sent(x0.at[:, fs, entries(d), :], end_send)
        bias_copy(mid).wait_send()
        near_tower(mid).wait_send()
        pass_in(mid).wait_send()
        unit_in(mid).wait_send()
        landed(out, give_recv)

    @pl.when(is_mid)
    def _():
        far_tower(d, far).wait_send()
        pass_on().wait_send()
        sent(tw.at[pl.ds(0, dim_count)], both_send)
        sent(unit_raw.at[pl.ds(0, 6)], unit_send)
        sent(x0.at[:, fs, entries(mid), :], cross_send.at[0])
        sent(x0.at[:, fs, entries(end), :], cross_send.at[1])
        sent(x1.at[:, fs, ss, :], cross_send.at[2])
        sent(x0.at[:, fs], pair_send)
        sent(x1.at[:, fs], one_send)
        sent(y.at[:, :, :, pl.ds(0, lanes)], two_send)
        sent(out, give_send)
        pltpu.make_async_copy(out, out, out_sem).wait()
        for group in range(CROSS + 3):
            sent(plane_bytes(group, 3), plane_send.at[group])

    @pl.when(giver)
    def _():
        sent(pre_out, part_send)

    @pl.when(owner)
    def _():
        for k in range(1, members):
            sent(losses, loss_send.at[k])
        pltpu.make_async_copy(losses, losses, loss_send.at[0]).wait()


def line_body(
    counts, features, cross_weight, cross_bias, tower_weight, tower_bias, query_weight,
    user_vec, candidates, positive,
):
    batch_count, field_count, dim_count = counts
    members = field_count * dim_count
    fl, el, row_count = features.shape
    units, fields, width = tower_weight.shape
    rc = row_count // CHUNKS
    lanes = rc // field_count
    wide = 2 * el
    quarter = units // batch_count
    packed = fields * wide + width
    items = CANDS + 1
    dma = pltpu.SemaphoreType.DMA
    vmem = pltpu.VMEM
    bf16 = jnp.bfloat16
    f32 = jnp.float32
    far = pl.BlockSpec(memory_space=pl.ANY)
    crossed, losses = pl.pallas_call(
        functools.partial(line_kernel, counts),
        out_shape=(
            jax.ShapeDtypeStruct(features.shape, bf16),
            jax.ShapeDtypeStruct((CHUNKS * field_count, 1, lanes), f32),
        ),
        in_specs=[far] * 9,
        out_specs=(far, far),
        scratch_shapes=[
            vmem((CHUNKS, fields, width, rc), bf16),
            vmem((CHUNKS, fields, width, rc), bf16),
            vmem((CHUNKS, fl, wide, rc), bf16),
            vmem((CHUNKS, fields, wide, lanes), bf16),
            vmem((CROSS, fl, wide, fields * width), bf16),
            vmem((members, units, packed), bf16),
            vmem((units, packed), bf16),
            vmem((quarter, packed), bf16),
            vmem((quarter, packed), bf16),
            vmem((fields, units, width), bf16),
            vmem((units, width), bf16),
            vmem((CHUNKS, members * units, lanes), bf16),
            vmem((CHUNKS, members * units, lanes), bf16),
            vmem((CHUNKS, members * units, lanes), f32),
            vmem((2, fl, CROSS, el), f32),
            vmem((CROSS, fl * wide, width), f32),
            vmem((members, 1, units), f32),
            vmem((members * units, lanes), f32),
            vmem((batch_count,) + candidates.shape, bf16),
            vmem(user_vec.shape, bf16),
            vmem((CHUNKS * field_count, 1, lanes), jnp.int32),
            vmem((CHUNKS, 1, lanes), f32),
            dma((CHUNKS,)), dma((CROSS,)), dma((7,)),
            dma, dma((CHUNKS,)), dma((3,)), dma((3, CHUNKS)),
            dma, dma((CHUNKS,)), dma, dma((CHUNKS,)),
            dma((CROSS,)), dma((CROSS, PIECES)), dma, dma, dma, dma((CROSS + 3,)), dma((items,)), dma((CROSS + 3,)),
            dma((2,)), dma((dim_count,)), dma, dma, dma,
            dma, dma, dma, dma, dma,
            dma, dma((CHUNKS,)), dma, dma, dma, dma, dma((CHUNKS,)), dma((members,)), dma,
        ],
        compiler_params=pltpu.CompilerParams(
            collective_id=0, has_side_effects=True, vmem_limit_bytes=48 * 2**20),
        name="line_forward",
    )(*(pltpu.with_memory_space_constraint(value, pltpu.HBM) for value in (
        features,
        cross_weight.transpose(0, 1, 3, 2, 4),
        cross_bias.transpose(1, 0, 2),
        tower_weight.transpose(1, 0, 2),
        tower_bias.reshape(1, units),
        query_weight,
        user_vec,
        candidates,
        positive.reshape(CHUNKS * field_count, 1, lanes),
    )))
    return (crossed, losses.reshape(row_count))


def body(
    features, cross_weight, cross_bias, tower_weight, tower_bias, query_weight,
    user_vec, candidates, positive,
):
    counts = tuple(lax.axis_size(name) for name in ("batch", "field", "dim"))
    if line_fits(counts, features, tower_weight, candidates):
        return line_body(
            counts, features, cross_weight, cross_bias, tower_weight, tower_bias, query_weight,
            user_vec, candidates, positive)
    batch_count, field_count, dim_count = counts
    members = field_count * dim_count
    fl, el, row_count = features.shape
    columns = fl * el
    units, fields, width = tower_weight.shape
    low, held = tower_levels(dim_count)
    chunks = chunk_count(row_count, field_count, held)
    split = batch_count if units % (batch_count * 16) == 0 else 1
    part = units // split
    rc = row_count // chunks
    sub = rc // held
    run = chunks // field_count
    share = run * sub
    steps = (CROSS, chunks, dim_count)
    small = (3, dim_count)
    dma = pltpu.SemaphoreType.DMA
    vmem = pltpu.VMEM
    bf16 = jnp.bfloat16
    far = pl.BlockSpec(memory_space=pl.ANY)
    near = pl.BlockSpec(memory_space=pltpu.VMEM)
    crossed, losses = pl.pallas_call(
        functools.partial(rank_kernel, counts, (chunks, split)),
        out_shape=(
            jax.ShapeDtypeStruct(features.shape, bf16),
            jax.ShapeDtypeStruct((chunks * held, 1, sub), jnp.float32),
        ),
        in_specs=[far, far, near, far, far, far, near, far, near],
        out_specs=(near, near),
        scratch_shapes=[
            vmem((chunks, fields, width, rc), bf16),
            vmem((chunks, fields, width, rc), bf16),
            vmem((CROSS, fl, el, fields * width), bf16),
            vmem((chunks, held, fl, el, sub), bf16),
            vmem((fields, width, share), bf16),
            vmem((split, members, part, fields * width), bf16),
            vmem((members, 1, units), jnp.float32),
            vmem((split, members, part, share), jnp.float32),
            vmem((split, members, part, width), bf16),
            vmem((batch_count,) + candidates.shape, bf16),
            vmem((held, chunks, 1, sub), jnp.float32),
            dma((chunks,)), dma((CROSS, fields)), dma((fields,)), dma((3,)),
            dma(steps), dma(steps), dma(steps), dma(steps), dma(steps),
            dma((chunks, held)), dma((run, members)), dma(small), dma(small), dma(small),
            dma((3,)), dma((3,)),
            dma((split,)), dma((split,)), dma((split,)), dma((split,)),
            dma((batch_count,)), dma((batch_count,)), dma((members,)), dma((field_count, held)),
        ],
        compiler_params=pltpu.CompilerParams(
            collective_id=0, has_side_effects=True, vmem_limit_bytes=56 * 2**20),
        name="rank_forward",
    )(
        features,
        cross_weight.transpose(0, 1, 3, 2, 4),
        cross_bias.reshape(CROSS, columns, 1),
        tower_weight.transpose(1, 0, 2),
        tower_bias.reshape(1, units),
        query_weight.reshape(split, part, width),
        user_vec,
        candidates,
        positive.reshape(chunks * held, 1, sub),
    )
    return (crossed, losses.reshape(row_count))


def solution(mesh):
    placed = (
        P("field", "dim", "batch"),
        P(None, "field", "dim", None, None),
        P(None, "field", "dim"),
        P(("field", "dim"), None, None),
        P(("field", "dim")),
        P(("field", "dim"), None),
        P("batch", None),
        P("batch", None),
        P("batch"),
    )
    return jax.shard_map(
        body,
        mesh=mesh,
        in_specs=placed,
        out_specs=(P("field", "dim", "batch"), P("batch")),
        check_vma=False,
    )
```

```python
import functools
import math

import jax
import jax.numpy as jnp
from jax import lax
from jax.experimental import pallas as pl
from jax.experimental.pallas import tpu as pltpu
from jax.sharding import PartitionSpec as P

CROSS = 2
MESH = pl.DeviceIdType.MESH


def tower_levels(dim_count):
    held = min(2, dim_count)
    return (dim_count - held) // 2, held


def chunk_count(row_count, field_count, held):
    chunks = 2
    while chunks > field_count and row_count % (chunks * held * 128):
        chunks //= 2
    return chunks


def rank_kernel(
    counts, splits,
    feat, weight, bias, tower, tower_bias, query_weight, user, cand, positive,
    out, loss_out,
    x0, x1, flat, sent, rows, towers, biases, columns_bias, queries, cands, losses,
    feat_sem, weight_sem, tower_sem, small_sem,
    right_sem, left_sem, pair_sem, recv_sem, pair_recv,
    row_send, row_recv, chain_right, chain_left, chain_recv, both_send, both_recv,
    plane_send, plane_recv, plane_pair, plane_pair_recv,
    cand_send, cand_recv, loss_send, loss_recv,
):
    batch_count, field_count, dim_count = counts
    chunks, split = splits
    b = lax.axis_index("batch")
    f = lax.axis_index("field")
    d = lax.axis_index("dim")
    me = f * dim_count + d
    members = field_count * dim_count
    fl, el, row_count = feat.shape
    columns = fl * el
    fields, width, rc = x0.shape[1:]
    low, held = tower_levels(dim_count)
    high = low + held - 1
    level_of = d - low
    active = (d >= low) & (d <= high)
    sub = rc // held
    run = chunks // field_count
    share = run * sub
    part = towers.shape[2]
    units = split * part
    buffers = (x0, x1)
    other = field_count - 1 - f
    mine = b if split > 1 else 0
    to_right = jnp.minimum(d + 1, dim_count - 1)
    to_left = jnp.maximum(d - 1, 0)

    def remote(ref, send, recv, **where):
        return pltpu.make_async_remote_copy(
            ref, ref, send, recv, device_id=where, device_id_type=MESH)

    def place(ff, o):
        return pl.ds(ff * fl, fl), pl.ds(pl.multiple_of(o * el, el), el)

    def piece(ph, c, ff, o):
        fs, ds = place(ff, o)
        return buffers[ph].at[c, fs, ds, :]

    def right(ph, c, o):
        return remote(piece(ph, c, f, o), right_sem.at[ph, c, o], recv_sem.at[ph, c, o], dim=to_right)

    def left(ph, c, o):
        return remote(piece(ph, c, f, o), left_sem.at[ph, c, o], recv_sem.at[ph, c, o], dim=to_left)

    def pair(ph, c, o, ff):
        return remote(
            piece(ph, c, ff, o), pair_sem.at[ph, c, o], pair_recv.at[ph, c, o], field=other)

    def issue_own(ph, c):
        @pl.when(d < dim_count - 1)
        def _():
            right(ph, c, d).start()

        @pl.when(d > 0)
        def _():
            left(ph, c, d).start()

        pair(ph, c, d, f).start()

    def forwards(ph, c):
        for s in range(1, dim_count):
            @pl.when(d - s >= 0)
            def _():
                right(ph, c, d - s).wait_recv()

                @pl.when(d < dim_count - 1)
                def _():
                    right(ph, c, d - s).start()

                pair(ph, c, d - s, f).start()

            @pl.when(d + s < dim_count)
            def _():
                left(ph, c, d + s).wait_recv()

                @pl.when(d > 0)
                def _():
                    left(ph, c, d + s).start()

                pair(ph, c, d + s, f).start()
        for o in range(dim_count):
            pair(ph, c, o, other).wait_recv()

    def weight_copy(level, ff):
        return pltpu.make_async_copy(
            weight.at[level, :, ff],
            flat.at[level, :, :, pl.ds(pl.multiple_of(ff * width, width), width)],
            weight_sem.at[level, ff])

    def tower_copy(ff):
        return pltpu.make_async_copy(
            tower.at[ff, pl.ds(pl.multiple_of(mine * part, part), part), :],
            towers.at[mine, me, :, pl.ds(pl.multiple_of(ff * width, width), width)],
            tower_sem.at[ff])

    def each_field(act):
        def step(ff, carry):
            act(ff)
            return carry

        lax.fori_loop(0, fields, step, 0)

    small_refs = (
        lambda o: towers.at[mine, f * dim_count + o],
        lambda o: queries.at[:, f * dim_count + o],
        lambda o: biases.at[f * dim_count + o],
    )
    small_wide = (
        lambda ff: towers.at[mine, pl.ds(ff * dim_count, dim_count)],
        lambda ff: queries.at[:, pl.ds(ff * dim_count, dim_count)],
        lambda ff: biases.at[pl.ds(ff * dim_count, dim_count)],
    )

    def chain_to(k, o, sems, target):
        return remote(small_refs[k](o), sems.at[k, o], chain_recv.at[k, o], dim=target)

    def chain_own():
        for k in range(3):
            @pl.when(d < high)
            def _():
                chain_to(k, d, chain_right, to_right).start()

            @pl.when(d > low)
            def _():
                chain_to(k, d, chain_left, to_left).start()

    def chain_step(s):
        for k in range(3):
            @pl.when((d - s >= 0) & (d <= high))
            def _():
                chain_to(k, d - s, chain_right, to_right).wait_recv()

                @pl.when(d < high)
                def _():
                    chain_to(k, d - s, chain_right, to_right).start()

            @pl.when((d + s < dim_count) & (d >= low))
            def _():
                chain_to(k, d + s, chain_left, to_left).wait_recv()

                @pl.when(d > low)
                def _():
                    chain_to(k, d + s, chain_left, to_left).start()

    def both(k, ff):
        return remote(small_wide[k](ff), both_send.at[k], both_recv.at[k], field=other)

    def plane(t, source):
        return remote(
            towers.at[source, pl.ds(f * dim_count, dim_count)],
            plane_send.at[t], plane_recv.at[source], batch=t)

    def plane_both(source, ff):
        return remote(
            towers.at[source, pl.ds(ff * dim_count, dim_count)],
            plane_pair.at[source], plane_pair_recv.at[source], field=other)

    def cand_copy(t, source):
        return remote(cands.at[source], cand_send.at[t], cand_recv.at[source], batch=t)

    def loss_copy(m, ff, level):
        ref = losses.at[level, pl.ds(ff * run, run)]
        return remote(
            ref, loss_send.at[m], loss_recv.at[ff, level], field=m // dim_count, dim=m % dim_count)

    def row_copy(c, level):
        fs, ds = place(f, d)
        return pltpu.make_async_remote_copy(
            sent.at[c, level],
            rows.at[fs, ds, pl.ds(pl.multiple_of(lax.rem(c, run) * sub, sub), sub)],
            row_send.at[c, level], row_recv.at[lax.rem(c, run), me],
            device_id={"field": c // run, "dim": low + level}, device_id_type=MESH)

    def own_rows(c, level):
        return (c // run == f) & (level_of == level)

    def advance(ph, c):
        whole = buffers[ph][c].reshape(fields * width, rc)
        matrix = flat[ph].reshape(columns, fields * width)
        product = jnp.dot(matrix, whole, preferred_element_type=jnp.float32) + bias[ph]
        fs, ds = place(f, d)
        anchor = x0[c, fs, ds, :].astype(jnp.float32).reshape(columns, rc)
        current = buffers[ph][c, fs, ds, :].astype(jnp.float32).reshape(columns, rc)
        return (anchor * product + current).astype(jnp.bfloat16).reshape(fl, el, rc)

    own_copies = []
    for c in range(chunks):
        own_copies.append(pltpu.make_async_copy(
            feat.at[:, :, pl.ds(c * rc, rc)], piece(0, c, f, d), feat_sem.at[c]))
    small_copies = [
        pltpu.make_async_copy(query_weight, queries.at[:, me], small_sem.at[0]),
        pltpu.make_async_copy(tower_bias, biases.at[me], small_sem.at[1]),
        pltpu.make_async_copy(cand, cands.at[b], small_sem.at[2]),
    ]
    for copy in own_copies + small_copies:
        copy.start()
    each_field(lambda ff: tower_copy(ff).start())
    for level in range(CROSS):
        each_field(lambda ff: weight_copy(level, ff).start())

    barrier = pltpu.get_barrier_semaphore()
    for k in range(1, members):
        m = lax.rem(me + k, members)
        pl.semaphore_signal(
            barrier, inc=1, device_id={"field": m // dim_count, "dim": m % dim_count},
            device_id_type=MESH)
    for k in range(1, batch_count):
        pl.semaphore_signal(
            barrier, inc=1, device_id={"batch": lax.rem(b + k, batch_count)}, device_id_type=MESH)
    pl.semaphore_wait(barrier, members + batch_count - 2)
    for copy in own_copies:
        copy.wait()
    issue_own(0, 0)
    if chunks > 1:
        issue_own(0, 1)
    each_field(lambda ff: tower_copy(ff).wait())
    for copy in small_copies:
        copy.wait()
    chain_own()

    @pl.when(active)
    def _():
        for k in range(1, batch_count):
            cand_copy(lax.rem(b + k, batch_count), b).start()

    for level in range(CROSS):
        each_field(lambda ff: weight_copy(level, ff).wait())

    def first(c, carry):
        @pl.when(c + 2 < chunks)
        def _():
            issue_own(0, c + 2)

        forwards(0, c)
        fs, ds = place(f, d)
        x1[c, fs, ds, :] = advance(0, c)
        issue_own(1, c)

        for s in range(1, min(chunks, dim_count)):
            @pl.when(c == s)
            def _():
                chain_step(s)

        return carry

    lax.fori_loop(0, chunks, first, 0)
    for s in range(min(chunks, dim_count), dim_count):
        chain_step(s)

    @pl.when(active)
    def _():
        for k in range(3):
            both(k, f).start()
        if split > 1:
            for k in range(1, split):
                plane(lax.rem(b + k, split), b).start()

    def second(c, carry):
        forwards(1, c)
        new = advance(1, c)
        out[:, :, pl.ds(pl.multiple_of(c * rc, 128), rc)] = new
        for level in range(held):
            block = new[:, :, level * sub:(level + 1) * sub]

            @pl.when(own_rows(c, level))
            def _():
                fs, ds = place(f, d)
                rows[fs, ds, pl.ds(pl.multiple_of(lax.rem(c, run) * sub, sub), sub)] = block

            @pl.when(jnp.logical_not(own_rows(c, level)))
            def _():
                sent[c, level] = block
                row_copy(c, level).start()

        return carry

    lax.fori_loop(0, chunks, second, 0)

    def tower_block(s, query):
        matrix = towers[s].reshape(members * part, fields * width)
        pre = jnp.dot(
            matrix, rows[...].reshape(fields * width, share), preferred_element_type=jnp.float32)
        pre = pre + columns_bias[s].reshape(members * part, share)
        hidden = jnp.maximum(pre, 0.0).astype(jnp.bfloat16)
        return query + lax.dot_general(
            hidden, queries[s].reshape(members * part, width), (((0,), (0,)), ((), ())),
            preferred_element_type=jnp.float32)

    @pl.when(active)
    def _():
        if split > 1:
            for k in range(1, split):
                source = lax.rem(b + k, split)
                plane(source, source).wait_recv()
                plane_both(source, f).start()
        for k in range(3):
            both(k, other).wait_recv()
        for k in range(1, batch_count):
            source = lax.rem(b + k, batch_count)
            cand_copy(source, source).wait_recv()
        for m in range(members):
            block = jnp.broadcast_to(biases[m], (share, units)).T
            columns_bias[:, m] = block.reshape(split, part, share)
        if split > 1:
            for k in range(1, split):
                plane_both(lax.rem(b + k, split), other).wait_recv()
        for j in range(run):
            for k in range(1, members):
                m = lax.rem(me + k, members)
                fs, ds = place(m // dim_count, m % dim_count)
                remote(rows.at[fs, ds, pl.ds(j * sub, sub)], row_send.at[0, 0], row_recv.at[j, m],
                       field=m // dim_count, dim=m % dim_count).wait_recv()

        query = lax.fori_loop(0, split, tower_block, jnp.zeros((share, width), jnp.float32))
        all_cands = cands[...].reshape(-1, width)
        for j in range(run):
            c = f * run + j
            start = pl.multiple_of(c * rc + level_of * sub, sub)
            query_vec = (
                query[j * sub:(j + 1) * sub] + user[pl.ds(start, sub), :].astype(jnp.float32)
            ).astype(jnp.bfloat16)
            logits = lax.dot_general(
                all_cands, query_vec, (((1,), (1,)), ((), ())), preferred_element_type=jnp.float32
            ) * (1.0 / math.sqrt(width))
            labels = lax.broadcasted_iota(jnp.int32, logits.shape, 0)
            target = positive[c * held + level_of]
            picked = jnp.sum(jnp.where(labels == target, logits, 0.0), axis=0, keepdims=True)
            best = jnp.max(logits, axis=0, keepdims=True)
            total = jnp.sum(jnp.exp(logits - best), axis=0, keepdims=True)
            losses[level_of, c] = best + jnp.log(total) - picked
        for k in range(1, members):
            loss_copy(lax.rem(me + k, members), f, level_of).start()

    def drain(c, carry):
        for ph in range(CROSS):
            for o in range(dim_count):
                @pl.when((o <= d) & (d < dim_count - 1))
                def _():
                    right(ph, c, o).wait_send()

                @pl.when((o >= d) & (d > 0))
                def _():
                    left(ph, c, o).wait_send()

                pair(ph, c, o, f).wait_send()
        return carry

    lax.fori_loop(0, chunks, drain, 0)
    for k in range(3):
        for o in range(dim_count):
            @pl.when((o <= d) & (d < high))
            def _():
                chain_to(k, o, chain_right, to_right).wait_send()

            @pl.when((o >= d) & (d > low))
            def _():
                chain_to(k, o, chain_left, to_left).wait_send()

    @pl.when(active)
    def _():
        for k in range(3):
            both(k, f).wait_send()
        if split > 1:
            for k in range(1, split):
                t = lax.rem(b + k, split)
                plane(t, b).wait_send()
                plane_both(t, f).wait_send()
        for k in range(1, batch_count):
            cand_copy(lax.rem(b + k, batch_count), b).wait_send()
        for k in range(1, members):
            loss_copy(lax.rem(me + k, members), f, level_of).wait_send()

    for c in range(chunks):
        for level in range(held):
            @pl.when(jnp.logical_not(own_rows(c, level)))
            def _():
                row_copy(c, level).wait_send()

    for ff in range(field_count):
        for level in range(held):
            @pl.when(jnp.logical_not((f == ff) & (level_of == level)))
            def _():
                loss_copy(ff * dim_count + low + level, ff, level).wait_recv()

    for c in range(chunks):
        for level in range(held):
            loss_out[c * held + level] = losses[level, c]


def line_pieces(count, parts):
    base, extra = divmod(count, parts)
    bounds, start = [], 0
    for k in range(parts):
        size = base + (k < extra)
        bounds.append((start, size))
        start += size
    return bounds


def line_fits(counts, features, tower_weight, candidates):
    batch_count, field_count, dim_count = counts
    fl, el, row_count = features.shape
    units, fields, width = tower_weight.shape
    relayed = line_pieces(fl, PIECES)[RELAYED][0]
    return (
        (fl + relayed) % 2 == 0 and (2 * fl + relayed) % 3 == 0 and
        dim_count == 4 and batch_count == 4 and field_count == 2
        and fields % 2 == 0 and fl >= PIECES and el % 32 == 0 and 4 * el == width and width == 128
        and row_count % (CHUNKS * field_count * 128) == 0 and units % (16 * batch_count) == 0)


PIECES = 4
RELAYED = 2
CHUNKS = 4
FAR_TOWER = CROSS * PIECES
END_TOWER = FAR_TOWER + 1
CANDS = END_TOWER + 1


def line_kernel(
    counts,
    feat, weight, bias, tower, tower_bias, query_weight, user, cand, positive,
    out, loss_out,
    x0, x1, y, x2, flat, tw, tw_near, tw_far, tw_pass, tw_raw, q_raw, pre_out, pre_in, pre_own,
    bias_raw, bias_cols, unit_raw, unit_cols, query_cols, cands, users, user_cols, targets, losses,
    feat_sem, weight_sem, small_sem,
    end_send, end_recv, cross_send, cross_recv, pair_send, pair_recv, one_send, one_recv,
    piece_send, piece_recv, direct_load, direct_send, direct_recv, plane_send, plane_recv, rest_recv,
    tower_send, tower_recv, near_recv, both_send, both_recv,
    bias_send, bias_recv, unit_send, unit_recv, near_unit,
    two_send, two_recv, out_sem, give_send, give_recv, part_send, part_recv, loss_send, loss_recv,
):
    batch_count, field_count, dim_count = counts
    b = lax.axis_index("batch")
    f = lax.axis_index("field")
    d = lax.axis_index("dim")
    members = field_count * dim_count
    me = f * dim_count + d
    chunks, fields, width, rc = x0.shape
    fl, el, _ = feat.shape
    wide = 2 * el
    half_k = fields // 2 * width
    quarter_units = tw_far.shape[0]
    units = tw.shape[1]
    side_k = fields * wide
    lanes = rc // field_count
    rows_in_part = el // 2
    side = d // 2
    mid = 1 + side
    far = 2 - side
    end = 3 * side
    far_end = 3 - end
    is_mid = d == mid
    is_end = d == end
    owner = is_mid & (f == 1)
    giver = is_mid & (f == 0)
    part_of = jnp.where(f == 1, side, 1 - side)
    other = field_count - 1 - f
    x_next = b + 1 - 2 * lax.rem(b, 2)
    y_next = lax.rem(b + 2, 4)
    diagonal = 3 - b
    fs = pl.ds(f * fl, fl)
    ss = pl.ds(pl.multiple_of(side * wide, wide), wide)

    def remote(ref, send, recv, to=None, **where):
        return pltpu.make_async_remote_copy(
            ref, ref if to is None else to, send, recv, device_id=where, device_id_type=MESH)

    def sent(ref, sem):
        remote(ref, sem, sem, field=other).wait_send()

    def landed(ref, sem):
        remote(ref, sem, sem, field=other).wait_recv()

    def entries(o):
        return pl.ds(pl.multiple_of(o * el, el), el)

    def within(o):
        return pl.ds(pl.multiple_of(lax.rem(o, 2) * el, el), el)

    def block(c, ff, o):
        return x0.at[c, pl.ds(ff * fl, fl), entries(o), :]

    def from_end(c, target):
        return remote(block(c, f, end), end_send, end_recv.at[c], dim=target)

    def cross(k, c, o):
        return remote(block(c, f, o), cross_send.at[k], cross_recv.at[k, c], dim=far)

    def cross_one(c, s):
        ref = x1.at[c, fs, pl.ds(pl.multiple_of(s * wide, wide), wide), :]
        return remote(ref, cross_send.at[2], cross_recv.at[2, c], dim=far)

    def pair(c, o):
        return remote(block(c, f, o), pair_send, pair_recv.at[c], field=other)

    def pair_one(c, s):
        ref = x1.at[c, fs, pl.ds(pl.multiple_of(s * wide, wide), wide), :]
        return remote(ref, one_send, one_recv.at[c], field=other)

    def weight_piece(level, p, source):
        start, size = line_pieces(fl, PIECES)[p]
        return weight_part(level, start, size, source)

    def weight_part(level, start, size, source):
        row = pl.multiple_of(lax.rem(end, 2) * el + lax.rem(source, 2) * rows_in_part, rows_in_part)
        lane = pl.multiple_of(source // 2 * half_k, half_k)
        return flat.at[level, pl.ds(start, size), pl.ds(row, rows_in_part), pl.ds(lane, half_k)]

    def piece(level, p, target):
        ref = weight_piece(level, p, b)
        return remote(ref, piece_send.at[level], piece_recv.at[level, p], dim=target)

    def direct(p, target):
        ref = weight_piece(1, p, diagonal)
        return remote(ref, direct_send, direct_recv, dim=target)

    def direct_part():
        start = line_pieces(fl, PIECES)[RELAYED][0]
        return weight_part(1, start, fl - start, diagonal)

    def tower_rows(member, source):
        return tw.at[member, pl.ds(pl.multiple_of(source * quarter_units, quarter_units), quarter_units), :]

    def item(i, source):
        if i < CROSS * PIECES:
            return weight_piece(i // PIECES, i % PIECES, source)
        if i == CANDS:
            return cands.at[source]
        return tower_rows(f * dim_count + (far if i == FAR_TOWER else far_end), source)

    def relay(i):
        return (x_next, y_next) if i % 2 == 0 else (y_next, x_next)

    def group_of(i):
        return i // PIECES if i < FAR_TOWER else CROSS + i - FAR_TOWER

    def plane(i, source, target, arrival):
        return remote(item(i, source), plane_send.at[group_of(i)], arrival, batch=target)

    def plane_out(i):
        first, second = relay(i)
        plane(i, b, first, plane_recv.at[i]).start()
        plane(i, b, second, rest_recv.at[group_of(i)]).start()

    def plane_forward(i):
        source, target = relay(i)
        plane(i, source, target, plane_recv.at[i]).wait_recv()
        plane(i, source, target, rest_recv.at[group_of(i)]).start()

    def plane_keep(i):
        source, target = relay(i)
        plane(i, source, target, plane_recv.at[i]).wait_recv()

    def plane_rest(group):
        landed(plane_bytes(group, 2), rest_recv.at[group])

    def plane_bytes(group, copies):
        if group == 1:
            total = (copies - 1) * fl + line_pieces(fl, PIECES)[RELAYED][0]
            return flat.at[1, pl.ds(0, total // copies), pl.ds(0, copies * rows_in_part), pl.ds(0, half_k)]
        if group < CROSS:
            return flat.at[group, :, pl.ds(0, copies * rows_in_part), pl.ds(0, half_k)]
        if group == CROSS + 2:
            return cands.at[pl.ds(0, copies)]
        return tw.at[pl.ds(0, copies), pl.ds(0, quarter_units), :]

    def near_tower(target):
        return remote(
            tw_near, tower_send.at[0], near_recv, to=tw.at[f * dim_count + end], dim=target)

    def far_tower(source, target):
        return remote(
            tw_far, tower_send.at[1], tower_recv.at[source],
            to=tower_rows(f * dim_count + source, b), dim=target)

    def pass_in(target):
        return remote(tw_far, tower_send.at[1], tower_recv.at[mid], to=tw_pass, dim=target)

    def pass_on():
        return remote(
            tw_pass, tower_send.at[0], tower_recv.at[end],
            to=tower_rows(f * dim_count + end, b), dim=far)

    def both(z, ff):
        return remote(tw.at[ff * dim_count + z], both_send, both_recv, field=other)

    def bias_copy(target):
        return remote(bias_raw.at[lax.rem(end, 2)], bias_send, bias_recv, dim=target)

    def unit_in(target):
        return remote(unit_raw.at[f * dim_count + end], unit_send, near_unit, dim=target)

    def unit_out(ff, z):
        rows = unit_raw.at[pl.ds(f * dim_count + 2 * side, 2)]
        return remote(rows, unit_send, unit_recv, field=ff, dim=z)

    def two(c, ff):
        lane = pl.multiple_of((1 - part_of) * lanes, lanes)
        return remote(
            y.at[c, :, :, pl.ds(lane, lanes)], two_send, two_recv.at[c],
            to=x2.at[c, pl.ds(ff * fl, fl)], field=other)

    def rows_of(c):
        return pl.ds(pl.multiple_of(c * rc, rc), rc)

    def keep(c):
        return pltpu.make_async_copy(y.at[c, :, within(mid), :], out.at[:, :, rows_of(c)], out_sem)

    def give(c):
        return remote(
            y.at[c, :, within(end), :], give_send, give_recv,
            to=out.at[:, :, rows_of(c)], dim=end)

    def part(c):
        return remote(
            pre_out.at[c], part_send, part_recv.at[c], to=pre_in.at[c], field=other, dim=far)

    def loss_copy(k, c):
        m = lax.rem(me + k, members)
        return remote(
            losses.at[c], loss_send.at[k], loss_recv, to=loss_out.at[c * field_count + part_of],
            field=m // dim_count, dim=lax.rem(m, dim_count))

    def keep_loss(c):
        return pltpu.make_async_copy(losses.at[c], loss_out.at[c * field_count + part_of], loss_send.at[0])

    def own_weight(level, ff):
        return pltpu.make_async_copy(
            weight.at[level, :, ff],
            flat.at[level, :, within(mid), pl.ds(pl.multiple_of(ff * width, width), width)],
            weight_sem.at[level])

    def end_weight(level, k):
        row = pl.multiple_of(lax.rem(b, 2) * rows_in_part, rows_in_part)
        ff = b // 2 * (fields // 2) + k
        to = pl.multiple_of(lax.rem(end, 2) * el + row, rows_in_part)
        return pltpu.make_async_copy(
            weight.at[level, :, ff, pl.ds(row, rows_in_part), :],
            flat.at[level, :, pl.ds(to, rows_in_part), pl.ds(pl.multiple_of(ff * width, width), width)],
            weight_sem.at[level])

    def direct_weight(k):
        start = line_pieces(fl, PIECES)[RELAYED][0]
        row = pl.multiple_of(lax.rem(diagonal, 2) * rows_in_part, rows_in_part)
        ff = diagonal // 2 * (fields // 2) + k
        to = pl.multiple_of(lax.rem(end, 2) * el + row, rows_in_part)
        return pltpu.make_async_copy(
            weight.at[1, pl.ds(start, fl - start), ff, pl.ds(row, rows_in_part), :],
            flat.at[1, pl.ds(start, fl - start), pl.ds(to, rows_in_part),
                    pl.ds(pl.multiple_of(ff * width, width), width)],
            direct_load)

    def each(count, act):
        def step(k, carry):
            act(k)
            return carry

        lax.fori_loop(0, count, step, 0)

    own_features = [
        pltpu.make_async_copy(feat.at[:, :, pl.ds(c * rc, rc)], block(c, f, d), feat_sem.at[c])
        for c in range(chunks)]
    quarter = pl.ds(pl.multiple_of(b * quarter_units, quarter_units), quarter_units)
    small = [
        pltpu.make_async_copy(bias, bias_raw.at[lax.rem(d, 2)], small_sem.at[0]),
        pltpu.make_async_copy(tower_bias, unit_raw.at[me], small_sem.at[1]),
        pltpu.make_async_copy(cand, cands.at[b], small_sem.at[2]),
        pltpu.make_async_copy(tower, tw_raw, small_sem.at[3]),
        pltpu.make_async_copy(query_weight, q_raw, small_sem.at[4]),
        pltpu.make_async_copy(user, users, small_sem.at[5]),
        pltpu.make_async_copy(positive, targets, small_sem.at[6]),
    ]
    barrier = pltpu.get_barrier_semaphore()

    def greet(**where):
        pl.semaphore_signal(barrier, inc=1, device_id=where, device_id_type=MESH)

    @pl.when(is_end)
    def _():
        for ff in range(field_count):
            for z in (1, 2):
                greet(field=ff, dim=z)

    @pl.when(is_mid)
    def _():
        greet(dim=end)
        greet(dim=far)
        greet(batch=x_next)
        greet(batch=y_next)
        greet(field=other, dim=far)
        greet(field=other)

    for copy in own_features:
        copy.start()

    @pl.when(is_end)
    def _():
        each(fields // 2, lambda k: end_weight(0, k).start())

    for copy in small:
        copy.start()

    @pl.when(is_mid)
    def _():
        each(fields, lambda k: own_weight(0, k).start())
        each(fields, lambda k: own_weight(1, k).start())

    @pl.when(is_end)
    def _():
        each(fields // 2, lambda k: end_weight(1, k).start())
        each(fields // 2, lambda k: direct_weight(k).start())

    pl.semaphore_wait(barrier, jnp.where(is_mid, 2 * field_count + 5, 1))

    def loaded_own(level):
        ref = flat.at[level, :, within(mid), :]
        pltpu.make_async_copy(ref, ref, weight_sem.at[level]).wait()

    def loaded_end(level):
        ref = weight_part(level, 0, fl, b)
        pltpu.make_async_copy(ref, ref, weight_sem.at[level]).wait()

    def pack_tower():
        def halves(rows, j):
            first = tw_raw[2 * j, rows, :]
            second = tw_raw[2 * j + 1, rows, :]
            low = jnp.concatenate([first[:, :wide], second[:, :wide]], axis=1)
            high = jnp.concatenate([first[:, wide:], second[:, wide:]], axis=1)
            return low, high

        for j in range(fields // 2):
            low, high = halves(slice(None), j)
            tw_near[:, j * width:(j + 1) * width] = jnp.where(side == 0, low, high)
            low, high = halves(quarter, j)
            tw_far[:, j * width:(j + 1) * width] = jnp.where(side == 0, high, low)
        tw_near[:, side_k:] = q_raw[...]
        tw_far[:, side_k:] = q_raw[quarter, :]

    @pl.when(is_end)
    def _():
        loaded_end(0)
        for p in range(PIECES - 1):
            piece(0, p, mid).start()
        for copy in own_features:
            copy.wait()
        from_end(0, mid).start()
        piece(0, PIECES - 1, mid).start()
        from_end(1, mid).start()
        for copy in small:
            copy.wait()
        bias_copy(mid).start()
        unit_in(mid).start()
        for c in range(2, chunks):
            from_end(c, mid).start()
        pack_tower()
        pass_in(mid).start()
        loaded_end(1)
        for p in range(PIECES):
            piece(1, p, mid).start()
        pltpu.make_async_copy(direct_part(), direct_part(), direct_load).wait()
        for p in range(RELAYED, PIECES):
            direct(p, mid).start()
        near_tower(mid).start()

    def expect_piece(level, p):
        piece(level, p, end).wait_recv()
        plane_out(level * PIECES + p)

    def expect_end(c):
        from_end(c, end).wait_recv()
        cross(1, c, end).start()
        pair(c, end).start()

    def expect_far(k, c, o):
        cross(k, c, o).wait_recv()
        pair(c, o).start()

    def expect_tower(i, z):
        far_tower(z, end).wait_recv()
        plane_out(i)

    def half(source, level, c, ff):
        matrix = flat[level, :, :, pl.ds(pl.multiple_of(ff * half_k, half_k), half_k)]
        return jnp.dot(
            matrix.reshape(fl * wide, half_k), source[c, pl.ds(ff * fl, fl)].reshape(half_k, rc),
            preferred_element_type=jnp.float32)

    def advance(source, level, c, wait_pair):
        product = half(source, level, c, f)
        wait_pair()
        product = product + half(source, level, c, other)
        column = bias_cols[level]
        product = product + jnp.concatenate([column] * (rc // column.shape[1]), axis=1)
        anchor = x0[c, fs, ss, :].astype(jnp.float32).reshape(fl * wide, rc)
        current = source[c, fs, ss, :].astype(jnp.float32).reshape(fl * wide, rc)
        return (anchor * product + current).astype(jnp.bfloat16).reshape(fl, wide, rc)

    def build_bias():
        pick = (lax.broadcasted_iota(jnp.int32, (el, el), 0) == lax.broadcasted_iota(jnp.int32, (el, el), 1))
        for level in range(CROSS):
            for k in range(fl):
                for s in range(2):
                    line = bias_raw[s, k, level:level + 1, :]
                    column = jnp.sum(jnp.where(pick, line, 0.0), axis=1, keepdims=True)
                    start = (2 * k + s) * el
                    bias_cols[level, start:start + el, :] = jnp.broadcast_to(column, (el, width))

    def build_units():
        for m in range(members):
            unit_cols[m * units:(m + 1) * units, :] = jnp.broadcast_to(unit_raw[m], (lanes, units)).T

    def build_users():
        for c in range(chunks):
            start = pl.multiple_of(c * rc + part_of * lanes, lanes)
            user_cols[c] = users[pl.ds(start, lanes), :].astype(jnp.float32).T

    def build_queries():
        for m in range(members):
            block = tw[m, :, side_k:].astype(jnp.float32).T
            query_cols[:, m * units:(m + 1) * units] = block.astype(jnp.bfloat16)

    def first(c, carry):
        @pl.when(c == 1)
        def _():
            pass_in(end).wait_recv()
            pass_on().start()

        @pl.when(c == 2)
        def _():
            expect_far(1, 2, far_end)
            plane_forward(FAR_TOWER)
            expect_piece(1, 0)

        @pl.when(c == 3)
        def _():
            expect_far(1, 3, far_end)
            expect_piece(1, 1)

        def wait_pair():
            landed(x0.at[c, fs], pair_recv.at[c])

        x1[c, fs, ss, :] = advance(x0, 0, c, wait_pair)
        cross_one(c, side).start()
        pair_one(c, side).start()
        return carry

    def tower_part(c):
        matrix = tw[:, :, :side_k].reshape(members * units, side_k)
        return jnp.dot(matrix, x2[c].reshape(side_k, lanes), preferred_element_type=jnp.float32)

    def expect_one(c):
        cross_one(c, 1 - side).wait_recv()
        pair_one(c, 1 - side).start()

    def layer_two(c):
        def wait_pair():
            landed(x1.at[c, fs], one_recv.at[c])

        y[c] = advance(x1, 1, c, wait_pair)
        two(c, f).start()
        give(c).start()
        keep(c).start()
        for k in range(2):
            @pl.when(part_of == k)
            def _():
                x2[c, fs] = y[c, :, :, k * lanes:(k + 1) * lanes]

    def layer_three(c):
        two(c, other).wait_recv()
        pre = tower_part(c)

        @pl.when(owner)
        def _():
            pre_own[c] = pre + unit_cols[...]

        @pl.when(giver)
        def _():
            pre_out[c] = pre.astype(jnp.bfloat16)
            part(c).start()

    def second(c, carry):
        layer_two(c)

        @pl.when(c == 1)
        def _():
            near_tower(end).wait_recv()
            both(end, f).start()
            expect_one(2)
            landed(tw.at[pl.ds(0, dim_count)], both_recv)

        def tower_step(k, carry):
            layer_three(k)
            return carry

        last = c == chunks - 1
        lax.fori_loop(
            jnp.where(last, c, jnp.maximum(c - 1, 0)), jnp.where(c < chunks - 2, c, c + 1),
            tower_step, 0)

        @pl.when(c == 2)
        def _():
            expect_one(3)

        return carry

    def finish(c):
        part(c).wait_recv()
        pre = pre_own[c] + pre_in[c].astype(jnp.float32)
        hidden = jnp.maximum(pre, 0.0).astype(jnp.bfloat16)
        query = jnp.dot(query_cols[...], hidden, preferred_element_type=jnp.float32)
        query_vec = (query + user_cols[c]).astype(jnp.bfloat16)
        logits = jnp.dot(
            cands[...].reshape(-1, width), query_vec,
            preferred_element_type=jnp.float32) * (1.0 / math.sqrt(width))
        labels = lax.broadcasted_iota(jnp.int32, logits.shape, 0)
        target = targets[c * field_count + part_of]
        picked = jnp.sum(jnp.where(labels == target, logits, 0.0), axis=0, keepdims=True)
        best = jnp.max(logits, axis=0, keepdims=True)
        total = jnp.sum(jnp.exp(logits - best), axis=0, keepdims=True)
        losses[c] = best + jnp.log(total) - picked
        for k in range(1, members):
            loss_copy(k, c).start()
        keep_loss(c).start()

    @pl.when(is_mid)
    def _():
        for c in range(chunks):
            own_features[c].wait()
            cross(0, c, mid).start()
            pair(c, mid).start()
        for copy in small:
            copy.wait()
        plane_out(CANDS)
        pack_tower()
        far_tower(d, far).start()
        tw[me] = tw_near[...]
        both(mid, f).start()
        expect_piece(0, 0)
        expect_far(0, 0, far)
        expect_piece(0, 1)
        expect_far(0, 1, far)
        plane_forward(CANDS)
        expect_piece(0, 2)
        expect_far(0, 2, far)
        plane_forward(0)
        plane_forward(1)
        expect_far(0, 3, far)
        expect_end(0)
        expect_piece(0, 3)
        plane_forward(2)
        expect_end(1)
        plane_forward(3)
        expect_far(1, 0, far_end)
        expect_tower(FAR_TOWER, far)
        bias_copy(end).wait_recv()
        build_bias()
        unit_in(end).wait_recv()
        unit_out(other, d).start()
        unit_out(f, far).start()
        unit_out(other, far).start()
        for level in range(CROSS):
            loaded_own(level)
        expect_end(2)
        plane_rest(0)
        expect_far(1, 1, far_end)
        expect_end(3)
        lax.fori_loop(0, chunks, first, 0)
        plane_rest(4)
        plane_rest(2)
        both(far, f).start()
        expect_piece(1, 2)
        expect_piece(1, 3)
        expect_tower(END_TOWER, far_end)
        for p in range(RELAYED):
            plane_forward(PIECES + p)
        expect_one(0)
        plane_forward(END_TOWER)
        for p in range(RELAYED, PIECES):
            plane_keep(PIECES + p)
        expect_one(1)
        landed(unit_raw.at[pl.ds(0, 6)], unit_recv)
        build_units()
        build_users()
        plane_rest(3)
        both(far_end, f).start()
        landed(direct_part(), direct_recv)
        plane_rest(1)
        lax.fori_loop(0, chunks, second, 0)

        @pl.when(owner)
        def _():
            build_queries()
            for c in range(chunks):
                finish(c)

    @pl.when(owner)
    def _():
        landed(losses, loss_recv)

    @pl.when(jnp.logical_not(owner))
    def _():
        landed(loss_out, loss_recv)

    @pl.when(is_end)
    def _():
        for level in range(CROSS):
            sent(weight_part(level, 0, fl, b), piece_send.at[level])
        sent(direct_part(), direct_send)
        sent(x0.at[:, fs, entries(d), :], end_send)
        bias_copy(mid).wait_send()
        near_tower(mid).wait_send()
        pass_in(mid).wait_send()
        unit_in(mid).wait_send()
        landed(out, give_recv)

    @pl.when(is_mid)
    def _():
        far_tower(d, far).wait_send()
        pass_on().wait_send()
        sent(tw.at[pl.ds(0, dim_count)], both_send)
        sent(unit_raw.at[pl.ds(0, 6)], unit_send)
        sent(x0.at[:, fs, entries(mid), :], cross_send.at[0])
        sent(x0.at[:, fs, entries(end), :], cross_send.at[1])
        sent(x1.at[:, fs, ss, :], cross_send.at[2])
        sent(x0.at[:, fs], pair_send)
        sent(x1.at[:, fs], one_send)
        sent(y.at[:, :, :, pl.ds(0, lanes)], two_send)
        sent(out, give_send)
        pltpu.make_async_copy(out, out, out_sem).wait()
        for group in range(CROSS + 3):
            sent(plane_bytes(group, 3), plane_send.at[group])

    @pl.when(giver)
    def _():
        sent(pre_out, part_send)

    @pl.when(owner)
    def _():
        for k in range(1, members):
            sent(losses, loss_send.at[k])
        pltpu.make_async_copy(losses, losses, loss_send.at[0]).wait()


def emit_kernel(crossed, losses, crossed_out, losses_out, sems):
    copies = [
        pltpu.make_async_copy(crossed, crossed_out, sems.at[0]),
        pltpu.make_async_copy(losses, losses_out, sems.at[1]),
    ]
    for copy in copies:
        copy.start()
    for copy in copies:
        copy.wait()


def line_body(
    counts, features, cross_weight, cross_bias, tower_weight, tower_bias, query_weight,
    user_vec, candidates, positive,
):
    batch_count, field_count, dim_count = counts
    members = field_count * dim_count
    fl, el, row_count = features.shape
    units, fields, width = tower_weight.shape
    rc = row_count // CHUNKS
    lanes = rc // field_count
    wide = 2 * el
    quarter = units // batch_count
    packed = fields * wide + width
    items = CANDS + 1
    dma = pltpu.SemaphoreType.DMA
    vmem = pltpu.VMEM
    bf16 = jnp.bfloat16
    f32 = jnp.float32
    far = pl.BlockSpec(memory_space=pl.ANY)
    crossed, losses = pl.pallas_call(
        functools.partial(line_kernel, counts),
        out_shape=(
            jax.ShapeDtypeStruct(features.shape, bf16),
            jax.ShapeDtypeStruct((CHUNKS * field_count, 1, lanes), f32),
        ),
        in_specs=[far] * 9,
        out_specs=(far, far),
        scratch_shapes=[
            vmem((CHUNKS, fields, width, rc), bf16),
            vmem((CHUNKS, fields, width, rc), bf16),
            vmem((CHUNKS, fl, wide, rc), bf16),
            vmem((CHUNKS, fields, wide, lanes), bf16),
            vmem((CROSS, fl, wide, fields * width), bf16),
            vmem((members, units, packed), bf16),
            vmem((units, packed), bf16),
            vmem((quarter, packed), bf16),
            vmem((quarter, packed), bf16),
            vmem((fields, units, width), bf16),
            vmem((units, width), bf16),
            vmem((CHUNKS, members * units, lanes), bf16),
            vmem((CHUNKS, members * units, lanes), bf16),
            vmem((CHUNKS, members * units, lanes), f32),
            vmem((2, fl, CROSS, el), f32),
            vmem((CROSS, fl * wide, width), f32),
            vmem((members, 1, units), f32),
            vmem((members * units, lanes), f32),
            vmem((width, members * units), bf16),
            vmem((batch_count,) + candidates.shape, bf16),
            vmem(user_vec.shape, bf16),
            vmem((CHUNKS, width, lanes), f32),
            vmem((CHUNKS * field_count, 1, lanes), jnp.int32),
            vmem((CHUNKS, 1, lanes), f32),
            dma((CHUNKS,)), dma((CROSS,)), dma((7,)),
            dma, dma((CHUNKS,)), dma((3,)), dma((3, CHUNKS)),
            dma, dma((CHUNKS,)), dma, dma((CHUNKS,)),
            dma((CROSS,)), dma((CROSS, PIECES)), dma, dma, dma, dma((CROSS + 3,)), dma((items,)), dma((CROSS + 3,)),
            dma((2,)), dma((dim_count,)), dma, dma, dma,
            dma, dma, dma, dma, dma,
            dma, dma((CHUNKS,)), dma, dma, dma, dma, dma((CHUNKS,)), dma((members,)), dma,
        ],
        compiler_params=pltpu.CompilerParams(
            collective_id=0, has_side_effects=True, vmem_limit_bytes=48 * 2**20),
        name="line_forward",
    )(*(pltpu.with_memory_space_constraint(value, pltpu.HBM) for value in (
        features,
        cross_weight.transpose(0, 1, 3, 2, 4),
        cross_bias.transpose(1, 0, 2),
        tower_weight.transpose(1, 0, 2),
        tower_bias.reshape(1, units),
        query_weight,
        user_vec,
        candidates,
        positive.reshape(CHUNKS * field_count, 1, lanes),
    )))
    crossed, losses = pl.pallas_call(
        emit_kernel,
        out_shape=(
            jax.ShapeDtypeStruct(features.shape, bf16),
            jax.ShapeDtypeStruct((CHUNKS * field_count, 1, lanes), f32),
        ),
        in_specs=[far] * 2,
        out_specs=(pl.BlockSpec(memory_space=pltpu.HBM),) * 2,
        scratch_shapes=[dma((2,))],
        compiler_params=pltpu.CompilerParams(vmem_limit_bytes=4 * 2**20),
        name="emit",
    )(crossed, losses)
    return (crossed, losses.reshape(row_count))


def body(
    features, cross_weight, cross_bias, tower_weight, tower_bias, query_weight,
    user_vec, candidates, positive,
):
    counts = tuple(lax.axis_size(name) for name in ("batch", "field", "dim"))
    if line_fits(counts, features, tower_weight, candidates):
        return line_body(
            counts, features, cross_weight, cross_bias, tower_weight, tower_bias, query_weight,
            user_vec, candidates, positive)
    batch_count, field_count, dim_count = counts
    members = field_count * dim_count
    fl, el, row_count = features.shape
    columns = fl * el
    units, fields, width = tower_weight.shape
    low, held = tower_levels(dim_count)
    chunks = chunk_count(row_count, field_count, held)
    split = batch_count if units % (batch_count * 16) == 0 else 1
    part = units // split
    rc = row_count // chunks
    sub = rc // held
    run = chunks // field_count
    share = run * sub
    steps = (CROSS, chunks, dim_count)
    small = (3, dim_count)
    dma = pltpu.SemaphoreType.DMA
    vmem = pltpu.VMEM
    bf16 = jnp.bfloat16
    far = pl.BlockSpec(memory_space=pl.ANY)
    near = pl.BlockSpec(memory_space=pltpu.VMEM)
    crossed, losses = pl.pallas_call(
        functools.partial(rank_kernel, counts, (chunks, split)),
        out_shape=(
            jax.ShapeDtypeStruct(features.shape, bf16),
            jax.ShapeDtypeStruct((chunks * held, 1, sub), jnp.float32),
        ),
        in_specs=[far, far, near, far, far, far, near, far, near],
        out_specs=(near, near),
        scratch_shapes=[
            vmem((chunks, fields, width, rc), bf16),
            vmem((chunks, fields, width, rc), bf16),
            vmem((CROSS, fl, el, fields * width), bf16),
            vmem((chunks, held, fl, el, sub), bf16),
            vmem((fields, width, share), bf16),
            vmem((split, members, part, fields * width), bf16),
            vmem((members, 1, units), jnp.float32),
            vmem((split, members, part, share), jnp.float32),
            vmem((split, members, part, width), bf16),
            vmem((batch_count,) + candidates.shape, bf16),
            vmem((held, chunks, 1, sub), jnp.float32),
            dma((chunks,)), dma((CROSS, fields)), dma((fields,)), dma((3,)),
            dma(steps), dma(steps), dma(steps), dma(steps), dma(steps),
            dma((chunks, held)), dma((run, members)), dma(small), dma(small), dma(small),
            dma((3,)), dma((3,)),
            dma((split,)), dma((split,)), dma((split,)), dma((split,)),
            dma((batch_count,)), dma((batch_count,)), dma((members,)), dma((field_count, held)),
        ],
        compiler_params=pltpu.CompilerParams(
            collective_id=0, has_side_effects=True, vmem_limit_bytes=56 * 2**20),
        name="rank_forward",
    )(
        features,
        cross_weight.transpose(0, 1, 3, 2, 4),
        cross_bias.reshape(CROSS, columns, 1),
        tower_weight.transpose(1, 0, 2),
        tower_bias.reshape(1, units),
        query_weight.reshape(split, part, width),
        user_vec,
        candidates,
        positive.reshape(chunks * held, 1, sub),
    )
    return (crossed, losses.reshape(row_count))


def solution(mesh):
    placed = (
        P("field", "dim", "batch"),
        P(None, "field", "dim", None, None),
        P(None, "field", "dim"),
        P(("field", "dim"), None, None),
        P(("field", "dim")),
        P(("field", "dim"), None),
        P("batch", None),
        P("batch", None),
        P("batch"),
    )
    return jax.shard_map(
        body,
        mesh=mesh,
        in_specs=placed,
        out_specs=(P("field", "dim", "batch"), P("batch")),
        check_vma=False,
    )
```

```python
import functools
import math

import jax
import jax.numpy as jnp
from jax import lax
from jax.experimental import pallas as pl
from jax.experimental.pallas import tpu as pltpu
from jax.sharding import PartitionSpec as P

CROSS = 2
MESH = pl.DeviceIdType.MESH


def tower_levels(dim_count):
    held = min(2, dim_count)
    return (dim_count - held) // 2, held


def chunk_count(row_count, field_count, held):
    chunks = 2
    while chunks > field_count and row_count % (chunks * held * 128):
        chunks //= 2
    return chunks


def rank_kernel(
    counts, splits,
    feat, weight, bias, tower, tower_bias, query_weight, user, cand, positive,
    out, loss_out,
    x0, x1, flat, sent, rows, towers, biases, columns_bias, queries, cands, losses,
    feat_sem, weight_sem, tower_sem, small_sem,
    right_sem, left_sem, pair_sem, recv_sem, pair_recv,
    row_send, row_recv, chain_right, chain_left, chain_recv, both_send, both_recv,
    plane_send, plane_recv, plane_pair, plane_pair_recv,
    cand_send, cand_recv, loss_send, loss_recv,
):
    batch_count, field_count, dim_count = counts
    chunks, split = splits
    b = lax.axis_index("batch")
    f = lax.axis_index("field")
    d = lax.axis_index("dim")
    me = f * dim_count + d
    members = field_count * dim_count
    fl, el, row_count = feat.shape
    columns = fl * el
    fields, width, rc = x0.shape[1:]
    low, held = tower_levels(dim_count)
    high = low + held - 1
    level_of = d - low
    active = (d >= low) & (d <= high)
    sub = rc // held
    run = chunks // field_count
    share = run * sub
    part = towers.shape[2]
    units = split * part
    buffers = (x0, x1)
    other = field_count - 1 - f
    mine = b if split > 1 else 0
    to_right = jnp.minimum(d + 1, dim_count - 1)
    to_left = jnp.maximum(d - 1, 0)

    def remote(ref, send, recv, **where):
        return pltpu.make_async_remote_copy(
            ref, ref, send, recv, device_id=where, device_id_type=MESH)

    def place(ff, o):
        return pl.ds(ff * fl, fl), pl.ds(pl.multiple_of(o * el, el), el)

    def piece(ph, c, ff, o):
        fs, ds = place(ff, o)
        return buffers[ph].at[c, fs, ds, :]

    def right(ph, c, o):
        return remote(piece(ph, c, f, o), right_sem.at[ph, c, o], recv_sem.at[ph, c, o], dim=to_right)

    def left(ph, c, o):
        return remote(piece(ph, c, f, o), left_sem.at[ph, c, o], recv_sem.at[ph, c, o], dim=to_left)

    def pair(ph, c, o, ff):
        return remote(
            piece(ph, c, ff, o), pair_sem.at[ph, c, o], pair_recv.at[ph, c, o], field=other)

    def issue_own(ph, c):
        @pl.when(d < dim_count - 1)
        def _():
            right(ph, c, d).start()

        @pl.when(d > 0)
        def _():
            left(ph, c, d).start()

        pair(ph, c, d, f).start()

    def forwards(ph, c):
        for s in range(1, dim_count):
            @pl.when(d - s >= 0)
            def _():
                right(ph, c, d - s).wait_recv()

                @pl.when(d < dim_count - 1)
                def _():
                    right(ph, c, d - s).start()

                pair(ph, c, d - s, f).start()

            @pl.when(d + s < dim_count)
            def _():
                left(ph, c, d + s).wait_recv()

                @pl.when(d > 0)
                def _():
                    left(ph, c, d + s).start()

                pair(ph, c, d + s, f).start()
        for o in range(dim_count):
            pair(ph, c, o, other).wait_recv()

    def weight_copy(level, ff):
        return pltpu.make_async_copy(
            weight.at[level, :, ff],
            flat.at[level, :, :, pl.ds(pl.multiple_of(ff * width, width), width)],
            weight_sem.at[level, ff])

    def tower_copy(ff):
        return pltpu.make_async_copy(
            tower.at[ff, pl.ds(pl.multiple_of(mine * part, part), part), :],
            towers.at[mine, me, :, pl.ds(pl.multiple_of(ff * width, width), width)],
            tower_sem.at[ff])

    def each_field(act):
        def step(ff, carry):
            act(ff)
            return carry

        lax.fori_loop(0, fields, step, 0)

    small_refs = (
        lambda o: towers.at[mine, f * dim_count + o],
        lambda o: queries.at[:, f * dim_count + o],
        lambda o: biases.at[f * dim_count + o],
    )
    small_wide = (
        lambda ff: towers.at[mine, pl.ds(ff * dim_count, dim_count)],
        lambda ff: queries.at[:, pl.ds(ff * dim_count, dim_count)],
        lambda ff: biases.at[pl.ds(ff * dim_count, dim_count)],
    )

    def chain_to(k, o, sems, target):
        return remote(small_refs[k](o), sems.at[k, o], chain_recv.at[k, o], dim=target)

    def chain_own():
        for k in range(3):
            @pl.when(d < high)
            def _():
                chain_to(k, d, chain_right, to_right).start()

            @pl.when(d > low)
            def _():
                chain_to(k, d, chain_left, to_left).start()

    def chain_step(s):
        for k in range(3):
            @pl.when((d - s >= 0) & (d <= high))
            def _():
                chain_to(k, d - s, chain_right, to_right).wait_recv()

                @pl.when(d < high)
                def _():
                    chain_to(k, d - s, chain_right, to_right).start()

            @pl.when((d + s < dim_count) & (d >= low))
            def _():
                chain_to(k, d + s, chain_left, to_left).wait_recv()

                @pl.when(d > low)
                def _():
                    chain_to(k, d + s, chain_left, to_left).start()

    def both(k, ff):
        return remote(small_wide[k](ff), both_send.at[k], both_recv.at[k], field=other)

    def plane(t, source):
        return remote(
            towers.at[source, pl.ds(f * dim_count, dim_count)],
            plane_send.at[t], plane_recv.at[source], batch=t)

    def plane_both(source, ff):
        return remote(
            towers.at[source, pl.ds(ff * dim_count, dim_count)],
            plane_pair.at[source], plane_pair_recv.at[source], field=other)

    def cand_copy(t, source):
        return remote(cands.at[source], cand_send.at[t], cand_recv.at[source], batch=t)

    def loss_copy(m, ff, level):
        ref = losses.at[level, pl.ds(ff * run, run)]
        return remote(
            ref, loss_send.at[m], loss_recv.at[ff, level], field=m // dim_count, dim=m % dim_count)

    def row_copy(c, level):
        fs, ds = place(f, d)
        return pltpu.make_async_remote_copy(
            sent.at[c, level],
            rows.at[fs, ds, pl.ds(pl.multiple_of(lax.rem(c, run) * sub, sub), sub)],
            row_send.at[c, level], row_recv.at[lax.rem(c, run), me],
            device_id={"field": c // run, "dim": low + level}, device_id_type=MESH)

    def own_rows(c, level):
        return (c // run == f) & (level_of == level)

    def advance(ph, c):
        whole = buffers[ph][c].reshape(fields * width, rc)
        matrix = flat[ph].reshape(columns, fields * width)
        product = jnp.dot(matrix, whole, preferred_element_type=jnp.float32) + bias[ph]
        fs, ds = place(f, d)
        anchor = x0[c, fs, ds, :].astype(jnp.float32).reshape(columns, rc)
        current = buffers[ph][c, fs, ds, :].astype(jnp.float32).reshape(columns, rc)
        return (anchor * product + current).astype(jnp.bfloat16).reshape(fl, el, rc)

    own_copies = []
    for c in range(chunks):
        own_copies.append(pltpu.make_async_copy(
            feat.at[:, :, pl.ds(c * rc, rc)], piece(0, c, f, d), feat_sem.at[c]))
    small_copies = [
        pltpu.make_async_copy(query_weight, queries.at[:, me], small_sem.at[0]),
        pltpu.make_async_copy(tower_bias, biases.at[me], small_sem.at[1]),
        pltpu.make_async_copy(cand, cands.at[b], small_sem.at[2]),
    ]
    for copy in own_copies + small_copies:
        copy.start()
    each_field(lambda ff: tower_copy(ff).start())
    for level in range(CROSS):
        each_field(lambda ff: weight_copy(level, ff).start())

    barrier = pltpu.get_barrier_semaphore()
    for k in range(1, members):
        m = lax.rem(me + k, members)
        pl.semaphore_signal(
            barrier, inc=1, device_id={"field": m // dim_count, "dim": m % dim_count},
            device_id_type=MESH)
    for k in range(1, batch_count):
        pl.semaphore_signal(
            barrier, inc=1, device_id={"batch": lax.rem(b + k, batch_count)}, device_id_type=MESH)
    pl.semaphore_wait(barrier, members + batch_count - 2)
    for copy in own_copies:
        copy.wait()
    issue_own(0, 0)
    if chunks > 1:
        issue_own(0, 1)
    each_field(lambda ff: tower_copy(ff).wait())
    for copy in small_copies:
        copy.wait()
    chain_own()

    @pl.when(active)
    def _():
        for k in range(1, batch_count):
            cand_copy(lax.rem(b + k, batch_count), b).start()

    for level in range(CROSS):
        each_field(lambda ff: weight_copy(level, ff).wait())

    def first(c, carry):
        @pl.when(c + 2 < chunks)
        def _():
            issue_own(0, c + 2)

        forwards(0, c)
        fs, ds = place(f, d)
        x1[c, fs, ds, :] = advance(0, c)
        issue_own(1, c)

        for s in range(1, min(chunks, dim_count)):
            @pl.when(c == s)
            def _():
                chain_step(s)

        return carry

    lax.fori_loop(0, chunks, first, 0)
    for s in range(min(chunks, dim_count), dim_count):
        chain_step(s)

    @pl.when(active)
    def _():
        for k in range(3):
            both(k, f).start()
        if split > 1:
            for k in range(1, split):
                plane(lax.rem(b + k, split), b).start()

    def second(c, carry):
        forwards(1, c)
        new = advance(1, c)
        out[:, :, pl.ds(pl.multiple_of(c * rc, 128), rc)] = new
        for level in range(held):
            block = new[:, :, level * sub:(level + 1) * sub]

            @pl.when(own_rows(c, level))
            def _():
                fs, ds = place(f, d)
                rows[fs, ds, pl.ds(pl.multiple_of(lax.rem(c, run) * sub, sub), sub)] = block

            @pl.when(jnp.logical_not(own_rows(c, level)))
            def _():
                sent[c, level] = block
                row_copy(c, level).start()

        return carry

    lax.fori_loop(0, chunks, second, 0)

    def tower_block(s, query):
        matrix = towers[s].reshape(members * part, fields * width)
        pre = jnp.dot(
            matrix, rows[...].reshape(fields * width, share), preferred_element_type=jnp.float32)
        pre = pre + columns_bias[s].reshape(members * part, share)
        hidden = jnp.maximum(pre, 0.0).astype(jnp.bfloat16)
        return query + lax.dot_general(
            hidden, queries[s].reshape(members * part, width), (((0,), (0,)), ((), ())),
            preferred_element_type=jnp.float32)

    @pl.when(active)
    def _():
        if split > 1:
            for k in range(1, split):
                source = lax.rem(b + k, split)
                plane(source, source).wait_recv()
                plane_both(source, f).start()
        for k in range(3):
            both(k, other).wait_recv()
        for k in range(1, batch_count):
            source = lax.rem(b + k, batch_count)
            cand_copy(source, source).wait_recv()
        for m in range(members):
            block = jnp.broadcast_to(biases[m], (share, units)).T
            columns_bias[:, m] = block.reshape(split, part, share)
        if split > 1:
            for k in range(1, split):
                plane_both(lax.rem(b + k, split), other).wait_recv()
        for j in range(run):
            for k in range(1, members):
                m = lax.rem(me + k, members)
                fs, ds = place(m // dim_count, m % dim_count)
                remote(rows.at[fs, ds, pl.ds(j * sub, sub)], row_send.at[0, 0], row_recv.at[j, m],
                       field=m // dim_count, dim=m % dim_count).wait_recv()

        query = lax.fori_loop(0, split, tower_block, jnp.zeros((share, width), jnp.float32))
        all_cands = cands[...].reshape(-1, width)
        for j in range(run):
            c = f * run + j
            start = pl.multiple_of(c * rc + level_of * sub, sub)
            query_vec = (
                query[j * sub:(j + 1) * sub] + user[pl.ds(start, sub), :].astype(jnp.float32)
            ).astype(jnp.bfloat16)
            logits = lax.dot_general(
                all_cands, query_vec, (((1,), (1,)), ((), ())), preferred_element_type=jnp.float32
            ) * (1.0 / math.sqrt(width))
            labels = lax.broadcasted_iota(jnp.int32, logits.shape, 0)
            target = positive[c * held + level_of]
            picked = jnp.sum(jnp.where(labels == target, logits, 0.0), axis=0, keepdims=True)
            best = jnp.max(logits, axis=0, keepdims=True)
            total = jnp.sum(jnp.exp(logits - best), axis=0, keepdims=True)
            losses[level_of, c] = best + jnp.log(total) - picked
        for k in range(1, members):
            loss_copy(lax.rem(me + k, members), f, level_of).start()

    def drain(c, carry):
        for ph in range(CROSS):
            for o in range(dim_count):
                @pl.when((o <= d) & (d < dim_count - 1))
                def _():
                    right(ph, c, o).wait_send()

                @pl.when((o >= d) & (d > 0))
                def _():
                    left(ph, c, o).wait_send()

                pair(ph, c, o, f).wait_send()
        return carry

    lax.fori_loop(0, chunks, drain, 0)
    for k in range(3):
        for o in range(dim_count):
            @pl.when((o <= d) & (d < high))
            def _():
                chain_to(k, o, chain_right, to_right).wait_send()

            @pl.when((o >= d) & (d > low))
            def _():
                chain_to(k, o, chain_left, to_left).wait_send()

    @pl.when(active)
    def _():
        for k in range(3):
            both(k, f).wait_send()
        if split > 1:
            for k in range(1, split):
                t = lax.rem(b + k, split)
                plane(t, b).wait_send()
                plane_both(t, f).wait_send()
        for k in range(1, batch_count):
            cand_copy(lax.rem(b + k, batch_count), b).wait_send()
        for k in range(1, members):
            loss_copy(lax.rem(me + k, members), f, level_of).wait_send()

    for c in range(chunks):
        for level in range(held):
            @pl.when(jnp.logical_not(own_rows(c, level)))
            def _():
                row_copy(c, level).wait_send()

    for ff in range(field_count):
        for level in range(held):
            @pl.when(jnp.logical_not((f == ff) & (level_of == level)))
            def _():
                loss_copy(ff * dim_count + low + level, ff, level).wait_recv()

    for c in range(chunks):
        for level in range(held):
            loss_out[c * held + level] = losses[level, c]


def line_pieces(count, parts):
    base, extra = divmod(count, parts)
    bounds, start = [], 0
    for k in range(parts):
        size = base + (k < extra)
        bounds.append((start, size))
        start += size
    return bounds


def line_fits(counts, features, tower_weight, candidates):
    batch_count, field_count, dim_count = counts
    fl, el, row_count = features.shape
    units, fields, width = tower_weight.shape
    relayed = line_pieces(fl, PIECES)[RELAYED][0]
    return (
        (fl + relayed) % 2 == 0 and (2 * fl + relayed) % 3 == 0 and
        dim_count == 4 and batch_count == 4 and field_count == 2
        and fields % 2 == 0 and fl >= PIECES and el % 32 == 0 and 4 * el == width and width == 128
        and row_count % (CHUNKS * field_count * 128) == 0 and units % (16 * batch_count) == 0)


PIECES = 4
RELAYED = 2
CHUNKS = 4
FAR_TOWER = CROSS * PIECES
END_TOWER = FAR_TOWER + 1
CANDS = END_TOWER + 1


def line_kernel(
    counts,
    feat, weight, bias, tower, tower_bias, query_weight, user, cand, positive,
    out, loss_out,
    x0, x1, y, x2, flat, tw, tw_near, tw_far, tw_pass, tw_raw, q_raw, pre_out, pre_in, pre_own,
    bias_raw, bias_cols, unit_raw, unit_cols, query_cols, cands, users, user_cols, targets, losses,
    feat_sem, weight_sem, small_sem,
    end_send, end_recv, cross_send, cross_recv, pair_send, pair_recv, one_send, one_recv,
    piece_send, piece_recv, direct_load, direct_send, direct_recv, plane_send, plane_recv, rest_recv,
    tower_send, tower_recv, near_recv, both_send, both_recv,
    bias_send, bias_recv, unit_send, unit_recv, near_unit,
    two_send, two_recv, out_sem, give_send, give_recv, part_send, part_recv, loss_send, loss_recv,
):
    batch_count, field_count, dim_count = counts
    b = lax.axis_index("batch")
    f = lax.axis_index("field")
    d = lax.axis_index("dim")
    members = field_count * dim_count
    me = f * dim_count + d
    chunks, fields, width, rc = x0.shape
    fl, el, _ = feat.shape
    wide = 2 * el
    half_k = fields // 2 * width
    quarter_units = tw_far.shape[0]
    units = tw.shape[1]
    side_k = fields * wide
    lanes = rc // field_count
    rows_in_part = el // 2
    side = d // 2
    mid = 1 + side
    far = 2 - side
    end = 3 * side
    far_end = 3 - end
    is_mid = d == mid
    is_end = d == end
    owner = is_mid & (f == 1)
    giver = is_mid & (f == 0)
    part_of = jnp.where(f == 1, side, 1 - side)
    other = field_count - 1 - f
    x_next = b + 1 - 2 * lax.rem(b, 2)
    y_next = lax.rem(b + 2, 4)
    diagonal = 3 - b
    fs = pl.ds(f * fl, fl)
    ss = pl.ds(pl.multiple_of(side * wide, wide), wide)

    def remote(ref, send, recv, to=None, **where):
        return pltpu.make_async_remote_copy(
            ref, ref if to is None else to, send, recv, device_id=where, device_id_type=MESH)

    def sent(ref, sem):
        remote(ref, sem, sem, field=other).wait_send()

    def landed(ref, sem):
        remote(ref, sem, sem, field=other).wait_recv()

    def entries(o):
        return pl.ds(pl.multiple_of(o * el, el), el)

    def within(o):
        return pl.ds(pl.multiple_of(lax.rem(o, 2) * el, el), el)

    def block(c, ff, o):
        return x0.at[c, pl.ds(ff * fl, fl), entries(o), :]

    def from_end(c, target):
        return remote(block(c, f, end), end_send, end_recv.at[c], dim=target)

    def cross(k, c, o):
        return remote(block(c, f, o), cross_send.at[k], cross_recv.at[k, c], dim=far)

    def cross_one(c, s):
        ref = x1.at[c, fs, pl.ds(pl.multiple_of(s * wide, wide), wide), :]
        return remote(ref, cross_send.at[2], cross_recv.at[2, c], dim=far)

    def pair(c, o):
        return remote(block(c, f, o), pair_send, pair_recv.at[c], field=other)

    def pair_one(c, s):
        ref = x1.at[c, fs, pl.ds(pl.multiple_of(s * wide, wide), wide), :]
        return remote(ref, one_send, one_recv.at[c], field=other)

    def weight_piece(level, p, source):
        start, size = line_pieces(fl, PIECES)[p]
        return weight_part(level, start, size, source)

    def weight_part(level, start, size, source):
        row = pl.multiple_of(lax.rem(end, 2) * el + lax.rem(source, 2) * rows_in_part, rows_in_part)
        lane = pl.multiple_of(source // 2 * half_k, half_k)
        return flat.at[level, pl.ds(start, size), pl.ds(row, rows_in_part), pl.ds(lane, half_k)]

    def piece(level, p, target):
        ref = weight_piece(level, p, b)
        return remote(ref, piece_send.at[level], piece_recv.at[level, p], dim=target)

    def direct(p, target):
        ref = weight_piece(1, p, diagonal)
        return remote(ref, direct_send, direct_recv, dim=target)

    def direct_part():
        start = line_pieces(fl, PIECES)[RELAYED][0]
        return weight_part(1, start, fl - start, diagonal)

    def tower_rows(member, source):
        return tw.at[member, pl.ds(pl.multiple_of(source * quarter_units, quarter_units), quarter_units), :]

    def item(i, source):
        if i < CROSS * PIECES:
            return weight_piece(i // PIECES, i % PIECES, source)
        if i == CANDS:
            return cands.at[source]
        return tower_rows(f * dim_count + (far if i == FAR_TOWER else far_end), source)

    def relay(i):
        return (x_next, y_next) if i % 2 == 0 else (y_next, x_next)

    def group_of(i):
        return i // PIECES if i < FAR_TOWER else CROSS + i - FAR_TOWER

    def plane(i, source, target, arrival):
        return remote(item(i, source), plane_send.at[group_of(i)], arrival, batch=target)

    def plane_out(i):
        first, second = relay(i)
        plane(i, b, first, plane_recv.at[i]).start()
        plane(i, b, second, rest_recv.at[group_of(i)]).start()

    def plane_forward(i):
        source, target = relay(i)
        plane(i, source, target, plane_recv.at[i]).wait_recv()
        plane(i, source, target, rest_recv.at[group_of(i)]).start()

    def plane_keep(i):
        source, target = relay(i)
        plane(i, source, target, plane_recv.at[i]).wait_recv()

    def plane_rest(group):
        landed(plane_bytes(group, 2), rest_recv.at[group])

    def plane_bytes(group, copies):
        if group == 1:
            total = (copies - 1) * fl + line_pieces(fl, PIECES)[RELAYED][0]
            return flat.at[1, pl.ds(0, total // copies), pl.ds(0, copies * rows_in_part), pl.ds(0, half_k)]
        if group < CROSS:
            return flat.at[group, :, pl.ds(0, copies * rows_in_part), pl.ds(0, half_k)]
        if group == CROSS + 2:
            return cands.at[pl.ds(0, copies)]
        return tw.at[pl.ds(0, copies), pl.ds(0, quarter_units), :]

    def near_tower(target):
        return remote(
            tw_near, tower_send.at[0], near_recv, to=tw.at[f * dim_count + end], dim=target)

    def far_tower(source, target):
        return remote(
            tw_far, tower_send.at[1], tower_recv.at[source],
            to=tower_rows(f * dim_count + source, b), dim=target)

    def pass_in(target):
        return remote(tw_far, tower_send.at[1], tower_recv.at[mid], to=tw_pass, dim=target)

    def pass_on():
        return remote(
            tw_pass, tower_send.at[0], tower_recv.at[end],
            to=tower_rows(f * dim_count + end, b), dim=far)

    def both(z, ff):
        return remote(tw.at[ff * dim_count + z], both_send, both_recv, field=other)

    def bias_copy(target):
        return remote(bias_raw.at[lax.rem(end, 2)], bias_send, bias_recv, dim=target)

    def unit_in(target):
        return remote(unit_raw.at[f * dim_count + end], unit_send, near_unit, dim=target)

    def unit_out(ff, z):
        rows = unit_raw.at[pl.ds(f * dim_count + 2 * side, 2)]
        return remote(rows, unit_send, unit_recv, field=ff, dim=z)

    def two(c, ff):
        lane = pl.multiple_of((1 - part_of) * lanes, lanes)
        return remote(
            y.at[c, :, :, pl.ds(lane, lanes)], two_send, two_recv.at[c],
            to=x2.at[c, pl.ds(ff * fl, fl)], field=other)

    def rows_of(c):
        return pl.ds(pl.multiple_of(c * rc, rc), rc)

    def keep(c):
        return pltpu.make_async_copy(y.at[c, :, within(mid), :], out.at[:, :, rows_of(c)], out_sem)

    def give(c):
        return remote(
            y.at[c, :, within(end), :], give_send, give_recv,
            to=out.at[:, :, rows_of(c)], dim=end)

    def part(c):
        return remote(
            pre_out.at[c], part_send, part_recv.at[c], to=pre_in.at[c], field=other, dim=far)

    def loss_copy(k, c):
        ff, z = (
            (other, far_end), (f, far_end), (other, end), (other, far), (f, end), (f, far), (other, d),
        )[k - 1]
        return remote(
            losses.at[c], loss_send.at[k], loss_recv, to=loss_out.at[c * field_count + part_of],
            field=ff, dim=z)

    def keep_loss(c):
        return pltpu.make_async_copy(losses.at[c], loss_out.at[c * field_count + part_of], loss_send.at[0])

    def own_weight(level, ff):
        return pltpu.make_async_copy(
            weight.at[level, :, ff],
            flat.at[level, :, within(mid), pl.ds(pl.multiple_of(ff * width, width), width)],
            weight_sem.at[level])

    def end_weight(level, k):
        row = pl.multiple_of(lax.rem(b, 2) * rows_in_part, rows_in_part)
        ff = b // 2 * (fields // 2) + k
        to = pl.multiple_of(lax.rem(end, 2) * el + row, rows_in_part)
        return pltpu.make_async_copy(
            weight.at[level, :, ff, pl.ds(row, rows_in_part), :],
            flat.at[level, :, pl.ds(to, rows_in_part), pl.ds(pl.multiple_of(ff * width, width), width)],
            weight_sem.at[level])

    def direct_weight(k):
        start = line_pieces(fl, PIECES)[RELAYED][0]
        row = pl.multiple_of(lax.rem(diagonal, 2) * rows_in_part, rows_in_part)
        ff = diagonal // 2 * (fields // 2) + k
        to = pl.multiple_of(lax.rem(end, 2) * el + row, rows_in_part)
        return pltpu.make_async_copy(
            weight.at[1, pl.ds(start, fl - start), ff, pl.ds(row, rows_in_part), :],
            flat.at[1, pl.ds(start, fl - start), pl.ds(to, rows_in_part),
                    pl.ds(pl.multiple_of(ff * width, width), width)],
            direct_load)

    def each(count, act):
        def step(k, carry):
            act(k)
            return carry

        lax.fori_loop(0, count, step, 0)

    own_features = [
        pltpu.make_async_copy(feat.at[:, :, pl.ds(c * rc, rc)], block(c, f, d), feat_sem.at[c])
        for c in range(chunks)]
    quarter = pl.ds(pl.multiple_of(b * quarter_units, quarter_units), quarter_units)
    small = [
        pltpu.make_async_copy(bias, bias_raw.at[lax.rem(d, 2)], small_sem.at[0]),
        pltpu.make_async_copy(tower_bias, unit_raw.at[me], small_sem.at[1]),
        pltpu.make_async_copy(cand, cands.at[b], small_sem.at[2]),
        pltpu.make_async_copy(tower, tw_raw, small_sem.at[3]),
        pltpu.make_async_copy(query_weight, q_raw, small_sem.at[4]),
        pltpu.make_async_copy(user, users, small_sem.at[5]),
        pltpu.make_async_copy(positive, targets, small_sem.at[6]),
    ]
    barrier = pltpu.get_barrier_semaphore()

    def greet(**where):
        pl.semaphore_signal(barrier, inc=1, device_id=where, device_id_type=MESH)

    @pl.when(is_end)
    def _():
        for ff in range(field_count):
            for z in (1, 2):
                greet(field=ff, dim=z)

    @pl.when(is_mid)
    def _():
        greet(dim=end)
        greet(dim=far)
        greet(batch=x_next)
        greet(batch=y_next)
        greet(field=other, dim=far)
        greet(field=other)

    for copy in own_features:
        copy.start()

    @pl.when(is_end)
    def _():
        each(fields // 2, lambda k: end_weight(0, k).start())

    for copy in small:
        copy.start()

    @pl.when(is_mid)
    def _():
        each(fields, lambda k: own_weight(0, k).start())
        each(fields, lambda k: own_weight(1, k).start())

    @pl.when(is_end)
    def _():
        each(fields // 2, lambda k: end_weight(1, k).start())
        each(fields // 2, lambda k: direct_weight(k).start())

    pl.semaphore_wait(barrier, jnp.where(is_mid, 2 * field_count + 5, 1))

    def loaded_own(level):
        ref = flat.at[level, :, within(mid), :]
        pltpu.make_async_copy(ref, ref, weight_sem.at[level]).wait()

    def loaded_end(level):
        ref = weight_part(level, 0, fl, b)
        pltpu.make_async_copy(ref, ref, weight_sem.at[level]).wait()

    def pack_tower():
        def halves(rows, j):
            first = tw_raw[2 * j, rows, :]
            second = tw_raw[2 * j + 1, rows, :]
            low = jnp.concatenate([first[:, :wide], second[:, :wide]], axis=1)
            high = jnp.concatenate([first[:, wide:], second[:, wide:]], axis=1)
            return low, high

        for j in range(fields // 2):
            low, high = halves(slice(None), j)
            tw_near[:, j * width:(j + 1) * width] = jnp.where(side == 0, low, high)
            low, high = halves(quarter, j)
            tw_far[:, j * width:(j + 1) * width] = jnp.where(side == 0, high, low)
        tw_near[:, side_k:] = q_raw[...]
        tw_far[:, side_k:] = q_raw[quarter, :]

    @pl.when(is_end)
    def _():
        loaded_end(0)
        for p in range(PIECES - 1):
            piece(0, p, mid).start()
        for copy in own_features:
            copy.wait()
        from_end(0, mid).start()
        piece(0, PIECES - 1, mid).start()
        from_end(1, mid).start()
        for copy in small:
            copy.wait()
        bias_copy(mid).start()
        unit_in(mid).start()
        for c in range(2, chunks):
            from_end(c, mid).start()
        pack_tower()
        pass_in(mid).start()
        loaded_end(1)
        for p in range(PIECES):
            piece(1, p, mid).start()
        pltpu.make_async_copy(direct_part(), direct_part(), direct_load).wait()
        for p in range(RELAYED, PIECES):
            direct(p, mid).start()
        near_tower(mid).start()

    def expect_piece(level, p):
        piece(level, p, end).wait_recv()
        plane_out(level * PIECES + p)

    def expect_end(c):
        from_end(c, end).wait_recv()
        cross(1, c, end).start()
        pair(c, end).start()

    def expect_far(k, c, o):
        cross(k, c, o).wait_recv()
        pair(c, o).start()

    def expect_tower(i, z):
        far_tower(z, end).wait_recv()
        plane_out(i)

    def half(source, level, c, ff):
        matrix = flat[level, :, :, pl.ds(pl.multiple_of(ff * half_k, half_k), half_k)]
        return jnp.dot(
            matrix.reshape(fl * wide, half_k), source[c, pl.ds(ff * fl, fl)].reshape(half_k, rc),
            preferred_element_type=jnp.float32)

    def advance(source, level, c, wait_pair):
        product = half(source, level, c, f)
        wait_pair()
        product = product + half(source, level, c, other)
        column = bias_cols[level]
        product = product + jnp.concatenate([column] * (rc // column.shape[1]), axis=1)
        anchor = x0[c, fs, ss, :].astype(jnp.float32).reshape(fl * wide, rc)
        current = source[c, fs, ss, :].astype(jnp.float32).reshape(fl * wide, rc)
        return (anchor * product + current).astype(jnp.bfloat16).reshape(fl, wide, rc)

    def build_bias():
        pick = (lax.broadcasted_iota(jnp.int32, (el, el), 0) == lax.broadcasted_iota(jnp.int32, (el, el), 1))
        for level in range(CROSS):
            for k in range(fl):
                for s in range(2):
                    line = bias_raw[s, k, level:level + 1, :]
                    column = jnp.sum(jnp.where(pick, line, 0.0), axis=1, keepdims=True)
                    start = (2 * k + s) * el
                    bias_cols[level, start:start + el, :] = jnp.broadcast_to(column, (el, width))

    def build_units():
        for m in range(members):
            unit_cols[m * units:(m + 1) * units, :] = jnp.broadcast_to(unit_raw[m], (lanes, units)).T

    def build_users():
        for c in range(chunks):
            start = pl.multiple_of(c * rc + part_of * lanes, lanes)
            user_cols[c] = users[pl.ds(start, lanes), :].astype(jnp.float32).T

    def build_queries():
        for m in range(members):
            block = tw[m, :, side_k:].astype(jnp.float32).T
            query_cols[:, m * units:(m + 1) * units] = block.astype(jnp.bfloat16)

    def first(c, carry):
        @pl.when(c == 1)
        def _():
            pass_in(end).wait_recv()
            pass_on().start()

        @pl.when(c == 2)
        def _():
            expect_far(1, 2, far_end)
            plane_forward(FAR_TOWER)
            expect_piece(1, 0)

        @pl.when(c == 3)
        def _():
            expect_far(1, 3, far_end)
            expect_piece(1, 1)

        def wait_pair():
            landed(x0.at[c, fs], pair_recv.at[c])

        x1[c, fs, ss, :] = advance(x0, 0, c, wait_pair)
        cross_one(c, side).start()
        pair_one(c, side).start()
        return carry

    def tower_part(c):
        matrix = tw[:, :, :side_k].reshape(members * units, side_k)
        return jnp.dot(matrix, x2[c].reshape(side_k, lanes), preferred_element_type=jnp.float32)

    def expect_one(c):
        cross_one(c, 1 - side).wait_recv()
        pair_one(c, 1 - side).start()

    def layer_two(c):
        def wait_pair():
            landed(x1.at[c, fs], one_recv.at[c])

        y[c] = advance(x1, 1, c, wait_pair)
        two(c, f).start()
        give(c).start()
        keep(c).start()
        for k in range(2):
            @pl.when(part_of == k)
            def _():
                x2[c, fs] = y[c, :, :, k * lanes:(k + 1) * lanes]

    def layer_three(c):
        two(c, other).wait_recv()
        pre = tower_part(c)

        @pl.when(owner)
        def _():
            pre_own[c] = pre + unit_cols[...]

        @pl.when(giver)
        def _():
            pre_out[c] = pre.astype(jnp.bfloat16)
            part(c).start()

    def second(c, carry):
        layer_two(c)

        @pl.when(c == 1)
        def _():
            near_tower(end).wait_recv()
            both(end, f).start()
            expect_one(2)
            landed(tw.at[pl.ds(0, dim_count)], both_recv)

        def tower_step(k, carry):
            layer_three(k)
            return carry

        last = c == chunks - 1
        lax.fori_loop(
            jnp.where(last, c, jnp.maximum(c - 1, 0)), jnp.where(c < chunks - 2, c, c + 1),
            tower_step, 0)

        @pl.when(c == 2)
        def _():
            expect_one(3)

        return carry

    def finish(c):
        part(c).wait_recv()
        pre = pre_own[c] + pre_in[c].astype(jnp.float32)
        hidden = jnp.maximum(pre, 0.0).astype(jnp.bfloat16)
        query = jnp.dot(query_cols[...], hidden, preferred_element_type=jnp.float32)
        query_vec = (query + user_cols[c]).astype(jnp.bfloat16)
        logits = jnp.dot(
            cands[...].reshape(-1, width), query_vec,
            preferred_element_type=jnp.float32) * (1.0 / math.sqrt(width))
        labels = lax.broadcasted_iota(jnp.int32, logits.shape, 0)
        target = targets[c * field_count + part_of]
        picked = jnp.sum(jnp.where(labels == target, logits, 0.0), axis=0, keepdims=True)
        best = jnp.max(logits, axis=0, keepdims=True)
        total = jnp.sum(jnp.exp(logits - best), axis=0, keepdims=True)
        losses[c] = best + jnp.log(total) - picked
        for k in range(1, members):
            loss_copy(k, c).start()
        keep_loss(c).start()

    @pl.when(is_mid)
    def _():
        for c in range(chunks):
            own_features[c].wait()
            cross(0, c, mid).start()
            pair(c, mid).start()
        for copy in small:
            copy.wait()
        plane_out(CANDS)
        pack_tower()
        far_tower(d, far).start()
        tw[me] = tw_near[...]
        both(mid, f).start()
        expect_piece(0, 0)
        expect_far(0, 0, far)
        expect_piece(0, 1)
        expect_far(0, 1, far)
        plane_forward(CANDS)
        expect_piece(0, 2)
        expect_far(0, 2, far)
        plane_forward(0)
        plane_forward(1)
        expect_far(0, 3, far)
        expect_end(0)
        expect_piece(0, 3)
        plane_forward(2)
        expect_end(1)
        plane_forward(3)
        expect_far(1, 0, far_end)
        expect_tower(FAR_TOWER, far)
        bias_copy(end).wait_recv()
        build_bias()
        unit_in(end).wait_recv()
        unit_out(other, d).start()
        unit_out(f, far).start()
        unit_out(other, far).start()
        for level in range(CROSS):
            loaded_own(level)
        expect_end(2)
        plane_rest(0)
        expect_far(1, 1, far_end)
        expect_end(3)
        lax.fori_loop(0, chunks, first, 0)
        plane_rest(4)
        plane_rest(2)
        both(far, f).start()
        expect_piece(1, 2)
        expect_piece(1, 3)
        expect_tower(END_TOWER, far_end)
        for p in range(RELAYED):
            plane_forward(PIECES + p)
        expect_one(0)
        plane_forward(END_TOWER)
        for p in range(RELAYED, PIECES):
            plane_keep(PIECES + p)
        expect_one(1)
        landed(unit_raw.at[pl.ds(0, 6)], unit_recv)
        build_units()
        build_users()
        plane_rest(3)
        both(far_end, f).start()
        landed(direct_part(), direct_recv)
        plane_rest(1)
        lax.fori_loop(0, chunks, second, 0)

        @pl.when(owner)
        def _():
            build_queries()
            for c in range(chunks):
                finish(c)

    @pl.when(owner)
    def _():
        landed(losses, loss_recv)

    @pl.when(jnp.logical_not(owner))
    def _():
        landed(loss_out, loss_recv)

    @pl.when(is_end)
    def _():
        for level in range(CROSS):
            sent(weight_part(level, 0, fl, b), piece_send.at[level])
        sent(direct_part(), direct_send)
        sent(x0.at[:, fs, entries(d), :], end_send)
        bias_copy(mid).wait_send()
        near_tower(mid).wait_send()
        pass_in(mid).wait_send()
        unit_in(mid).wait_send()
        landed(out, give_recv)

    @pl.when(is_mid)
    def _():
        far_tower(d, far).wait_send()
        pass_on().wait_send()
        sent(tw.at[pl.ds(0, dim_count)], both_send)
        sent(unit_raw.at[pl.ds(0, 6)], unit_send)
        sent(x0.at[:, fs, entries(mid), :], cross_send.at[0])
        sent(x0.at[:, fs, entries(end), :], cross_send.at[1])
        sent(x1.at[:, fs, ss, :], cross_send.at[2])
        sent(x0.at[:, fs], pair_send)
        sent(x1.at[:, fs], one_send)
        sent(y.at[:, :, :, pl.ds(0, lanes)], two_send)
        sent(out, give_send)
        pltpu.make_async_copy(out, out, out_sem).wait()
        for group in range(CROSS + 3):
            sent(plane_bytes(group, 3), plane_send.at[group])

    @pl.when(giver)
    def _():
        sent(pre_out, part_send)

    @pl.when(owner)
    def _():
        for k in range(1, members):
            sent(losses, loss_send.at[k])
        pltpu.make_async_copy(losses, losses, loss_send.at[0]).wait()


def emit_kernel(crossed, losses, crossed_out, losses_out, sems):
    copies = [
        pltpu.make_async_copy(crossed, crossed_out, sems.at[0]),
        pltpu.make_async_copy(losses, losses_out, sems.at[1]),
    ]
    for copy in copies:
        copy.start()
    for copy in copies:
        copy.wait()


def line_body(
    counts, features, cross_weight, cross_bias, tower_weight, tower_bias, query_weight,
    user_vec, candidates, positive,
):
    batch_count, field_count, dim_count = counts
    members = field_count * dim_count
    fl, el, row_count = features.shape
    units, fields, width = tower_weight.shape
    rc = row_count // CHUNKS
    lanes = rc // field_count
    wide = 2 * el
    quarter = units // batch_count
    packed = fields * wide + width
    items = CANDS + 1
    dma = pltpu.SemaphoreType.DMA
    vmem = pltpu.VMEM
    bf16 = jnp.bfloat16
    f32 = jnp.float32
    far = pl.BlockSpec(memory_space=pl.ANY)
    crossed, losses = pl.pallas_call(
        functools.partial(line_kernel, counts),
        out_shape=(
            jax.ShapeDtypeStruct(features.shape, bf16),
            jax.ShapeDtypeStruct((CHUNKS * field_count, 1, lanes), f32),
        ),
        in_specs=[far] * 9,
        out_specs=(far, far),
        scratch_shapes=[
            vmem((CHUNKS, fields, width, rc), bf16),
            vmem((CHUNKS, fields, width, rc), bf16),
            vmem((CHUNKS, fl, wide, rc), bf16),
            vmem((CHUNKS, fields, wide, lanes), bf16),
            vmem((CROSS, fl, wide, fields * width), bf16),
            vmem((members, units, packed), bf16),
            vmem((units, packed), bf16),
            vmem((quarter, packed), bf16),
            vmem((quarter, packed), bf16),
            vmem((fields, units, width), bf16),
            vmem((units, width), bf16),
            vmem((CHUNKS, members * units, lanes), bf16),
            vmem((CHUNKS, members * units, lanes), bf16),
            vmem((CHUNKS, members * units, lanes), f32),
            vmem((2, fl, CROSS, el), f32),
            vmem((CROSS, fl * wide, width), f32),
            vmem((members, 1, units), f32),
            vmem((members * units, lanes), f32),
            vmem((width, members * units), bf16),
            vmem((batch_count,) + candidates.shape, bf16),
            vmem(user_vec.shape, bf16),
            vmem((CHUNKS, width, lanes), f32),
            vmem((CHUNKS * field_count, 1, lanes), jnp.int32),
            vmem((CHUNKS, 1, lanes), f32),
            dma((CHUNKS,)), dma((CROSS,)), dma((7,)),
            dma, dma((CHUNKS,)), dma((3,)), dma((3, CHUNKS)),
            dma, dma((CHUNKS,)), dma, dma((CHUNKS,)),
            dma((CROSS,)), dma((CROSS, PIECES)), dma, dma, dma, dma((CROSS + 3,)), dma((items,)), dma((CROSS + 3,)),
            dma((2,)), dma((dim_count,)), dma, dma, dma,
            dma, dma, dma, dma, dma,
            dma, dma((CHUNKS,)), dma, dma, dma, dma, dma((CHUNKS,)), dma((members,)), dma,
        ],
        compiler_params=pltpu.CompilerParams(
            collective_id=0, has_side_effects=True, vmem_limit_bytes=48 * 2**20),
        name="line_forward",
    )(*(pltpu.with_memory_space_constraint(value, pltpu.HBM) for value in (
        features,
        cross_weight.transpose(0, 1, 3, 2, 4),
        cross_bias.transpose(1, 0, 2),
        tower_weight.transpose(1, 0, 2),
        tower_bias.reshape(1, units),
        query_weight,
        user_vec,
        candidates,
        positive.reshape(CHUNKS * field_count, 1, lanes),
    )))
    crossed, losses = pl.pallas_call(
        emit_kernel,
        out_shape=(
            jax.ShapeDtypeStruct(features.shape, bf16),
            jax.ShapeDtypeStruct((CHUNKS * field_count, 1, lanes), f32),
        ),
        in_specs=[far] * 2,
        out_specs=(pl.BlockSpec(memory_space=pltpu.HBM),) * 2,
        scratch_shapes=[dma((2,))],
        compiler_params=pltpu.CompilerParams(vmem_limit_bytes=4 * 2**20),
        name="emit",
    )(crossed, losses)
    return (crossed, losses.reshape(row_count))


def body(
    features, cross_weight, cross_bias, tower_weight, tower_bias, query_weight,
    user_vec, candidates, positive,
):
    counts = tuple(lax.axis_size(name) for name in ("batch", "field", "dim"))
    if line_fits(counts, features, tower_weight, candidates):
        return line_body(
            counts, features, cross_weight, cross_bias, tower_weight, tower_bias, query_weight,
            user_vec, candidates, positive)
    batch_count, field_count, dim_count = counts
    members = field_count * dim_count
    fl, el, row_count = features.shape
    columns = fl * el
    units, fields, width = tower_weight.shape
    low, held = tower_levels(dim_count)
    chunks = chunk_count(row_count, field_count, held)
    split = batch_count if units % (batch_count * 16) == 0 else 1
    part = units // split
    rc = row_count // chunks
    sub = rc // held
    run = chunks // field_count
    share = run * sub
    steps = (CROSS, chunks, dim_count)
    small = (3, dim_count)
    dma = pltpu.SemaphoreType.DMA
    vmem = pltpu.VMEM
    bf16 = jnp.bfloat16
    far = pl.BlockSpec(memory_space=pl.ANY)
    near = pl.BlockSpec(memory_space=pltpu.VMEM)
    crossed, losses = pl.pallas_call(
        functools.partial(rank_kernel, counts, (chunks, split)),
        out_shape=(
            jax.ShapeDtypeStruct(features.shape, bf16),
            jax.ShapeDtypeStruct((chunks * held, 1, sub), jnp.float32),
        ),
        in_specs=[far, far, near, far, far, far, near, far, near],
        out_specs=(near, near),
        scratch_shapes=[
            vmem((chunks, fields, width, rc), bf16),
            vmem((chunks, fields, width, rc), bf16),
            vmem((CROSS, fl, el, fields * width), bf16),
            vmem((chunks, held, fl, el, sub), bf16),
            vmem((fields, width, share), bf16),
            vmem((split, members, part, fields * width), bf16),
            vmem((members, 1, units), jnp.float32),
            vmem((split, members, part, share), jnp.float32),
            vmem((split, members, part, width), bf16),
            vmem((batch_count,) + candidates.shape, bf16),
            vmem((held, chunks, 1, sub), jnp.float32),
            dma((chunks,)), dma((CROSS, fields)), dma((fields,)), dma((3,)),
            dma(steps), dma(steps), dma(steps), dma(steps), dma(steps),
            dma((chunks, held)), dma((run, members)), dma(small), dma(small), dma(small),
            dma((3,)), dma((3,)),
            dma((split,)), dma((split,)), dma((split,)), dma((split,)),
            dma((batch_count,)), dma((batch_count,)), dma((members,)), dma((field_count, held)),
        ],
        compiler_params=pltpu.CompilerParams(
            collective_id=0, has_side_effects=True, vmem_limit_bytes=56 * 2**20),
        name="rank_forward",
    )(
        features,
        cross_weight.transpose(0, 1, 3, 2, 4),
        cross_bias.reshape(CROSS, columns, 1),
        tower_weight.transpose(1, 0, 2),
        tower_bias.reshape(1, units),
        query_weight.reshape(split, part, width),
        user_vec,
        candidates,
        positive.reshape(chunks * held, 1, sub),
    )
    return (crossed, losses.reshape(row_count))


def solution(mesh):
    placed = (
        P("field", "dim", "batch"),
        P(None, "field", "dim", None, None),
        P(None, "field", "dim"),
        P(("field", "dim"), None, None),
        P(("field", "dim")),
        P(("field", "dim"), None),
        P("batch", None),
        P("batch", None),
        P("batch"),
    )
    return jax.shard_map(
        body,
        mesh=mesh,
        in_specs=placed,
        out_specs=(P("field", "dim", "batch"), P("batch")),
        check_vma=False,
    )
```

```python
import functools
import math

import jax
import jax.numpy as jnp
from jax import lax
from jax.experimental import pallas as pl
from jax.experimental.pallas import tpu as pltpu
from jax.sharding import PartitionSpec as P

CROSS = 2
MESH = pl.DeviceIdType.MESH


def tower_levels(dim_count):
    held = min(2, dim_count)
    return (dim_count - held) // 2, held


def chunk_count(row_count, field_count, held):
    chunks = 2
    while chunks > field_count and row_count % (chunks * held * 128):
        chunks //= 2
    return chunks


def rank_kernel(
    counts, splits,
    feat, weight, bias, tower, tower_bias, query_weight, user, cand, positive,
    out, loss_out,
    x0, x1, flat, sent, rows, towers, biases, columns_bias, queries, cands, losses,
    feat_sem, weight_sem, tower_sem, small_sem,
    right_sem, left_sem, pair_sem, recv_sem, pair_recv,
    row_send, row_recv, chain_right, chain_left, chain_recv, both_send, both_recv,
    plane_send, plane_recv, plane_pair, plane_pair_recv,
    cand_send, cand_recv, loss_send, loss_recv,
):
    batch_count, field_count, dim_count = counts
    chunks, split = splits
    b = lax.axis_index("batch")
    f = lax.axis_index("field")
    d = lax.axis_index("dim")
    me = f * dim_count + d
    members = field_count * dim_count
    fl, el, row_count = feat.shape
    columns = fl * el
    fields, width, rc = x0.shape[1:]
    low, held = tower_levels(dim_count)
    high = low + held - 1
    level_of = d - low
    active = (d >= low) & (d <= high)
    sub = rc // held
    run = chunks // field_count
    share = run * sub
    part = towers.shape[2]
    units = split * part
    buffers = (x0, x1)
    other = field_count - 1 - f
    mine = b if split > 1 else 0
    to_right = jnp.minimum(d + 1, dim_count - 1)
    to_left = jnp.maximum(d - 1, 0)

    def remote(ref, send, recv, **where):
        return pltpu.make_async_remote_copy(
            ref, ref, send, recv, device_id=where, device_id_type=MESH)

    def place(ff, o):
        return pl.ds(ff * fl, fl), pl.ds(pl.multiple_of(o * el, el), el)

    def piece(ph, c, ff, o):
        fs, ds = place(ff, o)
        return buffers[ph].at[c, fs, ds, :]

    def right(ph, c, o):
        return remote(piece(ph, c, f, o), right_sem.at[ph, c, o], recv_sem.at[ph, c, o], dim=to_right)

    def left(ph, c, o):
        return remote(piece(ph, c, f, o), left_sem.at[ph, c, o], recv_sem.at[ph, c, o], dim=to_left)

    def pair(ph, c, o, ff):
        return remote(
            piece(ph, c, ff, o), pair_sem.at[ph, c, o], pair_recv.at[ph, c, o], field=other)

    def issue_own(ph, c):
        @pl.when(d < dim_count - 1)
        def _():
            right(ph, c, d).start()

        @pl.when(d > 0)
        def _():
            left(ph, c, d).start()

        pair(ph, c, d, f).start()

    def forwards(ph, c):
        for s in range(1, dim_count):
            @pl.when(d - s >= 0)
            def _():
                right(ph, c, d - s).wait_recv()

                @pl.when(d < dim_count - 1)
                def _():
                    right(ph, c, d - s).start()

                pair(ph, c, d - s, f).start()

            @pl.when(d + s < dim_count)
            def _():
                left(ph, c, d + s).wait_recv()

                @pl.when(d > 0)
                def _():
                    left(ph, c, d + s).start()

                pair(ph, c, d + s, f).start()
        for o in range(dim_count):
            pair(ph, c, o, other).wait_recv()

    def weight_copy(level, ff):
        return pltpu.make_async_copy(
            weight.at[level, :, ff],
            flat.at[level, :, :, pl.ds(pl.multiple_of(ff * width, width), width)],
            weight_sem.at[level, ff])

    def tower_copy(ff):
        return pltpu.make_async_copy(
            tower.at[ff, pl.ds(pl.multiple_of(mine * part, part), part), :],
            towers.at[mine, me, :, pl.ds(pl.multiple_of(ff * width, width), width)],
            tower_sem.at[ff])

    def each_field(act):
        def step(ff, carry):
            act(ff)
            return carry

        lax.fori_loop(0, fields, step, 0)

    small_refs = (
        lambda o: towers.at[mine, f * dim_count + o],
        lambda o: queries.at[:, f * dim_count + o],
        lambda o: biases.at[f * dim_count + o],
    )
    small_wide = (
        lambda ff: towers.at[mine, pl.ds(ff * dim_count, dim_count)],
        lambda ff: queries.at[:, pl.ds(ff * dim_count, dim_count)],
        lambda ff: biases.at[pl.ds(ff * dim_count, dim_count)],
    )

    def chain_to(k, o, sems, target):
        return remote(small_refs[k](o), sems.at[k, o], chain_recv.at[k, o], dim=target)

    def chain_own():
        for k in range(3):
            @pl.when(d < high)
            def _():
                chain_to(k, d, chain_right, to_right).start()

            @pl.when(d > low)
            def _():
                chain_to(k, d, chain_left, to_left).start()

    def chain_step(s):
        for k in range(3):
            @pl.when((d - s >= 0) & (d <= high))
            def _():
                chain_to(k, d - s, chain_right, to_right).wait_recv()

                @pl.when(d < high)
                def _():
                    chain_to(k, d - s, chain_right, to_right).start()

            @pl.when((d + s < dim_count) & (d >= low))
            def _():
                chain_to(k, d + s, chain_left, to_left).wait_recv()

                @pl.when(d > low)
                def _():
                    chain_to(k, d + s, chain_left, to_left).start()

    def both(k, ff):
        return remote(small_wide[k](ff), both_send.at[k], both_recv.at[k], field=other)

    def plane(t, source):
        return remote(
            towers.at[source, pl.ds(f * dim_count, dim_count)],
            plane_send.at[t], plane_recv.at[source], batch=t)

    def plane_both(source, ff):
        return remote(
            towers.at[source, pl.ds(ff * dim_count, dim_count)],
            plane_pair.at[source], plane_pair_recv.at[source], field=other)

    def cand_copy(t, source):
        return remote(cands.at[source], cand_send.at[t], cand_recv.at[source], batch=t)

    def loss_copy(m, ff, level):
        ref = losses.at[level, pl.ds(ff * run, run)]
        return remote(
            ref, loss_send.at[m], loss_recv.at[ff, level], field=m // dim_count, dim=m % dim_count)

    def row_copy(c, level):
        fs, ds = place(f, d)
        return pltpu.make_async_remote_copy(
            sent.at[c, level],
            rows.at[fs, ds, pl.ds(pl.multiple_of(lax.rem(c, run) * sub, sub), sub)],
            row_send.at[c, level], row_recv.at[lax.rem(c, run), me],
            device_id={"field": c // run, "dim": low + level}, device_id_type=MESH)

    def own_rows(c, level):
        return (c // run == f) & (level_of == level)

    def advance(ph, c):
        whole = buffers[ph][c].reshape(fields * width, rc)
        matrix = flat[ph].reshape(columns, fields * width)
        product = jnp.dot(matrix, whole, preferred_element_type=jnp.float32) + bias[ph]
        fs, ds = place(f, d)
        anchor = x0[c, fs, ds, :].astype(jnp.float32).reshape(columns, rc)
        current = buffers[ph][c, fs, ds, :].astype(jnp.float32).reshape(columns, rc)
        return (anchor * product + current).astype(jnp.bfloat16).reshape(fl, el, rc)

    own_copies = []
    for c in range(chunks):
        own_copies.append(pltpu.make_async_copy(
            feat.at[:, :, pl.ds(c * rc, rc)], piece(0, c, f, d), feat_sem.at[c]))
    small_copies = [
        pltpu.make_async_copy(query_weight, queries.at[:, me], small_sem.at[0]),
        pltpu.make_async_copy(tower_bias, biases.at[me], small_sem.at[1]),
        pltpu.make_async_copy(cand, cands.at[b], small_sem.at[2]),
    ]
    for copy in own_copies + small_copies:
        copy.start()
    each_field(lambda ff: tower_copy(ff).start())
    for level in range(CROSS):
        each_field(lambda ff: weight_copy(level, ff).start())

    barrier = pltpu.get_barrier_semaphore()
    for k in range(1, members):
        m = lax.rem(me + k, members)
        pl.semaphore_signal(
            barrier, inc=1, device_id={"field": m // dim_count, "dim": m % dim_count},
            device_id_type=MESH)
    for k in range(1, batch_count):
        pl.semaphore_signal(
            barrier, inc=1, device_id={"batch": lax.rem(b + k, batch_count)}, device_id_type=MESH)
    pl.semaphore_wait(barrier, members + batch_count - 2)
    for copy in own_copies:
        copy.wait()
    issue_own(0, 0)
    if chunks > 1:
        issue_own(0, 1)
    each_field(lambda ff: tower_copy(ff).wait())
    for copy in small_copies:
        copy.wait()
    chain_own()

    @pl.when(active)
    def _():
        for k in range(1, batch_count):
            cand_copy(lax.rem(b + k, batch_count), b).start()

    for level in range(CROSS):
        each_field(lambda ff: weight_copy(level, ff).wait())

    def first(c, carry):
        @pl.when(c + 2 < chunks)
        def _():
            issue_own(0, c + 2)

        forwards(0, c)
        fs, ds = place(f, d)
        x1[c, fs, ds, :] = advance(0, c)
        issue_own(1, c)

        for s in range(1, min(chunks, dim_count)):
            @pl.when(c == s)
            def _():
                chain_step(s)

        return carry

    lax.fori_loop(0, chunks, first, 0)
    for s in range(min(chunks, dim_count), dim_count):
        chain_step(s)

    @pl.when(active)
    def _():
        for k in range(3):
            both(k, f).start()
        if split > 1:
            for k in range(1, split):
                plane(lax.rem(b + k, split), b).start()

    def second(c, carry):
        forwards(1, c)
        new = advance(1, c)
        out[:, :, pl.ds(pl.multiple_of(c * rc, 128), rc)] = new
        for level in range(held):
            block = new[:, :, level * sub:(level + 1) * sub]

            @pl.when(own_rows(c, level))
            def _():
                fs, ds = place(f, d)
                rows[fs, ds, pl.ds(pl.multiple_of(lax.rem(c, run) * sub, sub), sub)] = block

            @pl.when(jnp.logical_not(own_rows(c, level)))
            def _():
                sent[c, level] = block
                row_copy(c, level).start()

        return carry

    lax.fori_loop(0, chunks, second, 0)

    def tower_block(s, query):
        matrix = towers[s].reshape(members * part, fields * width)
        pre = jnp.dot(
            matrix, rows[...].reshape(fields * width, share), preferred_element_type=jnp.float32)
        pre = pre + columns_bias[s].reshape(members * part, share)
        hidden = jnp.maximum(pre, 0.0).astype(jnp.bfloat16)
        return query + lax.dot_general(
            hidden, queries[s].reshape(members * part, width), (((0,), (0,)), ((), ())),
            preferred_element_type=jnp.float32)

    @pl.when(active)
    def _():
        if split > 1:
            for k in range(1, split):
                source = lax.rem(b + k, split)
                plane(source, source).wait_recv()
                plane_both(source, f).start()
        for k in range(3):
            both(k, other).wait_recv()
        for k in range(1, batch_count):
            source = lax.rem(b + k, batch_count)
            cand_copy(source, source).wait_recv()
        for m in range(members):
            block = jnp.broadcast_to(biases[m], (share, units)).T
            columns_bias[:, m] = block.reshape(split, part, share)
        if split > 1:
            for k in range(1, split):
                plane_both(lax.rem(b + k, split), other).wait_recv()
        for j in range(run):
            for k in range(1, members):
                m = lax.rem(me + k, members)
                fs, ds = place(m // dim_count, m % dim_count)
                remote(rows.at[fs, ds, pl.ds(j * sub, sub)], row_send.at[0, 0], row_recv.at[j, m],
                       field=m // dim_count, dim=m % dim_count).wait_recv()

        query = lax.fori_loop(0, split, tower_block, jnp.zeros((share, width), jnp.float32))
        all_cands = cands[...].reshape(-1, width)
        for j in range(run):
            c = f * run + j
            start = pl.multiple_of(c * rc + level_of * sub, sub)
            query_vec = (
                query[j * sub:(j + 1) * sub] + user[pl.ds(start, sub), :].astype(jnp.float32)
            ).astype(jnp.bfloat16)
            logits = lax.dot_general(
                all_cands, query_vec, (((1,), (1,)), ((), ())), preferred_element_type=jnp.float32
            ) * (1.0 / math.sqrt(width))
            labels = lax.broadcasted_iota(jnp.int32, logits.shape, 0)
            target = positive[c * held + level_of]
            picked = jnp.sum(jnp.where(labels == target, logits, 0.0), axis=0, keepdims=True)
            best = jnp.max(logits, axis=0, keepdims=True)
            total = jnp.sum(jnp.exp(logits - best), axis=0, keepdims=True)
            losses[level_of, c] = best + jnp.log(total) - picked
        for k in range(1, members):
            loss_copy(lax.rem(me + k, members), f, level_of).start()

    def drain(c, carry):
        for ph in range(CROSS):
            for o in range(dim_count):
                @pl.when((o <= d) & (d < dim_count - 1))
                def _():
                    right(ph, c, o).wait_send()

                @pl.when((o >= d) & (d > 0))
                def _():
                    left(ph, c, o).wait_send()

                pair(ph, c, o, f).wait_send()
        return carry

    lax.fori_loop(0, chunks, drain, 0)
    for k in range(3):
        for o in range(dim_count):
            @pl.when((o <= d) & (d < high))
            def _():
                chain_to(k, o, chain_right, to_right).wait_send()

            @pl.when((o >= d) & (d > low))
            def _():
                chain_to(k, o, chain_left, to_left).wait_send()

    @pl.when(active)
    def _():
        for k in range(3):
            both(k, f).wait_send()
        if split > 1:
            for k in range(1, split):
                t = lax.rem(b + k, split)
                plane(t, b).wait_send()
                plane_both(t, f).wait_send()
        for k in range(1, batch_count):
            cand_copy(lax.rem(b + k, batch_count), b).wait_send()
        for k in range(1, members):
            loss_copy(lax.rem(me + k, members), f, level_of).wait_send()

    for c in range(chunks):
        for level in range(held):
            @pl.when(jnp.logical_not(own_rows(c, level)))
            def _():
                row_copy(c, level).wait_send()

    for ff in range(field_count):
        for level in range(held):
            @pl.when(jnp.logical_not((f == ff) & (level_of == level)))
            def _():
                loss_copy(ff * dim_count + low + level, ff, level).wait_recv()

    for c in range(chunks):
        for level in range(held):
            loss_out[c * held + level] = losses[level, c]


def line_pieces(count, parts):
    base, extra = divmod(count, parts)
    bounds, start = [], 0
    for k in range(parts):
        size = base + (k < extra)
        bounds.append((start, size))
        start += size
    return bounds


def line_fits(counts, features, tower_weight, candidates):
    batch_count, field_count, dim_count = counts
    fl, el, row_count = features.shape
    units, fields, width = tower_weight.shape
    relayed = line_pieces(fl, PIECES)[RELAYED][0]
    return (
        (fl + relayed) % 2 == 0 and (2 * fl + relayed) % 3 == 0 and
        dim_count == 4 and batch_count == 4 and field_count == 2
        and fields % 2 == 0 and fl >= PIECES and el % 32 == 0 and 4 * el == width and width == 128
        and row_count % (CHUNKS * field_count * 128) == 0 and units % (16 * batch_count) == 0)


PIECES = 4
RELAYED = 2
CHUNKS = 4
FAR_TOWER = CROSS * PIECES
END_TOWER = FAR_TOWER + 1
CANDS = END_TOWER + 1


def line_kernel(
    counts,
    feat, weight, bias, tower, tower_bias, query_weight, user, cand, positive,
    out, loss_out,
    x0, x1, y, x2, flat, tw, tw_near, tw_far, tw_pass, tw_raw, q_raw, pre_out, pre_in, pre_own,
    bias_raw, bias_cols, unit_raw, unit_cols, query_cols, cands, users, user_cols, targets, losses,
    feat_sem, weight_sem, small_sem,
    end_send, end_recv, cross_send, cross_recv, pair_send, pair_recv, one_send, one_recv,
    piece_send, piece_recv, direct_load, direct_send, direct_recv, plane_send, plane_recv, rest_recv,
    tower_send, tower_recv, near_recv, both_send, both_recv,
    bias_send, bias_recv, unit_send, unit_recv, near_unit,
    two_send, two_recv, out_sem, give_send, give_recv, part_send, part_recv, loss_send, loss_recv,
):
    batch_count, field_count, dim_count = counts
    b = lax.axis_index("batch")
    f = lax.axis_index("field")
    d = lax.axis_index("dim")
    members = field_count * dim_count
    me = f * dim_count + d
    chunks, fields, width, rc = x0.shape
    fl, el, _ = feat.shape
    wide = 2 * el
    half_k = fields // 2 * width
    quarter_units = tw_far.shape[0]
    units = tw.shape[1]
    side_k = fields * wide
    lanes = rc // field_count
    rows_in_part = el // 2
    side = d // 2
    mid = 1 + side
    far = 2 - side
    end = 3 * side
    far_end = 3 - end
    is_mid = d == mid
    is_end = d == end
    owner = is_mid & (f == 1)
    giver = is_mid & (f == 0)
    part_of = jnp.where(f == 1, side, 1 - side)
    other = field_count - 1 - f
    x_next = b + 1 - 2 * lax.rem(b, 2)
    y_next = lax.rem(b + 2, 4)
    diagonal = 3 - b
    fs = pl.ds(f * fl, fl)
    ss = pl.ds(pl.multiple_of(side * wide, wide), wide)

    def remote(ref, send, recv, to=None, **where):
        return pltpu.make_async_remote_copy(
            ref, ref if to is None else to, send, recv, device_id=where, device_id_type=MESH)

    def sent(ref, sem):
        remote(ref, sem, sem, field=other).wait_send()

    def landed(ref, sem):
        remote(ref, sem, sem, field=other).wait_recv()

    def entries(o):
        return pl.ds(pl.multiple_of(o * el, el), el)

    def within(o):
        return pl.ds(pl.multiple_of(lax.rem(o, 2) * el, el), el)

    def block(c, ff, o):
        return x0.at[c, pl.ds(ff * fl, fl), entries(o), :]

    def from_end(c, target):
        return remote(block(c, f, end), end_send, end_recv.at[c], dim=target)

    def cross(k, c, o):
        return remote(block(c, f, o), cross_send.at[k], cross_recv.at[k, c], dim=far)

    def cross_one(c, s):
        ref = x1.at[c, fs, pl.ds(pl.multiple_of(s * wide, wide), wide), :]
        return remote(ref, cross_send.at[2], cross_recv.at[2, c], dim=far)

    def pair(c, o):
        return remote(block(c, f, o), pair_send, pair_recv.at[c], field=other)

    def pair_one(c, s):
        ref = x1.at[c, fs, pl.ds(pl.multiple_of(s * wide, wide), wide), :]
        return remote(ref, one_send, one_recv.at[c], field=other)

    def weight_piece(level, p, source):
        start, size = line_pieces(fl, PIECES)[p]
        return weight_part(level, start, size, source)

    def weight_part(level, start, size, source):
        row = pl.multiple_of(lax.rem(end, 2) * el + lax.rem(source, 2) * rows_in_part, rows_in_part)
        lane = pl.multiple_of(source // 2 * half_k, half_k)
        return flat.at[level, pl.ds(start, size), pl.ds(row, rows_in_part), pl.ds(lane, half_k)]

    def piece(level, p, target):
        ref = weight_piece(level, p, b)
        return remote(ref, piece_send.at[level], piece_recv.at[level, p], dim=target)

    def direct(p, target):
        ref = weight_piece(1, p, diagonal)
        return remote(ref, direct_send, direct_recv, dim=target)

    def direct_part():
        start = line_pieces(fl, PIECES)[RELAYED][0]
        return weight_part(1, start, fl - start, diagonal)

    def tower_rows(member, source):
        return tw.at[member, pl.ds(pl.multiple_of(source * quarter_units, quarter_units), quarter_units), :]

    def item(i, source):
        if i < CROSS * PIECES:
            return weight_piece(i // PIECES, i % PIECES, source)
        if i == CANDS:
            return cands.at[source]
        return tower_rows(f * dim_count + (far if i == FAR_TOWER else far_end), source)

    def relay(i):
        return (x_next, y_next) if i % 2 == 0 else (y_next, x_next)

    def group_of(i):
        return i // PIECES if i < FAR_TOWER else CROSS + i - FAR_TOWER

    def plane(i, source, target, arrival):
        return remote(item(i, source), plane_send.at[group_of(i)], arrival, batch=target)

    def plane_out(i):
        first, second = relay(i)
        plane(i, b, first, plane_recv.at[i]).start()
        plane(i, b, second, rest_recv.at[group_of(i)]).start()

    def plane_forward(i):
        source, target = relay(i)
        plane(i, source, target, plane_recv.at[i]).wait_recv()
        plane(i, source, target, rest_recv.at[group_of(i)]).start()

    def plane_keep(i):
        source, target = relay(i)
        plane(i, source, target, plane_recv.at[i]).wait_recv()

    def plane_rest(group):
        landed(plane_bytes(group, 2), rest_recv.at[group])

    def plane_bytes(group, copies):
        if group == 1:
            total = (copies - 1) * fl + line_pieces(fl, PIECES)[RELAYED][0]
            return flat.at[1, pl.ds(0, total // copies), pl.ds(0, copies * rows_in_part), pl.ds(0, half_k)]
        if group < CROSS:
            return flat.at[group, :, pl.ds(0, copies * rows_in_part), pl.ds(0, half_k)]
        if group == CROSS + 2:
            return cands.at[pl.ds(0, copies)]
        return tw.at[pl.ds(0, copies), pl.ds(0, quarter_units), :]

    def near_tower(target):
        return remote(
            tw_near, tower_send.at[0], near_recv, to=tw.at[f * dim_count + end], dim=target)

    def far_tower(source, target):
        return remote(
            tw_far, tower_send.at[1], tower_recv.at[source],
            to=tower_rows(f * dim_count + source, b), dim=target)

    def pass_in(target):
        return remote(tw_far, tower_send.at[1], tower_recv.at[mid], to=tw_pass, dim=target)

    def pass_on():
        return remote(
            tw_pass, tower_send.at[0], tower_recv.at[end],
            to=tower_rows(f * dim_count + end, b), dim=far)

    def both(z, ff):
        return remote(tw.at[ff * dim_count + z], both_send, both_recv, field=other)

    def bias_copy(target):
        return remote(bias_raw.at[lax.rem(end, 2)], bias_send, bias_recv, dim=target)

    def unit_in(target):
        return remote(unit_raw.at[f * dim_count + end], unit_send, near_unit, dim=target)

    def unit_out(ff, z):
        rows = unit_raw.at[pl.ds(f * dim_count + 2 * side, 2)]
        return remote(rows, unit_send, unit_recv, field=ff, dim=z)

    def two(c, ff):
        lane = pl.multiple_of((1 - part_of) * lanes, lanes)
        return remote(
            y.at[c, :, :, pl.ds(lane, lanes)], two_send, two_recv.at[c],
            to=x2.at[c, pl.ds(ff * fl, fl)], field=other)

    def rows_of(c):
        return pl.ds(pl.multiple_of(c * rc, rc), rc)

    def keep(c):
        return pltpu.make_async_copy(y.at[c, :, within(mid), :], out.at[:, :, rows_of(c)], out_sem)

    def give(c):
        return remote(
            y.at[c, :, within(end), :], give_send, give_recv,
            to=out.at[:, :, rows_of(c)], dim=end)

    def part(last):
        rows = pl.ds(chunks - 1, 1) if last else pl.ds(0, chunks - 1)
        return remote(
            pre_out.at[rows], part_send, part_recv.at[last], to=pre_in.at[rows],
            field=other, dim=far)

    def loss_copy(k, c):
        ff, z = (
            (other, far_end), (f, far_end), (other, end), (other, far), (f, end), (f, far), (other, d),
        )[k - 1]
        return remote(
            losses.at[c], loss_send.at[k], loss_recv, to=loss_out.at[c * field_count + part_of],
            field=ff, dim=z)

    def keep_loss(c):
        return pltpu.make_async_copy(losses.at[c], loss_out.at[c * field_count + part_of], loss_send.at[0])

    def own_weight(level, ff):
        return pltpu.make_async_copy(
            weight.at[level, :, ff],
            flat.at[level, :, within(mid), pl.ds(pl.multiple_of(ff * width, width), width)],
            weight_sem.at[level])

    def end_weight(level, k):
        row = pl.multiple_of(lax.rem(b, 2) * rows_in_part, rows_in_part)
        ff = b // 2 * (fields // 2) + k
        to = pl.multiple_of(lax.rem(end, 2) * el + row, rows_in_part)
        return pltpu.make_async_copy(
            weight.at[level, :, ff, pl.ds(row, rows_in_part), :],
            flat.at[level, :, pl.ds(to, rows_in_part), pl.ds(pl.multiple_of(ff * width, width), width)],
            weight_sem.at[level])

    def direct_weight(k):
        start = line_pieces(fl, PIECES)[RELAYED][0]
        row = pl.multiple_of(lax.rem(diagonal, 2) * rows_in_part, rows_in_part)
        ff = diagonal // 2 * (fields // 2) + k
        to = pl.multiple_of(lax.rem(end, 2) * el + row, rows_in_part)
        return pltpu.make_async_copy(
            weight.at[1, pl.ds(start, fl - start), ff, pl.ds(row, rows_in_part), :],
            flat.at[1, pl.ds(start, fl - start), pl.ds(to, rows_in_part),
                    pl.ds(pl.multiple_of(ff * width, width), width)],
            direct_load)

    def each(count, act):
        def step(k, carry):
            act(k)
            return carry

        lax.fori_loop(0, count, step, 0)

    own_features = [
        pltpu.make_async_copy(feat.at[:, :, pl.ds(c * rc, rc)], block(c, f, d), feat_sem.at[c])
        for c in range(chunks)]
    quarter = pl.ds(pl.multiple_of(b * quarter_units, quarter_units), quarter_units)
    small = [
        pltpu.make_async_copy(bias, bias_raw.at[lax.rem(d, 2)], small_sem.at[0]),
        pltpu.make_async_copy(tower_bias, unit_raw.at[me], small_sem.at[1]),
        pltpu.make_async_copy(cand, cands.at[b], small_sem.at[2]),
        pltpu.make_async_copy(tower, tw_raw, small_sem.at[3]),
        pltpu.make_async_copy(query_weight, q_raw, small_sem.at[4]),
        pltpu.make_async_copy(user, users, small_sem.at[5]),
        pltpu.make_async_copy(positive, targets, small_sem.at[6]),
    ]
    barrier = pltpu.get_barrier_semaphore()

    def greet(**where):
        pl.semaphore_signal(barrier, inc=1, device_id=where, device_id_type=MESH)

    @pl.when(is_end)
    def _():
        for ff in range(field_count):
            for z in (1, 2):
                greet(field=ff, dim=z)

    @pl.when(is_mid)
    def _():
        greet(dim=end)
        greet(dim=far)
        greet(batch=x_next)
        greet(batch=y_next)
        greet(field=other, dim=far)
        greet(field=other)

    for copy in own_features:
        copy.start()

    @pl.when(is_end)
    def _():
        each(fields // 2, lambda k: end_weight(0, k).start())

    for copy in small:
        copy.start()

    @pl.when(is_mid)
    def _():
        each(fields, lambda k: own_weight(0, k).start())
        each(fields, lambda k: own_weight(1, k).start())

    @pl.when(is_end)
    def _():
        each(fields // 2, lambda k: end_weight(1, k).start())
        each(fields // 2, lambda k: direct_weight(k).start())

    pl.semaphore_wait(barrier, jnp.where(is_mid, 2 * field_count + 5, 1))

    def loaded_own(level):
        ref = flat.at[level, :, within(mid), :]
        pltpu.make_async_copy(ref, ref, weight_sem.at[level]).wait()

    def loaded_end(level):
        ref = weight_part(level, 0, fl, b)
        pltpu.make_async_copy(ref, ref, weight_sem.at[level]).wait()

    def pack_tower():
        def halves(rows, j):
            first = tw_raw[2 * j, rows, :]
            second = tw_raw[2 * j + 1, rows, :]
            low = jnp.concatenate([first[:, :wide], second[:, :wide]], axis=1)
            high = jnp.concatenate([first[:, wide:], second[:, wide:]], axis=1)
            return low, high

        for j in range(fields // 2):
            low, high = halves(slice(None), j)
            tw_near[:, j * width:(j + 1) * width] = jnp.where(side == 0, low, high)
            low, high = halves(quarter, j)
            tw_far[:, j * width:(j + 1) * width] = jnp.where(side == 0, high, low)
        tw_near[:, side_k:] = q_raw[...]
        tw_far[:, side_k:] = q_raw[quarter, :]

    @pl.when(is_end)
    def _():
        loaded_end(0)
        for p in range(PIECES - 1):
            piece(0, p, mid).start()
        for copy in own_features:
            copy.wait()
        from_end(0, mid).start()
        piece(0, PIECES - 1, mid).start()
        from_end(1, mid).start()
        for copy in small:
            copy.wait()
        bias_copy(mid).start()
        unit_in(mid).start()
        for c in range(2, chunks):
            from_end(c, mid).start()
        pack_tower()
        pass_in(mid).start()
        loaded_end(1)
        for p in range(PIECES):
            piece(1, p, mid).start()
        pltpu.make_async_copy(direct_part(), direct_part(), direct_load).wait()
        for p in range(RELAYED, PIECES):
            direct(p, mid).start()
        near_tower(mid).start()

    def expect_piece(level, p):
        piece(level, p, end).wait_recv()
        plane_out(level * PIECES + p)

    def expect_end(c):
        from_end(c, end).wait_recv()
        cross(1, c, end).start()
        pair(c, end).start()

    def expect_far(k, c, o):
        cross(k, c, o).wait_recv()
        pair(c, o).start()

    def expect_tower(i, z):
        far_tower(z, end).wait_recv()
        plane_out(i)

    def half(source, level, c, ff):
        matrix = flat[level, :, :, pl.ds(pl.multiple_of(ff * half_k, half_k), half_k)]
        return jnp.dot(
            matrix.reshape(fl * wide, half_k), source[c, pl.ds(ff * fl, fl)].reshape(half_k, rc),
            preferred_element_type=jnp.float32)

    def advance(source, level, c, wait_pair):
        product = half(source, level, c, f)
        wait_pair()
        product = product + half(source, level, c, other)
        column = bias_cols[level]
        product = product + jnp.concatenate([column] * (rc // column.shape[1]), axis=1)
        anchor = x0[c, fs, ss, :].astype(jnp.float32).reshape(fl * wide, rc)
        current = source[c, fs, ss, :].astype(jnp.float32).reshape(fl * wide, rc)
        return (anchor * product + current).astype(jnp.bfloat16).reshape(fl, wide, rc)

    def build_bias():
        pick = (lax.broadcasted_iota(jnp.int32, (el, el), 0) == lax.broadcasted_iota(jnp.int32, (el, el), 1))
        for level in range(CROSS):
            for k in range(fl):
                for s in range(2):
                    line = bias_raw[s, k, level:level + 1, :]
                    column = jnp.sum(jnp.where(pick, line, 0.0), axis=1, keepdims=True)
                    start = (2 * k + s) * el
                    bias_cols[level, start:start + el, :] = jnp.broadcast_to(column, (el, width))

    def build_units():
        for m in range(members):
            unit_cols[m * units:(m + 1) * units, :] = jnp.broadcast_to(unit_raw[m], (lanes, units)).T

    def build_users():
        for c in range(chunks):
            start = pl.multiple_of(c * rc + part_of * lanes, lanes)
            user_cols[c] = users[pl.ds(start, lanes), :].astype(jnp.float32).T

    def build_queries():
        for m in range(members):
            block = tw[m, :, side_k:].astype(jnp.float32).T
            query_cols[:, m * units:(m + 1) * units] = block.astype(jnp.bfloat16)

    def first(c, carry):
        @pl.when(c == 1)
        def _():
            pass_in(end).wait_recv()
            pass_on().start()

        @pl.when(c == 2)
        def _():
            expect_far(1, 2, far_end)
            plane_forward(FAR_TOWER)
            expect_piece(1, 0)

        @pl.when(c == 3)
        def _():
            expect_far(1, 3, far_end)
            expect_piece(1, 1)

        def wait_pair():
            landed(x0.at[c, fs], pair_recv.at[c])

        x1[c, fs, ss, :] = advance(x0, 0, c, wait_pair)
        cross_one(c, side).start()
        pair_one(c, side).start()
        return carry

    def tower_part(c):
        matrix = tw[:, :, :side_k].reshape(members * units, side_k)
        return jnp.dot(matrix, x2[c].reshape(side_k, lanes), preferred_element_type=jnp.float32)

    def expect_one(c):
        cross_one(c, 1 - side).wait_recv()
        pair_one(c, 1 - side).start()

    def layer_two(c):
        def wait_pair():
            landed(x1.at[c, fs], one_recv.at[c])

        y[c] = advance(x1, 1, c, wait_pair)
        two(c, f).start()
        give(c).start()
        keep(c).start()
        for k in range(2):
            @pl.when(part_of == k)
            def _():
                x2[c, fs] = y[c, :, :, k * lanes:(k + 1) * lanes]

    def layer_three(c):
        two(c, other).wait_recv()
        pre = tower_part(c)

        @pl.when(owner)
        def _():
            pre_own[c] = pre + unit_cols[...]

        @pl.when(giver)
        def _():
            pre_out[c] = pre.astype(jnp.bfloat16)

    def give_parts(c):
        @pl.when(giver & (c == chunks - 2))
        def _():
            part(0).start()

        @pl.when(giver & (c == chunks - 1))
        def _():
            part(1).start()

    def second(c, carry):
        layer_two(c)

        @pl.when(c == 1)
        def _():
            near_tower(end).wait_recv()
            both(end, f).start()
            expect_one(2)
            landed(tw.at[pl.ds(0, dim_count)], both_recv)

        def tower_step(k, carry):
            layer_three(k)
            give_parts(k)
            return carry

        last = c == chunks - 1
        lax.fori_loop(
            jnp.where(last, c, jnp.maximum(c - 1, 0)), jnp.where(c < chunks - 2, c, c + 1),
            tower_step, 0)

        @pl.when(c == 2)
        def _():
            expect_one(3)

        return carry

    def finish(c):
        if c == 0:
            part(0).wait_recv()
        if c == chunks - 1:
            part(1).wait_recv()
        pre = pre_own[c] + pre_in[c].astype(jnp.float32)
        hidden = jnp.maximum(pre, 0.0).astype(jnp.bfloat16)
        query = jnp.dot(query_cols[...], hidden, preferred_element_type=jnp.float32)
        query_vec = (query + user_cols[c]).astype(jnp.bfloat16)
        logits = jnp.dot(
            cands[...].reshape(-1, width), query_vec,
            preferred_element_type=jnp.float32) * (1.0 / math.sqrt(width))
        labels = lax.broadcasted_iota(jnp.int32, logits.shape, 0)
        target = targets[c * field_count + part_of]
        picked = jnp.sum(jnp.where(labels == target, logits, 0.0), axis=0, keepdims=True)
        best = jnp.max(logits, axis=0, keepdims=True)
        total = jnp.sum(jnp.exp(logits - best), axis=0, keepdims=True)
        losses[c] = best + jnp.log(total) - picked
        for k in range(1, members):
            loss_copy(k, c).start()
        keep_loss(c).start()

    @pl.when(is_mid)
    def _():
        for c in range(chunks):
            own_features[c].wait()
            cross(0, c, mid).start()
            pair(c, mid).start()
        for copy in small:
            copy.wait()
        plane_out(CANDS)
        pack_tower()
        far_tower(d, far).start()
        tw[me] = tw_near[...]
        both(mid, f).start()
        expect_piece(0, 0)
        expect_far(0, 0, far)
        expect_piece(0, 1)
        expect_far(0, 1, far)
        plane_forward(CANDS)
        expect_piece(0, 2)
        expect_far(0, 2, far)
        plane_forward(0)
        plane_forward(1)
        expect_far(0, 3, far)
        expect_end(0)
        expect_piece(0, 3)
        plane_forward(2)
        expect_end(1)
        plane_forward(3)
        expect_far(1, 0, far_end)
        expect_tower(FAR_TOWER, far)
        bias_copy(end).wait_recv()
        build_bias()
        unit_in(end).wait_recv()
        unit_out(other, d).start()
        unit_out(f, far).start()
        unit_out(other, far).start()
        for level in range(CROSS):
            loaded_own(level)
        expect_end(2)
        plane_rest(0)
        expect_far(1, 1, far_end)
        expect_end(3)
        lax.fori_loop(0, chunks, first, 0)
        plane_rest(4)
        plane_rest(2)
        both(far, f).start()
        expect_piece(1, 2)
        expect_piece(1, 3)
        expect_tower(END_TOWER, far_end)
        for p in range(RELAYED):
            plane_forward(PIECES + p)
        expect_one(0)
        plane_forward(END_TOWER)
        for p in range(RELAYED, PIECES):
            plane_keep(PIECES + p)
        expect_one(1)
        landed(unit_raw.at[pl.ds(0, 6)], unit_recv)
        build_units()
        build_users()
        plane_rest(3)
        both(far_end, f).start()
        landed(direct_part(), direct_recv)
        plane_rest(1)
        lax.fori_loop(0, chunks, second, 0)

        @pl.when(owner)
        def _():
            build_queries()
            for c in range(chunks):
                finish(c)

    @pl.when(owner)
    def _():
        landed(losses, loss_recv)

    @pl.when(jnp.logical_not(owner))
    def _():
        landed(loss_out, loss_recv)

    @pl.when(is_end)
    def _():
        for level in range(CROSS):
            sent(weight_part(level, 0, fl, b), piece_send.at[level])
        sent(direct_part(), direct_send)
        sent(x0.at[:, fs, entries(d), :], end_send)
        bias_copy(mid).wait_send()
        near_tower(mid).wait_send()
        pass_in(mid).wait_send()
        unit_in(mid).wait_send()
        landed(out, give_recv)

    @pl.when(is_mid)
    def _():
        far_tower(d, far).wait_send()
        pass_on().wait_send()
        sent(tw.at[pl.ds(0, dim_count)], both_send)
        sent(unit_raw.at[pl.ds(0, 6)], unit_send)
        sent(x0.at[:, fs, entries(mid), :], cross_send.at[0])
        sent(x0.at[:, fs, entries(end), :], cross_send.at[1])
        sent(x1.at[:, fs, ss, :], cross_send.at[2])
        sent(x0.at[:, fs], pair_send)
        sent(x1.at[:, fs], one_send)
        sent(y.at[:, :, :, pl.ds(0, lanes)], two_send)
        sent(out, give_send)
        pltpu.make_async_copy(out, out, out_sem).wait()
        for group in range(CROSS + 3):
            sent(plane_bytes(group, 3), plane_send.at[group])

    @pl.when(giver)
    def _():
        sent(pre_out, part_send)

    @pl.when(owner)
    def _():
        for k in range(1, members):
            sent(losses, loss_send.at[k])
        pltpu.make_async_copy(losses, losses, loss_send.at[0]).wait()


def emit_kernel(crossed, losses, crossed_out, losses_out, sems):
    copies = [
        pltpu.make_async_copy(crossed, crossed_out, sems.at[0]),
        pltpu.make_async_copy(losses, losses_out, sems.at[1]),
    ]
    for copy in copies:
        copy.start()
    for copy in copies:
        copy.wait()


def line_body(
    counts, features, cross_weight, cross_bias, tower_weight, tower_bias, query_weight,
    user_vec, candidates, positive,
):
    batch_count, field_count, dim_count = counts
    members = field_count * dim_count
    fl, el, row_count = features.shape
    units, fields, width = tower_weight.shape
    rc = row_count // CHUNKS
    lanes = rc // field_count
    wide = 2 * el
    quarter = units // batch_count
    packed = fields * wide + width
    items = CANDS + 1
    dma = pltpu.SemaphoreType.DMA
    vmem = pltpu.VMEM
    bf16 = jnp.bfloat16
    f32 = jnp.float32
    far = pl.BlockSpec(memory_space=pl.ANY)
    crossed, losses = pl.pallas_call(
        functools.partial(line_kernel, counts),
        out_shape=(
            jax.ShapeDtypeStruct(features.shape, bf16),
            jax.ShapeDtypeStruct((CHUNKS * field_count, 1, lanes), f32),
        ),
        in_specs=[far] * 9,
        out_specs=(far, far),
        scratch_shapes=[
            vmem((CHUNKS, fields, width, rc), bf16),
            vmem((CHUNKS, fields, width, rc), bf16),
            vmem((CHUNKS, fl, wide, rc), bf16),
            vmem((CHUNKS, fields, wide, lanes), bf16),
            vmem((CROSS, fl, wide, fields * width), bf16),
            vmem((members, units, packed), bf16),
            vmem((units, packed), bf16),
            vmem((quarter, packed), bf16),
            vmem((quarter, packed), bf16),
            vmem((fields, units, width), bf16),
            vmem((units, width), bf16),
            vmem((CHUNKS, members * units, lanes), bf16),
            vmem((CHUNKS, members * units, lanes), bf16),
            vmem((CHUNKS, members * units, lanes), f32),
            vmem((2, fl, CROSS, el), f32),
            vmem((CROSS, fl * wide, width), f32),
            vmem((members, 1, units), f32),
            vmem((members * units, lanes), f32),
            vmem((width, members * units), bf16),
            vmem((batch_count,) + candidates.shape, bf16),
            vmem(user_vec.shape, bf16),
            vmem((CHUNKS, width, lanes), f32),
            vmem((CHUNKS * field_count, 1, lanes), jnp.int32),
            vmem((CHUNKS, 1, lanes), f32),
            dma((CHUNKS,)), dma((CROSS,)), dma((7,)),
            dma, dma((CHUNKS,)), dma((3,)), dma((3, CHUNKS)),
            dma, dma((CHUNKS,)), dma, dma((CHUNKS,)),
            dma((CROSS,)), dma((CROSS, PIECES)), dma, dma, dma, dma((CROSS + 3,)), dma((items,)), dma((CROSS + 3,)),
            dma((2,)), dma((dim_count,)), dma, dma, dma,
            dma, dma, dma, dma, dma,
            dma, dma((CHUNKS,)), dma, dma, dma, dma, dma((2,)), dma((members,)), dma,
        ],
        compiler_params=pltpu.CompilerParams(
            collective_id=0, has_side_effects=True, vmem_limit_bytes=48 * 2**20),
        name="line_forward",
    )(*(pltpu.with_memory_space_constraint(value, pltpu.HBM) for value in (
        features,
        cross_weight.transpose(0, 1, 3, 2, 4),
        cross_bias.transpose(1, 0, 2),
        tower_weight.transpose(1, 0, 2),
        tower_bias.reshape(1, units),
        query_weight,
        user_vec,
        candidates,
        positive.reshape(CHUNKS * field_count, 1, lanes),
    )))
    crossed, losses = pl.pallas_call(
        emit_kernel,
        out_shape=(
            jax.ShapeDtypeStruct(features.shape, bf16),
            jax.ShapeDtypeStruct((CHUNKS * field_count, 1, lanes), f32),
        ),
        in_specs=[far] * 2,
        out_specs=(pl.BlockSpec(memory_space=pltpu.HBM),) * 2,
        scratch_shapes=[dma((2,))],
        compiler_params=pltpu.CompilerParams(vmem_limit_bytes=4 * 2**20),
        name="emit",
    )(crossed, losses)
    return (crossed, losses.reshape(row_count))


def body(
    features, cross_weight, cross_bias, tower_weight, tower_bias, query_weight,
    user_vec, candidates, positive,
):
    counts = tuple(lax.axis_size(name) for name in ("batch", "field", "dim"))
    if line_fits(counts, features, tower_weight, candidates):
        return line_body(
            counts, features, cross_weight, cross_bias, tower_weight, tower_bias, query_weight,
            user_vec, candidates, positive)
    batch_count, field_count, dim_count = counts
    members = field_count * dim_count
    fl, el, row_count = features.shape
    columns = fl * el
    units, fields, width = tower_weight.shape
    low, held = tower_levels(dim_count)
    chunks = chunk_count(row_count, field_count, held)
    split = batch_count if units % (batch_count * 16) == 0 else 1
    part = units // split
    rc = row_count // chunks
    sub = rc // held
    run = chunks // field_count
    share = run * sub
    steps = (CROSS, chunks, dim_count)
    small = (3, dim_count)
    dma = pltpu.SemaphoreType.DMA
    vmem = pltpu.VMEM
    bf16 = jnp.bfloat16
    far = pl.BlockSpec(memory_space=pl.ANY)
    near = pl.BlockSpec(memory_space=pltpu.VMEM)
    crossed, losses = pl.pallas_call(
        functools.partial(rank_kernel, counts, (chunks, split)),
        out_shape=(
            jax.ShapeDtypeStruct(features.shape, bf16),
            jax.ShapeDtypeStruct((chunks * held, 1, sub), jnp.float32),
        ),
        in_specs=[far, far, near, far, far, far, near, far, near],
        out_specs=(near, near),
        scratch_shapes=[
            vmem((chunks, fields, width, rc), bf16),
            vmem((chunks, fields, width, rc), bf16),
            vmem((CROSS, fl, el, fields * width), bf16),
            vmem((chunks, held, fl, el, sub), bf16),
            vmem((fields, width, share), bf16),
            vmem((split, members, part, fields * width), bf16),
            vmem((members, 1, units), jnp.float32),
            vmem((split, members, part, share), jnp.float32),
            vmem((split, members, part, width), bf16),
            vmem((batch_count,) + candidates.shape, bf16),
            vmem((held, chunks, 1, sub), jnp.float32),
            dma((chunks,)), dma((CROSS, fields)), dma((fields,)), dma((3,)),
            dma(steps), dma(steps), dma(steps), dma(steps), dma(steps),
            dma((chunks, held)), dma((run, members)), dma(small), dma(small), dma(small),
            dma((3,)), dma((3,)),
            dma((split,)), dma((split,)), dma((split,)), dma((split,)),
            dma((batch_count,)), dma((batch_count,)), dma((members,)), dma((field_count, held)),
        ],
        compiler_params=pltpu.CompilerParams(
            collective_id=0, has_side_effects=True, vmem_limit_bytes=56 * 2**20),
        name="rank_forward",
    )(
        features,
        cross_weight.transpose(0, 1, 3, 2, 4),
        cross_bias.reshape(CROSS, columns, 1),
        tower_weight.transpose(1, 0, 2),
        tower_bias.reshape(1, units),
        query_weight.reshape(split, part, width),
        user_vec,
        candidates,
        positive.reshape(chunks * held, 1, sub),
    )
    return (crossed, losses.reshape(row_count))


def solution(mesh):
    placed = (
        P("field", "dim", "batch"),
        P(None, "field", "dim", None, None),
        P(None, "field", "dim"),
        P(("field", "dim"), None, None),
        P(("field", "dim")),
        P(("field", "dim"), None),
        P("batch", None),
        P("batch", None),
        P("batch"),
    )
    return jax.shard_map(
        body,
        mesh=mesh,
        in_specs=placed,
        out_specs=(P("field", "dim", "batch"), P("batch")),
        check_vma=False,
    )
```
